8 devices in a mesh: dp: 2 (over z, y), tp: 4 (over x, core).
Axes of the slice: x: 2, y: 2, z: 1, core: 2. Of those that a mesh axis runs over, the one named last changes fastest.
Arguments:
- hidden: bfloat16 [8, 5, 2048], P('dp'), parts along dimension 0
- norm_gain: float32 [2048], replicated
- w_head: bfloat16 [2048, 151936], P(None, 'tp')
- draft_probs: float32 [8, 4, 151936], P('dp', None, 'tp'), parts along dimension 0
- draft_tokens: int32 [8, 4], P('dp'), parts along dimension 0
- temperature: float32 [8], P('dp'), parts along dimension 0
Outputs:
- output 1: float32 [8, 4], P('dp'), parts along dimension 0
- output 2: float32 [8, 4], P('dp'), parts along dimension 0
- output 3: float32 [8, 4, 151936], P('dp', None, 'tp'), parts along dimension 0
- output 4: float32 [8], P('dp'), parts along dimension 0
There are 2 independent parts. The reference program is written for one: setup_inputs(seed, part) draws one part's arguments, and reference() takes and returns one part's arrays. A program takes and returns all parts, laid end to end along the dimension named above; an argument that names none is the same for every part.
All inputs are finite; a program needn't handle non-finite values.
Results may differ from the reference program's by a relative error of at most 0.001.
Values sent between devices are 32-bit elements.
A program may use at most 1 GiB of HBM per device.

```python
import jax
import jax.numpy as jnp
from jax import lax

BATCH_ROWS = 4
DRAFT_LEN = 4
D_MODEL = 2048
VOCAB_SIZE = 151936
CLUSTER_COUNT = 3
WEIGHT_BLOCK = 128
CLUSTER_SPAN = VOCAB_SIZE // 32


def setup_inputs(seed: int = 0, part: int = 0) -> dict:
    part_key = jax.random.fold_in(jax.random.key(seed), part)
    key_h, key_q, key_s, key_t, key_c, key_k, key_o = jax.random.split(part_key, 7)
    key_w, key_g = jax.random.split(jax.random.key(seed + 1), 2)
    hidden = jax.random.normal(key_h, (BATCH_ROWS, DRAFT_LEN + 1, D_MODEL), jnp.float32).astype(jnp.bfloat16)
    norm_gain = jax.random.uniform(key_g, (D_MODEL,), jnp.float32, 0.5, 1.5)

    def weight_block(block_idx):
        gauss_block = jax.random.normal(jax.random.fold_in(key_w, block_idx), (WEIGHT_BLOCK, VOCAB_SIZE), jnp.float32)
        return (gauss_block * D_MODEL ** -0.5).astype(jnp.bfloat16)

    w_head = lax.map(weight_block, jnp.arange(D_MODEL // WEIGHT_BLOCK)).reshape(D_MODEL, VOCAB_SIZE)
    q_scale = jax.random.uniform(key_s, (BATCH_ROWS, DRAFT_LEN, 1), jnp.float32, 0.7, 1.3)
    q_logits = jax.random.normal(key_q, (BATCH_ROWS, DRAFT_LEN, VOCAB_SIZE), jnp.float32) * q_scale
    draft_probs = jax.nn.softmax(q_logits, axis=-1)
    temperature = jax.random.uniform(key_t, (BATCH_ROWS,), jnp.float32, 0.6, 1.4)
    centers = jax.random.randint(key_c, (CLUSTER_COUNT,), 0, VOCAB_SIZE - CLUSTER_SPAN)
    choice = jax.random.randint(key_k, (BATCH_ROWS, DRAFT_LEN), 0, CLUSTER_COUNT)
    offsets = jax.random.randint(key_o, (BATCH_ROWS, DRAFT_LEN), 0, CLUSTER_SPAN)
    draft_tokens = (centers[choice] + offsets).astype(jnp.int32)
    return {'hidden': hidden, 'norm_gain': norm_gain, 'w_head': w_head, 'draft_probs': draft_probs, 'draft_tokens': draft_tokens, 'temperature': temperature}


def reference(hidden, norm_gain, w_head, draft_probs, draft_tokens, temperature):
    def one_row(row_args):
        row_hidden, row_probs, row_tokens, row_temp = row_args
        hidden_f32 = row_hidden.astype(jnp.float32)
        inv_rms = lax.rsqrt(jnp.mean(hidden_f32 * hidden_f32, axis=-1, keepdims=True) + 1e-5)
        normed = (hidden_f32 * inv_rms * norm_gain).astype(jnp.bfloat16)
        logits = jnp.dot(normed, w_head, preferred_element_type=jnp.float32)
        scaled = logits / row_temp
        row_max = jnp.max(scaled, axis=-1, keepdims=True)
        row_lse = row_max + jnp.log(jnp.sum(jnp.exp(scaled - row_max), axis=-1, keepdims=True))
        target = jnp.exp(scaled[:DRAFT_LEN] - row_lse[:DRAFT_LEN])
        tok_target = jnp.take_along_axis(target, row_tokens[:, None], axis=-1)[:, 0]
        tok_draft = jnp.take_along_axis(row_probs, row_tokens[:, None], axis=-1)[:, 0]
        accept = jnp.minimum(1.0, tok_target / tok_draft)
        excess = jnp.maximum(target - row_probs, 0.0)
        norm_sum = jnp.sum(excess, axis=-1)
        residual = excess / norm_sum[:, None]
        return accept, norm_sum, residual, row_lse[DRAFT_LEN, 0]

    accept, norm_sum, residual, bonus_lse = lax.map(one_row, (hidden, draft_probs, draft_tokens, temperature))
    return accept, norm_sum, residual, bonus_lse
```

```python
import jax
import jax.numpy as jnp
from jax import lax
from jax.experimental import pallas as pl
from jax.experimental.pallas import tpu as pltpu
from jax.sharding import PartitionSpec as P

MESH = pl.DeviceIdType.MESH
F32 = jnp.float32
LOWEST = float(jnp.finfo(jnp.float32).min)

TILE = 1024
SUB = 256
SLOTS = 4
SHARED = 14
FIRST = 5
PASS = 512


def verify_kernel(
    h_ref, g_ref, t_ref, dt_ref, w_ref, q_ref,
    ex_ref, norm_ref, acc_ref, lse_ref,
    wbuf, wtail, qv, s_scr, xf, xp, xrows, xb, tv, tp_recv, ct, dl, m_scr, l_scr, k_scr,
    zsend, pstat_s, pstat_r, e1s, e1r, e2s, e2r, e3s, e3r,
    w_sem, wt_sem, q_sem, x_sem, t_sem, zs_sem, zr_sem, ps_sem, e1_sem, e2_sem, e3_sem,
):
    dp, tp = lax.axis_index("dp"), lax.axis_index("tp")
    partner = (1 - dp, tp)
    peers = [(dp, lax.rem(tp + d, 4)) for d in (1, 2, 3)]
    n_ids = w_ref.shape[0]
    n_full = n_ids // TILE
    tail = n_ids - n_full * TILE
    tail_at = n_full * TILE
    last = n_full - 2 * SHARED - FIRST
    steps = FIRST + SHARED + last

    def column(i):
        in_shared = (i + steps - FIRST) // steps
        past_shared = (i + steps - FIRST - SHARED) // steps
        return pl.multiple_of((i + in_shared * dp * SHARED + past_shared * (SHARED - dp * SHARED)) * TILE, TILE)

    half = TILE // 2

    def tile_copies(i, slot):
        at = column(i)
        return [
            pltpu.make_async_copy(
                w_ref.at[pl.ds(at + k * half, half), :], wbuf.at[slot, pl.ds(k * half, half), :], w_sem.at[slot, k]
            )
            for k in (0, 1)
        ]

    tail_copy = pltpu.make_async_copy(w_ref.at[pl.ds(tail_at, tail), :], wtail, wt_sem)
    q_copy = pltpu.make_async_copy(q_ref, qv, q_sem)
    for c in tile_copies(0, 0):
        c.start()
    tail_copy.start()
    for i in range(1, SLOTS):
        for c in tile_copies(i, i):
            c.start()
    q_copy.start()

    barrier = pltpu.get_barrier_semaphore()
    for other in [partner] + peers:
        pl.semaphore_signal(barrier, inc=1, device_id=other, device_id_type=MESH)

    h = h_ref[...].astype(F32)
    inv_rms = lax.rsqrt(jnp.mean(h * h, axis=-1, keepdims=True) + 1e-5)
    xf[...] = h * inv_rms * g_ref[...][None]
    for b in range(4):
        tv[0, b : b + 1, :] = jnp.full((1, 128), 1.0, F32) / jnp.full((1, 128), t_ref[b], F32)
        for j in range(4):
            tv[1 + j, b : b + 1, :] = jnp.full((1, 128), dt_ref[b, j].astype(F32), F32)

    def lay_rows(src, t_src, at):
        xrows[...] = jnp.zeros_like(xrows)
        lane = lax.broadcasted_iota(jnp.int32, (1, 128), 1) + tp * n_ids
        for b in range(4):
            for j in range(5):
                xrows[8 * b + j : 8 * b + j + 1, :] = src[j, b : b + 1, :]
            ct[at + 8 * b : at + 8 * b + 8, :] = jnp.broadcast_to(t_src[0, b : b + 1, :], (8, 128))
            dl[at + 8 * b : at + 8 * b + 8, :] = jnp.full((8, 128), -1.0, F32)
            for j in range(4):
                dl[at + 8 * b + j : at + 8 * b + j + 1, :] = t_src[1 + j, b : b + 1, :] - lane.astype(F32)
        xb[at : at + 32, :] = xrows[...].astype(jnp.bfloat16)

    lay_rows(xf, tv, 0)
    m_scr[...] = jnp.full(m_scr.shape, LOWEST, F32)
    l_scr[...] = jnp.zeros_like(l_scr)
    k_scr[...] = jnp.zeros_like(k_scr)

    pl.semaphore_wait(barrier, 4)
    x_copy = pltpu.make_async_remote_copy(
        src_ref=xf, dst_ref=xp, send_sem=x_sem.at[0], recv_sem=x_sem.at[1], device_id=partner, device_id_type=MESH
    )
    t_copy = pltpu.make_async_remote_copy(
        src_ref=tv, dst_ref=tp_recv, send_sem=t_sem.at[0], recv_sem=t_sem.at[1], device_id=partner, device_id_type=MESH
    )
    x_copy.start()
    t_copy.start()

    def product(rows, w):
        return lax.dot_general(xb[0:rows, :], w, (((1,), (1,)), ((), ())), preferred_element_type=F32)

    def fold(rows, parts):
        m_old = m_scr[0:rows, :]
        m_new = m_old
        for p in parts:
            m_new = jnp.maximum(m_new, p)
        total = l_scr[0:rows, :] * jnp.exp(m_old - m_new)
        for p in parts:
            total = total + jnp.exp(p - m_new)
        m_scr[0:rows, :] = m_new
        l_scr[0:rows, :] = total

    tail_copy.wait()
    z = product(32, wtail[...])
    s = z * ct[0:32, 0:tail]
    for b in range(4):
        s_scr[b, :, tail_at : tail_at + tail] = s[8 * b : 8 * b + 4, :]
    k_scr[0:32, 0:tail] = jnp.where(dl[0:32, 0:tail] == float(tail_at), s, 0.0)
    m_tail = jnp.max(s, axis=1, keepdims=True)
    l_tail = jnp.sum(jnp.exp(s - m_tail), axis=1, keepdims=True)
    lane0 = lax.broadcasted_iota(jnp.int32, (32, 128), 1) == 0
    m_scr[0:32, :] = jnp.where(lane0, m_tail, LOWEST)
    l_scr[0:32, :] = jnp.where(lane0, l_tail, 0.0)

    def z_copy(k):
        at = column(FIRST + k)
        return pltpu.make_async_remote_copy(
            src_ref=zsend.at[k], dst_ref=s_scr.at[:, :, pl.ds(at, TILE)], send_sem=zs_sem.at[k], recv_sem=zr_sem.at[k],
            device_id=partner, device_id_type=MESH,
        )

    def step(i, rows):
        slot = i % SLOTS
        for c in tile_copies(i, slot):
            c.wait()
        if rows == 64:
            k = i - FIRST

            @pl.when(k > 0)
            def _():
                z_copy(k - 1).start()

        at = column(i)
        kept = k_scr[0:rows, :]
        for c in range(TILE // SUB):
            z = product(rows, wbuf[slot, c * SUB : (c + 1) * SUB, :])
            parts = []
            for lane in range(0, SUB, 128):
                s = z[:, lane : lane + 128] * ct[0:rows, :]
                parts.append(s)
                off = c * SUB + lane
                kept = jnp.where(dl[0:rows, :] == (at + off).astype(F32), s, kept)
                for b in range(4):
                    s_scr[b, :, pl.ds(at + off, 128)] = s[8 * b : 8 * b + 4, :]
                    if rows == 64:
                        zsend[k, b, :, off : off + 128] = s[32 + 8 * b : 32 + 8 * b + 4, :]
            fold(rows, parts)
        k_scr[0:rows, :] = kept

        @pl.when(i + SLOTS < steps)
        def _():
            for c in tile_copies(i + SLOTS, slot):
                c.start()

    lax.fori_loop(0, FIRST, lambda i, _: step(i, 32), None)
    x_copy.wait()
    t_copy.wait()
    lay_rows(xp, tp_recv, 32)
    lax.fori_loop(FIRST, FIRST + SHARED, lambda i, _: step(i, 64), None)
    pstat_s[0] = m_scr[32:64, :]
    pstat_s[1] = l_scr[32:64, :]
    pstat_s[2] = k_scr[32:64, :]
    z_copy(SHARED - 1).start()
    stat_copy = pltpu.make_async_remote_copy(
        src_ref=pstat_s, dst_ref=pstat_r, send_sem=ps_sem.at[0], recv_sem=ps_sem.at[1],
        device_id=partner, device_id_type=MESH,
    )
    stat_copy.start()
    lax.fori_loop(FIRST + SHARED, steps, lambda i, _: step(i, 32), None)

    group = lax.broadcasted_iota(jnp.int32, (8, 128), 1) // 32

    def pack(cols):
        size = cols[0].shape[0]
        packed = jnp.broadcast_to(cols[0], (size, 128))
        for b in range(1, 4):
            packed = jnp.where(group[:size] == b, cols[b], packed)
        return packed

    def unpack(packed, b):
        size = packed.shape[0]
        lane = lax.broadcasted_iota(jnp.int32, (size, 128), 1)
        return jnp.sum(jnp.where(lane == 32 * b, packed, 0.0), axis=1, keepdims=True)

    def exchange(src, dst, sem):
        return [
            pltpu.make_async_remote_copy(
                src_ref=src, dst_ref=dst.at[d], send_sem=sem.at[0, d], recv_sem=sem.at[1, d],
                device_id=peers[d], device_id_type=MESH,
            )
            for d in range(3)
        ]

    stat_copy.wait()
    m = jnp.maximum(m_scr[0:32, :], pstat_r[0])
    total = l_scr[0:32, :] * jnp.exp(m_scr[0:32, :] - m) + pstat_r[1] * jnp.exp(pstat_r[0] - m)
    row_max = jnp.max(m, axis=1, keepdims=True)
    row_lse = row_max + jnp.log(jnp.sum(total * jnp.exp(m - row_max), axis=1, keepdims=True))
    e1s[...] = pack([row_lse[8 * b : 8 * b + 8, :] for b in range(4)])
    e1 = exchange(e1s, e1r, e1_sem)
    for c in e1:
        c.start()

    q_copy.wait()
    own = [dl[8 * b : 8 * b + 4, :] for b in range(4)]

    def pick(i, found):
        at = pl.multiple_of(i * PASS, PASS)
        out = []
        for b in range(4):
            f = found[b]
            for off in range(0, PASS, 128):
                f = jnp.where(own[b] == (at + off).astype(F32), qv[b, :, pl.ds(at + off, 128)], f)
            out.append(f)
        return tuple(out)

    zero = jnp.zeros((4, 128), F32)
    found = lax.fori_loop(0, tail_at // PASS, pick, (zero,) * 4)
    token_q, token_s = [], []
    for b in range(4):
        f = jnp.where(own[b][:, :tail] == float(tail_at), qv[b, :, tail_at : tail_at + tail], 0.0)
        token_q.append(jnp.sum(found[b], axis=1, keepdims=True) + jnp.sum(f, axis=1, keepdims=True))
        kept = k_scr[8 * b : 8 * b + 4, :] + pstat_r[2, 8 * b : 8 * b + 4, :]
        token_s.append(jnp.sum(kept, axis=1, keepdims=True))
    e3s[0] = pack(token_s)
    e3s[1] = pack(token_q)
    e3 = exchange(e3s, e3r, e3_sem)
    for c in e3:
        c.start()

    def await_z(k, _):
        z_copy(k).wait_send()
        pltpu.make_async_remote_copy(
            src_ref=zsend.at[k], dst_ref=s_scr.at[:, :, pl.ds(pl.multiple_of((FIRST + (1 - dp) * SHARED + k) * TILE, TILE), TILE)],
            send_sem=zs_sem.at[k], recv_sem=zr_sem.at[k], device_id=partner, device_id_type=MESH,
        ).wait_recv()
        return None

    lax.fori_loop(0, SHARED, await_z, None)
    for c in e1:
        c.wait()
    lses = [e1s[...]] + [e1r[d] for d in range(3)]
    top = jnp.maximum(jnp.maximum(lses[0], lses[1]), jnp.maximum(lses[2], lses[3]))
    sums = jnp.exp(lses[0] - top) + jnp.exp(lses[1] - top) + jnp.exp(lses[2] - top) + jnp.exp(lses[3] - top)
    lse = top + jnp.log(sums)
    lse_ref[...] = lse
    row_l = [jnp.broadcast_to(unpack(lse[0:4, :], b), (4, 128)) for b in range(4)]

    def excess(b, at, size):
        e = jnp.maximum(jnp.exp(s_scr[b, :, pl.ds(at, size)] - row_l[b][:, :size]) - qv[b, :, pl.ds(at, size)], 0.0)
        ex_ref[b, :, pl.ds(at, size)] = e
        return e

    def last_pass(i, sums):
        at = pl.multiple_of(i * PASS, PASS)
        out = []
        for b in range(4):
            acc = sums[b]
            for off in range(0, PASS, 128):
                acc = acc + excess(b, at + off, 128)
            out.append(acc)
        return tuple(out)

    sums = lax.fori_loop(0, tail_at // PASS, last_pass, (zero,) * 4)
    rows = []
    for b in range(4):
        e = excess(b, tail_at, tail)
        rows.append(jnp.sum(sums[b], axis=1, keepdims=True) + jnp.sum(e, axis=1, keepdims=True))
    e2s[...] = pack(rows)
    e2 = exchange(e2s, e2r, e2_sem)
    for c in e2:
        c.start()

    for c in e3:
        c.wait()
    at_token = (e3s[...] + e3r[0]) + (e3r[1] + e3r[2])
    acc_ref[...] = jnp.minimum(jnp.exp(at_token[0] - lse[0:4, :]) / at_token[1], 1.0)

    for c in e2:
        c.wait()
    norm = (e2s[...] + e2r[0]) + (e2r[1] + e2r[2])
    for b in range(4):
        norm_ref[b] = jnp.broadcast_to(unpack(norm, b), (4, 128))


def solution(mesh):
    def local_step(hidden, norm_gain, w_head, draft_probs, draft_tokens, temperature):
        n_ids = w_head.shape[1]
        width = w_head.shape[0]
        pad_ids = -(-n_ids // 128) * 128
        tail = n_ids % TILE
        vmem, smem, hbm = pltpu.VMEM, pltpu.SMEM, pltpu.HBM
        dma = pltpu.SemaphoreType.DMA
        ex, norm, acc, lse = pl.pallas_call(
            verify_kernel,
            out_shape=[
                jax.ShapeDtypeStruct((4, 4, n_ids), F32),
                jax.ShapeDtypeStruct((4, 4, 128), F32),
                jax.ShapeDtypeStruct((4, 128), F32),
                jax.ShapeDtypeStruct((8, 128), F32),
            ],
            in_specs=[pl.BlockSpec(memory_space=s) for s in (vmem, vmem, smem, smem, hbm, hbm)],
            out_specs=[pl.BlockSpec(memory_space=vmem)] * 4,
            scratch_shapes=[
                vmem((SLOTS, TILE, width), jnp.bfloat16),
                vmem((tail, width), jnp.bfloat16),
                vmem((4, 4, n_ids), F32),
                vmem((4, 4, pad_ids), F32),
                vmem((5, 4, width), F32),
                vmem((5, 4, width), F32),
                vmem((32, width), F32),
                vmem((64, width), jnp.bfloat16),
                vmem((5, 4, 128), F32),
                vmem((5, 4, 128), F32),
                vmem((64, 128), F32),
                vmem((64, 128), F32),
                vmem((64, 128), F32),
                vmem((64, 128), F32),
                vmem((64, 128), F32),
                vmem((SHARED, 4, 4, TILE), F32),
                vmem((3, 32, 128), F32),
                vmem((3, 32, 128), F32),
                vmem((8, 128), F32),
                vmem((3, 8, 128), F32),
                vmem((4, 128), F32),
                vmem((3, 4, 128), F32),
                vmem((2, 4, 128), F32),
                vmem((3, 2, 4, 128), F32),
                dma((SLOTS, 2)), dma, dma, dma((2,)), dma((2,)), dma((SHARED,)), dma((SHARED,)), dma((2,)),
                dma((2, 3)), dma((2, 3)), dma((2, 3)),
            ],
            compiler_params=pltpu.CompilerParams(collective_id=0, has_side_effects=True),
            name="verify",
        )(
            hidden.transpose(1, 0, 2), norm_gain.reshape(1, width), temperature, draft_tokens,
            w_head.T, draft_probs,
        )
        residual = ex / norm[:, :, :1]
        return acc[:, ::32].T, norm[:, :, 0], residual, lse[4, ::32]

    return jax.shard_map(
        local_step,
        mesh=mesh,
        in_specs=(P("dp", None, None), P(), P(None, "tp"), P("dp", None, "tp"), P("dp", None), P("dp")),
        out_specs=(P("dp", None), P("dp", None), P("dp", None, "tp"), P("dp")),
        check_vma=False,
    )
```

```python
import jax
import jax.numpy as jnp
from jax import lax
from jax.experimental import pallas as pl
from jax.experimental.pallas import tpu as pltpu
from jax.sharding import PartitionSpec as P

MESH = pl.DeviceIdType.MESH
F32 = jnp.float32
LOWEST = float(jnp.finfo(jnp.float32).min)

TILE = 1024
SUB = 256
SLOTS = 4
SHARED = 8
FIRST = 5
PASS = 512


def verify_kernel(
    h_ref, g_ref, t_ref, dt_ref, w_ref, q_ref,
    ex_ref, norm_ref, acc_ref, lse_ref,
    wbuf, wtail, qv, s_scr, xf, xp, xrows, xb, tv, tp_recv, ct, dl, m_scr, l_scr, k_scr,
    zsend, pstat_s, pstat_r, e1s, e1r, e2s, e2r, e3s, e3r,
    w_sem, wt_sem, q_sem, x_sem, t_sem, zs_sem, zr_sem, ps_sem, e1_sem, e2_sem, e3_sem,
):
    dp, tp = lax.axis_index("dp"), lax.axis_index("tp")
    partner = (1 - dp, tp)
    peers = [(dp, lax.rem(tp + d, 4)) for d in (1, 2, 3)]
    n_ids = w_ref.shape[0]
    n_full = n_ids // TILE
    tail = n_ids - n_full * TILE
    tail_at = n_full * TILE
    last = n_full - 2 * SHARED - FIRST
    steps = FIRST + SHARED + last

    def column(i):
        in_shared = (i + steps - FIRST) // steps
        past_shared = (i + steps - FIRST - SHARED) // steps
        return pl.multiple_of((i + in_shared * dp * SHARED + past_shared * (SHARED - dp * SHARED)) * TILE, TILE)

    half = TILE // 2

    def tile_copies(i, slot):
        at = column(i)
        return [
            pltpu.make_async_copy(
                w_ref.at[pl.ds(at + k * half, half), :], wbuf.at[slot, pl.ds(k * half, half), :], w_sem.at[slot, k]
            )
            for k in (0, 1)
        ]

    tail_copy = pltpu.make_async_copy(w_ref.at[pl.ds(tail_at, tail), :], wtail, wt_sem)
    q_copy = pltpu.make_async_copy(q_ref, qv, q_sem)
    for c in tile_copies(0, 0):
        c.start()
    tail_copy.start()
    for i in range(1, SLOTS):
        for c in tile_copies(i, i):
            c.start()
    q_copy.start()

    barrier = pltpu.get_barrier_semaphore()
    for other in [partner] + peers:
        pl.semaphore_signal(barrier, inc=1, device_id=other, device_id_type=MESH)

    h = h_ref[...].astype(F32)
    inv_rms = lax.rsqrt(jnp.mean(h * h, axis=-1, keepdims=True) + 1e-5)
    xf[...] = h * inv_rms * g_ref[...][None]
    for b in range(4):
        tv[0, b : b + 1, :] = jnp.full((1, 128), 1.0, F32) / jnp.full((1, 128), t_ref[b], F32)
        for j in range(4):
            tv[1 + j, b : b + 1, :] = jnp.full((1, 128), dt_ref[b, j].astype(F32), F32)

    def lay_rows(src, t_src, at):
        xrows[...] = jnp.zeros_like(xrows)
        lane = lax.broadcasted_iota(jnp.int32, (1, 128), 1) + tp * n_ids
        for b in range(4):
            for j in range(5):
                xrows[8 * b + j : 8 * b + j + 1, :] = src[j, b : b + 1, :]
            ct[at + 8 * b : at + 8 * b + 8, :] = jnp.broadcast_to(t_src[0, b : b + 1, :], (8, 128))
            dl[at + 8 * b : at + 8 * b + 8, :] = jnp.full((8, 128), -1.0, F32)
            for j in range(4):
                dl[at + 8 * b + j : at + 8 * b + j + 1, :] = t_src[1 + j, b : b + 1, :] - lane.astype(F32)
        xb[at : at + 32, :] = xrows[...].astype(jnp.bfloat16)

    lay_rows(xf, tv, 0)
    m_scr[...] = jnp.full(m_scr.shape, LOWEST, F32)
    l_scr[...] = jnp.zeros_like(l_scr)
    k_scr[...] = jnp.zeros_like(k_scr)

    pl.semaphore_wait(barrier, 4)
    x_copy = pltpu.make_async_remote_copy(
        src_ref=xf, dst_ref=xp, send_sem=x_sem.at[0], recv_sem=x_sem.at[1], device_id=partner, device_id_type=MESH
    )
    t_copy = pltpu.make_async_remote_copy(
        src_ref=tv, dst_ref=tp_recv, send_sem=t_sem.at[0], recv_sem=t_sem.at[1], device_id=partner, device_id_type=MESH
    )
    x_copy.start()
    t_copy.start()

    def product(rows, w):
        return lax.dot_general(xb[0:rows, :], w, (((1,), (1,)), ((), ())), preferred_element_type=F32)

    def fold(rows, parts):
        m_old = m_scr[0:rows, :]
        m_new = m_old
        for p in parts:
            m_new = jnp.maximum(m_new, p)
        total = l_scr[0:rows, :] * jnp.exp(m_old - m_new)
        for p in parts:
            total = total + jnp.exp(p - m_new)
        m_scr[0:rows, :] = m_new
        l_scr[0:rows, :] = total

    tail_copy.wait()
    z = product(32, wtail[...])
    s = z * ct[0:32, 0:tail]
    for b in range(4):
        s_scr[b, :, tail_at : tail_at + tail] = s[8 * b : 8 * b + 4, :]
    k_scr[0:32, 0:tail] = jnp.where(dl[0:32, 0:tail] == float(tail_at), s, 0.0)
    m_tail = jnp.max(s, axis=1, keepdims=True)
    l_tail = jnp.sum(jnp.exp(s - m_tail), axis=1, keepdims=True)
    lane0 = lax.broadcasted_iota(jnp.int32, (32, 128), 1) == 0
    m_scr[0:32, :] = jnp.where(lane0, m_tail, LOWEST)
    l_scr[0:32, :] = jnp.where(lane0, l_tail, 0.0)

    def z_copy(k):
        at = column(FIRST + k)
        return pltpu.make_async_remote_copy(
            src_ref=zsend.at[k], dst_ref=s_scr.at[:, :, pl.ds(at, TILE)], send_sem=zs_sem.at[k], recv_sem=zr_sem.at[k],
            device_id=partner, device_id_type=MESH,
        )

    def step(i, rows):
        slot = i % SLOTS
        for c in tile_copies(i, slot):
            c.wait()
        if rows == 64:
            k = i - FIRST

            @pl.when(k > 0)
            def _():
                z_copy(k - 1).start()

        at = column(i)
        kept = k_scr[0:rows, :]
        for c in range(TILE // SUB):
            z = product(rows, wbuf[slot, c * SUB : (c + 1) * SUB, :])
            parts = []
            for lane in range(0, SUB, 128):
                s = z[:, lane : lane + 128] * ct[0:rows, :]
                parts.append(s)
                off = c * SUB + lane
                kept = jnp.where(dl[0:rows, :] == (at + off).astype(F32), s, kept)
                for b in range(4):
                    s_scr[b, :, pl.ds(at + off, 128)] = s[8 * b : 8 * b + 4, :]
                    if rows == 64:
                        zsend[k, b, :, off : off + 128] = s[32 + 8 * b : 32 + 8 * b + 4, :]
            fold(rows, parts)
        k_scr[0:rows, :] = kept

        @pl.when(i + SLOTS < steps)
        def _():
            for c in tile_copies(i + SLOTS, slot):
                c.start()

    lax.fori_loop(0, FIRST, lambda i, _: step(i, 32), None)
    x_copy.wait()
    t_copy.wait()
    lay_rows(xp, tp_recv, 32)
    lax.fori_loop(FIRST, FIRST + SHARED, lambda i, _: step(i, 64), None)
    pstat_s[0] = m_scr[32:64, :]
    pstat_s[1] = l_scr[32:64, :]
    pstat_s[2] = k_scr[32:64, :]
    z_copy(SHARED - 1).start()
    stat_copy = pltpu.make_async_remote_copy(
        src_ref=pstat_s, dst_ref=pstat_r, send_sem=ps_sem.at[0], recv_sem=ps_sem.at[1],
        device_id=partner, device_id_type=MESH,
    )
    stat_copy.start()
    lax.fori_loop(FIRST + SHARED, steps, lambda i, _: step(i, 32), None)

    group = lax.broadcasted_iota(jnp.int32, (8, 128), 1) // 32

    def pack(cols):
        size = cols[0].shape[0]
        packed = jnp.broadcast_to(cols[0], (size, 128))
        for b in range(1, 4):
            packed = jnp.where(group[:size] == b, cols[b], packed)
        return packed

    def unpack(packed, b):
        size = packed.shape[0]
        lane = lax.broadcasted_iota(jnp.int32, (size, 128), 1)
        return jnp.sum(jnp.where(lane == 32 * b, packed, 0.0), axis=1, keepdims=True)

    def exchange(src, dst, sem):
        return [
            pltpu.make_async_remote_copy(
                src_ref=src, dst_ref=dst.at[d], send_sem=sem.at[0, d], recv_sem=sem.at[1, d],
                device_id=peers[d], device_id_type=MESH,
            )
            for d in range(3)
        ]

    stat_copy.wait()
    m = jnp.maximum(m_scr[0:32, :], pstat_r[0])
    total = l_scr[0:32, :] * jnp.exp(m_scr[0:32, :] - m) + pstat_r[1] * jnp.exp(pstat_r[0] - m)
    row_max = jnp.max(m, axis=1, keepdims=True)
    row_lse = row_max + jnp.log(jnp.sum(total * jnp.exp(m - row_max), axis=1, keepdims=True))
    e1s[...] = pack([row_lse[8 * b : 8 * b + 8, :] for b in range(4)])
    e1 = exchange(e1s, e1r, e1_sem)
    for c in e1:
        c.start()

    q_copy.wait()
    own = [dl[8 * b : 8 * b + 4, :] for b in range(4)]

    def pick(i, found):
        at = pl.multiple_of(i * PASS, PASS)
        out = []
        for b in range(4):
            f = found[b]
            for off in range(0, PASS, 128):
                f = jnp.where(own[b] == (at + off).astype(F32), qv[b, :, pl.ds(at + off, 128)], f)
            out.append(f)
        return tuple(out)

    zero = jnp.zeros((4, 128), F32)
    found = lax.fori_loop(0, tail_at // PASS, pick, (zero,) * 4)
    token_q, token_s = [], []
    for b in range(4):
        f = jnp.where(own[b][:, :tail] == float(tail_at), qv[b, :, tail_at : tail_at + tail], 0.0)
        token_q.append(jnp.sum(found[b], axis=1, keepdims=True) + jnp.sum(f, axis=1, keepdims=True))
        kept = k_scr[8 * b : 8 * b + 4, :] + pstat_r[2, 8 * b : 8 * b + 4, :]
        token_s.append(jnp.sum(kept, axis=1, keepdims=True))
    e3s[0] = pack(token_s)
    e3s[1] = pack(token_q)
    e3 = exchange(e3s, e3r, e3_sem)
    for c in e3:
        c.start()

    def await_z(k, _):
        z_copy(k).wait_send()
        pltpu.make_async_remote_copy(
            src_ref=zsend.at[k], dst_ref=s_scr.at[:, :, pl.ds(pl.multiple_of((FIRST + (1 - dp) * SHARED + k) * TILE, TILE), TILE)],
            send_sem=zs_sem.at[k], recv_sem=zr_sem.at[k], device_id=partner, device_id_type=MESH,
        ).wait_recv()
        return None

    lax.fori_loop(0, SHARED, await_z, None)
    for c in e1:
        c.wait()
    lses = [e1s[...]] + [e1r[d] for d in range(3)]
    top = jnp.maximum(jnp.maximum(lses[0], lses[1]), jnp.maximum(lses[2], lses[3]))
    sums = jnp.exp(lses[0] - top) + jnp.exp(lses[1] - top) + jnp.exp(lses[2] - top) + jnp.exp(lses[3] - top)
    lse = top + jnp.log(sums)
    lse_ref[...] = lse
    row_l = [jnp.broadcast_to(unpack(lse[0:4, :], b), (4, 128)) for b in range(4)]

    def excess(b, at, size):
        e = jnp.maximum(jnp.exp(s_scr[b, :, pl.ds(at, size)] - row_l[b][:, :size]) - qv[b, :, pl.ds(at, size)], 0.0)
        ex_ref[b, :, pl.ds(at, size)] = e
        return e

    def last_pass(i, sums):
        at = pl.multiple_of(i * PASS, PASS)
        out = []
        for b in range(4):
            acc = sums[b]
            for off in range(0, PASS, 128):
                acc = acc + excess(b, at + off, 128)
            out.append(acc)
        return tuple(out)

    sums = lax.fori_loop(0, tail_at // PASS, last_pass, (zero,) * 4)
    rows = []
    for b in range(4):
        e = excess(b, tail_at, tail)
        rows.append(jnp.sum(sums[b], axis=1, keepdims=True) + jnp.sum(e, axis=1, keepdims=True))
    e2s[...] = pack(rows)
    e2 = exchange(e2s, e2r, e2_sem)
    for c in e2:
        c.start()

    for c in e3:
        c.wait()
    at_token = (e3s[...] + e3r[0]) + (e3r[1] + e3r[2])
    acc_ref[...] = jnp.minimum(jnp.exp(at_token[0] - lse[0:4, :]) / at_token[1], 1.0)

    for c in e2:
        c.wait()
    norm_ref[...] = (e2s[...] + e2r[0]) + (e2r[1] + e2r[2])


def finish_kernel(
    ex_ref, norm_ref, acc_ref, lse_ref, acc_out, norm_out, res_out, bonus_out, acc_v, norm_v, bonus_v, stage, sem, r_sem
):
    n_ids = ex_ref.shape[2]
    n_full = n_ids // PASS
    lane = lax.broadcasted_iota(jnp.int32, (4, 128), 1)
    norm = norm_ref[...]
    writes = []
    for b in range(4):
        total = jnp.sum(jnp.where(lane == 32 * b, norm, 0.0), axis=1, keepdims=True)
        scale = jnp.broadcast_to(1.0 / jnp.broadcast_to(total, (4, 128)), (4, 128))

        def body(i, _):
            at = pl.multiple_of(i * PASS, PASS)
            for off in range(0, PASS, 128):
                stage[b, :, pl.ds(at + off, 128)] = ex_ref[b, :, pl.ds(at + off, 128)] * scale

        lax.fori_loop(0, n_full, body, None)
        for at in range(n_full * PASS, n_ids, 128):
            size = min(128, n_ids - at)
            stage[b, :, at : at + size] = ex_ref[b, :, at : at + size] * scale[:, :size]
        writes.append(pltpu.make_async_copy(stage.at[b], res_out.at[b], r_sem.at[b]))
        writes[-1].start()

    sub = lax.broadcasted_iota(jnp.int32, (4, 128), 0)
    for src, dst, out, k in ((acc_ref[...], acc_v, acc_out, 0), (norm, norm_v, norm_out, 1)):
        row = jnp.sum(jnp.where(lane % 32 == sub, src, 0.0), axis=0, keepdims=True)
        for b in range(4):
            dst[b : b + 1, :] = (row if b == 0 else pltpu.roll(row, 128 - 32 * b, 1))[:, 0:4]
        writes.append(pltpu.make_async_copy(dst, out, sem.at[k]))
        writes[-1].start()
    row = lse_ref[4:5, :]
    lane = lane[0:1, :]
    packed = row
    for b in range(1, 4):
        packed = jnp.where(lane == b, pltpu.roll(row, 128 - 31 * b, 1), packed)
    bonus_v[...] = packed[:, 0:4]
    writes.append(pltpu.make_async_copy(bonus_v, bonus_out, sem.at[2]))
    writes[-1].start()
    for c in writes:
        c.wait()


def solution(mesh):
    def local_step(hidden, norm_gain, w_head, draft_probs, draft_tokens, temperature):
        n_ids = w_head.shape[1]
        width = w_head.shape[0]
        pad_ids = -(-n_ids // 128) * 128
        tail = n_ids % TILE
        vmem, smem, hbm = pltpu.VMEM, pltpu.SMEM, pltpu.HBM
        dma = pltpu.SemaphoreType.DMA
        ex, norm, acc, lse = pl.pallas_call(
            verify_kernel,
            out_shape=[vmem((4, 4, n_ids), F32), vmem((4, 128), F32), vmem((4, 128), F32), vmem((8, 128), F32)],
            in_specs=[pl.BlockSpec(memory_space=s) for s in (vmem, vmem, smem, smem, hbm, hbm)],
            out_specs=[pl.BlockSpec(memory_space=vmem)] * 4,
            scratch_shapes=[
                vmem((SLOTS, TILE, width), jnp.bfloat16),
                vmem((tail, width), jnp.bfloat16),
                vmem((4, 4, n_ids), F32),
                vmem((4, 4, pad_ids), F32),
                vmem((5, 4, width), F32),
                vmem((5, 4, width), F32),
                vmem((32, width), F32),
                vmem((64, width), jnp.bfloat16),
                vmem((5, 4, 128), F32),
                vmem((5, 4, 128), F32),
                vmem((64, 128), F32),
                vmem((64, 128), F32),
                vmem((64, 128), F32),
                vmem((64, 128), F32),
                vmem((64, 128), F32),
                vmem((SHARED, 4, 4, TILE), F32),
                vmem((3, 32, 128), F32),
                vmem((3, 32, 128), F32),
                vmem((8, 128), F32),
                vmem((3, 8, 128), F32),
                vmem((4, 128), F32),
                vmem((3, 4, 128), F32),
                vmem((2, 4, 128), F32),
                vmem((3, 2, 4, 128), F32),
                dma((SLOTS, 2)), dma, dma, dma((2,)), dma((2,)), dma((SHARED,)), dma((SHARED,)), dma((2,)),
                dma((2, 3)), dma((2, 3)), dma((2, 3)),
            ],
            compiler_params=pltpu.CompilerParams(collective_id=0, has_side_effects=True),
            name="verify",
        )(
            hidden.transpose(1, 0, 2), norm_gain.reshape(1, width), temperature, draft_tokens,
            w_head.T, draft_probs,
        )
        acc, norm, residual, bonus = pl.pallas_call(
            finish_kernel,
            out_shape=[
                jax.ShapeDtypeStruct((4, 4), F32),
                jax.ShapeDtypeStruct((4, 4), F32),
                jax.ShapeDtypeStruct((4, 4, n_ids), F32),
                jax.ShapeDtypeStruct((1, 4), F32),
            ],
            in_specs=[pl.BlockSpec(memory_space=vmem)] * 4,
            out_specs=[pl.BlockSpec(memory_space=hbm)] * 4,
            scratch_shapes=[
                vmem((4, 4), F32), vmem((4, 4), F32), vmem((1, 4), F32), vmem((4, 4, n_ids), F32), dma((3,)), dma((4,)),
            ],
            compiler_params=pltpu.CompilerParams(vmem_limit_bytes=16 * 1024 * 1024),
            name="finish",
        )(ex, norm, acc, lse)
        return acc, norm, residual, bonus.reshape(4)

    return jax.shard_map(
        local_step,
        mesh=mesh,
        in_specs=(P("dp", None, None), P(), P(None, "tp"), P("dp", None, "tp"), P("dp", None), P("dp")),
        out_specs=(P("dp", None), P("dp", None), P("dp", None, "tp"), P("dp")),
        check_vma=False,
    )
```

```python
import jax
import jax.numpy as jnp
from jax import lax
from jax.experimental import pallas as pl
from jax.experimental.pallas import tpu as pltpu
from jax.sharding import PartitionSpec as P

MESH = pl.DeviceIdType.MESH
F32 = jnp.float32
LOWEST = float(jnp.finfo(jnp.float32).min)

TILE = 1024
SUB = 256
SLOTS = 4
SHARED = 14
FIRST = 5
PASS = 1024


def verify_kernel(
    h_hbm, g_hbm, t_hbm, dt_hbm, w_ref, q_ref,
    ex_ref, norm_ref, acc_ref, lse_ref,
    h_ref, g_ref, t_ref, dt_ref, wbuf, wtail, qv, s_scr, xf, xp, xrows, xb, tv, tp_recv, ct, dl, m_scr, l_scr, k_scr,
    zsend, pstat_s, pstat_r, e1s, e1r, e2s, e2r, e3s, e3r,
    in_sem, w_sem, wt_sem, q_sem, x_sem, t_sem, zs_sem, zr_sem, ps_sem, e1_sem, e2_sem, e3_sem,
):
    dp, tp = lax.axis_index("dp"), lax.axis_index("tp")
    partner = (1 - dp, tp)
    peers = [(dp, lax.rem(tp + d, 4)) for d in (1, 2, 3)]
    n_ids = w_ref.shape[0]
    n_full = n_ids // TILE
    tail = n_ids - n_full * TILE
    tail_at = n_full * TILE
    last = n_full - 2 * SHARED - FIRST
    steps = FIRST + SHARED + last

    def column(i):
        in_shared = (i + steps - FIRST) // steps
        past_shared = (i + steps - FIRST - SHARED) // steps
        return pl.multiple_of((i + in_shared * dp * SHARED + past_shared * (SHARED - dp * SHARED)) * TILE, TILE)

    half = TILE // 2

    def tile_copies(i, slot):
        at = column(i)
        return [
            pltpu.make_async_copy(
                w_ref.at[pl.ds(at + k * half, half), :], wbuf.at[slot, pl.ds(k * half, half), :], w_sem.at[slot, k]
            )
            for k in (0, 1)
        ]

    tail_copy = pltpu.make_async_copy(w_ref.at[pl.ds(tail_at, tail), :], wtail, wt_sem)
    q_copy = pltpu.make_async_copy(q_ref, qv, q_sem)
    small = [
        pltpu.make_async_copy(src, dst, in_sem.at[k])
        for k, (src, dst) in enumerate(((h_hbm, h_ref), (g_hbm, g_ref), (t_hbm, t_ref), (dt_hbm, dt_ref)))
    ]
    for c in small:
        c.start()
    tail_copy.start()
    for i in range(SLOTS):
        for c in tile_copies(i, i):
            c.start()
    q_copy.start()

    barrier = pltpu.get_barrier_semaphore()
    for other in [partner] + peers:
        pl.semaphore_signal(barrier, inc=1, device_id=other, device_id_type=MESH)

    for c in small:
        c.wait()
    h = h_ref[...].astype(F32)
    inv_rms = lax.rsqrt(jnp.mean(h * h, axis=-1, keepdims=True) + 1e-5)
    xf[...] = h * inv_rms * g_ref[...][None]
    for b in range(4):
        tv[0, b : b + 1, :] = jnp.full((1, 128), 1.0, F32) / jnp.full((1, 128), t_ref[b], F32)
        for j in range(4):
            tv[1 + j, b : b + 1, :] = jnp.full((1, 128), dt_ref[b, j].astype(F32), F32)

    def lay_rows(src, t_src, at):
        xrows[...] = jnp.zeros_like(xrows)
        lane = lax.broadcasted_iota(jnp.int32, (1, 128), 1) + tp * n_ids
        for b in range(4):
            for j in range(5):
                xrows[8 * b + j : 8 * b + j + 1, :] = src[j, b : b + 1, :]
            ct[at + 8 * b : at + 8 * b + 8, :] = jnp.broadcast_to(t_src[0, b : b + 1, :], (8, 128))
            dl[at + 8 * b : at + 8 * b + 8, :] = jnp.full((8, 128), -1.0, F32)
            for j in range(4):
                dl[at + 8 * b + j : at + 8 * b + j + 1, :] = t_src[1 + j, b : b + 1, :] - lane.astype(F32)
        xb[at : at + 32, :] = xrows[...].astype(jnp.bfloat16)

    lay_rows(xf, tv, 0)
    m_scr[...] = jnp.full(m_scr.shape, LOWEST, F32)
    l_scr[...] = jnp.zeros_like(l_scr)
    k_scr[...] = jnp.zeros_like(k_scr)

    pl.semaphore_wait(barrier, 4)
    x_copy = pltpu.make_async_remote_copy(
        src_ref=xf, dst_ref=xp, send_sem=x_sem.at[0], recv_sem=x_sem.at[1], device_id=partner, device_id_type=MESH
    )
    t_copy = pltpu.make_async_remote_copy(
        src_ref=tv, dst_ref=tp_recv, send_sem=t_sem.at[0], recv_sem=t_sem.at[1], device_id=partner, device_id_type=MESH
    )
    x_copy.start()
    t_copy.start()

    def product(rows, w):
        return lax.dot_general(xb[0:rows, :], w, (((1,), (1,)), ((), ())), preferred_element_type=F32)

    def fold(rows, parts):
        m_old = m_scr[0:rows, :]
        m_new = m_old
        for p in parts:
            m_new = jnp.maximum(m_new, p)
        total = l_scr[0:rows, :] * jnp.exp(m_old - m_new)
        for p in parts:
            total = total + jnp.exp(p - m_new)
        m_scr[0:rows, :] = m_new
        l_scr[0:rows, :] = total

    tail_copy.wait()
    z = product(32, wtail[...])
    s = z * ct[0:32, 0:tail]
    for b in range(4):
        s_scr[b, :, tail_at : tail_at + tail] = s[8 * b : 8 * b + 4, :]
    k_scr[0:32, 0:tail] = jnp.where(dl[0:32, 0:tail] == float(tail_at), s, 0.0)
    m_tail = jnp.max(s, axis=1, keepdims=True)
    l_tail = jnp.sum(jnp.exp(s - m_tail), axis=1, keepdims=True)
    lane0 = lax.broadcasted_iota(jnp.int32, (32, 128), 1) == 0
    m_scr[0:32, :] = jnp.where(lane0, m_tail, LOWEST)
    l_scr[0:32, :] = jnp.where(lane0, l_tail, 0.0)

    def z_copy(k):
        at = column(FIRST + k)
        return pltpu.make_async_remote_copy(
            src_ref=zsend.at[k], dst_ref=s_scr.at[:, :, pl.ds(at, TILE)], send_sem=zs_sem.at[k], recv_sem=zr_sem.at[k],
            device_id=partner, device_id_type=MESH,
        )

    def step(i, rows):
        slot = i % SLOTS
        for c in tile_copies(i, slot):
            c.wait()
        if rows == 64:
            k = i - FIRST

            @pl.when(k > 0)
            def _():
                z_copy(k - 1).start()

        at = column(i)
        kept = k_scr[0:rows, :]
        for c in range(TILE // SUB):
            z = product(rows, wbuf[slot, c * SUB : (c + 1) * SUB, :])
            parts = []
            for lane in range(0, SUB, 128):
                s = z[:, lane : lane + 128] * ct[0:rows, :]
                parts.append(s)
                off = c * SUB + lane
                kept = jnp.where(dl[0:rows, :] == (at + off).astype(F32), s, kept)
                for b in range(4):
                    s_scr[b, :, pl.ds(at + off, 128)] = s[8 * b : 8 * b + 4, :]
                    if rows == 64:
                        zsend[k, b, :, off : off + 128] = s[32 + 8 * b : 32 + 8 * b + 4, :]
            fold(rows, parts)
        k_scr[0:rows, :] = kept

        @pl.when(i + SLOTS < steps)
        def _():
            for c in tile_copies(i + SLOTS, slot):
                c.start()

    lax.fori_loop(0, FIRST, lambda i, _: step(i, 32), None)
    x_copy.wait()
    t_copy.wait()
    lay_rows(xp, tp_recv, 32)
    lax.fori_loop(FIRST, FIRST + SHARED, lambda i, _: step(i, 64), None)
    pstat_s[0] = m_scr[32:64, :]
    pstat_s[1] = l_scr[32:64, :]
    pstat_s[2] = k_scr[32:64, :]
    z_copy(SHARED - 1).start()
    stat_copy = pltpu.make_async_remote_copy(
        src_ref=pstat_s, dst_ref=pstat_r, send_sem=ps_sem.at[0], recv_sem=ps_sem.at[1],
        device_id=partner, device_id_type=MESH,
    )
    stat_copy.start()
    lax.fori_loop(FIRST + SHARED, steps, lambda i, _: step(i, 32), None)

    group = lax.broadcasted_iota(jnp.int32, (8, 128), 1) // 32

    def pack(cols):
        size = cols[0].shape[0]
        packed = jnp.broadcast_to(cols[0], (size, 128))
        for b in range(1, 4):
            packed = jnp.where(group[:size] == b, cols[b], packed)
        return packed

    def unpack(packed, b):
        size = packed.shape[0]
        lane = lax.broadcasted_iota(jnp.int32, (size, 128), 1)
        return jnp.sum(jnp.where(lane == 32 * b, packed, 0.0), axis=1, keepdims=True)

    def exchange(src, dst, sem):
        return [
            pltpu.make_async_remote_copy(
                src_ref=src, dst_ref=dst.at[d], send_sem=sem.at[0, d], recv_sem=sem.at[1, d],
                device_id=peers[d], device_id_type=MESH,
            )
            for d in range(3)
        ]

    stat_copy.wait()
    m = jnp.maximum(m_scr[0:32, :], pstat_r[0])
    total = l_scr[0:32, :] * jnp.exp(m_scr[0:32, :] - m) + pstat_r[1] * jnp.exp(pstat_r[0] - m)
    row_max = jnp.max(m, axis=1, keepdims=True)
    row_lse = row_max + jnp.log(jnp.sum(total * jnp.exp(m - row_max), axis=1, keepdims=True))
    e1s[...] = pack([row_lse[8 * b : 8 * b + 8, :] for b in range(4)])
    e1 = exchange(e1s, e1r, e1_sem)
    for c in e1:
        c.start()

    q_copy.wait()
    own = [dl[8 * b : 8 * b + 4, :] for b in range(4)]

    def pick(i, found):
        at = pl.multiple_of(i * PASS, PASS)
        out = []
        for b in range(4):
            f = found[b]
            for off in range(0, PASS, 128):
                f = jnp.where(own[b] == (at + off).astype(F32), qv[b, :, pl.ds(at + off, 128)], f)
            out.append(f)
        return tuple(out)

    zero = jnp.zeros((4, 128), F32)
    found = lax.fori_loop(0, tail_at // PASS, pick, (zero,) * 4)
    token_q, token_s = [], []
    for b in range(4):
        f = jnp.where(own[b][:, :tail] == float(tail_at), qv[b, :, tail_at : tail_at + tail], 0.0)
        token_q.append(jnp.sum(found[b], axis=1, keepdims=True) + jnp.sum(f, axis=1, keepdims=True))
        kept = k_scr[8 * b : 8 * b + 4, :] + pstat_r[2, 8 * b : 8 * b + 4, :]
        token_s.append(jnp.sum(kept, axis=1, keepdims=True))
    e3s[0] = pack(token_s)
    e3s[1] = pack(token_q)
    e3 = exchange(e3s, e3r, e3_sem)
    for c in e3:
        c.start()

    def await_z(k, _):
        z_copy(k).wait_send()
        pltpu.make_async_remote_copy(
            src_ref=zsend.at[k], dst_ref=s_scr.at[:, :, pl.ds(pl.multiple_of((FIRST + (1 - dp) * SHARED + k) * TILE, TILE), TILE)],
            send_sem=zs_sem.at[k], recv_sem=zr_sem.at[k], device_id=partner, device_id_type=MESH,
        ).wait_recv()
        return None

    lax.fori_loop(0, SHARED, await_z, None)
    for c in e1:
        c.wait()
    lses = [e1s[...]] + [e1r[d] for d in range(3)]
    top = jnp.maximum(jnp.maximum(lses[0], lses[1]), jnp.maximum(lses[2], lses[3]))
    sums = jnp.exp(lses[0] - top) + jnp.exp(lses[1] - top) + jnp.exp(lses[2] - top) + jnp.exp(lses[3] - top)
    lse = top + jnp.log(sums)
    lse_ref[...] = lse
    row_l = [jnp.broadcast_to(unpack(lse[0:4, :], b), (4, 128)) for b in range(4)]

    def excess(b, at, size):
        e = jnp.maximum(jnp.exp(s_scr[b, :, pl.ds(at, size)] - row_l[b][:, :size]) - qv[b, :, pl.ds(at, size)], 0.0)
        ex_ref[b, :, pl.ds(at, size)] = e
        return e

    def last_pass(i, sums):
        at = pl.multiple_of(i * PASS, PASS)
        out = []
        for b in range(4):
            acc = sums[b]
            for off in range(0, PASS, 128):
                acc = acc + excess(b, at + off, 128)
            out.append(acc)
        return tuple(out)

    sums = lax.fori_loop(0, tail_at // PASS, last_pass, (zero,) * 4)
    rows = []
    for b in range(4):
        e = excess(b, tail_at, tail)
        rows.append(jnp.sum(sums[b], axis=1, keepdims=True) + jnp.sum(e, axis=1, keepdims=True))
    e2s[...] = pack(rows)
    e2 = exchange(e2s, e2r, e2_sem)
    for c in e2:
        c.start()

    for c in e3:
        c.wait()
    at_token = (e3s[...] + e3r[0]) + (e3r[1] + e3r[2])
    acc_ref[...] = jnp.minimum(jnp.exp(at_token[0] - lse[0:4, :]) / at_token[1], 1.0)

    for c in e2:
        c.wait()
    norm_ref[...] = (e2s[...] + e2r[0]) + (e2r[1] + e2r[2])


def finish_kernel(
    ex_ref, norm_ref, acc_ref, lse_ref, acc_out, norm_out, res_out, bonus_out, acc_v, norm_v, bonus_v, stage, sem, r_sem
):
    n_ids = ex_ref.shape[2]
    lane = lax.broadcasted_iota(jnp.int32, (4, 128), 1)
    norm = norm_ref[...]
    writes = []
    for b in range(4):
        total = jnp.sum(jnp.where(lane == 32 * b, norm, 0.0), axis=1, keepdims=True)
        scale = jnp.broadcast_to(1.0 / jnp.broadcast_to(total, (4, 128)), (4, 128))

        for at in range(0, n_ids, 128):
            size = min(128, n_ids - at)
            stage[b, :, at : at + size] = ex_ref[b, :, at : at + size] * scale[:, :size]
        writes.append(pltpu.make_async_copy(stage.at[b], res_out.at[b], r_sem.at[b]))
        writes[-1].start()

    sub = lax.broadcasted_iota(jnp.int32, (4, 128), 0)
    for src, dst, out, k in ((acc_ref[...], acc_v, acc_out, 0), (norm, norm_v, norm_out, 1)):
        row = jnp.sum(jnp.where(lane % 32 == sub, src, 0.0), axis=0, keepdims=True)
        for b in range(4):
            dst[b : b + 1, :] = (row if b == 0 else pltpu.roll(row, 128 - 32 * b, 1))[:, 0:4]
        writes.append(pltpu.make_async_copy(dst, out, sem.at[k]))
        writes[-1].start()
    row = lse_ref[4:5, :]
    lane = lane[0:1, :]
    packed = row
    for b in range(1, 4):
        packed = jnp.where(lane == b, pltpu.roll(row, 128 - 31 * b, 1), packed)
    bonus_v[...] = packed[:, 0:4]
    writes.append(pltpu.make_async_copy(bonus_v, bonus_out, sem.at[2]))
    writes[-1].start()
    for c in writes:
        c.wait()


def solution(mesh):
    def local_step(hidden, norm_gain, w_head, draft_probs, draft_tokens, temperature):
        n_ids = w_head.shape[1]
        width = w_head.shape[0]
        pad_ids = -(-n_ids // 128) * 128
        tail = n_ids % TILE
        vmem, smem, hbm = pltpu.VMEM, pltpu.SMEM, pltpu.HBM
        dma = pltpu.SemaphoreType.DMA
        ex, norm, acc, lse = pl.pallas_call(
            verify_kernel,
            out_shape=[vmem((4, 4, n_ids), F32), vmem((4, 128), F32), vmem((4, 128), F32), vmem((8, 128), F32)],
            in_specs=[pl.BlockSpec(memory_space=s) for s in (hbm,) * 6],
            out_specs=[pl.BlockSpec(memory_space=vmem)] * 4,
            scratch_shapes=[
                vmem((5, 4, width), jnp.bfloat16),
                vmem((1, width), F32),
                smem((4,), F32),
                smem((4, 4), jnp.int32),
                vmem((SLOTS, TILE, width), jnp.bfloat16),
                vmem((tail, width), jnp.bfloat16),
                vmem((4, 4, n_ids), F32),
                vmem((4, 4, pad_ids), F32),
                vmem((5, 4, width), F32),
                vmem((5, 4, width), F32),
                vmem((32, width), F32),
                vmem((64, width), jnp.bfloat16),
                vmem((5, 4, 128), F32),
                vmem((5, 4, 128), F32),
                vmem((64, 128), F32),
                vmem((64, 128), F32),
                vmem((64, 128), F32),
                vmem((64, 128), F32),
                vmem((64, 128), F32),
                vmem((SHARED, 4, 4, TILE), F32),
                vmem((3, 32, 128), F32),
                vmem((3, 32, 128), F32),
                vmem((8, 128), F32),
                vmem((3, 8, 128), F32),
                vmem((4, 128), F32),
                vmem((3, 4, 128), F32),
                vmem((2, 4, 128), F32),
                vmem((3, 2, 4, 128), F32),
                dma((4,)), dma((SLOTS, 2)), dma, dma, dma((2,)), dma((2,)), dma((SHARED,)), dma((SHARED,)), dma((2,)),
                dma((2, 3)), dma((2, 3)), dma((2, 3)),
            ],
            compiler_params=pltpu.CompilerParams(collective_id=0, has_side_effects=True),
            name="verify",
        )(
            hidden.transpose(1, 0, 2), norm_gain.reshape(1, width), temperature, draft_tokens,
            w_head.T, draft_probs,
        )
        acc, norm, residual, bonus = pl.pallas_call(
            finish_kernel,
            out_shape=[
                jax.ShapeDtypeStruct((4, 4), F32),
                jax.ShapeDtypeStruct((4, 4), F32),
                jax.ShapeDtypeStruct((4, 4, n_ids), F32),
                jax.ShapeDtypeStruct((1, 4), F32),
            ],
            in_specs=[pl.BlockSpec(memory_space=vmem)] * 4,
            out_specs=[pl.BlockSpec(memory_space=hbm)] * 4,
            scratch_shapes=[
                vmem((4, 4), F32), vmem((4, 4), F32), vmem((1, 4), F32), vmem((4, 4, n_ids), F32), dma((3,)), dma((4,)),
            ],
            compiler_params=pltpu.CompilerParams(vmem_limit_bytes=16 * 1024 * 1024),
            name="finish",
        )(ex, norm, acc, lse)
        return acc, norm, residual, bonus.reshape(4)

    return jax.shard_map(
        local_step,
        mesh=mesh,
        in_specs=(P("dp", None, None), P(), P(None, "tp"), P("dp", None, "tp"), P("dp", None), P("dp")),
        out_specs=(P("dp", None), P("dp", None), P("dp", None, "tp"), P("dp")),
        check_vma=False,
    )
```

```python
import jax
import jax.numpy as jnp
from jax import lax
from jax.experimental import pallas as pl
from jax.experimental.pallas import tpu as pltpu
from jax.sharding import PartitionSpec as P

MESH = pl.DeviceIdType.MESH
F32 = jnp.float32
LOWEST = float(jnp.finfo(jnp.float32).min)

TILE = 1024
SUB = 256
SLOTS = 4
SHARED = 11
FIRST = 8
PASS = 1024


def verify_kernel(
    h_hbm, g_hbm, t_hbm, dt_hbm, w_ref, q_ref,
    ex_ref, norm_ref, acc_ref, lse_ref,
    h_ref, g_ref, t_ref, dt_ref, wbuf, wtail, qv, s_scr, xf, xp, xrows, xb, tv, tp_recv, ct, dl, m_scr, l_scr, k_scr,
    zsend, pstat_s, pstat_r, e1s, e1r, e2s, e2r, e3s, e3r,
    in_sem, w_sem, wt_sem, q_sem, x_sem, t_sem, zs_sem, zr_sem, ps_sem, e1_sem, e2_sem, e3_sem,
):
    dp, tp = lax.axis_index("dp"), lax.axis_index("tp")
    partner = (1 - dp, tp)
    peers = [(dp, lax.rem(tp + d, 4)) for d in (1, 2, 3)]
    n_ids = w_ref.shape[0]
    n_full = n_ids // TILE
    tail = n_ids - n_full * TILE
    tail_at = n_full * TILE
    last = n_full - 2 * SHARED - FIRST
    steps = FIRST + SHARED + last

    def column(i):
        in_shared = (i + steps - FIRST) // steps
        past_shared = (i + steps - FIRST - SHARED) // steps
        return pl.multiple_of((i + in_shared * dp * SHARED + past_shared * (SHARED - dp * SHARED)) * TILE, TILE)

    half = TILE // 2

    def tile_copies(i, slot):
        at = column(i)
        return [
            pltpu.make_async_copy(
                w_ref.at[pl.ds(at + k * half, half), :], wbuf.at[slot, pl.ds(k * half, half), :], w_sem.at[slot, k]
            )
            for k in (0, 1)
        ]

    tail_copy = pltpu.make_async_copy(w_ref.at[pl.ds(tail_at, tail), :], wtail, wt_sem)
    q_copy = pltpu.make_async_copy(q_ref, qv, q_sem)
    small = [
        pltpu.make_async_copy(src, dst, in_sem.at[k])
        for k, (src, dst) in enumerate(((h_hbm, h_ref), (g_hbm, g_ref), (t_hbm, t_ref), (dt_hbm, dt_ref)))
    ]
    for c in small:
        c.start()
    tail_copy.start()
    for i in range(SLOTS):
        for c in tile_copies(i, i):
            c.start()
    q_copy.start()

    barrier = pltpu.get_barrier_semaphore()
    for other in [partner] + peers:
        pl.semaphore_signal(barrier, inc=1, device_id=other, device_id_type=MESH)

    for c in small:
        c.wait()
    h = h_ref[...].astype(F32)
    inv_rms = lax.rsqrt(jnp.mean(h * h, axis=-1, keepdims=True) + 1e-5)
    xf[...] = h * inv_rms * g_ref[...][None]
    for b in range(4):
        tv[0, b : b + 1, :] = jnp.full((1, 128), 1.0, F32) / jnp.full((1, 128), t_ref[b], F32)
        for j in range(4):
            tv[1 + j, b : b + 1, :] = jnp.full((1, 128), dt_ref[b, j].astype(F32), F32)

    def lay_rows(src, t_src, at):
        xrows[...] = jnp.zeros_like(xrows)
        lane = lax.broadcasted_iota(jnp.int32, (1, 128), 1) + tp * n_ids
        for b in range(4):
            for j in range(5):
                xrows[8 * b + j : 8 * b + j + 1, :] = src[j, b : b + 1, :]
            ct[at + 8 * b : at + 8 * b + 8, :] = jnp.broadcast_to(t_src[0, b : b + 1, :], (8, 128))
            dl[at + 8 * b : at + 8 * b + 8, :] = jnp.full((8, 128), -1.0, F32)
            for j in range(4):
                dl[at + 8 * b + j : at + 8 * b + j + 1, :] = t_src[1 + j, b : b + 1, :] - lane.astype(F32)
        xb[at : at + 32, :] = xrows[...].astype(jnp.bfloat16)

    lay_rows(xf, tv, 0)
    m_scr[...] = jnp.full(m_scr.shape, LOWEST, F32)
    l_scr[...] = jnp.zeros_like(l_scr)
    k_scr[...] = jnp.zeros_like(k_scr)

    pl.semaphore_wait(barrier, 4)
    x_copy = pltpu.make_async_remote_copy(
        src_ref=xf, dst_ref=xp, send_sem=x_sem.at[0], recv_sem=x_sem.at[1], device_id=partner, device_id_type=MESH
    )
    t_copy = pltpu.make_async_remote_copy(
        src_ref=tv, dst_ref=tp_recv, send_sem=t_sem.at[0], recv_sem=t_sem.at[1], device_id=partner, device_id_type=MESH
    )
    x_copy.start()
    t_copy.start()

    def product(rows, w):
        return lax.dot_general(xb[0:rows, :], w, (((1,), (1,)), ((), ())), preferred_element_type=F32)

    def fold(rows, parts):
        m_old = m_scr[0:rows, :]
        m_new = m_old
        for p in parts:
            m_new = jnp.maximum(m_new, p)
        total = l_scr[0:rows, :] * jnp.exp(m_old - m_new)
        for p in parts:
            total = total + jnp.exp(p - m_new)
        m_scr[0:rows, :] = m_new
        l_scr[0:rows, :] = total

    tail_copy.wait()
    z = product(32, wtail[...])
    s = z * ct[0:32, 0:tail]
    for b in range(4):
        s_scr[b, :, tail_at : tail_at + tail] = s[8 * b : 8 * b + 4, :]
    k_scr[0:32, 0:tail] = jnp.where(dl[0:32, 0:tail] == float(tail_at), s, 0.0)
    m_tail = jnp.max(s, axis=1, keepdims=True)
    l_tail = jnp.sum(jnp.exp(s - m_tail), axis=1, keepdims=True)
    lane0 = lax.broadcasted_iota(jnp.int32, (32, 128), 1) == 0
    m_scr[0:32, :] = jnp.where(lane0, m_tail, LOWEST)
    l_scr[0:32, :] = jnp.where(lane0, l_tail, 0.0)

    def z_copy(k):
        at = column(FIRST + k)
        return pltpu.make_async_remote_copy(
            src_ref=zsend.at[k], dst_ref=s_scr.at[:, :, pl.ds(at, TILE)], send_sem=zs_sem.at[k], recv_sem=zr_sem.at[k],
            device_id=partner, device_id_type=MESH,
        )

    def step(i, rows):
        slot = i % SLOTS
        for c in tile_copies(i, slot):
            c.wait()
        if rows == 64:
            k = i - FIRST

            @pl.when(k > 0)
            def _():
                z_copy(k - 1).start()

        at = column(i)
        kept = k_scr[0:rows, :]
        for c in range(TILE // SUB):
            z = product(rows, wbuf[slot, c * SUB : (c + 1) * SUB, :])
            parts = []
            for lane in range(0, SUB, 128):
                s = z[:, lane : lane + 128] * ct[0:rows, :]
                parts.append(s)
                off = c * SUB + lane
                kept = jnp.where(dl[0:rows, :] == (at + off).astype(F32), s, kept)
                for b in range(4):
                    s_scr[b, :, pl.ds(at + off, 128)] = s[8 * b : 8 * b + 4, :]
                    if rows == 64:
                        zsend[k, b, :, off : off + 128] = s[32 + 8 * b : 32 + 8 * b + 4, :]
            fold(rows, parts)
        k_scr[0:rows, :] = kept

        @pl.when(i + SLOTS < steps)
        def _():
            for c in tile_copies(i + SLOTS, slot):
                c.start()

    lax.fori_loop(0, FIRST, lambda i, _: step(i, 32), None)
    x_copy.wait()
    t_copy.wait()
    lay_rows(xp, tp_recv, 32)
    lax.fori_loop(FIRST, FIRST + SHARED, lambda i, _: step(i, 64), None)
    pstat_s[0] = m_scr[32:64, :]
    pstat_s[1] = l_scr[32:64, :]
    pstat_s[2] = k_scr[32:64, :]
    z_copy(SHARED - 1).start()
    stat_copy = pltpu.make_async_remote_copy(
        src_ref=pstat_s, dst_ref=pstat_r, send_sem=ps_sem.at[0], recv_sem=ps_sem.at[1],
        device_id=partner, device_id_type=MESH,
    )
    stat_copy.start()
    lax.fori_loop(FIRST + SHARED, steps, lambda i, _: step(i, 32), None)

    group = lax.broadcasted_iota(jnp.int32, (8, 128), 1) // 32

    def pack(cols):
        size = cols[0].shape[0]
        packed = jnp.broadcast_to(cols[0], (size, 128))
        for b in range(1, 4):
            packed = jnp.where(group[:size] == b, cols[b], packed)
        return packed

    def unpack(packed, b):
        size = packed.shape[0]
        lane = lax.broadcasted_iota(jnp.int32, (size, 128), 1)
        return jnp.sum(jnp.where(lane == 32 * b, packed, 0.0), axis=1, keepdims=True)

    def exchange(src, dst, sem):
        return [
            pltpu.make_async_remote_copy(
                src_ref=src, dst_ref=dst.at[d], send_sem=sem.at[0, d], recv_sem=sem.at[1, d],
                device_id=peers[d], device_id_type=MESH,
            )
            for d in range(3)
        ]

    stat_copy.wait()
    m = jnp.maximum(m_scr[0:32, :], pstat_r[0])
    total = l_scr[0:32, :] * jnp.exp(m_scr[0:32, :] - m) + pstat_r[1] * jnp.exp(pstat_r[0] - m)
    row_max = jnp.max(m, axis=1, keepdims=True)
    row_lse = row_max + jnp.log(jnp.sum(total * jnp.exp(m - row_max), axis=1, keepdims=True))
    e1s[...] = pack([row_lse[8 * b : 8 * b + 8, :] for b in range(4)])
    e1 = exchange(e1s, e1r, e1_sem)
    for c in e1:
        c.start()

    q_copy.wait()
    own = [dl[8 * b : 8 * b + 4, :] for b in range(4)]

    def pick(i, found):
        at = pl.multiple_of(i * PASS, PASS)
        out = []
        for b in range(4):
            f = found[b]
            for off in range(0, PASS, 128):
                f = jnp.where(own[b] == (at + off).astype(F32), qv[b, :, pl.ds(at + off, 128)], f)
            out.append(f)
        return tuple(out)

    zero = jnp.zeros((4, 128), F32)
    found = lax.fori_loop(0, tail_at // PASS, pick, (zero,) * 4)
    token_q, token_s = [], []
    for b in range(4):
        f = jnp.where(own[b][:, :tail] == float(tail_at), qv[b, :, tail_at : tail_at + tail], 0.0)
        token_q.append(jnp.sum(found[b], axis=1, keepdims=True) + jnp.sum(f, axis=1, keepdims=True))
        kept = k_scr[8 * b : 8 * b + 4, :] + pstat_r[2, 8 * b : 8 * b + 4, :]
        token_s.append(jnp.sum(kept, axis=1, keepdims=True))
    e3s[0] = pack(token_s)
    e3s[1] = pack(token_q)
    e3 = exchange(e3s, e3r, e3_sem)
    for c in e3:
        c.start()

    def await_z(k, _):
        z_copy(k).wait_send()
        pltpu.make_async_remote_copy(
            src_ref=zsend.at[k], dst_ref=s_scr.at[:, :, pl.ds(pl.multiple_of((FIRST + (1 - dp) * SHARED + k) * TILE, TILE), TILE)],
            send_sem=zs_sem.at[k], recv_sem=zr_sem.at[k], device_id=partner, device_id_type=MESH,
        ).wait_recv()
        return None

    lax.fori_loop(0, SHARED, await_z, None)
    for c in e1:
        c.wait()
    lses = [e1s[...]] + [e1r[d] for d in range(3)]
    top = jnp.maximum(jnp.maximum(lses[0], lses[1]), jnp.maximum(lses[2], lses[3]))
    sums = jnp.exp(lses[0] - top) + jnp.exp(lses[1] - top) + jnp.exp(lses[2] - top) + jnp.exp(lses[3] - top)
    lse = top + jnp.log(sums)
    lse_ref[...] = lse
    row_l = [jnp.broadcast_to(unpack(lse[0:4, :], b), (4, 128)) for b in range(4)]

    def excess(b, at, size):
        e = jnp.maximum(jnp.exp(s_scr[b, :, pl.ds(at, size)] - row_l[b][:, :size]) - qv[b, :, pl.ds(at, size)], 0.0)
        ex_ref[b, :, pl.ds(at, size)] = e
        return e

    def last_pass(i, sums):
        at = pl.multiple_of(i * PASS, PASS)
        out = []
        for b in range(4):
            acc = sums[b]
            for off in range(0, PASS, 128):
                acc = acc + excess(b, at + off, 128)
            out.append(acc)
        return tuple(out)

    sums = lax.fori_loop(0, tail_at // PASS, last_pass, (zero,) * 4)
    rows = []
    for b in range(4):
        e = excess(b, tail_at, tail)
        rows.append(jnp.sum(sums[b], axis=1, keepdims=True) + jnp.sum(e, axis=1, keepdims=True))
    e2s[...] = pack(rows)
    e2 = exchange(e2s, e2r, e2_sem)
    for c in e2:
        c.start()

    for c in e3:
        c.wait()
    at_token = (e3s[...] + e3r[0]) + (e3r[1] + e3r[2])
    acc_ref[...] = jnp.minimum(jnp.exp(at_token[0] - lse[0:4, :]) / at_token[1], 1.0)

    for c in e2:
        c.wait()
    norm_ref[...] = (e2s[...] + e2r[0]) + (e2r[1] + e2r[2])


def finish_kernel(
    ex_ref, norm_ref, acc_ref, lse_ref, acc_out, norm_out, res_out, bonus_out, acc_v, norm_v, bonus_v, stage, sem, r_sem
):
    n_ids = ex_ref.shape[2]
    lane = lax.broadcasted_iota(jnp.int32, (4, 128), 1)
    norm = norm_ref[...]
    writes = []
    for b in range(4):
        total = jnp.sum(jnp.where(lane == 32 * b, norm, 0.0), axis=1, keepdims=True)
        scale = jnp.broadcast_to(1.0 / jnp.broadcast_to(total, (4, 128)), (4, 128))

        for at in range(0, n_ids, 128):
            size = min(128, n_ids - at)
            stage[b, :, at : at + size] = ex_ref[b, :, at : at + size] * scale[:, :size]
        writes.append(pltpu.make_async_copy(stage.at[b], res_out.at[b], r_sem.at[b]))
        writes[-1].start()

    sub = lax.broadcasted_iota(jnp.int32, (4, 128), 0)
    for src, dst, out, k in ((acc_ref[...], acc_v, acc_out, 0), (norm, norm_v, norm_out, 1)):
        row = jnp.sum(jnp.where(lane % 32 == sub, src, 0.0), axis=0, keepdims=True)
        for b in range(4):
            dst[b : b + 1, :] = (row if b == 0 else pltpu.roll(row, 128 - 32 * b, 1))[:, 0:4]
        writes.append(pltpu.make_async_copy(dst, out, sem.at[k]))
        writes[-1].start()
    row = lse_ref[4:5, :]
    lane = lane[0:1, :]
    packed = row
    for b in range(1, 4):
        packed = jnp.where(lane == b, pltpu.roll(row, 128 - 31 * b, 1), packed)
    bonus_v[...] = packed[:, 0:4]
    writes.append(pltpu.make_async_copy(bonus_v, bonus_out, sem.at[2]))
    writes[-1].start()
    for c in writes:
        c.wait()


def solution(mesh):
    def local_step(hidden, norm_gain, w_head, draft_probs, draft_tokens, temperature):
        n_ids = w_head.shape[1]
        width = w_head.shape[0]
        pad_ids = -(-n_ids // 128) * 128
        tail = n_ids % TILE
        vmem, smem, hbm = pltpu.VMEM, pltpu.SMEM, pltpu.HBM
        dma = pltpu.SemaphoreType.DMA
        ex, norm, acc, lse = pl.pallas_call(
            verify_kernel,
            out_shape=[vmem((4, 4, n_ids), F32), vmem((4, 128), F32), vmem((4, 128), F32), vmem((8, 128), F32)],
            in_specs=[pl.BlockSpec(memory_space=s) for s in (hbm,) * 6],
            out_specs=[pl.BlockSpec(memory_space=vmem)] * 4,
            scratch_shapes=[
                vmem((5, 4, width), jnp.bfloat16),
                vmem((1, width), F32),
                smem((4,), F32),
                smem((4, 4), jnp.int32),
                vmem((SLOTS, TILE, width), jnp.bfloat16),
                vmem((tail, width), jnp.bfloat16),
                vmem((4, 4, n_ids), F32),
                vmem((4, 4, pad_ids), F32),
                vmem((5, 4, width), F32),
                vmem((5, 4, width), F32),
                vmem((32, width), F32),
                vmem((64, width), jnp.bfloat16),
                vmem((5, 4, 128), F32),
                vmem((5, 4, 128), F32),
                vmem((64, 128), F32),
                vmem((64, 128), F32),
                vmem((64, 128), F32),
                vmem((64, 128), F32),
                vmem((64, 128), F32),
                vmem((SHARED, 4, 4, TILE), F32),
                vmem((3, 32, 128), F32),
                vmem((3, 32, 128), F32),
                vmem((8, 128), F32),
                vmem((3, 8, 128), F32),
                vmem((4, 128), F32),
                vmem((3, 4, 128), F32),
                vmem((2, 4, 128), F32),
                vmem((3, 2, 4, 128), F32),
                dma((4,)), dma((SLOTS, 2)), dma, dma, dma((2,)), dma((2,)), dma((SHARED,)), dma((SHARED,)), dma((2,)),
                dma((2, 3)), dma((2, 3)), dma((2, 3)),
            ],
            compiler_params=pltpu.CompilerParams(collective_id=0, has_side_effects=True),
            name="verify",
        )(
            hidden.transpose(1, 0, 2), norm_gain.reshape(1, width), temperature, draft_tokens,
            w_head.T, draft_probs,
        )
        acc, norm, residual, bonus = pl.pallas_call(
            finish_kernel,
            out_shape=[
                jax.ShapeDtypeStruct((4, 4), F32),
                jax.ShapeDtypeStruct((4, 4), F32),
                jax.ShapeDtypeStruct((4, 4, n_ids), F32),
                jax.ShapeDtypeStruct((1, 4), F32),
            ],
            in_specs=[pl.BlockSpec(memory_space=vmem)] * 4,
            out_specs=[pl.BlockSpec(memory_space=hbm)] * 4,
            scratch_shapes=[
                vmem((4, 4), F32), vmem((4, 4), F32), vmem((1, 4), F32), vmem((4, 4, n_ids), F32), dma((3,)), dma((4,)),
            ],
            compiler_params=pltpu.CompilerParams(vmem_limit_bytes=16 * 1024 * 1024),
            name="finish",
        )(ex, norm, acc, lse)
        return acc, norm, residual, bonus.reshape(4)

    return jax.shard_map(
        local_step,
        mesh=mesh,
        in_specs=(P("dp", None, None), P(), P(None, "tp"), P("dp", None, "tp"), P("dp", None), P("dp")),
        out_specs=(P("dp", None), P("dp", None), P("dp", None, "tp"), P("dp")),
        check_vma=False,
    )
```

```python
import jax
import jax.numpy as jnp
from jax import lax
from jax.experimental import pallas as pl
from jax.experimental.pallas import tpu as pltpu
from jax.sharding import PartitionSpec as P

MESH = pl.DeviceIdType.MESH
F32 = jnp.float32
LOWEST = float(jnp.finfo(jnp.float32).min)

TILE = 1024
SUB = 256
DEPTH = 256
SLOTS = 4
SHARED = 14
FIRST = 5
PASS = 1024


def verify_kernel(
    h_hbm, g_hbm, t_hbm, dt_hbm, w_ref, q_ref,
    ex_ref, norm_ref, acc_ref, lse_ref,
    h_ref, g_ref, t_ref, dt_ref, wbuf, wtail, qv, s_scr, xf, xp, xrows, xb, xt, tv, tp_recv, ct, dl, m_scr, l_scr, k_scr,
    zsend, pstat_s, pstat_r, e1s, e1r, e2s, e2r, e3s, e3r,
    in_sem, w_sem, wt_sem, q_sem, x_sem, t_sem, zs_sem, zr_sem, ps_sem, e1_sem, e2_sem, e3_sem,
):
    dp, tp = lax.axis_index("dp"), lax.axis_index("tp")
    partner = (1 - dp, tp)
    peers = [(dp, lax.rem(tp + d, 4)) for d in (1, 2, 3)]
    n_ids, width = w_ref.shape
    n_full = n_ids // TILE
    tail = n_ids - n_full * TILE
    tail_at = n_full * TILE
    last = n_full - 2 * SHARED - FIRST
    steps = FIRST + SHARED + last

    def column(i):
        in_shared = (i + steps - FIRST) // steps
        past_shared = (i + steps - FIRST - SHARED) // steps
        return pl.multiple_of((i + in_shared * dp * SHARED + past_shared * (SHARED - dp * SHARED)) * TILE, TILE)

    half = TILE // 2

    def tile_copies(i, slot):
        at = column(i)
        return [
            pltpu.make_async_copy(
                w_ref.at[pl.ds(at + k * half, half), :], wbuf.at[slot, pl.ds(k * half, half), :], w_sem.at[slot, k]
            )
            for k in (0, 1)
        ]

    tail_copy = pltpu.make_async_copy(w_ref.at[pl.ds(tail_at, tail), :], wtail, wt_sem)
    q_copy = pltpu.make_async_copy(q_ref, qv, q_sem)
    small = [
        pltpu.make_async_copy(src, dst, in_sem.at[k])
        for k, (src, dst) in enumerate(((h_hbm, h_ref), (g_hbm, g_ref), (t_hbm, t_ref), (dt_hbm, dt_ref)))
    ]
    for c in small:
        c.start()
    tail_copy.start()
    for i in range(SLOTS):
        for c in tile_copies(i, i):
            c.start()
    q_copy.start()

    barrier = pltpu.get_barrier_semaphore()
    for other in [partner] + peers:
        pl.semaphore_signal(barrier, inc=1, device_id=other, device_id_type=MESH)

    for c in small:
        c.wait()
    h = h_ref[...].astype(F32)
    inv_rms = lax.rsqrt(jnp.mean(h * h, axis=-1, keepdims=True) + 1e-5)
    xf[...] = h * inv_rms * g_ref[...][None]
    for b in range(4):
        tv[0, b : b + 1, :] = jnp.full((1, 128), 1.0, F32) / jnp.full((1, 128), t_ref[b], F32)
        for j in range(4):
            tv[1 + j, b : b + 1, :] = jnp.full((1, 128), dt_ref[b, j].astype(F32), F32)

    def lay_rows(src, t_src, at):
        xrows[...] = jnp.zeros_like(xrows)
        lane = lax.broadcasted_iota(jnp.int32, (1, 128), 1) + tp * n_ids
        for b in range(4):
            for j in range(5):
                xrows[8 * b + j : 8 * b + j + 1, :] = src[j, b : b + 1, :]
            ct[at + 8 * b : at + 8 * b + 8, :] = jnp.broadcast_to(t_src[0, b : b + 1, :], (8, 128))
            dl[at + 8 * b : at + 8 * b + 8, :] = jnp.full((8, 128), -1.0, F32)
            for j in range(4):
                dl[at + 8 * b + j : at + 8 * b + j + 1, :] = t_src[1 + j, b : b + 1, :] - lane.astype(F32)
        rows = xrows[...].astype(jnp.bfloat16)
        xb[at : at + 32, :] = rows
        for k in range(0, width, 128):
            block = jnp.concatenate([xrows[:, k : k + 128], jnp.zeros((96, 128), F32)], axis=0).T
            both = block if at == 0 else xt[k : k + 128, :].astype(F32) + pltpu.roll(block, at, 1)
            xt[k : k + 128, :] = both.astype(jnp.bfloat16)

    xb[32:64, :] = jnp.zeros((32, width), jnp.bfloat16)
    lay_rows(xf, tv, 0)
    m_scr[...] = jnp.full(m_scr.shape, LOWEST, F32)
    l_scr[...] = jnp.zeros_like(l_scr)
    k_scr[...] = jnp.zeros_like(k_scr)

    pl.semaphore_wait(barrier, 4)
    x_copy = pltpu.make_async_remote_copy(
        src_ref=xf, dst_ref=xp, send_sem=x_sem.at[0], recv_sem=x_sem.at[1], device_id=partner, device_id_type=MESH
    )
    t_copy = pltpu.make_async_remote_copy(
        src_ref=tv, dst_ref=tp_recv, send_sem=t_sem.at[0], recv_sem=t_sem.at[1], device_id=partner, device_id_type=MESH
    )
    x_copy.start()
    t_copy.start()

    def by_rows(w, depth):
        return lax.dot_general(xb[:, depth], w, (((1,), (1,)), ((), ())), preferred_element_type=F32)

    def by_ids(w, depth):
        return lax.dot_general(w, xt[depth, :], (((1,), (0,)), ((), ())), preferred_element_type=F32)

    def tile_products(slot):
        sums = [None] * 4
        for k in range(0, width, DEPTH):
            depth = slice(k, k + DEPTH)
            for q in range(4):
                w = wbuf[slot, q * SUB : (q + 1) * SUB, depth]
                z = by_rows(w, depth) if q < 2 else by_ids(w, depth)
                sums[q] = z if k == 0 else sums[q] + z
        pieces = []
        for z in sums[:2]:
            pieces += [z[:, 0:128], z[:, 128:256]]
        for z in sums[2:]:
            pieces += [z[at : at + 128, :].T[0:64] for at in (0, 128)]
        return pieces

    def fold(rows, parts):
        m_old = m_scr[0:rows, :]
        m_new = m_old
        for p in parts:
            m_new = jnp.maximum(m_new, p)
        total = l_scr[0:rows, :] * jnp.exp(m_old - m_new)
        for p in parts:
            total = total + jnp.exp(p - m_new)
        m_scr[0:rows, :] = m_new
        l_scr[0:rows, :] = total

    tail_copy.wait()
    s = by_rows(wtail[...], slice(0, width))[0:32] * ct[0:32, 0:tail]
    for b in range(4):
        s_scr[b, :, tail_at : tail_at + tail] = s[8 * b : 8 * b + 4, :]
    k_scr[0:32, 0:tail] = jnp.where(dl[0:32, 0:tail] == float(tail_at), s, 0.0)
    m_tail = jnp.max(s, axis=1, keepdims=True)
    l_tail = jnp.sum(jnp.exp(s - m_tail), axis=1, keepdims=True)
    lane0 = lax.broadcasted_iota(jnp.int32, (32, 128), 1) == 0
    m_scr[0:32, :] = jnp.where(lane0, m_tail, LOWEST)
    l_scr[0:32, :] = jnp.where(lane0, l_tail, 0.0)

    def z_copy(k):
        at = column(FIRST + k)
        return pltpu.make_async_remote_copy(
            src_ref=zsend.at[k], dst_ref=s_scr.at[:, :, pl.ds(at, TILE)], send_sem=zs_sem.at[k], recv_sem=zr_sem.at[k],
            device_id=partner, device_id_type=MESH,
        )

    def step(i, rows):
        slot = i % SLOTS
        for c in tile_copies(i, slot):
            c.wait()
        if rows == 64:
            k = i - FIRST

            @pl.when(k > 0)
            def _():
                z_copy(k - 1).start()

        at = column(i)
        kept = k_scr[0:rows, :]
        parts = []
        for n, z in enumerate(tile_products(slot)):
            s = z[0:rows] * ct[0:rows, :]
            parts.append(s)
            off = n * 128
            kept = jnp.where(dl[0:rows, :] == (at + off).astype(F32), s, kept)
            for b in range(4):
                s_scr[b, :, pl.ds(at + off, 128)] = s[8 * b : 8 * b + 4, :]
                if rows == 64:
                    zsend[k, b, :, off : off + 128] = s[32 + 8 * b : 32 + 8 * b + 4, :]
            if n % 2:
                fold(rows, parts)
                parts = []
        k_scr[0:rows, :] = kept

        @pl.when(i + SLOTS < steps)
        def _():
            for c in tile_copies(i + SLOTS, slot):
                c.start()

    lax.fori_loop(0, FIRST, lambda i, _: step(i, 32), None)
    x_copy.wait()
    t_copy.wait()
    lay_rows(xp, tp_recv, 32)
    lax.fori_loop(FIRST, FIRST + SHARED, lambda i, _: step(i, 64), None)
    pstat_s[0] = m_scr[32:64, :]
    pstat_s[1] = l_scr[32:64, :]
    pstat_s[2] = k_scr[32:64, :]
    z_copy(SHARED - 1).start()
    stat_copy = pltpu.make_async_remote_copy(
        src_ref=pstat_s, dst_ref=pstat_r, send_sem=ps_sem.at[0], recv_sem=ps_sem.at[1],
        device_id=partner, device_id_type=MESH,
    )
    stat_copy.start()
    lax.fori_loop(FIRST + SHARED, steps, lambda i, _: step(i, 32), None)

    group = lax.broadcasted_iota(jnp.int32, (8, 128), 1) // 32

    def pack(cols):
        size = cols[0].shape[0]
        packed = jnp.broadcast_to(cols[0], (size, 128))
        for b in range(1, 4):
            packed = jnp.where(group[:size] == b, cols[b], packed)
        return packed

    def unpack(packed, b):
        size = packed.shape[0]
        lane = lax.broadcasted_iota(jnp.int32, (size, 128), 1)
        return jnp.sum(jnp.where(lane == 32 * b, packed, 0.0), axis=1, keepdims=True)

    def exchange(src, dst, sem):
        return [
            pltpu.make_async_remote_copy(
                src_ref=src, dst_ref=dst.at[d], send_sem=sem.at[0, d], recv_sem=sem.at[1, d],
                device_id=peers[d], device_id_type=MESH,
            )
            for d in range(3)
        ]

    stat_copy.wait()
    m = jnp.maximum(m_scr[0:32, :], pstat_r[0])
    total = l_scr[0:32, :] * jnp.exp(m_scr[0:32, :] - m) + pstat_r[1] * jnp.exp(pstat_r[0] - m)
    row_max = jnp.max(m, axis=1, keepdims=True)
    row_lse = row_max + jnp.log(jnp.sum(total * jnp.exp(m - row_max), axis=1, keepdims=True))
    e1s[...] = pack([row_lse[8 * b : 8 * b + 8, :] for b in range(4)])
    e1 = exchange(e1s, e1r, e1_sem)
    for c in e1:
        c.start()

    q_copy.wait()
    own = [dl[8 * b : 8 * b + 4, :] for b in range(4)]

    def pick(i, found):
        at = pl.multiple_of(i * PASS, PASS)
        out = []
        for b in range(4):
            f = found[b]
            for off in range(0, PASS, 128):
                f = jnp.where(own[b] == (at + off).astype(F32), qv[b, :, pl.ds(at + off, 128)], f)
            out.append(f)
        return tuple(out)

    zero = jnp.zeros((4, 128), F32)
    found = lax.fori_loop(0, tail_at // PASS, pick, (zero,) * 4)
    token_q, token_s = [], []
    for b in range(4):
        f = jnp.where(own[b][:, :tail] == float(tail_at), qv[b, :, tail_at : tail_at + tail], 0.0)
        token_q.append(jnp.sum(found[b], axis=1, keepdims=True) + jnp.sum(f, axis=1, keepdims=True))
        kept = k_scr[8 * b : 8 * b + 4, :] + pstat_r[2, 8 * b : 8 * b + 4, :]
        token_s.append(jnp.sum(kept, axis=1, keepdims=True))
    e3s[0] = pack(token_s)
    e3s[1] = pack(token_q)
    e3 = exchange(e3s, e3r, e3_sem)
    for c in e3:
        c.start()

    def await_z(k, _):
        z_copy(k).wait_send()
        pltpu.make_async_remote_copy(
            src_ref=zsend.at[k], dst_ref=s_scr.at[:, :, pl.ds(pl.multiple_of((FIRST + (1 - dp) * SHARED + k) * TILE, TILE), TILE)],
            send_sem=zs_sem.at[k], recv_sem=zr_sem.at[k], device_id=partner, device_id_type=MESH,
        ).wait_recv()
        return None

    lax.fori_loop(0, SHARED, await_z, None)
    for c in e1:
        c.wait()
    lses = [e1s[...]] + [e1r[d] for d in range(3)]
    top = jnp.maximum(jnp.maximum(lses[0], lses[1]), jnp.maximum(lses[2], lses[3]))
    sums = jnp.exp(lses[0] - top) + jnp.exp(lses[1] - top) + jnp.exp(lses[2] - top) + jnp.exp(lses[3] - top)
    lse = top + jnp.log(sums)
    lse_ref[...] = lse
    row_l = [jnp.broadcast_to(unpack(lse[0:4, :], b), (4, 128)) for b in range(4)]

    def excess(b, at, size):
        e = jnp.maximum(jnp.exp(s_scr[b, :, pl.ds(at, size)] - row_l[b][:, :size]) - qv[b, :, pl.ds(at, size)], 0.0)
        ex_ref[b, :, pl.ds(at, size)] = e
        return e

    def last_pass(i, sums):
        at = pl.multiple_of(i * PASS, PASS)
        out = []
        for b in range(4):
            acc = sums[b]
            for off in range(0, PASS, 128):
                acc = acc + excess(b, at + off, 128)
            out.append(acc)
        return tuple(out)

    sums = lax.fori_loop(0, tail_at // PASS, last_pass, (zero,) * 4)
    rows = []
    for b in range(4):
        e = excess(b, tail_at, tail)
        rows.append(jnp.sum(sums[b], axis=1, keepdims=True) + jnp.sum(e, axis=1, keepdims=True))
    e2s[...] = pack(rows)
    e2 = exchange(e2s, e2r, e2_sem)
    for c in e2:
        c.start()

    for c in e3:
        c.wait()
    at_token = (e3s[...] + e3r[0]) + (e3r[1] + e3r[2])
    acc_ref[...] = jnp.minimum(jnp.exp(at_token[0] - lse[0:4, :]) / at_token[1], 1.0)

    for c in e2:
        c.wait()
    norm_ref[...] = (e2s[...] + e2r[0]) + (e2r[1] + e2r[2])


def finish_kernel(
    ex_ref, norm_ref, acc_ref, lse_ref, acc_out, norm_out, res_out, bonus_out, acc_v, norm_v, bonus_v, stage, sem, r_sem
):
    n_ids = ex_ref.shape[2]
    lane = lax.broadcasted_iota(jnp.int32, (4, 128), 1)
    norm = norm_ref[...]
    writes = []
    for b in range(4):
        total = jnp.sum(jnp.where(lane == 32 * b, norm, 0.0), axis=1, keepdims=True)
        scale = jnp.broadcast_to(1.0 / jnp.broadcast_to(total, (4, 128)), (4, 128))

        for at in range(0, n_ids, 128):
            size = min(128, n_ids - at)
            stage[b, :, at : at + size] = ex_ref[b, :, at : at + size] * scale[:, :size]
        writes.append(pltpu.make_async_copy(stage.at[b], res_out.at[b], r_sem.at[b]))
        writes[-1].start()

    sub = lax.broadcasted_iota(jnp.int32, (4, 128), 0)
    for src, dst, out, k in ((acc_ref[...], acc_v, acc_out, 0), (norm, norm_v, norm_out, 1)):
        row = jnp.sum(jnp.where(lane % 32 == sub, src, 0.0), axis=0, keepdims=True)
        for b in range(4):
            dst[b : b + 1, :] = (row if b == 0 else pltpu.roll(row, 128 - 32 * b, 1))[:, 0:4]
        writes.append(pltpu.make_async_copy(dst, out, sem.at[k]))
        writes[-1].start()
    row = lse_ref[4:5, :]
    lane = lane[0:1, :]
    packed = row
    for b in range(1, 4):
        packed = jnp.where(lane == b, pltpu.roll(row, 128 - 31 * b, 1), packed)
    bonus_v[...] = packed[:, 0:4]
    writes.append(pltpu.make_async_copy(bonus_v, bonus_out, sem.at[2]))
    writes[-1].start()
    for c in writes:
        c.wait()


def solution(mesh):
    def local_step(hidden, norm_gain, w_head, draft_probs, draft_tokens, temperature):
        n_ids = w_head.shape[1]
        width = w_head.shape[0]
        pad_ids = -(-n_ids // 128) * 128
        tail = n_ids % TILE
        vmem, smem, hbm = pltpu.VMEM, pltpu.SMEM, pltpu.HBM
        dma = pltpu.SemaphoreType.DMA
        ex, norm, acc, lse = pl.pallas_call(
            verify_kernel,
            out_shape=[vmem((4, 4, n_ids), F32), vmem((4, 128), F32), vmem((4, 128), F32), vmem((8, 128), F32)],
            in_specs=[pl.BlockSpec(memory_space=s) for s in (hbm,) * 6],
            out_specs=[pl.BlockSpec(memory_space=vmem)] * 4,
            scratch_shapes=[
                vmem((5, 4, width), jnp.bfloat16),
                vmem((1, width), F32),
                smem((4,), F32),
                smem((4, 4), jnp.int32),
                vmem((SLOTS, TILE, width), jnp.bfloat16),
                vmem((tail, width), jnp.bfloat16),
                vmem((4, 4, n_ids), F32),
                vmem((4, 4, pad_ids), F32),
                vmem((5, 4, width), F32),
                vmem((5, 4, width), F32),
                vmem((32, width), F32),
                vmem((64, width), jnp.bfloat16),
                vmem((width, 128), jnp.bfloat16),
                vmem((5, 4, 128), F32),
                vmem((5, 4, 128), F32),
                vmem((64, 128), F32),
                vmem((64, 128), F32),
                vmem((64, 128), F32),
                vmem((64, 128), F32),
                vmem((64, 128), F32),
                vmem((SHARED, 4, 4, TILE), F32),
                vmem((3, 32, 128), F32),
                vmem((3, 32, 128), F32),
                vmem((8, 128), F32),
                vmem((3, 8, 128), F32),
                vmem((4, 128), F32),
                vmem((3, 4, 128), F32),
                vmem((2, 4, 128), F32),
                vmem((3, 2, 4, 128), F32),
                dma((4,)), dma((SLOTS, 2)), dma, dma, dma((2,)), dma((2,)), dma((SHARED,)), dma((SHARED,)), dma((2,)),
                dma((2, 3)), dma((2, 3)), dma((2, 3)),
            ],
            compiler_params=pltpu.CompilerParams(collective_id=0, has_side_effects=True),
            name="verify",
        )(
            hidden.transpose(1, 0, 2), norm_gain.reshape(1, width), temperature, draft_tokens,
            w_head.T, draft_probs,
        )
        acc, norm, residual, bonus = pl.pallas_call(
            finish_kernel,
            out_shape=[
                jax.ShapeDtypeStruct((4, 4), F32),
                jax.ShapeDtypeStruct((4, 4), F32),
                jax.ShapeDtypeStruct((4, 4, n_ids), F32),
                jax.ShapeDtypeStruct((1, 4), F32),
            ],
            in_specs=[pl.BlockSpec(memory_space=vmem)] * 4,
            out_specs=[pl.BlockSpec(memory_space=hbm)] * 4,
            scratch_shapes=[
                vmem((4, 4), F32), vmem((4, 4), F32), vmem((1, 4), F32), vmem((4, 4, n_ids), F32), dma((3,)), dma((4,)),
            ],
            compiler_params=pltpu.CompilerParams(vmem_limit_bytes=16 * 1024 * 1024),
            name="finish",
        )(ex, norm, acc, lse)
        return acc, norm, residual, bonus.reshape(4)

    return jax.shard_map(
        local_step,
        mesh=mesh,
        in_specs=(P("dp", None, None), P(), P(None, "tp"), P("dp", None, "tp"), P("dp", None), P("dp")),
        out_specs=(P("dp", None), P("dp", None), P("dp", None, "tp"), P("dp")),
        check_vma=False,
    )
```

```python
import jax
import jax.numpy as jnp
from jax import lax
from jax.experimental import pallas as pl
from jax.experimental.pallas import tpu as pltpu
from jax.sharding import PartitionSpec as P

MESH = pl.DeviceIdType.MESH
F32 = jnp.float32
LOWEST = float(jnp.finfo(jnp.float32).min)

TILE = 1024
SUB = 256
DEPTH = 256
SLOTS = 4
SHARED = 12
FIRST = 5
PASS = 1024


def verify_kernel(
    h_hbm, g_hbm, t_hbm, dt_hbm, w_ref, q_ref,
    ex_ref, norm_ref, acc_ref, lse_ref,
    h_ref, g_ref, t_ref, dt_ref, wbuf, wtail, qv, s_scr, xf, xp, xrows, xb, xt, tv, tp_recv, ct, dl, m_scr, l_scr, k_scr,
    zsend, pstat_s, pstat_r, e1s, e1r, e2s, e2r, e3s, e3r,
    in_sem, w_sem, wt_sem, q_sem, x_sem, t_sem, zs_sem, zr_sem, ps_sem, e1_sem, e2_sem, e3_sem,
):
    dp, tp = lax.axis_index("dp"), lax.axis_index("tp")
    partner = (1 - dp, tp)
    peers = [(dp, lax.rem(tp + d, 4)) for d in (1, 2, 3)]
    n_ids, width = w_ref.shape
    n_full = n_ids // TILE
    tail = n_ids - n_full * TILE
    tail_at = n_full * TILE
    last = n_full - 2 * SHARED - FIRST
    steps = FIRST + SHARED + last

    def column(i):
        in_shared = (i + steps - FIRST) // steps
        past_shared = (i + steps - FIRST - SHARED) // steps
        return pl.multiple_of((i + in_shared * dp * SHARED + past_shared * (SHARED - dp * SHARED)) * TILE, TILE)

    half = TILE // 2

    def tile_copies(i, slot):
        at = column(i)
        return [
            pltpu.make_async_copy(
                w_ref.at[pl.ds(at + k * half, half), :], wbuf.at[slot, pl.ds(k * half, half), :], w_sem.at[slot, k]
            )
            for k in (0, 1)
        ]

    tail_copy = pltpu.make_async_copy(w_ref.at[pl.ds(tail_at, tail), :], wtail, wt_sem)
    q_copy = pltpu.make_async_copy(q_ref, qv, q_sem)
    small = [
        pltpu.make_async_copy(src, dst, in_sem.at[k])
        for k, (src, dst) in enumerate(((h_hbm, h_ref), (g_hbm, g_ref), (t_hbm, t_ref), (dt_hbm, dt_ref)))
    ]
    for c in small:
        c.start()
    tail_copy.start()
    for i in range(SLOTS):
        for c in tile_copies(i, i):
            c.start()
    q_copy.start()

    barrier = pltpu.get_barrier_semaphore()
    for other in [partner] + peers:
        pl.semaphore_signal(barrier, inc=1, device_id=other, device_id_type=MESH)

    for c in small:
        c.wait()
    h = h_ref[...].astype(F32)
    inv_rms = lax.rsqrt(jnp.mean(h * h, axis=-1, keepdims=True) + 1e-5)
    xf[...] = h * inv_rms * g_ref[...][None]
    for b in range(4):
        tv[0, b : b + 1, :] = jnp.full((1, 128), 1.0, F32) / jnp.full((1, 128), t_ref[b], F32)
        for j in range(4):
            tv[1 + j, b : b + 1, :] = jnp.full((1, 128), dt_ref[b, j].astype(F32), F32)

    def lay_rows(src, t_src, at):
        xrows[...] = jnp.zeros_like(xrows)
        lane = lax.broadcasted_iota(jnp.int32, (1, 128), 1) + tp * n_ids
        for b in range(4):
            for j in range(5):
                xrows[8 * b + j : 8 * b + j + 1, :] = src[j, b : b + 1, :]
            ct[at + 8 * b : at + 8 * b + 8, :] = jnp.broadcast_to(t_src[0, b : b + 1, :], (8, 128))
            dl[at + 8 * b : at + 8 * b + 8, :] = jnp.full((8, 128), -1.0, F32)
            for j in range(4):
                dl[at + 8 * b + j : at + 8 * b + j + 1, :] = t_src[1 + j, b : b + 1, :] - lane.astype(F32)
        rows = xrows[...].astype(jnp.bfloat16)
        xb[at : at + 32, :] = rows
        for k in range(0, width, 128):
            block = jnp.concatenate([xrows[:, k : k + 128], jnp.zeros((96, 128), F32)], axis=0).T
            both = block if at == 0 else xt[k : k + 128, :].astype(F32) + pltpu.roll(block, at, 1)
            xt[k : k + 128, :] = both.astype(jnp.bfloat16)

    xb[32:64, :] = jnp.zeros((32, width), jnp.bfloat16)
    lay_rows(xf, tv, 0)
    m_scr[...] = jnp.full(m_scr.shape, LOWEST, F32)
    l_scr[...] = jnp.zeros_like(l_scr)
    k_scr[...] = jnp.zeros_like(k_scr)

    pl.semaphore_wait(barrier, 4)
    x_copy = pltpu.make_async_remote_copy(
        src_ref=xf, dst_ref=xp, send_sem=x_sem.at[0], recv_sem=x_sem.at[1], device_id=partner, device_id_type=MESH
    )
    t_copy = pltpu.make_async_remote_copy(
        src_ref=tv, dst_ref=tp_recv, send_sem=t_sem.at[0], recv_sem=t_sem.at[1], device_id=partner, device_id_type=MESH
    )
    x_copy.start()
    t_copy.start()

    def by_rows(w, depth):
        return lax.dot_general(xb[:, depth], w, (((1,), (1,)), ((), ())), preferred_element_type=F32)

    def by_ids(w, depth):
        return lax.dot_general(w, xt[depth, :], (((1,), (0,)), ((), ())), preferred_element_type=F32)

    def tile_products(slot):
        sums = [None] * 4
        for k in range(0, width, DEPTH):
            depth = slice(k, k + DEPTH)
            for q in range(4):
                w = wbuf[slot, q * SUB : (q + 1) * SUB, depth]
                z = by_rows(w, depth) if q < 2 else by_ids(w, depth)
                sums[q] = z if k == 0 else sums[q] + z
        pieces = []
        for z in sums[:2]:
            pieces += [z[:, 0:128], z[:, 128:256]]
        for z in sums[2:]:
            pieces += [z[at : at + 128, :].T[0:64] for at in (0, 128)]
        return pieces

    def fold(rows, parts):
        m_old = m_scr[0:rows, :]
        m_new = m_old
        for p in parts:
            m_new = jnp.maximum(m_new, p)
        total = l_scr[0:rows, :] * jnp.exp(m_old - m_new)
        for p in parts:
            total = total + jnp.exp(p - m_new)
        m_scr[0:rows, :] = m_new
        l_scr[0:rows, :] = total

    tail_copy.wait()
    s = by_rows(wtail[...], slice(0, width))[0:32] * ct[0:32, 0:tail]
    for b in range(4):
        s_scr[b, :, tail_at : tail_at + tail] = s[8 * b : 8 * b + 4, :]
    k_scr[0:32, 0:tail] = jnp.where(dl[0:32, 0:tail] == float(tail_at), s, 0.0)
    m_tail = jnp.max(s, axis=1, keepdims=True)
    l_tail = jnp.sum(jnp.exp(s - m_tail), axis=1, keepdims=True)
    lane0 = lax.broadcasted_iota(jnp.int32, (32, 128), 1) == 0
    m_scr[0:32, :] = jnp.where(lane0, m_tail, LOWEST)
    l_scr[0:32, :] = jnp.where(lane0, l_tail, 0.0)

    def z_copy(k):
        at = column(FIRST + k)
        return pltpu.make_async_remote_copy(
            src_ref=zsend.at[k], dst_ref=s_scr.at[:, :, pl.ds(at, TILE)], send_sem=zs_sem.at[k], recv_sem=zr_sem.at[k],
            device_id=partner, device_id_type=MESH,
        )

    def step(i, rows):
        slot = i % SLOTS
        for c in tile_copies(i, slot):
            c.wait()
        if rows == 64:
            k = i - FIRST

            @pl.when(k > 0)
            def _():
                z_copy(k - 1).start()

        at = column(i)
        kept = k_scr[0:rows, :]
        parts = []
        for n, z in enumerate(tile_products(slot)):
            s = z[0:rows] * ct[0:rows, :]
            parts.append(s)
            off = n * 128
            kept = jnp.where(dl[0:rows, :] == (at + off).astype(F32), s, kept)
            for b in range(4):
                s_scr[b, :, pl.ds(at + off, 128)] = s[8 * b : 8 * b + 4, :]
                if rows == 64:
                    zsend[k, b, :, off : off + 128] = s[32 + 8 * b : 32 + 8 * b + 4, :]
            if n % 2:
                fold(rows, parts)
                parts = []
        k_scr[0:rows, :] = kept

        @pl.when(i + SLOTS < steps)
        def _():
            for c in tile_copies(i + SLOTS, slot):
                c.start()

    lax.fori_loop(0, FIRST, lambda i, _: step(i, 32), None)
    x_copy.wait()
    t_copy.wait()
    lay_rows(xp, tp_recv, 32)
    lax.fori_loop(FIRST, FIRST + SHARED, lambda i, _: step(i, 64), None)
    pstat_s[0] = m_scr[32:64, :]
    pstat_s[1] = l_scr[32:64, :]
    pstat_s[2] = k_scr[32:64, :]
    z_copy(SHARED - 1).start()
    stat_copy = pltpu.make_async_remote_copy(
        src_ref=pstat_s, dst_ref=pstat_r, send_sem=ps_sem.at[0], recv_sem=ps_sem.at[1],
        device_id=partner, device_id_type=MESH,
    )
    stat_copy.start()
    lax.fori_loop(FIRST + SHARED, steps, lambda i, _: step(i, 32), None)

    group = lax.broadcasted_iota(jnp.int32, (8, 128), 1) // 32

    def pack(cols):
        size = cols[0].shape[0]
        packed = jnp.broadcast_to(cols[0], (size, 128))
        for b in range(1, 4):
            packed = jnp.where(group[:size] == b, cols[b], packed)
        return packed

    def unpack(packed, b):
        size = packed.shape[0]
        lane = lax.broadcasted_iota(jnp.int32, (size, 128), 1)
        return jnp.sum(jnp.where(lane == 32 * b, packed, 0.0), axis=1, keepdims=True)

    def exchange(src, dst, sem):
        return [
            pltpu.make_async_remote_copy(
                src_ref=src, dst_ref=dst.at[d], send_sem=sem.at[0, d], recv_sem=sem.at[1, d],
                device_id=peers[d], device_id_type=MESH,
            )
            for d in range(3)
        ]

    stat_copy.wait()
    m = jnp.maximum(m_scr[0:32, :], pstat_r[0])
    total = l_scr[0:32, :] * jnp.exp(m_scr[0:32, :] - m) + pstat_r[1] * jnp.exp(pstat_r[0] - m)
    row_max = jnp.max(m, axis=1, keepdims=True)
    row_lse = row_max + jnp.log(jnp.sum(total * jnp.exp(m - row_max), axis=1, keepdims=True))
    e1s[...] = pack([row_lse[8 * b : 8 * b + 8, :] for b in range(4)])
    e1 = exchange(e1s, e1r, e1_sem)
    for c in e1:
        c.start()

    q_copy.wait()
    own = [dl[8 * b : 8 * b + 4, :] for b in range(4)]

    def pick(i, found):
        at = pl.multiple_of(i * PASS, PASS)
        out = []
        for b in range(4):
            f = found[b]
            for off in range(0, PASS, 128):
                f = jnp.where(own[b] == (at + off).astype(F32), qv[b, :, pl.ds(at + off, 128)], f)
            out.append(f)
        return tuple(out)

    zero = jnp.zeros((4, 128), F32)
    found = lax.fori_loop(0, tail_at // PASS, pick, (zero,) * 4)
    token_q, token_s = [], []
    for b in range(4):
        f = jnp.where(own[b][:, :tail] == float(tail_at), qv[b, :, tail_at : tail_at + tail], 0.0)
        token_q.append(jnp.sum(found[b], axis=1, keepdims=True) + jnp.sum(f, axis=1, keepdims=True))
        kept = k_scr[8 * b : 8 * b + 4, :] + pstat_r[2, 8 * b : 8 * b + 4, :]
        token_s.append(jnp.sum(kept, axis=1, keepdims=True))
    e3s[0] = pack(token_s)
    e3s[1] = pack(token_q)
    e3 = exchange(e3s, e3r, e3_sem)
    for c in e3:
        c.start()

    def await_z(k, _):
        z_copy(k).wait_send()
        pltpu.make_async_remote_copy(
            src_ref=zsend.at[k], dst_ref=s_scr.at[:, :, pl.ds(pl.multiple_of((FIRST + (1 - dp) * SHARED + k) * TILE, TILE), TILE)],
            send_sem=zs_sem.at[k], recv_sem=zr_sem.at[k], device_id=partner, device_id_type=MESH,
        ).wait_recv()
        return None

    lax.fori_loop(0, SHARED, await_z, None)
    for c in e1:
        c.wait()
    lses = [e1s[...]] + [e1r[d] for d in range(3)]
    top = jnp.maximum(jnp.maximum(lses[0], lses[1]), jnp.maximum(lses[2], lses[3]))
    sums = jnp.exp(lses[0] - top) + jnp.exp(lses[1] - top) + jnp.exp(lses[2] - top) + jnp.exp(lses[3] - top)
    lse = top + jnp.log(sums)
    lse_ref[...] = lse
    row_l = [jnp.broadcast_to(unpack(lse[0:4, :], b), (4, 128)) for b in range(4)]

    def excess(b, at, size):
        e = jnp.maximum(jnp.exp(s_scr[b, :, pl.ds(at, size)] - row_l[b][:, :size]) - qv[b, :, pl.ds(at, size)], 0.0)
        ex_ref[b, :, pl.ds(at, size)] = e
        return e

    def last_pass(i, sums):
        at = pl.multiple_of(i * PASS, PASS)
        out = []
        for b in range(4):
            acc = sums[b]
            for off in range(0, PASS, 128):
                acc = acc + excess(b, at + off, 128)
            out.append(acc)
        return tuple(out)

    sums = lax.fori_loop(0, tail_at // PASS, last_pass, (zero,) * 4)
    rows = []
    for b in range(4):
        e = excess(b, tail_at, tail)
        rows.append(jnp.sum(sums[b], axis=1, keepdims=True) + jnp.sum(e, axis=1, keepdims=True))
    e2s[...] = pack(rows)
    e2 = exchange(e2s, e2r, e2_sem)
    for c in e2:
        c.start()

    for c in e3:
        c.wait()
    at_token = (e3s[...] + e3r[0]) + (e3r[1] + e3r[2])
    acc_ref[...] = jnp.minimum(jnp.exp(at_token[0] - lse[0:4, :]) / at_token[1], 1.0)

    for c in e2:
        c.wait()
    norm_ref[...] = (e2s[...] + e2r[0]) + (e2r[1] + e2r[2])


def finish_kernel(
    ex_ref, norm_ref, acc_ref, lse_ref, acc_out, norm_out, res_out, bonus_out, acc_v, norm_v, bonus_v, stage, sem, r_sem
):
    n_ids = ex_ref.shape[2]
    lane = lax.broadcasted_iota(jnp.int32, (4, 128), 1)
    norm = norm_ref[...]
    writes = []
    for b in range(4):
        total = jnp.sum(jnp.where(lane == 32 * b, norm, 0.0), axis=1, keepdims=True)
        scale = jnp.broadcast_to(1.0 / jnp.broadcast_to(total, (4, 128)), (4, 128))

        for at in range(0, n_ids, 128):
            size = min(128, n_ids - at)
            stage[b, :, at : at + size] = ex_ref[b, :, at : at + size] * scale[:, :size]
        writes.append(pltpu.make_async_copy(stage.at[b], res_out.at[b], r_sem.at[b]))
        writes[-1].start()

    sub = lax.broadcasted_iota(jnp.int32, (4, 128), 0)
    for src, dst, out, k in ((acc_ref[...], acc_v, acc_out, 0), (norm, norm_v, norm_out, 1)):
        row = jnp.sum(jnp.where(lane % 32 == sub, src, 0.0), axis=0, keepdims=True)
        for b in range(4):
            dst[b : b + 1, :] = (row if b == 0 else pltpu.roll(row, 128 - 32 * b, 1))[:, 0:4]
        writes.append(pltpu.make_async_copy(dst, out, sem.at[k]))
        writes[-1].start()
    row = lse_ref[4:5, :]
    lane = lane[0:1, :]
    packed = row
    for b in range(1, 4):
        packed = jnp.where(lane == b, pltpu.roll(row, 128 - 31 * b, 1), packed)
    bonus_v[...] = packed[:, 0:4]
    writes.append(pltpu.make_async_copy(bonus_v, bonus_out, sem.at[2]))
    writes[-1].start()
    for c in writes:
        c.wait()


def solution(mesh):
    def local_step(hidden, norm_gain, w_head, draft_probs, draft_tokens, temperature):
        n_ids = w_head.shape[1]
        width = w_head.shape[0]
        pad_ids = -(-n_ids // 128) * 128
        tail = n_ids % TILE
        vmem, smem, hbm = pltpu.VMEM, pltpu.SMEM, pltpu.HBM
        dma = pltpu.SemaphoreType.DMA
        ex, norm, acc, lse = pl.pallas_call(
            verify_kernel,
            out_shape=[vmem((4, 4, n_ids), F32), vmem((4, 128), F32), vmem((4, 128), F32), vmem((8, 128), F32)],
            in_specs=[pl.BlockSpec(memory_space=s) for s in (hbm,) * 6],
            out_specs=[pl.BlockSpec(memory_space=vmem)] * 4,
            scratch_shapes=[
                vmem((5, 4, width), jnp.bfloat16),
                vmem((1, width), F32),
                smem((4,), F32),
                smem((4, 4), jnp.int32),
                vmem((SLOTS, TILE, width), jnp.bfloat16),
                vmem((tail, width), jnp.bfloat16),
                vmem((4, 4, n_ids), F32),
                vmem((4, 4, pad_ids), F32),
                vmem((5, 4, width), F32),
                vmem((5, 4, width), F32),
                vmem((32, width), F32),
                vmem((64, width), jnp.bfloat16),
                vmem((width, 128), jnp.bfloat16),
                vmem((5, 4, 128), F32),
                vmem((5, 4, 128), F32),
                vmem((64, 128), F32),
                vmem((64, 128), F32),
                vmem((64, 128), F32),
                vmem((64, 128), F32),
                vmem((64, 128), F32),
                vmem((SHARED, 4, 4, TILE), F32),
                vmem((3, 32, 128), F32),
                vmem((3, 32, 128), F32),
                vmem((8, 128), F32),
                vmem((3, 8, 128), F32),
                vmem((4, 128), F32),
                vmem((3, 4, 128), F32),
                vmem((2, 4, 128), F32),
                vmem((3, 2, 4, 128), F32),
                dma((4,)), dma((SLOTS, 2)), dma, dma, dma((2,)), dma((2,)), dma((SHARED,)), dma((SHARED,)), dma((2,)),
                dma((2, 3)), dma((2, 3)), dma((2, 3)),
            ],
            compiler_params=pltpu.CompilerParams(collective_id=0, has_side_effects=True),
            name="verify",
        )(
            hidden.transpose(1, 0, 2), norm_gain.reshape(1, width), temperature, draft_tokens,
            w_head.T, draft_probs,
        )
        acc, norm, residual, bonus = pl.pallas_call(
            finish_kernel,
            out_shape=[
                jax.ShapeDtypeStruct((4, 4), F32),
                jax.ShapeDtypeStruct((4, 4), F32),
                jax.ShapeDtypeStruct((4, 4, n_ids), F32),
                jax.ShapeDtypeStruct((1, 4), F32),
            ],
            in_specs=[pl.BlockSpec(memory_space=vmem)] * 4,
            out_specs=[pl.BlockSpec(memory_space=hbm)] * 4,
            scratch_shapes=[
                vmem((4, 4), F32), vmem((4, 4), F32), vmem((1, 4), F32), vmem((4, 4, n_ids), F32), dma((3,)), dma((4,)),
            ],
            compiler_params=pltpu.CompilerParams(vmem_limit_bytes=16 * 1024 * 1024),
            name="finish",
        )(ex, norm, acc, lse)
        return acc, norm, residual, bonus.reshape(4)

    return jax.shard_map(
        local_step,
        mesh=mesh,
        in_specs=(P("dp", None, None), P(), P(None, "tp"), P("dp", None, "tp"), P("dp", None), P("dp")),
        out_specs=(P("dp", None), P("dp", None), P("dp", None, "tp"), P("dp")),
        check_vma=False,
    )
```

```python
import jax
import jax.numpy as jnp
from jax import lax
from jax.experimental import pallas as pl
from jax.experimental.pallas import tpu as pltpu
from jax.sharding import PartitionSpec as P

MESH = pl.DeviceIdType.MESH
F32 = jnp.float32
LOWEST = float(jnp.finfo(jnp.float32).min)

TILE = 1024
SUB = 256
DEPTH = 256
SLOTS = 4
SHARED = 14
FIRST = 5
RELAY = 3
PASS = 1024


def verify_kernel(
    h_hbm, g_hbm, t_hbm, dt_hbm, w_ref, q_ref,
    ex_ref, norm_ref, acc_ref, lse_ref,
    h_ref, g_ref, t_ref, dt_ref, wbuf, wtail, qv, s_scr, xf, xp, xrows, xb, xt, tv, tp_recv, ct, dl, m_scr, l_scr, k_scr,
    zsend, pstat_s, pstat_r, e1s, e1r, e2s, e2r, e3s, e3r,
    in_sem, w_sem, wt_sem, q_sem, x_sem, t_sem, zs_sem, zr_sem, ps_sem, e1_sem, e2_sem, e3_sem,
):
    dp, tp = lax.axis_index("dp"), lax.axis_index("tp")
    partner = (1 - dp, tp)
    peers = [(dp, lax.rem(tp + d, 4)) for d in (1, 2, 3)]
    n_ids, width = w_ref.shape
    n_full = n_ids // TILE
    tail = n_ids - n_full * TILE
    tail_at = n_full * TILE
    last = n_full - 2 * SHARED - FIRST
    steps = FIRST + SHARED + last

    def column(i):
        in_shared = (i + steps - FIRST) // steps
        past_shared = (i + steps - FIRST - SHARED) // steps
        return pl.multiple_of((i + in_shared * dp * SHARED + past_shared * (SHARED - dp * SHARED)) * TILE, TILE)

    half = TILE // 2

    def tile_copies(i, slot):
        at = column(i)
        return [
            pltpu.make_async_copy(
                w_ref.at[pl.ds(at + k * half, half), :], wbuf.at[slot, pl.ds(k * half, half), :], w_sem.at[slot, k]
            )
            for k in (0, 1)
        ]

    tail_copy = pltpu.make_async_copy(w_ref.at[pl.ds(tail_at, tail), :], wtail, wt_sem)
    q_copy = pltpu.make_async_copy(q_ref, qv, q_sem)
    small = [
        pltpu.make_async_copy(src, dst, in_sem.at[k])
        for k, (src, dst) in enumerate(((h_hbm, h_ref), (g_hbm, g_ref), (t_hbm, t_ref), (dt_hbm, dt_ref)))
    ]
    for c in small:
        c.start()
    tail_copy.start()
    for i in range(SLOTS):
        for c in tile_copies(i, i):
            c.start()
    q_copy.start()

    barrier = pltpu.get_barrier_semaphore()
    for other in [partner] + peers:
        pl.semaphore_signal(barrier, inc=1, device_id=other, device_id_type=MESH)

    for c in small:
        c.wait()
    h = h_ref[...].astype(F32)
    inv_rms = lax.rsqrt(jnp.mean(h * h, axis=-1, keepdims=True) + 1e-5)
    xf[...] = h * inv_rms * g_ref[...][None]
    for b in range(4):
        tv[0, b : b + 1, :] = jnp.full((1, 128), 1.0, F32) / jnp.full((1, 128), t_ref[b], F32)
        for j in range(4):
            tv[1 + j, b : b + 1, :] = jnp.full((1, 128), dt_ref[b, j].astype(F32), F32)

    def lay_rows(src, t_src, at):
        xrows[...] = jnp.zeros_like(xrows)
        lane = lax.broadcasted_iota(jnp.int32, (1, 128), 1) + tp * n_ids
        for b in range(4):
            for j in range(5):
                xrows[8 * b + j : 8 * b + j + 1, :] = src[j, b : b + 1, :]
            ct[at + 8 * b : at + 8 * b + 8, :] = jnp.broadcast_to(t_src[0, b : b + 1, :], (8, 128))
            dl[at + 8 * b : at + 8 * b + 8, :] = jnp.full((8, 128), -1.0, F32)
            for j in range(4):
                dl[at + 8 * b + j : at + 8 * b + j + 1, :] = t_src[1 + j, b : b + 1, :] - lane.astype(F32)
        rows = xrows[...].astype(jnp.bfloat16)
        xb[at : at + 32, :] = rows
        for k in range(0, width, 128):
            xt[k : k + 128, at : at + 32] = xrows[:, k : k + 128].T.astype(jnp.bfloat16)

    xt[:, 32:128] = jnp.zeros((width, 96), jnp.bfloat16)
    xb[32:64, :] = jnp.zeros((32, width), jnp.bfloat16)
    lay_rows(xf, tv, 0)
    m_scr[...] = jnp.full(m_scr.shape, LOWEST, F32)
    l_scr[...] = jnp.zeros_like(l_scr)
    k_scr[...] = jnp.zeros_like(k_scr)

    pl.semaphore_wait(barrier, 4)
    core = lax.rem(tp, 2)
    sibling = (dp, tp + 1 - 2 * core)

    def width_half(ref, c):
        return ref.at[:, :, pl.ds(pl.multiple_of(c * (width // 2), width // 2), width // 2)]

    def x_copy(src, c, to, k):
        return pltpu.make_async_remote_copy(
            src_ref=width_half(src, c), dst_ref=width_half(xp, c), send_sem=x_sem.at[0, k], recv_sem=x_sem.at[1, k],
            device_id=to, device_id_type=MESH,
        )

    x_direct = x_copy(xf, core, partner, 0)
    x_relay = x_copy(xp, core, sibling, 1)
    t_copy = pltpu.make_async_remote_copy(
        src_ref=tv, dst_ref=tp_recv, send_sem=t_sem.at[0], recv_sem=t_sem.at[1], device_id=partner, device_id_type=MESH
    )
    x_direct.start()
    t_copy.start()

    def by_rows(w, depth):
        return lax.dot_general(xb[:, depth], w, (((1,), (1,)), ((), ())), preferred_element_type=F32)

    def by_ids(w, depth):
        return lax.dot_general(w, xt[depth, :], (((1,), (0,)), ((), ())), preferred_element_type=F32)

    def tile_products(slot):
        sums = [None] * 4
        for k in range(0, width, DEPTH):
            depth = slice(k, k + DEPTH)
            for q in range(4):
                w = wbuf[slot, q * SUB : (q + 1) * SUB, depth]
                z = by_rows(w, depth) if q < 2 else by_ids(w, depth)
                sums[q] = z if k == 0 else sums[q] + z
        pieces = []
        for z in sums[:2]:
            pieces += [z[:, 0:128], z[:, 128:256]]
        for z in sums[2:]:
            pieces += [z[at : at + 128, :].T[0:64] for at in (0, 128)]
        return pieces

    def fold(rows, parts):
        m_old = m_scr[0:rows, :]
        m_new = m_old
        for p in parts:
            m_new = jnp.maximum(m_new, p)
        total = l_scr[0:rows, :] * jnp.exp(m_old - m_new)
        for p in parts:
            total = total + jnp.exp(p - m_new)
        m_scr[0:rows, :] = m_new
        l_scr[0:rows, :] = total

    tail_copy.wait()
    s = by_rows(wtail[...], slice(0, width))[0:32] * ct[0:32, 0:tail]
    for b in range(4):
        s_scr[b, :, tail_at : tail_at + tail] = s[8 * b : 8 * b + 4, :]
    k_scr[0:32, 0:tail] = jnp.where(dl[0:32, 0:tail] == float(tail_at), s, 0.0)
    m_tail = jnp.max(s, axis=1, keepdims=True)
    l_tail = jnp.sum(jnp.exp(s - m_tail), axis=1, keepdims=True)
    lane0 = lax.broadcasted_iota(jnp.int32, (32, 128), 1) == 0
    m_scr[0:32, :] = jnp.where(lane0, m_tail, LOWEST)
    l_scr[0:32, :] = jnp.where(lane0, l_tail, 0.0)

    def z_copy(k):
        at = column(FIRST + k)
        return pltpu.make_async_remote_copy(
            src_ref=zsend.at[k], dst_ref=s_scr.at[:, :, pl.ds(at, TILE)], send_sem=zs_sem.at[k], recv_sem=zr_sem.at[k],
            device_id=partner, device_id_type=MESH,
        )

    def step(i, rows):
        slot = i % SLOTS
        for c in tile_copies(i, slot):
            c.wait()
        k = i - FIRST
        at = column(i)
        kept = k_scr[0:rows, :]
        parts = []
        for n, z in enumerate(tile_products(slot)):
            s = z[0:rows] * ct[0:rows, :]
            parts.append(s)
            off = n * 128
            kept = jnp.where(dl[0:rows, :] == (at + off).astype(F32), s, kept)
            for b in range(4):
                s_scr[b, :, pl.ds(at + off, 128)] = s[8 * b : 8 * b + 4, :]
                if rows == 64:
                    zsend[k, b, :, off : off + 128] = s[32 + 8 * b : 32 + 8 * b + 4, :]
            if n % 2:
                fold(rows, parts)
                parts = []
        k_scr[0:rows, :] = kept

        @pl.when(i + SLOTS < steps)
        def _():
            for c in tile_copies(i + SLOTS, slot):
                c.start()

        if rows == 64:
            z_copy(k).start()

    lax.fori_loop(0, RELAY, lambda i, _: step(i, 32), None)
    x_direct.wait()
    x_relay.start()
    lax.fori_loop(RELAY, FIRST, lambda i, _: step(i, 32), None)
    x_copy(xp, 1 - core, sibling, 1).wait_recv()
    x_relay.wait_send()
    t_copy.wait()
    lay_rows(xp, tp_recv, 32)
    lax.fori_loop(FIRST, FIRST + SHARED, lambda i, _: step(i, 64), None)
    pstat_s[0] = m_scr[32:64, :]
    pstat_s[1] = l_scr[32:64, :]
    pstat_s[2] = k_scr[32:64, :]
    stat_copy = pltpu.make_async_remote_copy(
        src_ref=pstat_s, dst_ref=pstat_r, send_sem=ps_sem.at[0], recv_sem=ps_sem.at[1],
        device_id=partner, device_id_type=MESH,
    )
    stat_copy.start()
    lax.fori_loop(FIRST + SHARED, steps, lambda i, _: step(i, 32), None)

    group = lax.broadcasted_iota(jnp.int32, (8, 128), 1) // 32

    def pack(cols):
        size = cols[0].shape[0]
        packed = jnp.broadcast_to(cols[0], (size, 128))
        for b in range(1, 4):
            packed = jnp.where(group[:size] == b, cols[b], packed)
        return packed

    def unpack(packed, b):
        size = packed.shape[0]
        lane = lax.broadcasted_iota(jnp.int32, (size, 128), 1)
        return jnp.sum(jnp.where(lane == 32 * b, packed, 0.0), axis=1, keepdims=True)

    def exchange(src, dst, sem):
        return [
            pltpu.make_async_remote_copy(
                src_ref=src, dst_ref=dst.at[d], send_sem=sem.at[0, d], recv_sem=sem.at[1, d],
                device_id=peers[d], device_id_type=MESH,
            )
            for d in range(3)
        ]

    stat_copy.wait()
    m = jnp.maximum(m_scr[0:32, :], pstat_r[0])
    total = l_scr[0:32, :] * jnp.exp(m_scr[0:32, :] - m) + pstat_r[1] * jnp.exp(pstat_r[0] - m)
    row_max = jnp.max(m, axis=1, keepdims=True)
    row_lse = row_max + jnp.log(jnp.sum(total * jnp.exp(m - row_max), axis=1, keepdims=True))
    e1s[...] = pack([row_lse[8 * b : 8 * b + 8, :] for b in range(4)])
    e1 = exchange(e1s, e1r, e1_sem)
    for c in e1:
        c.start()

    q_copy.wait()
    own = [dl[8 * b : 8 * b + 4, :] for b in range(4)]

    row_m = [jnp.broadcast_to(row_max[8 * b : 8 * b + 4, :], (4, 128)) for b in range(4)]

    def prepare(b, at, size, found):
        s_scr[b, :, pl.ds(at, size)] = jnp.exp(s_scr[b, :, pl.ds(at, size)] - row_m[b][:, :size])
        return jnp.where(own[b][:, :size] == jnp.asarray(at).astype(F32), qv[b, :, pl.ds(at, size)], found)

    def prepare_tile(at, found):
        out = []
        for b in range(4):
            f = found[b]
            for off in range(0, TILE, 128):
                f = prepare(b, at + off, 128, f)
            out.append(f)
        return tuple(out)

    zero = jnp.zeros((4, 128), F32)
    found = lax.fori_loop(0, steps, lambda i, f: prepare_tile(column(i), f), (zero,) * 4)

    def take_z(k, found):
        z_copy(k).wait_send()
        at = pl.multiple_of((FIRST + (1 - dp) * SHARED + k) * TILE, TILE)
        pltpu.make_async_remote_copy(
            src_ref=zsend.at[k], dst_ref=s_scr.at[:, :, pl.ds(at, TILE)], send_sem=zs_sem.at[k], recv_sem=zr_sem.at[k],
            device_id=partner, device_id_type=MESH,
        ).wait_recv()
        return prepare_tile(at, found)

    found = lax.fori_loop(0, SHARED, take_z, found)
    token_q, token_s = [], []
    for b in range(4):
        f = prepare(b, tail_at, tail, jnp.zeros((4, tail), F32))
        token_q.append(jnp.sum(found[b], axis=1, keepdims=True) + jnp.sum(f, axis=1, keepdims=True))
        kept = k_scr[8 * b : 8 * b + 4, :] + pstat_r[2, 8 * b : 8 * b + 4, :]
        token_s.append(jnp.sum(kept, axis=1, keepdims=True))
    e3s[0] = pack(token_s)
    e3s[1] = pack(token_q)
    e3 = exchange(e3s, e3r, e3_sem)
    for c in e3:
        c.start()

    for c in e1:
        c.wait()
    lses = [e1s[...]] + [e1r[d] for d in range(3)]
    top = jnp.maximum(jnp.maximum(lses[0], lses[1]), jnp.maximum(lses[2], lses[3]))
    sums = jnp.exp(lses[0] - top) + jnp.exp(lses[1] - top) + jnp.exp(lses[2] - top) + jnp.exp(lses[3] - top)
    lse = top + jnp.log(sums)
    lse_ref[...] = lse
    scale = [jnp.exp(row_m[b] - jnp.broadcast_to(unpack(lse[0:4, :], b), (4, 128))) for b in range(4)]

    def excess(b, at, size):
        e = jnp.maximum(s_scr[b, :, pl.ds(at, size)] * scale[b][:, :size] - qv[b, :, pl.ds(at, size)], 0.0)
        ex_ref[b, :, pl.ds(at, size)] = e
        return e

    def last_pass(i, sums):
        at = pl.multiple_of(i * PASS, PASS)
        out = []
        for b in range(4):
            acc = sums[b]
            for off in range(0, PASS, 128):
                acc = acc + excess(b, at + off, 128)
            out.append(acc)
        return tuple(out)

    sums = lax.fori_loop(0, tail_at // PASS, last_pass, (zero,) * 4)
    rows = []
    for b in range(4):
        e = excess(b, tail_at, tail)
        rows.append(jnp.sum(sums[b], axis=1, keepdims=True) + jnp.sum(e, axis=1, keepdims=True))
    e2s[...] = pack(rows)
    e2 = exchange(e2s, e2r, e2_sem)
    for c in e2:
        c.start()

    for c in e3:
        c.wait()
    at_token = (e3s[...] + e3r[0]) + (e3r[1] + e3r[2])
    acc_ref[...] = jnp.minimum(jnp.exp(at_token[0] - lse[0:4, :]) / at_token[1], 1.0)

    for c in e2:
        c.wait()
    norm_ref[...] = (e2s[...] + e2r[0]) + (e2r[1] + e2r[2])


def finish_kernel(
    ex_ref, norm_ref, acc_ref, lse_ref, acc_out, norm_out, res_out, bonus_out, acc_v, norm_v, bonus_v, stage, sem, r_sem
):
    n_ids = ex_ref.shape[2]
    lane = lax.broadcasted_iota(jnp.int32, (4, 128), 1)
    norm = norm_ref[...]
    writes = []
    for b in range(4):
        total = jnp.sum(jnp.where(lane == 32 * b, norm, 0.0), axis=1, keepdims=True)
        scale = jnp.broadcast_to(1.0 / jnp.broadcast_to(total, (4, 128)), (4, 128))

        for at in range(0, n_ids, 128):
            size = min(128, n_ids - at)
            stage[b, :, at : at + size] = ex_ref[b, :, at : at + size] * scale[:, :size]
        writes.append(pltpu.make_async_copy(stage.at[b], res_out.at[b], r_sem.at[b]))
        writes[-1].start()

    sub = lax.broadcasted_iota(jnp.int32, (4, 128), 0)
    for src, dst, out, k in ((acc_ref[...], acc_v, acc_out, 0), (norm, norm_v, norm_out, 1)):
        row = jnp.sum(jnp.where(lane % 32 == sub, src, 0.0), axis=0, keepdims=True)
        for b in range(4):
            dst[b : b + 1, :] = (row if b == 0 else pltpu.roll(row, 128 - 32 * b, 1))[:, 0:4]
        writes.append(pltpu.make_async_copy(dst, out, sem.at[k]))
        writes[-1].start()
    row = lse_ref[4:5, :]
    lane = lane[0:1, :]
    packed = row
    for b in range(1, 4):
        packed = jnp.where(lane == b, pltpu.roll(row, 128 - 31 * b, 1), packed)
    bonus_v[...] = packed[:, 0:4]
    writes.append(pltpu.make_async_copy(bonus_v, bonus_out, sem.at[2]))
    writes[-1].start()
    for c in writes:
        c.wait()


def solution(mesh):
    def local_step(hidden, norm_gain, w_head, draft_probs, draft_tokens, temperature):
        n_ids = w_head.shape[1]
        width = w_head.shape[0]
        pad_ids = -(-n_ids // 128) * 128
        tail = n_ids % TILE
        vmem, smem, hbm = pltpu.VMEM, pltpu.SMEM, pltpu.HBM
        dma = pltpu.SemaphoreType.DMA
        ex, norm, acc, lse = pl.pallas_call(
            verify_kernel,
            out_shape=[vmem((4, 4, n_ids), F32), vmem((4, 128), F32), vmem((4, 128), F32), vmem((8, 128), F32)],
            in_specs=[pl.BlockSpec(memory_space=s) for s in (hbm,) * 6],
            out_specs=[pl.BlockSpec(memory_space=vmem)] * 4,
            scratch_shapes=[
                vmem((5, 4, width), jnp.bfloat16),
                vmem((1, width), F32),
                smem((4,), F32),
                smem((4, 4), jnp.int32),
                vmem((SLOTS, TILE, width), jnp.bfloat16),
                vmem((tail, width), jnp.bfloat16),
                vmem((4, 4, n_ids), F32),
                vmem((4, 4, pad_ids), F32),
                vmem((5, 4, width), F32),
                vmem((5, 4, width), F32),
                vmem((32, width), F32),
                vmem((64, width), jnp.bfloat16),
                vmem((width, 128), jnp.bfloat16),
                vmem((5, 4, 128), F32),
                vmem((5, 4, 128), F32),
                vmem((64, 128), F32),
                vmem((64, 128), F32),
                vmem((64, 128), F32),
                vmem((64, 128), F32),
                vmem((64, 128), F32),
                vmem((SHARED, 4, 4, TILE), F32),
                vmem((3, 32, 128), F32),
                vmem((3, 32, 128), F32),
                vmem((8, 128), F32),
                vmem((3, 8, 128), F32),
                vmem((4, 128), F32),
                vmem((3, 4, 128), F32),
                vmem((2, 4, 128), F32),
                vmem((3, 2, 4, 128), F32),
                dma((4,)), dma((SLOTS, 2)), dma, dma, dma((2, 2)), dma((2,)), dma((SHARED,)), dma((SHARED,)), dma((2,)),
                dma((2, 3)), dma((2, 3)), dma((2, 3)),
            ],
            compiler_params=pltpu.CompilerParams(collective_id=0, has_side_effects=True),
            name="verify",
        )(
            hidden.transpose(1, 0, 2), norm_gain.reshape(1, width), temperature, draft_tokens,
            w_head.T, draft_probs,
        )
        acc, norm, residual, bonus = pl.pallas_call(
            finish_kernel,
            out_shape=[
                jax.ShapeDtypeStruct((4, 4), F32),
                jax.ShapeDtypeStruct((4, 4), F32),
                jax.ShapeDtypeStruct((4, 4, n_ids), F32),
                jax.ShapeDtypeStruct((1, 4), F32),
            ],
            in_specs=[pl.BlockSpec(memory_space=vmem)] * 4,
            out_specs=[pl.BlockSpec(memory_space=hbm)] * 4,
            scratch_shapes=[
                vmem((4, 4), F32), vmem((4, 4), F32), vmem((1, 4), F32), vmem((4, 4, n_ids), F32), dma((3,)), dma((4,)),
            ],
            compiler_params=pltpu.CompilerParams(vmem_limit_bytes=16 * 1024 * 1024),
            name="finish",
        )(ex, norm, acc, lse)
        return acc, norm, residual, bonus.reshape(4)

    return jax.shard_map(
        local_step,
        mesh=mesh,
        in_specs=(P("dp", None, None), P(), P(None, "tp"), P("dp", None, "tp"), P("dp", None), P("dp")),
        out_specs=(P("dp", None), P("dp", None), P("dp", None, "tp"), P("dp")),
        check_vma=False,
    )
```

```python
import jax
import jax.numpy as jnp
from jax import lax
from jax.experimental import pallas as pl
from jax.experimental.pallas import tpu as pltpu
from jax.sharding import PartitionSpec as P

MESH = pl.DeviceIdType.MESH
F32 = jnp.float32
LOWEST = float(jnp.finfo(jnp.float32).min)

TILE = 1024
SUB = 256
DEPTH = 256
SLOTS = 4
SHARED = 14
FIRST = 5
RELAY = 3
PASS = 1024


def verify_kernel(
    h_hbm, g_hbm, t_hbm, dt_hbm, w_ref, q_ref,
    ex_ref, norm_ref, acc_ref, lse_ref,
    h_ref, g_ref, t_ref, dt_ref, wbuf, wtail, qv, s_scr, xf, xp, xrows, xb, xt, tv, tp_recv, ct, dl, m_scr, l_scr, k_scr,
    zsend, pstat_s, pstat_r, e1s, e1r, e2s, e2r, e3s, e3r,
    in_sem, w_sem, wt_sem, q_sem, x_sem, t_sem, zs_sem, zr_sem, ps_sem, e1_sem, e2_sem, e3_sem,
):
    dp, tp = lax.axis_index("dp"), lax.axis_index("tp")
    partner = (1 - dp, tp)
    peers = [(dp, lax.rem(tp + d, 4)) for d in (1, 2, 3)]
    n_ids, width = w_ref.shape
    n_full = n_ids // TILE
    tail = n_ids - n_full * TILE
    tail_at = n_full * TILE
    last = n_full - 2 * SHARED - FIRST
    steps = FIRST + SHARED + last

    def column(i):
        in_shared = (i + steps - FIRST) // steps
        past_shared = (i + steps - FIRST - SHARED) // steps
        return pl.multiple_of((i + in_shared * dp * SHARED + past_shared * (SHARED - dp * SHARED)) * TILE, TILE)

    half = TILE // 2

    def tile_copies(i, slot):
        at = column(i)
        return [
            pltpu.make_async_copy(
                w_ref.at[pl.ds(at + k * half, half), :], wbuf.at[slot, pl.ds(k * half, half), :], w_sem.at[slot, k]
            )
            for k in (0, 1)
        ]

    tail_copy = pltpu.make_async_copy(w_ref.at[pl.ds(tail_at, tail), :], wtail, wt_sem)
    q_copy = pltpu.make_async_copy(q_ref, qv, q_sem)
    small = [
        pltpu.make_async_copy(src, dst, in_sem.at[k])
        for k, (src, dst) in enumerate(((h_hbm, h_ref), (g_hbm, g_ref), (t_hbm, t_ref), (dt_hbm, dt_ref)))
    ]
    for c in small:
        c.start()
    tail_copy.start()
    for i in range(SLOTS):
        for c in tile_copies(i, i):
            c.start()
    q_copy.start()

    barrier = pltpu.get_barrier_semaphore()
    for other in [partner] + peers:
        pl.semaphore_signal(barrier, inc=1, device_id=other, device_id_type=MESH)

    for c in small:
        c.wait()
    h = h_ref[...].astype(F32)
    inv_rms = lax.rsqrt(jnp.mean(h * h, axis=-1, keepdims=True) + 1e-5)
    xf[...] = h * inv_rms * g_ref[...][None]
    for b in range(4):
        tv[0, b : b + 1, :] = jnp.full((1, 128), 1.0, F32) / jnp.full((1, 128), t_ref[b], F32)
        for j in range(4):
            tv[1 + j, b : b + 1, :] = jnp.full((1, 128), dt_ref[b, j].astype(F32), F32)

    def lay_rows(src, t_src, at):
        xrows[...] = jnp.zeros_like(xrows)
        lane = lax.broadcasted_iota(jnp.int32, (1, 128), 1) + tp * n_ids
        for b in range(4):
            for j in range(5):
                xrows[8 * b + j : 8 * b + j + 1, :] = src[j, b : b + 1, :]
            ct[at + 8 * b : at + 8 * b + 8, :] = jnp.broadcast_to(t_src[0, b : b + 1, :], (8, 128))
            dl[at + 8 * b : at + 8 * b + 8, :] = jnp.full((8, 128), -1.0, F32)
            for j in range(4):
                dl[at + 8 * b + j : at + 8 * b + j + 1, :] = t_src[1 + j, b : b + 1, :] - lane.astype(F32)
        rows = xrows[...].astype(jnp.bfloat16)
        xb[at : at + 32, :] = rows
        for k in range(0, width, 128):
            xt[k : k + 128, at : at + 32] = xrows[:, k : k + 128].T.astype(jnp.bfloat16)

    xt[:, 32:128] = jnp.zeros((width, 96), jnp.bfloat16)
    xb[32:64, :] = jnp.zeros((32, width), jnp.bfloat16)
    lay_rows(xf, tv, 0)
    m_scr[...] = jnp.full(m_scr.shape, LOWEST, F32)
    l_scr[...] = jnp.zeros_like(l_scr)
    k_scr[...] = jnp.zeros_like(k_scr)

    pl.semaphore_wait(barrier, 4)
    core = lax.rem(tp, 2)
    sibling = (dp, tp + 1 - 2 * core)

    def width_half(ref, c):
        return ref.at[:, :, pl.ds(pl.multiple_of(c * (width // 2), width // 2), width // 2)]

    def x_copy(src, c, to, k):
        return pltpu.make_async_remote_copy(
            src_ref=width_half(src, c), dst_ref=width_half(xp, c), send_sem=x_sem.at[0, k], recv_sem=x_sem.at[1, k],
            device_id=to, device_id_type=MESH,
        )

    x_direct = x_copy(xf, core, partner, 0)
    x_relay = x_copy(xp, core, sibling, 1)
    t_copy = pltpu.make_async_remote_copy(
        src_ref=tv, dst_ref=tp_recv, send_sem=t_sem.at[0], recv_sem=t_sem.at[1], device_id=partner, device_id_type=MESH
    )
    x_direct.start()
    t_copy.start()

    def by_rows(w, depth):
        return lax.dot_general(xb[:, depth], w, (((1,), (1,)), ((), ())), preferred_element_type=F32)

    def by_ids(w, depth):
        return lax.dot_general(w, xt[depth, :], (((1,), (0,)), ((), ())), preferred_element_type=F32)

    def tile_products(slot):
        sums = [None] * 4
        for k in range(0, width, DEPTH):
            depth = slice(k, k + DEPTH)
            for q in range(4):
                w = wbuf[slot, q * SUB : (q + 1) * SUB, depth]
                z = by_rows(w, depth) if q < 2 else by_ids(w, depth)
                sums[q] = z if k == 0 else sums[q] + z
        pieces = []
        for z in sums[:2]:
            pieces += [z[:, 0:128], z[:, 128:256]]
        for z in sums[2:]:
            pieces += [z[at : at + 128, :].T[0:64] for at in (0, 128)]
        return pieces

    def fold(rows, parts):
        m_old = m_scr[0:rows, :]
        m_new = m_old
        for p in parts:
            m_new = jnp.maximum(m_new, p)
        total = l_scr[0:rows, :] * jnp.exp(m_old - m_new)
        for p in parts:
            total = total + jnp.exp(p - m_new)
        m_scr[0:rows, :] = m_new
        l_scr[0:rows, :] = total

    tail_copy.wait()
    s = by_rows(wtail[...], slice(0, width))[0:32] * ct[0:32, 0:tail]
    for b in range(4):
        s_scr[b, :, tail_at : tail_at + tail] = s[8 * b : 8 * b + 4, :]
    k_scr[0:32, 0:tail] = jnp.where(dl[0:32, 0:tail] == float(tail_at), s, 0.0)
    m_tail = jnp.max(s, axis=1, keepdims=True)
    l_tail = jnp.sum(jnp.exp(s - m_tail), axis=1, keepdims=True)
    lane0 = lax.broadcasted_iota(jnp.int32, (32, 128), 1) == 0
    m_scr[0:32, :] = jnp.where(lane0, m_tail, LOWEST)
    l_scr[0:32, :] = jnp.where(lane0, l_tail, 0.0)

    def z_copy(k):
        at = column(FIRST + k)
        return pltpu.make_async_remote_copy(
            src_ref=zsend.at[k], dst_ref=s_scr.at[:, :, pl.ds(at, TILE)], send_sem=zs_sem.at[k], recv_sem=zr_sem.at[k],
            device_id=partner, device_id_type=MESH,
        )

    def step(i, rows):
        slot = i % SLOTS
        for c in tile_copies(i, slot):
            c.wait()
        k = i - FIRST
        at = column(i)
        kept = k_scr[0:rows, :]
        parts = []
        for n, z in enumerate(tile_products(slot)):
            s = z[0:rows] * ct[0:rows, :]
            parts.append(s)
            off = n * 128
            kept = jnp.where(dl[0:rows, :] == (at + off).astype(F32), s, kept)
            for b in range(4):
                s_scr[b, :, pl.ds(at + off, 128)] = s[8 * b : 8 * b + 4, :]
                if rows == 64:
                    zsend[k, b, :, off : off + 128] = s[32 + 8 * b : 32 + 8 * b + 4, :]
            if n % 2:
                fold(rows, parts)
                parts = []
        k_scr[0:rows, :] = kept

        @pl.when(i + SLOTS < steps)
        def _():
            for c in tile_copies(i + SLOTS, slot):
                c.start()

        if rows == 64:
            z_copy(k).start()

    lax.fori_loop(0, RELAY, lambda i, _: step(i, 32), None)
    x_direct.wait()
    x_relay.start()
    lax.fori_loop(RELAY, FIRST, lambda i, _: step(i, 32), None)
    x_copy(xp, 1 - core, sibling, 1).wait_recv()
    x_relay.wait_send()
    t_copy.wait()
    lay_rows(xp, tp_recv, 32)
    lax.fori_loop(FIRST, FIRST + SHARED, lambda i, _: step(i, 64), None)
    pstat_s[0] = m_scr[32:64, :]
    pstat_s[1] = l_scr[32:64, :]
    pstat_s[2] = k_scr[32:64, :]
    stat_copy = pltpu.make_async_remote_copy(
        src_ref=pstat_s, dst_ref=pstat_r, send_sem=ps_sem.at[0], recv_sem=ps_sem.at[1],
        device_id=partner, device_id_type=MESH,
    )
    stat_copy.start()
    lax.fori_loop(FIRST + SHARED, steps, lambda i, _: step(i, 32), None)

    group = lax.broadcasted_iota(jnp.int32, (8, 128), 1) // 32

    def pack(cols):
        size = cols[0].shape[0]
        packed = jnp.broadcast_to(cols[0], (size, 128))
        for b in range(1, 4):
            packed = jnp.where(group[:size] == b, cols[b], packed)
        return packed

    def unpack(packed, b):
        size = packed.shape[0]
        lane = lax.broadcasted_iota(jnp.int32, (size, 128), 1)
        return jnp.sum(jnp.where(lane == 32 * b, packed, 0.0), axis=1, keepdims=True)

    def exchange(src, dst, sem):
        return [
            pltpu.make_async_remote_copy(
                src_ref=src, dst_ref=dst.at[d], send_sem=sem.at[0, d], recv_sem=sem.at[1, d],
                device_id=peers[d], device_id_type=MESH,
            )
            for d in range(3)
        ]

    stat_copy.wait()
    m = jnp.maximum(m_scr[0:32, :], pstat_r[0])
    total = l_scr[0:32, :] * jnp.exp(m_scr[0:32, :] - m) + pstat_r[1] * jnp.exp(pstat_r[0] - m)
    row_max = jnp.max(m, axis=1, keepdims=True)
    row_lse = row_max + jnp.log(jnp.sum(total * jnp.exp(m - row_max), axis=1, keepdims=True))
    e1s[...] = pack([row_lse[8 * b : 8 * b + 8, :] for b in range(4)])
    e1 = exchange(e1s, e1r, e1_sem)
    for c in e1:
        c.start()

    q_copy.wait()
    own = [dl[8 * b : 8 * b + 4, :] for b in range(4)]

    row_m = [jnp.broadcast_to(row_max[8 * b : 8 * b + 4, :], (4, 128)) for b in range(4)]

    def prepare(at, size, found):
        places = [(b, at + off, min(size, 128)) for b in range(4) for off in range(0, size, 128)]
        values = [s_scr[b, :, pl.ds(a, n)] for b, a, n in places]
        values = [jnp.exp(v - row_m[b][:, :n]) for v, (b, _, n) in zip(values, places)]
        for v, (b, a, n) in zip(values, places):
            s_scr[b, :, pl.ds(a, n)] = v
        found = list(found)
        for b, a, n in places:
            found[b] = jnp.where(own[b][:, :n] == jnp.asarray(a).astype(F32), qv[b, :, pl.ds(a, n)], found[b])
        return tuple(found)

    zero = jnp.zeros((4, 128), F32)
    found = lax.fori_loop(0, steps, lambda i, f: prepare(column(i), TILE, f), (zero,) * 4)

    def take_z(k, found):
        z_copy(k).wait_send()
        at = pl.multiple_of((FIRST + (1 - dp) * SHARED + k) * TILE, TILE)
        pltpu.make_async_remote_copy(
            src_ref=zsend.at[k], dst_ref=s_scr.at[:, :, pl.ds(at, TILE)], send_sem=zs_sem.at[k], recv_sem=zr_sem.at[k],
            device_id=partner, device_id_type=MESH,
        ).wait_recv()
        return prepare(at, TILE, found)

    found = lax.fori_loop(0, SHARED, take_z, found)
    token_q, token_s = [], []
    found_tail = prepare(tail_at, tail, (jnp.zeros((4, tail), F32),) * 4)
    for b in range(4):
        f = found_tail[b]
        token_q.append(jnp.sum(found[b], axis=1, keepdims=True) + jnp.sum(f, axis=1, keepdims=True))
        kept = k_scr[8 * b : 8 * b + 4, :] + pstat_r[2, 8 * b : 8 * b + 4, :]
        token_s.append(jnp.sum(kept, axis=1, keepdims=True))
    e3s[0] = pack(token_s)
    e3s[1] = pack(token_q)
    e3 = exchange(e3s, e3r, e3_sem)
    for c in e3:
        c.start()

    for c in e1:
        c.wait()
    lses = [e1s[...]] + [e1r[d] for d in range(3)]
    top = jnp.maximum(jnp.maximum(lses[0], lses[1]), jnp.maximum(lses[2], lses[3]))
    sums = jnp.exp(lses[0] - top) + jnp.exp(lses[1] - top) + jnp.exp(lses[2] - top) + jnp.exp(lses[3] - top)
    lse = top + jnp.log(sums)
    lse_ref[...] = lse
    scale = [jnp.exp(row_m[b] - jnp.broadcast_to(unpack(lse[0:4, :], b), (4, 128))) for b in range(4)]

    def excess(b, at, size):
        e = jnp.maximum(s_scr[b, :, pl.ds(at, size)] * scale[b][:, :size] - qv[b, :, pl.ds(at, size)], 0.0)
        ex_ref[b, :, pl.ds(at, size)] = e
        return e

    def last_pass(i, sums):
        at = pl.multiple_of(i * PASS, PASS)
        out = []
        for b in range(4):
            acc = sums[b]
            for off in range(0, PASS, 128):
                acc = acc + excess(b, at + off, 128)
            out.append(acc)
        return tuple(out)

    sums = lax.fori_loop(0, tail_at // PASS, last_pass, (zero,) * 4)
    rows = []
    for b in range(4):
        e = excess(b, tail_at, tail)
        rows.append(jnp.sum(sums[b], axis=1, keepdims=True) + jnp.sum(e, axis=1, keepdims=True))
    e2s[...] = pack(rows)
    e2 = exchange(e2s, e2r, e2_sem)
    for c in e2:
        c.start()

    for c in e3:
        c.wait()
    at_token = (e3s[...] + e3r[0]) + (e3r[1] + e3r[2])
    acc_ref[...] = jnp.minimum(jnp.exp(at_token[0] - lse[0:4, :]) / at_token[1], 1.0)

    for c in e2:
        c.wait()
    norm_ref[...] = (e2s[...] + e2r[0]) + (e2r[1] + e2r[2])


def finish_kernel(
    ex_ref, norm_ref, acc_ref, lse_ref, acc_out, norm_out, res_out, bonus_out, acc_v, norm_v, bonus_v, stage, sem, r_sem
):
    n_ids = ex_ref.shape[2]
    lane = lax.broadcasted_iota(jnp.int32, (4, 128), 1)
    norm = norm_ref[...]
    writes = []
    for b in range(4):
        total = jnp.sum(jnp.where(lane == 32 * b, norm, 0.0), axis=1, keepdims=True)
        scale = jnp.broadcast_to(1.0 / jnp.broadcast_to(total, (4, 128)), (4, 128))

        for at in range(0, n_ids, 128):
            size = min(128, n_ids - at)
            stage[b, :, at : at + size] = ex_ref[b, :, at : at + size] * scale[:, :size]
        writes.append(pltpu.make_async_copy(stage.at[b], res_out.at[b], r_sem.at[b]))
        writes[-1].start()

    sub = lax.broadcasted_iota(jnp.int32, (4, 128), 0)
    for src, dst, out, k in ((acc_ref[...], acc_v, acc_out, 0), (norm, norm_v, norm_out, 1)):
        row = jnp.sum(jnp.where(lane % 32 == sub, src, 0.0), axis=0, keepdims=True)
        for b in range(4):
            dst[b : b + 1, :] = (row if b == 0 else pltpu.roll(row, 128 - 32 * b, 1))[:, 0:4]
        writes.append(pltpu.make_async_copy(dst, out, sem.at[k]))
        writes[-1].start()
    row = lse_ref[4:5, :]
    lane = lane[0:1, :]
    packed = row
    for b in range(1, 4):
        packed = jnp.where(lane == b, pltpu.roll(row, 128 - 31 * b, 1), packed)
    bonus_v[...] = packed[:, 0:4]
    writes.append(pltpu.make_async_copy(bonus_v, bonus_out, sem.at[2]))
    writes[-1].start()
    for c in writes:
        c.wait()


def solution(mesh):
    def local_step(hidden, norm_gain, w_head, draft_probs, draft_tokens, temperature):
        n_ids = w_head.shape[1]
        width = w_head.shape[0]
        pad_ids = -(-n_ids // 128) * 128
        tail = n_ids % TILE
        vmem, smem, hbm = pltpu.VMEM, pltpu.SMEM, pltpu.HBM
        dma = pltpu.SemaphoreType.DMA
        ex, norm, acc, lse = pl.pallas_call(
            verify_kernel,
            out_shape=[vmem((4, 4, n_ids), F32), vmem((4, 128), F32), vmem((4, 128), F32), vmem((8, 128), F32)],
            in_specs=[pl.BlockSpec(memory_space=s) for s in (hbm,) * 6],
            out_specs=[pl.BlockSpec(memory_space=vmem)] * 4,
            scratch_shapes=[
                vmem((5, 4, width), jnp.bfloat16),
                vmem((1, width), F32),
                smem((4,), F32),
                smem((4, 4), jnp.int32),
                vmem((SLOTS, TILE, width), jnp.bfloat16),
                vmem((tail, width), jnp.bfloat16),
                vmem((4, 4, n_ids), F32),
                vmem((4, 4, pad_ids), F32),
                vmem((5, 4, width), F32),
                vmem((5, 4, width), F32),
                vmem((32, width), F32),
                vmem((64, width), jnp.bfloat16),
                vmem((width, 128), jnp.bfloat16),
                vmem((5, 4, 128), F32),
                vmem((5, 4, 128), F32),
                vmem((64, 128), F32),
                vmem((64, 128), F32),
                vmem((64, 128), F32),
                vmem((64, 128), F32),
                vmem((64, 128), F32),
                vmem((SHARED, 4, 4, TILE), F32),
                vmem((3, 32, 128), F32),
                vmem((3, 32, 128), F32),
                vmem((8, 128), F32),
                vmem((3, 8, 128), F32),
                vmem((4, 128), F32),
                vmem((3, 4, 128), F32),
                vmem((2, 4, 128), F32),
                vmem((3, 2, 4, 128), F32),
                dma((4,)), dma((SLOTS, 2)), dma, dma, dma((2, 2)), dma((2,)), dma((SHARED,)), dma((SHARED,)), dma((2,)),
                dma((2, 3)), dma((2, 3)), dma((2, 3)),
            ],
            compiler_params=pltpu.CompilerParams(collective_id=0, has_side_effects=True),
            name="verify",
        )(
            hidden.transpose(1, 0, 2), norm_gain.reshape(1, width), temperature, draft_tokens,
            w_head.T, draft_probs,
        )
        acc, norm, residual, bonus = pl.pallas_call(
            finish_kernel,
            out_shape=[
                jax.ShapeDtypeStruct((4, 4), F32),
                jax.ShapeDtypeStruct((4, 4), F32),
                jax.ShapeDtypeStruct((4, 4, n_ids), F32),
                jax.ShapeDtypeStruct((1, 4), F32),
            ],
            in_specs=[pl.BlockSpec(memory_space=vmem)] * 4,
            out_specs=[pl.BlockSpec(memory_space=hbm)] * 4,
            scratch_shapes=[
                vmem((4, 4), F32), vmem((4, 4), F32), vmem((1, 4), F32), vmem((4, 4, n_ids), F32), dma((3,)), dma((4,)),
            ],
            compiler_params=pltpu.CompilerParams(vmem_limit_bytes=16 * 1024 * 1024),
            name="finish",
        )(ex, norm, acc, lse)
        return acc, norm, residual, bonus.reshape(4)

    return jax.shard_map(
        local_step,
        mesh=mesh,
        in_specs=(P("dp", None, None), P(), P(None, "tp"), P("dp", None, "tp"), P("dp", None), P("dp")),
        out_specs=(P("dp", None), P("dp", None), P("dp", None, "tp"), P("dp")),
        check_vma=False,
    )
```

```python
import jax
import jax.numpy as jnp
from jax import lax
from jax.experimental import pallas as pl
from jax.experimental.pallas import tpu as pltpu
from jax.sharding import PartitionSpec as P

MESH = pl.DeviceIdType.MESH
F32 = jnp.float32
LOWEST = float(jnp.finfo(jnp.float32).min)

TILE = 1024
SUB = 256
DEPTH = 256
SLOTS = 4
SHARED = 14
FIRST = 5
HELD = 2
RELAY = 3
PASS = 1024


def verify_kernel(
    h_hbm, g_hbm, t_hbm, dt_hbm, w_ref, q_ref,
    ex_ref, norm_ref, acc_ref, lse_ref,
    h_ref, g_ref, t_ref, dt_ref, wbuf, wtail, qv, s_scr, xf, xp, xrows, xb, xt, tv, tp_recv, ct, dl, m_scr, l_scr, k_scr,
    zsend, pstat_s, pstat_r, e1s, e1r, e2s, e2r, e3s, e3r,
    in_sem, w_sem, wt_sem, q_sem, x_sem, t_sem, zs_sem, zr_sem, ps_sem, e1_sem, e2_sem, e3_sem,
):
    dp, tp = lax.axis_index("dp"), lax.axis_index("tp")
    partner = (1 - dp, tp)
    peers = [(dp, lax.rem(tp + d, 4)) for d in (1, 2, 3)]
    n_ids, width = w_ref.shape
    n_full = n_ids // TILE
    tail = n_ids - n_full * TILE
    tail_at = n_full * TILE
    last = n_full - 2 * SHARED - FIRST
    steps = FIRST + SHARED + last

    def column(i):
        in_shared = (i + steps - FIRST) // steps
        past_shared = (i + steps - FIRST - SHARED) // steps
        return pl.multiple_of((i + in_shared * dp * SHARED + past_shared * (SHARED - dp * SHARED)) * TILE, TILE)

    half = TILE // 2

    def tile_copies(i, slot):
        at = column(i)
        return [
            pltpu.make_async_copy(
                w_ref.at[pl.ds(at + k * half, half), :], wbuf.at[slot, pl.ds(k * half, half), :], w_sem.at[slot, k]
            )
            for k in (0, 1)
        ]

    tail_copy = pltpu.make_async_copy(w_ref.at[pl.ds(tail_at, tail), :], wtail, wt_sem)
    q_copy = pltpu.make_async_copy(q_ref, qv, q_sem)
    small = [
        pltpu.make_async_copy(src, dst, in_sem.at[k])
        for k, (src, dst) in enumerate(((h_hbm, h_ref), (g_hbm, g_ref), (t_hbm, t_ref), (dt_hbm, dt_ref)))
    ]
    for c in small:
        c.start()
    tail_copy.start()
    for i in range(SLOTS):
        for c in tile_copies(i, i):
            c.start()
    q_copy.start()

    barrier = pltpu.get_barrier_semaphore()
    for other in [partner] + peers:
        pl.semaphore_signal(barrier, inc=1, device_id=other, device_id_type=MESH)

    for c in small:
        c.wait()
    h = h_ref[...].astype(F32)
    inv_rms = lax.rsqrt(jnp.mean(h * h, axis=-1, keepdims=True) + 1e-5)
    xf[...] = h * inv_rms * g_ref[...][None]
    for b in range(4):
        tv[0, b : b + 1, :] = jnp.full((1, 128), 1.0, F32) / jnp.full((1, 128), t_ref[b], F32)
        for j in range(4):
            tv[1 + j, b : b + 1, :] = jnp.full((1, 128), dt_ref[b, j].astype(F32), F32)

    def lay_rows(src, t_src, at):
        xrows[...] = jnp.zeros_like(xrows)
        lane = lax.broadcasted_iota(jnp.int32, (1, 128), 1) + tp * n_ids
        for b in range(4):
            for j in range(5):
                xrows[8 * b + j : 8 * b + j + 1, :] = src[j, b : b + 1, :]
            ct[at + 8 * b : at + 8 * b + 8, :] = jnp.broadcast_to(t_src[0, b : b + 1, :], (8, 128))
            dl[at + 8 * b : at + 8 * b + 8, :] = jnp.full((8, 128), -1.0, F32)
            for j in range(4):
                dl[at + 8 * b + j : at + 8 * b + j + 1, :] = t_src[1 + j, b : b + 1, :] - lane.astype(F32)
        rows = xrows[...].astype(jnp.bfloat16)
        xb[at : at + 32, :] = rows
        for k in range(0, width, 128):
            xt[k : k + 128, at : at + 32] = xrows[:, k : k + 128].T.astype(jnp.bfloat16)

    xt[:, 32:128] = jnp.zeros((width, 96), jnp.bfloat16)
    xb[32:64, :] = jnp.zeros((32, width), jnp.bfloat16)
    lay_rows(xf, tv, 0)
    m_scr[...] = jnp.full(m_scr.shape, LOWEST, F32)
    l_scr[...] = jnp.zeros_like(l_scr)
    k_scr[...] = jnp.zeros_like(k_scr)

    pl.semaphore_wait(barrier, 4)
    core = lax.rem(tp, 2)
    sibling = (dp, tp + 1 - 2 * core)

    def width_half(ref, c):
        return ref.at[:, :, pl.ds(pl.multiple_of(c * (width // 2), width // 2), width // 2)]

    def x_copy(src, c, to, k):
        return pltpu.make_async_remote_copy(
            src_ref=width_half(src, c), dst_ref=width_half(xp, c), send_sem=x_sem.at[0, k], recv_sem=x_sem.at[1, k],
            device_id=to, device_id_type=MESH,
        )

    x_direct = x_copy(xf, core, partner, 0)
    x_relay = x_copy(xp, core, sibling, 1)
    t_copy = pltpu.make_async_remote_copy(
        src_ref=tv, dst_ref=tp_recv, send_sem=t_sem.at[0], recv_sem=t_sem.at[1], device_id=partner, device_id_type=MESH
    )
    x_direct.start()
    t_copy.start()

    def by_rows(w, depth):
        return lax.dot_general(xb[:, depth], w, (((1,), (1,)), ((), ())), preferred_element_type=F32)

    def by_ids(w, depth):
        return lax.dot_general(w, xt[depth, :], (((1,), (0,)), ((), ())), preferred_element_type=F32)

    def tile_products(slot):
        sums = [None] * 4
        for k in range(0, width, DEPTH):
            depth = slice(k, k + DEPTH)
            for q in range(4):
                w = wbuf[slot, q * SUB : (q + 1) * SUB, depth]
                z = by_rows(w, depth) if q < 2 else by_ids(w, depth)
                sums[q] = z if k == 0 else sums[q] + z
        pieces = []
        for z in sums[:2]:
            pieces += [z[:, 0:128], z[:, 128:256]]
        for z in sums[2:]:
            pieces += [z[at : at + 128, :].T[0:64] for at in (0, 128)]
        return pieces

    def fold(rows, parts):
        m_old = m_scr[0:rows, :]
        m_new = m_old
        for p in parts:
            m_new = jnp.maximum(m_new, p)
        total = l_scr[0:rows, :] * jnp.exp(m_old - m_new)
        for p in parts:
            total = total + jnp.exp(p - m_new)
        m_scr[0:rows, :] = m_new
        l_scr[0:rows, :] = total

    tail_copy.wait()
    s = by_rows(wtail[...], slice(0, width))[0:32] * ct[0:32, 0:tail]
    for b in range(4):
        s_scr[b, :, tail_at : tail_at + tail] = s[8 * b : 8 * b + 4, :]
    k_scr[0:32, 0:tail] = jnp.where(dl[0:32, 0:tail] == float(tail_at), s, 0.0)
    m_tail = jnp.max(s, axis=1, keepdims=True)
    l_tail = jnp.sum(jnp.exp(s - m_tail), axis=1, keepdims=True)
    lane0 = lax.broadcasted_iota(jnp.int32, (32, 128), 1) == 0
    m_scr[0:32, :] = jnp.where(lane0, m_tail, LOWEST)
    l_scr[0:32, :] = jnp.where(lane0, l_tail, 0.0)

    def z_copy(k):
        at = column(FIRST + k)
        return pltpu.make_async_remote_copy(
            src_ref=zsend.at[k], dst_ref=s_scr.at[:, :, pl.ds(at, TILE)], send_sem=zs_sem.at[k], recv_sem=zr_sem.at[k],
            device_id=partner, device_id_type=MESH,
        )

    def step(i, rows):
        slot = i % SLOTS
        for c in tile_copies(i, slot):
            c.wait()
        k = i - FIRST
        at = column(i)
        kept = k_scr[0:rows, :]
        parts = []
        for n, z in enumerate(tile_products(slot)):
            s = z[0:rows] * ct[0:rows, :]
            parts.append(s)
            off = n * 128
            kept = jnp.where(dl[0:rows, :] == (at + off).astype(F32), s, kept)
            for b in range(4):
                s_scr[b, :, pl.ds(at + off, 128)] = s[8 * b : 8 * b + 4, :]
                if rows == 64:
                    zsend[k, b, :, off : off + 128] = s[32 + 8 * b : 32 + 8 * b + 4, :]
            if n % 2:
                fold(rows, parts)
                parts = []
        k_scr[0:rows, :] = kept

        @pl.when(i + SLOTS < steps)
        def _():
            for c in tile_copies(i + SLOTS, slot):
                c.start()

        if rows == 64:

            @pl.when(k < SHARED - HELD)
            def _():
                z_copy(k).start()

    group = lax.broadcasted_iota(jnp.int32, (8, 128), 1) // 32

    def pack(cols):
        size = cols[0].shape[0]
        packed = jnp.broadcast_to(cols[0], (size, 128))
        for b in range(1, 4):
            packed = jnp.where(group[:size] == b, cols[b], packed)
        return packed

    def unpack(packed, b):
        size = packed.shape[0]
        lane = lax.broadcasted_iota(jnp.int32, (size, 128), 1)
        return jnp.sum(jnp.where(lane == 32 * b, packed, 0.0), axis=1, keepdims=True)

    def packed_lse(at):
        m = m_scr[at : at + 32, :]
        top = jnp.max(m, axis=1, keepdims=True)
        lse = top + jnp.log(jnp.sum(l_scr[at : at + 32, :] * jnp.exp(m - top), axis=1, keepdims=True))
        return pack([lse[8 * b : 8 * b + 8, :] for b in range(4)])

    def packed_token(at):
        kept = jnp.sum(k_scr[at : at + 32, :], axis=1, keepdims=True)
        return pack([kept[8 * b : 8 * b + 8, :] for b in range(4)])

    lax.fori_loop(0, RELAY, lambda i, _: step(i, 32), None)
    x_direct.wait()
    x_relay.start()
    lax.fori_loop(RELAY, FIRST, lambda i, _: step(i, 32), None)
    x_copy(xp, 1 - core, sibling, 1).wait_recv()
    x_relay.wait_send()
    t_copy.wait()
    lay_rows(xp, tp_recv, 32)
    lax.fori_loop(FIRST, FIRST + SHARED, lambda i, _: step(i, 64), None)
    pstat_s[0] = packed_lse(32)
    pstat_s[1] = packed_token(32)
    stat_copy = pltpu.make_async_remote_copy(
        src_ref=pstat_s, dst_ref=pstat_r, send_sem=ps_sem.at[0], recv_sem=ps_sem.at[1],
        device_id=partner, device_id_type=MESH,
    )
    stat_copy.start()
    for k in range(SHARED - HELD, SHARED):
        z_copy(k).start()
    lax.fori_loop(FIRST + SHARED, steps, lambda i, _: step(i, 32), None)

    def exchange(src, dst, sem):
        return [
            pltpu.make_async_remote_copy(
                src_ref=src, dst_ref=dst.at[d], send_sem=sem.at[0, d], recv_sem=sem.at[1, d],
                device_id=peers[d], device_id_type=MESH,
            )
            for d in range(3)
        ]

    mine = packed_lse(0)
    stat_copy.wait()
    theirs = pstat_r[0]
    top = jnp.maximum(mine, theirs)
    near = top + jnp.log(jnp.exp(mine - top) + jnp.exp(theirs - top))
    e1s[...] = near
    e1 = exchange(e1s, e1r, e1_sem)
    for c in e1:
        c.start()

    q_copy.wait()
    own = [dl[8 * b : 8 * b + 4, :] for b in range(4)]

    row_m = [jnp.broadcast_to(unpack(near[0:4, :], b), (4, 128)) for b in range(4)]

    def prepare(at, size, found):
        places = [(b, at + off, min(size, 128)) for b in range(4) for off in range(0, size, 128)]
        values = [s_scr[b, :, pl.ds(a, n)] for b, a, n in places]
        values = [jnp.exp(v - row_m[b][:, :n]) for v, (b, _, n) in zip(values, places)]
        for v, (b, a, n) in zip(values, places):
            s_scr[b, :, pl.ds(a, n)] = v
        found = list(found)
        for b, a, n in places:
            found[b] = jnp.where(own[b][:, :n] == jnp.asarray(a).astype(F32), qv[b, :, pl.ds(a, n)], found[b])
        return tuple(found)

    zero = jnp.zeros((4, 128), F32)
    found = lax.fori_loop(0, steps, lambda i, f: prepare(column(i), TILE, f), (zero,) * 4)

    def take_z(k, found):
        z_copy(k).wait_send()
        at = pl.multiple_of((FIRST + (1 - dp) * SHARED + k) * TILE, TILE)
        pltpu.make_async_remote_copy(
            src_ref=zsend.at[k], dst_ref=s_scr.at[:, :, pl.ds(at, TILE)], send_sem=zs_sem.at[k], recv_sem=zr_sem.at[k],
            device_id=partner, device_id_type=MESH,
        ).wait_recv()
        return prepare(at, TILE, found)

    found = lax.fori_loop(0, SHARED, take_z, found)
    token_q = []
    found_tail = prepare(tail_at, tail, (jnp.zeros((4, tail), F32),) * 4)
    for b in range(4):
        f = found_tail[b]
        token_q.append(jnp.sum(found[b], axis=1, keepdims=True) + jnp.sum(f, axis=1, keepdims=True))
    e3s[0] = (packed_token(0) + pstat_r[1])[0:4, :]
    e3s[1] = pack(token_q)
    e3 = exchange(e3s, e3r, e3_sem)
    for c in e3:
        c.start()

    for c in e1:
        c.wait()
    lses = [near] + [e1r[d] for d in range(3)]
    top = jnp.maximum(jnp.maximum(lses[0], lses[1]), jnp.maximum(lses[2], lses[3]))
    sums = jnp.exp(lses[0] - top) + jnp.exp(lses[1] - top) + jnp.exp(lses[2] - top) + jnp.exp(lses[3] - top)
    lse = top + jnp.log(sums)
    lse_ref[...] = lse
    scale = [jnp.exp(row_m[b] - jnp.broadcast_to(unpack(lse[0:4, :], b), (4, 128))) for b in range(4)]

    def excess(b, at, size):
        e = jnp.maximum(s_scr[b, :, pl.ds(at, size)] * scale[b][:, :size] - qv[b, :, pl.ds(at, size)], 0.0)
        ex_ref[b, :, pl.ds(at, size)] = e
        return e

    def last_pass(i, sums):
        at = pl.multiple_of(i * PASS, PASS)
        out = []
        for b in range(4):
            acc = sums[b]
            for off in range(0, PASS, 128):
                acc = acc + excess(b, at + off, 128)
            out.append(acc)
        return tuple(out)

    sums = lax.fori_loop(0, tail_at // PASS, last_pass, (zero,) * 4)
    rows = []
    for b in range(4):
        e = excess(b, tail_at, tail)
        rows.append(jnp.sum(sums[b], axis=1, keepdims=True) + jnp.sum(e, axis=1, keepdims=True))
    e2s[...] = pack(rows)
    e2 = exchange(e2s, e2r, e2_sem)
    for c in e2:
        c.start()

    for c in e3:
        c.wait()
    at_token = (e3s[...] + e3r[0]) + (e3r[1] + e3r[2])
    acc_ref[...] = jnp.minimum(jnp.exp(at_token[0] - lse[0:4, :]) / at_token[1], 1.0)

    for c in e2:
        c.wait()
    norm_ref[...] = (e2s[...] + e2r[0]) + (e2r[1] + e2r[2])


def finish_kernel(
    ex_ref, norm_ref, acc_ref, lse_ref, acc_out, norm_out, res_out, bonus_out, acc_v, norm_v, bonus_v, stage, sem, r_sem
):
    n_ids = ex_ref.shape[2]
    lane = lax.broadcasted_iota(jnp.int32, (4, 128), 1)
    norm = norm_ref[...]
    writes = []
    for b in range(4):
        total = jnp.sum(jnp.where(lane == 32 * b, norm, 0.0), axis=1, keepdims=True)
        scale = jnp.broadcast_to(1.0 / jnp.broadcast_to(total, (4, 128)), (4, 128))

        for at in range(0, n_ids, 128):
            size = min(128, n_ids - at)
            stage[b, :, at : at + size] = ex_ref[b, :, at : at + size] * scale[:, :size]
        writes.append(pltpu.make_async_copy(stage.at[b], res_out.at[b], r_sem.at[b]))
        writes[-1].start()

    sub = lax.broadcasted_iota(jnp.int32, (4, 128), 0)
    for src, dst, out, k in ((acc_ref[...], acc_v, acc_out, 0), (norm, norm_v, norm_out, 1)):
        row = jnp.sum(jnp.where(lane % 32 == sub, src, 0.0), axis=0, keepdims=True)
        for b in range(4):
            dst[b : b + 1, :] = (row if b == 0 else pltpu.roll(row, 128 - 32 * b, 1))[:, 0:4]
        writes.append(pltpu.make_async_copy(dst, out, sem.at[k]))
        writes[-1].start()
    row = lse_ref[4:5, :]
    lane = lane[0:1, :]
    packed = row
    for b in range(1, 4):
        packed = jnp.where(lane == b, pltpu.roll(row, 128 - 31 * b, 1), packed)
    bonus_v[...] = packed[:, 0:4]
    writes.append(pltpu.make_async_copy(bonus_v, bonus_out, sem.at[2]))
    writes[-1].start()
    for c in writes:
        c.wait()


def solution(mesh):
    def local_step(hidden, norm_gain, w_head, draft_probs, draft_tokens, temperature):
        n_ids = w_head.shape[1]
        width = w_head.shape[0]
        pad_ids = -(-n_ids // 128) * 128
        tail = n_ids % TILE
        vmem, smem, hbm = pltpu.VMEM, pltpu.SMEM, pltpu.HBM
        dma = pltpu.SemaphoreType.DMA
        ex, norm, acc, lse = pl.pallas_call(
            verify_kernel,
            out_shape=[vmem((4, 4, n_ids), F32), vmem((4, 128), F32), vmem((4, 128), F32), vmem((8, 128), F32)],
            in_specs=[pl.BlockSpec(memory_space=s) for s in (hbm,) * 6],
            out_specs=[pl.BlockSpec(memory_space=vmem)] * 4,
            scratch_shapes=[
                vmem((5, 4, width), jnp.bfloat16),
                vmem((1, width), F32),
                smem((4,), F32),
                smem((4, 4), jnp.int32),
                vmem((SLOTS, TILE, width), jnp.bfloat16),
                vmem((tail, width), jnp.bfloat16),
                vmem((4, 4, n_ids), F32),
                vmem((4, 4, pad_ids), F32),
                vmem((5, 4, width), F32),
                vmem((5, 4, width), F32),
                vmem((32, width), F32),
                vmem((64, width), jnp.bfloat16),
                vmem((width, 128), jnp.bfloat16),
                vmem((5, 4, 128), F32),
                vmem((5, 4, 128), F32),
                vmem((64, 128), F32),
                vmem((64, 128), F32),
                vmem((64, 128), F32),
                vmem((64, 128), F32),
                vmem((64, 128), F32),
                vmem((SHARED, 4, 4, TILE), F32),
                vmem((2, 8, 128), F32),
                vmem((2, 8, 128), F32),
                vmem((8, 128), F32),
                vmem((3, 8, 128), F32),
                vmem((4, 128), F32),
                vmem((3, 4, 128), F32),
                vmem((2, 4, 128), F32),
                vmem((3, 2, 4, 128), F32),
                dma((4,)), dma((SLOTS, 2)), dma, dma, dma((2, 2)), dma((2,)), dma((SHARED,)), dma((SHARED,)), dma((2,)),
                dma((2, 3)), dma((2, 3)), dma((2, 3)),
            ],
            compiler_params=pltpu.CompilerParams(collective_id=0, has_side_effects=True),
            name="verify",
        )(
            hidden.transpose(1, 0, 2), norm_gain.reshape(1, width), temperature, draft_tokens,
            w_head.T, draft_probs,
        )
        acc, norm, residual, bonus = pl.pallas_call(
            finish_kernel,
            out_shape=[
                jax.ShapeDtypeStruct((4, 4), F32),
                jax.ShapeDtypeStruct((4, 4), F32),
                jax.ShapeDtypeStruct((4, 4, n_ids), F32),
                jax.ShapeDtypeStruct((1, 4), F32),
            ],
            in_specs=[pl.BlockSpec(memory_space=vmem)] * 4,
            out_specs=[pl.BlockSpec(memory_space=hbm)] * 4,
            scratch_shapes=[
                vmem((4, 4), F32), vmem((4, 4), F32), vmem((1, 4), F32), vmem((4, 4, n_ids), F32), dma((3,)), dma((4,)),
            ],
            compiler_params=pltpu.CompilerParams(vmem_limit_bytes=16 * 1024 * 1024),
            name="finish",
        )(ex, norm, acc, lse)
        return acc, norm, residual, bonus.reshape(4)

    return jax.shard_map(
        local_step,
        mesh=mesh,
        in_specs=(P("dp", None, None), P(), P(None, "tp"), P("dp", None, "tp"), P("dp", None), P("dp")),
        out_specs=(P("dp", None), P("dp", None), P("dp", None, "tp"), P("dp")),
        check_vma=False,
    )
```

```python
import jax
import jax.numpy as jnp
from jax import lax
from jax.experimental import pallas as pl
from jax.experimental.pallas import tpu as pltpu
from jax.sharding import PartitionSpec as P

MESH = pl.DeviceIdType.MESH
F32 = jnp.float32
LOWEST = float(jnp.finfo(jnp.float32).min)

TILE = 1024
SUB = 256
DEPTH = 256
SLOTS = 4
SHARED = 13
FIRST = 4
HELD = 2
RELAY = 2
PASS = 1024


def verify_kernel(
    h_hbm, g_hbm, t_hbm, dt_hbm, w_ref, q_ref,
    ex_ref, norm_ref, acc_ref, lse_ref,
    h_ref, g_ref, t_ref, dt_ref, wbuf, wtail, qv, s_scr, xf, xp, xrows, xb, xt, tv, tp_recv, ct, dl, m_scr, l_scr, k_scr,
    zsend, pstat_s, pstat_r, e1s, e1r, e2s, e2r, e3s, e3r,
    in_sem, w_sem, wt_sem, q_sem, x_sem, t_sem, zs_sem, zr_sem, ps_sem, e1_sem, e2_sem, e3_sem,
):
    dp, tp = lax.axis_index("dp"), lax.axis_index("tp")
    partner = (1 - dp, tp)
    peers = [(dp, lax.rem(tp + d, 4)) for d in (1, 2, 3)]
    n_ids, width = w_ref.shape
    n_full = n_ids // TILE
    tail = n_ids - n_full * TILE
    tail_at = n_full * TILE
    last = n_full - 2 * SHARED - FIRST
    steps = FIRST + SHARED + last

    def column(i):
        in_shared = (i + steps - FIRST) // steps
        past_shared = (i + steps - FIRST - SHARED) // steps
        return pl.multiple_of((i + in_shared * dp * SHARED + past_shared * (SHARED - dp * SHARED)) * TILE, TILE)

    half = TILE // 2

    def tile_copies(i, slot):
        at = column(i)
        return [
            pltpu.make_async_copy(
                w_ref.at[pl.ds(at + k * half, half), :], wbuf.at[slot, pl.ds(k * half, half), :], w_sem.at[slot, k]
            )
            for k in (0, 1)
        ]

    tail_copy = pltpu.make_async_copy(w_ref.at[pl.ds(tail_at, tail), :], wtail, wt_sem)
    q_copy = pltpu.make_async_copy(q_ref, qv, q_sem)
    small = [
        pltpu.make_async_copy(src, dst, in_sem.at[k])
        for k, (src, dst) in enumerate(((h_hbm, h_ref), (g_hbm, g_ref), (t_hbm, t_ref), (dt_hbm, dt_ref)))
    ]
    for c in small:
        c.start()
    tail_copy.start()
    for i in range(SLOTS):
        for c in tile_copies(i, i):
            c.start()
    q_copy.start()

    barrier = pltpu.get_barrier_semaphore()
    for other in [partner] + peers:
        pl.semaphore_signal(barrier, inc=1, device_id=other, device_id_type=MESH)

    for c in small:
        c.wait()
    h = h_ref[...].astype(F32)
    inv_rms = lax.rsqrt(jnp.mean(h * h, axis=-1, keepdims=True) + 1e-5)
    xf[...] = h * inv_rms * g_ref[...][None]
    for b in range(4):
        tv[0, b : b + 1, :] = jnp.full((1, 128), 1.0, F32) / jnp.full((1, 128), t_ref[b], F32)
        for j in range(4):
            tv[1 + j, b : b + 1, :] = jnp.full((1, 128), dt_ref[b, j].astype(F32), F32)

    def lay_rows(src, t_src, at):
        xrows[...] = jnp.zeros_like(xrows)
        lane = lax.broadcasted_iota(jnp.int32, (1, 128), 1) + tp * n_ids
        for b in range(4):
            for j in range(5):
                xrows[8 * b + j : 8 * b + j + 1, :] = src[j, b : b + 1, :]
            ct[at + 8 * b : at + 8 * b + 8, :] = jnp.broadcast_to(t_src[0, b : b + 1, :], (8, 128))
            dl[at + 8 * b : at + 8 * b + 8, :] = jnp.full((8, 128), -1.0, F32)
            for j in range(4):
                dl[at + 8 * b + j : at + 8 * b + j + 1, :] = t_src[1 + j, b : b + 1, :] - lane.astype(F32)
        rows = xrows[...].astype(jnp.bfloat16)
        xb[at : at + 32, :] = rows
        for k in range(0, width, 128):
            xt[k : k + 128, at : at + 32] = xrows[:, k : k + 128].T.astype(jnp.bfloat16)

    xt[:, 32:128] = jnp.zeros((width, 96), jnp.bfloat16)
    xb[32:64, :] = jnp.zeros((32, width), jnp.bfloat16)
    lay_rows(xf, tv, 0)
    m_scr[...] = jnp.full(m_scr.shape, LOWEST, F32)
    l_scr[...] = jnp.zeros_like(l_scr)
    k_scr[...] = jnp.zeros_like(k_scr)

    pl.semaphore_wait(barrier, 4)
    core = lax.rem(tp, 2)
    sibling = (dp, tp + 1 - 2 * core)

    def width_half(ref, c):
        return ref.at[:, :, pl.ds(pl.multiple_of(c * (width // 2), width // 2), width // 2)]

    def x_copy(src, c, to, k):
        return pltpu.make_async_remote_copy(
            src_ref=width_half(src, c), dst_ref=width_half(xp, c), send_sem=x_sem.at[0, k], recv_sem=x_sem.at[1, k],
            device_id=to, device_id_type=MESH,
        )

    x_direct = x_copy(xf, core, partner, 0)
    x_relay = x_copy(xp, core, sibling, 1)
    t_copy = pltpu.make_async_remote_copy(
        src_ref=tv, dst_ref=tp_recv, send_sem=t_sem.at[0], recv_sem=t_sem.at[1], device_id=partner, device_id_type=MESH
    )
    x_direct.start()
    t_copy.start()

    def by_rows(w, depth):
        return lax.dot_general(xb[:, depth], w, (((1,), (1,)), ((), ())), preferred_element_type=F32)

    def by_ids(w, depth):
        return lax.dot_general(w, xt[depth, :], (((1,), (0,)), ((), ())), preferred_element_type=F32)

    def tile_products(slot):
        sums = [None] * 4
        for k in range(0, width, DEPTH):
            depth = slice(k, k + DEPTH)
            for q in range(4):
                w = wbuf[slot, q * SUB : (q + 1) * SUB, depth]
                z = by_rows(w, depth) if q < 2 else by_ids(w, depth)
                sums[q] = z if k == 0 else sums[q] + z
        pieces = []
        for z in sums[:2]:
            pieces += [z[:, 0:128], z[:, 128:256]]
        for z in sums[2:]:
            pieces += [z[at : at + 128, :].T[0:64] for at in (0, 128)]
        return pieces

    def fold(rows, parts):
        m_old = m_scr[0:rows, :]
        m_new = m_old
        for p in parts:
            m_new = jnp.maximum(m_new, p)
        total = l_scr[0:rows, :] * jnp.exp(m_old - m_new)
        for p in parts:
            total = total + jnp.exp(p - m_new)
        m_scr[0:rows, :] = m_new
        l_scr[0:rows, :] = total

    tail_copy.wait()
    s = by_rows(wtail[...], slice(0, width))[0:32] * ct[0:32, 0:tail]
    for b in range(4):
        s_scr[b, :, tail_at : tail_at + tail] = s[8 * b : 8 * b + 4, :]
    k_scr[0:32, 0:tail] = jnp.where(dl[0:32, 0:tail] == float(tail_at), s, 0.0)
    m_tail = jnp.max(s, axis=1, keepdims=True)
    l_tail = jnp.sum(jnp.exp(s - m_tail), axis=1, keepdims=True)
    lane0 = lax.broadcasted_iota(jnp.int32, (32, 128), 1) == 0
    m_scr[0:32, :] = jnp.where(lane0, m_tail, LOWEST)
    l_scr[0:32, :] = jnp.where(lane0, l_tail, 0.0)

    def z_copy(k):
        at = column(FIRST + k)
        return pltpu.make_async_remote_copy(
            src_ref=zsend.at[k], dst_ref=s_scr.at[:, :, pl.ds(at, TILE)], send_sem=zs_sem.at[k], recv_sem=zr_sem.at[k],
            device_id=partner, device_id_type=MESH,
        )

    def step(i, rows):
        slot = i % SLOTS
        for c in tile_copies(i, slot):
            c.wait()
        k = i - FIRST
        at = column(i)
        kept = k_scr[0:rows, :]
        parts = []
        for n, z in enumerate(tile_products(slot)):
            s = z[0:rows] * ct[0:rows, :]
            parts.append(s)
            off = n * 128
            kept = jnp.where(dl[0:rows, :] == (at + off).astype(F32), s, kept)
            for b in range(4):
                s_scr[b, :, pl.ds(at + off, 128)] = s[8 * b : 8 * b + 4, :]
                if rows == 64:
                    zsend[k, b, :, off : off + 128] = s[32 + 8 * b : 32 + 8 * b + 4, :]
            if n % 2:
                fold(rows, parts)
                parts = []
        k_scr[0:rows, :] = kept

        @pl.when(i + SLOTS < steps)
        def _():
            for c in tile_copies(i + SLOTS, slot):
                c.start()

        if rows == 64:

            @pl.when(k < SHARED - HELD)
            def _():
                z_copy(k).start()

    group = lax.broadcasted_iota(jnp.int32, (8, 128), 1) // 32

    def pack(cols):
        size = cols[0].shape[0]
        packed = jnp.broadcast_to(cols[0], (size, 128))
        for b in range(1, 4):
            packed = jnp.where(group[:size] == b, cols[b], packed)
        return packed

    def unpack(packed, b):
        size = packed.shape[0]
        lane = lax.broadcasted_iota(jnp.int32, (size, 128), 1)
        return jnp.sum(jnp.where(lane == 32 * b, packed, 0.0), axis=1, keepdims=True)

    def packed_lse(at):
        m = m_scr[at : at + 32, :]
        top = jnp.max(m, axis=1, keepdims=True)
        lse = top + jnp.log(jnp.sum(l_scr[at : at + 32, :] * jnp.exp(m - top), axis=1, keepdims=True))
        return pack([lse[8 * b : 8 * b + 8, :] for b in range(4)])

    def packed_token(at):
        kept = jnp.sum(k_scr[at : at + 32, :], axis=1, keepdims=True)
        return pack([kept[8 * b : 8 * b + 8, :] for b in range(4)])

    lax.fori_loop(0, RELAY, lambda i, _: step(i, 32), None)
    x_direct.wait()
    x_relay.start()
    lax.fori_loop(RELAY, FIRST, lambda i, _: step(i, 32), None)
    x_copy(xp, 1 - core, sibling, 1).wait_recv()
    x_relay.wait_send()
    t_copy.wait()
    lay_rows(xp, tp_recv, 32)
    lax.fori_loop(FIRST, FIRST + SHARED, lambda i, _: step(i, 64), None)
    pstat_s[0] = packed_lse(32)
    pstat_s[1] = packed_token(32)
    stat_copy = pltpu.make_async_remote_copy(
        src_ref=pstat_s, dst_ref=pstat_r, send_sem=ps_sem.at[0], recv_sem=ps_sem.at[1],
        device_id=partner, device_id_type=MESH,
    )
    stat_copy.start()
    for k in range(SHARED - HELD, SHARED):
        z_copy(k).start()
    lax.fori_loop(FIRST + SHARED, steps, lambda i, _: step(i, 32), None)

    def exchange(src, dst, sem):
        return [
            pltpu.make_async_remote_copy(
                src_ref=src, dst_ref=dst.at[d], send_sem=sem.at[0, d], recv_sem=sem.at[1, d],
                device_id=peers[d], device_id_type=MESH,
            )
            for d in range(3)
        ]

    mine = packed_lse(0)
    stat_copy.wait()
    theirs = pstat_r[0]
    top = jnp.maximum(mine, theirs)
    near = top + jnp.log(jnp.exp(mine - top) + jnp.exp(theirs - top))
    e1s[...] = near
    e1 = exchange(e1s, e1r, e1_sem)
    for c in e1:
        c.start()

    q_copy.wait()
    own = [dl[8 * b : 8 * b + 4, :] for b in range(4)]

    row_m = [jnp.broadcast_to(unpack(near[0:4, :], b), (4, 128)) for b in range(4)]

    def prepare(at, size, found):
        places = [(b, at + off, min(size, 128)) for b in range(4) for off in range(0, size, 128)]
        values = [s_scr[b, :, pl.ds(a, n)] for b, a, n in places]
        values = [jnp.exp(v - row_m[b][:, :n]) for v, (b, _, n) in zip(values, places)]
        for v, (b, a, n) in zip(values, places):
            s_scr[b, :, pl.ds(a, n)] = v
        found = list(found)
        for b, a, n in places:
            found[b] = jnp.where(own[b][:, :n] == jnp.asarray(a).astype(F32), qv[b, :, pl.ds(a, n)], found[b])
        return tuple(found)

    zero = jnp.zeros((4, 128), F32)
    found = lax.fori_loop(0, steps, lambda i, f: prepare(column(i), TILE, f), (zero,) * 4)

    def take_z(k, found):
        z_copy(k).wait_send()
        at = pl.multiple_of((FIRST + (1 - dp) * SHARED + k) * TILE, TILE)
        pltpu.make_async_remote_copy(
            src_ref=zsend.at[k], dst_ref=s_scr.at[:, :, pl.ds(at, TILE)], send_sem=zs_sem.at[k], recv_sem=zr_sem.at[k],
            device_id=partner, device_id_type=MESH,
        ).wait_recv()
        return prepare(at, TILE, found)

    found = lax.fori_loop(0, SHARED, take_z, found)
    token_q = []
    found_tail = prepare(tail_at, tail, (jnp.zeros((4, tail), F32),) * 4)
    for b in range(4):
        f = found_tail[b]
        token_q.append(jnp.sum(found[b], axis=1, keepdims=True) + jnp.sum(f, axis=1, keepdims=True))
    e3s[0] = (packed_token(0) + pstat_r[1])[0:4, :]
    e3s[1] = pack(token_q)
    e3 = exchange(e3s, e3r, e3_sem)
    for c in e3:
        c.start()

    for c in e1:
        c.wait()
    lses = [near] + [e1r[d] for d in range(3)]
    top = jnp.maximum(jnp.maximum(lses[0], lses[1]), jnp.maximum(lses[2], lses[3]))
    sums = jnp.exp(lses[0] - top) + jnp.exp(lses[1] - top) + jnp.exp(lses[2] - top) + jnp.exp(lses[3] - top)
    lse = top + jnp.log(sums)
    lse_ref[...] = lse
    scale = [jnp.exp(row_m[b] - jnp.broadcast_to(unpack(lse[0:4, :], b), (4, 128))) for b in range(4)]

    def excess(b, at, size):
        e = jnp.maximum(s_scr[b, :, pl.ds(at, size)] * scale[b][:, :size] - qv[b, :, pl.ds(at, size)], 0.0)
        ex_ref[b, :, pl.ds(at, size)] = e
        return e

    def last_pass(i, sums):
        at = pl.multiple_of(i * PASS, PASS)
        out = []
        for b in range(4):
            acc = sums[b]
            for off in range(0, PASS, 128):
                acc = acc + excess(b, at + off, 128)
            out.append(acc)
        return tuple(out)

    sums = lax.fori_loop(0, tail_at // PASS, last_pass, (zero,) * 4)
    rows = []
    for b in range(4):
        e = excess(b, tail_at, tail)
        rows.append(jnp.sum(sums[b], axis=1, keepdims=True) + jnp.sum(e, axis=1, keepdims=True))
    e2s[...] = pack(rows)
    e2 = exchange(e2s, e2r, e2_sem)
    for c in e2:
        c.start()

    for c in e3:
        c.wait()
    at_token = (e3s[...] + e3r[0]) + (e3r[1] + e3r[2])
    acc_ref[...] = jnp.minimum(jnp.exp(at_token[0] - lse[0:4, :]) / at_token[1], 1.0)

    for c in e2:
        c.wait()
    norm_ref[...] = (e2s[...] + e2r[0]) + (e2r[1] + e2r[2])


def finish_kernel(
    ex_ref, norm_ref, acc_ref, lse_ref, acc_out, norm_out, res_out, bonus_out, acc_v, norm_v, bonus_v, stage, sem, r_sem
):
    n_ids = ex_ref.shape[2]
    lane = lax.broadcasted_iota(jnp.int32, (4, 128), 1)
    norm = norm_ref[...]
    writes = []
    for b in range(4):
        total = jnp.sum(jnp.where(lane == 32 * b, norm, 0.0), axis=1, keepdims=True)
        scale = jnp.broadcast_to(1.0 / jnp.broadcast_to(total, (4, 128)), (4, 128))

        for at in range(0, n_ids, 128):
            size = min(128, n_ids - at)
            stage[b, :, at : at + size] = ex_ref[b, :, at : at + size] * scale[:, :size]
        writes.append(pltpu.make_async_copy(stage.at[b], res_out.at[b], r_sem.at[b]))
        writes[-1].start()

    sub = lax.broadcasted_iota(jnp.int32, (4, 128), 0)
    for src, dst, out, k in ((acc_ref[...], acc_v, acc_out, 0), (norm, norm_v, norm_out, 1)):
        row = jnp.sum(jnp.where(lane % 32 == sub, src, 0.0), axis=0, keepdims=True)
        for b in range(4):
            dst[b : b + 1, :] = (row if b == 0 else pltpu.roll(row, 128 - 32 * b, 1))[:, 0:4]
        writes.append(pltpu.make_async_copy(dst, out, sem.at[k]))
        writes[-1].start()
    row = lse_ref[4:5, :]
    lane = lane[0:1, :]
    packed = row
    for b in range(1, 4):
        packed = jnp.where(lane == b, pltpu.roll(row, 128 - 31 * b, 1), packed)
    bonus_v[...] = packed[:, 0:4]
    writes.append(pltpu.make_async_copy(bonus_v, bonus_out, sem.at[2]))
    writes[-1].start()
    for c in writes:
        c.wait()


def solution(mesh):
    def local_step(hidden, norm_gain, w_head, draft_probs, draft_tokens, temperature):
        n_ids = w_head.shape[1]
        width = w_head.shape[0]
        pad_ids = -(-n_ids // 128) * 128
        tail = n_ids % TILE
        vmem, smem, hbm = pltpu.VMEM, pltpu.SMEM, pltpu.HBM
        dma = pltpu.SemaphoreType.DMA
        ex, norm, acc, lse = pl.pallas_call(
            verify_kernel,
            out_shape=[vmem((4, 4, n_ids), F32), vmem((4, 128), F32), vmem((4, 128), F32), vmem((8, 128), F32)],
            in_specs=[pl.BlockSpec(memory_space=s) for s in (hbm,) * 6],
            out_specs=[pl.BlockSpec(memory_space=vmem)] * 4,
            scratch_shapes=[
                vmem((5, 4, width), jnp.bfloat16),
                vmem((1, width), F32),
                smem((4,), F32),
                smem((4, 4), jnp.int32),
                vmem((SLOTS, TILE, width), jnp.bfloat16),
                vmem((tail, width), jnp.bfloat16),
                vmem((4, 4, n_ids), F32),
                vmem((4, 4, pad_ids), F32),
                vmem((5, 4, width), F32),
                vmem((5, 4, width), F32),
                vmem((32, width), F32),
                vmem((64, width), jnp.bfloat16),
                vmem((width, 128), jnp.bfloat16),
                vmem((5, 4, 128), F32),
                vmem((5, 4, 128), F32),
                vmem((64, 128), F32),
                vmem((64, 128), F32),
                vmem((64, 128), F32),
                vmem((64, 128), F32),
                vmem((64, 128), F32),
                vmem((SHARED, 4, 4, TILE), F32),
                vmem((2, 8, 128), F32),
                vmem((2, 8, 128), F32),
                vmem((8, 128), F32),
                vmem((3, 8, 128), F32),
                vmem((4, 128), F32),
                vmem((3, 4, 128), F32),
                vmem((2, 4, 128), F32),
                vmem((3, 2, 4, 128), F32),
                dma((4,)), dma((SLOTS, 2)), dma, dma, dma((2, 2)), dma((2,)), dma((SHARED,)), dma((SHARED,)), dma((2,)),
                dma((2, 3)), dma((2, 3)), dma((2, 3)),
            ],
            compiler_params=pltpu.CompilerParams(collective_id=0, has_side_effects=True),
            name="verify",
        )(
            hidden.transpose(1, 0, 2), norm_gain.reshape(1, width), temperature, draft_tokens,
            w_head.T, draft_probs,
        )
        acc, norm, residual, bonus = pl.pallas_call(
            finish_kernel,
            out_shape=[
                jax.ShapeDtypeStruct((4, 4), F32),
                jax.ShapeDtypeStruct((4, 4), F32),
                jax.ShapeDtypeStruct((4, 4, n_ids), F32),
                jax.ShapeDtypeStruct((1, 4), F32),
            ],
            in_specs=[pl.BlockSpec(memory_space=vmem)] * 4,
            out_specs=[pl.BlockSpec(memory_space=hbm)] * 4,
            scratch_shapes=[
                vmem((4, 4), F32), vmem((4, 4), F32), vmem((1, 4), F32), vmem((4, 4, n_ids), F32), dma((3,)), dma((4,)),
            ],
            compiler_params=pltpu.CompilerParams(vmem_limit_bytes=16 * 1024 * 1024),
            name="finish",
        )(ex, norm, acc, lse)
        return acc, norm, residual, bonus.reshape(4)

    return jax.shard_map(
        local_step,
        mesh=mesh,
        in_specs=(P("dp", None, None), P(), P(None, "tp"), P("dp", None, "tp"), P("dp", None), P("dp")),
        out_specs=(P("dp", None), P("dp", None), P("dp", None, "tp"), P("dp")),
        check_vma=False,
    )
```

```python
import jax
import jax.numpy as jnp
from jax import lax
from jax.experimental import pallas as pl
from jax.experimental.pallas import tpu as pltpu
from jax.sharding import PartitionSpec as P

MESH = pl.DeviceIdType.MESH
F32 = jnp.float32
LOWEST = float(jnp.finfo(jnp.float32).min)

TILE = 1024
SUB = 256
DEPTH = 256
SLOTS = 4
SHARED = 14
FIRST = 4
HELD = 2
RELAY = 2
PARTS = 4
PASS = 4736


def verify_kernel(
    h_hbm, g_hbm, t_hbm, dt_hbm, w_ref, q_ref,
    ex_ref, norm_ref, acc_ref, lse_ref,
    h_ref, g_ref, t_ref, dt_ref, wbuf, wtail, qv, s_scr, xf, xp, xrows, xb, xt, tv, tp_recv, ct, dl, m_scr, l_scr, k_scr,
    zsend, pstat_s, pstat_r, e1s, e1r, e2s, e2r, e3s, e3r,
    in_sem, w_sem, wt_sem, q_sem, x_sem, t_sem, zs_sem, zr_sem, ps_sem, e1_sem, e2_sem, e3_sem,
):
    dp, tp = lax.axis_index("dp"), lax.axis_index("tp")
    partner = (1 - dp, tp)
    peers = [(dp, lax.rem(tp + d, 4)) for d in (1, 2, 3)]
    n_ids, width = w_ref.shape
    n_full = n_ids // TILE
    tail = n_ids - n_full * TILE
    tail_at = n_full * TILE
    last = n_full - 2 * SHARED - FIRST
    steps = FIRST + SHARED + last

    def column(i):
        in_shared = (i + steps - FIRST) // steps
        past_shared = (i + steps - FIRST - SHARED) // steps
        return pl.multiple_of((i + in_shared * dp * SHARED + past_shared * (SHARED - dp * SHARED)) * TILE, TILE)

    part = TILE // PARTS

    def tile_copies(i, slot):
        at = column(i)
        return [
            pltpu.make_async_copy(
                w_ref.at[pl.ds(at + k * part, part), :], wbuf.at[slot, pl.ds(k * part, part), :], w_sem.at[slot, k]
            )
            for k in range(PARTS)
        ]

    tail_copy = pltpu.make_async_copy(w_ref.at[pl.ds(tail_at, tail), :], wtail, wt_sem)
    q_copy = pltpu.make_async_copy(q_ref, qv, q_sem)
    small = [
        pltpu.make_async_copy(src, dst, in_sem.at[k])
        for k, (src, dst) in enumerate(((h_hbm, h_ref), (g_hbm, g_ref), (t_hbm, t_ref), (dt_hbm, dt_ref)))
    ]
    for c in small:
        c.start()
    tail_copy.start()
    for i in range(SLOTS):
        for c in tile_copies(i, i):
            c.start()

    barrier = pltpu.get_barrier_semaphore()
    for other in [partner] + peers:
        pl.semaphore_signal(barrier, inc=1, device_id=other, device_id_type=MESH)

    for c in small:
        c.wait()
    h = h_ref[...].astype(F32)
    inv_rms = lax.rsqrt(jnp.mean(h * h, axis=-1, keepdims=True) + 1e-5)
    xf[...] = h * inv_rms * g_ref[...][None]
    for b in range(4):
        tv[0, b : b + 1, :] = jnp.full((1, 128), 1.0, F32) / jnp.full((1, 128), t_ref[b], F32)
        for j in range(4):
            tv[1 + j, b : b + 1, :] = jnp.full((1, 128), dt_ref[b, j].astype(F32), F32)

    def lay_rows(src, t_src, at):
        xrows[...] = jnp.zeros_like(xrows)
        lane = lax.broadcasted_iota(jnp.int32, (1, 128), 1) + tp * n_ids
        for b in range(4):
            for j in range(5):
                xrows[8 * b + j : 8 * b + j + 1, :] = src[j, b : b + 1, :]
            ct[at + 8 * b : at + 8 * b + 8, :] = jnp.broadcast_to(t_src[0, b : b + 1, :], (8, 128))
            dl[at + 8 * b : at + 8 * b + 8, :] = jnp.full((8, 128), -1.0, F32)
            for j in range(4):
                dl[at + 8 * b + j : at + 8 * b + j + 1, :] = t_src[1 + j, b : b + 1, :] - lane.astype(F32)
        rows = xrows[...].astype(jnp.bfloat16)
        xb[at : at + 32, :] = rows
        for k in range(0, width, 128):
            xt[k : k + 128, at : at + 32] = xrows[:, k : k + 128].T.astype(jnp.bfloat16)

    xt[:, 32:128] = jnp.zeros((width, 96), jnp.bfloat16)
    xb[32:64, :] = jnp.zeros((32, width), jnp.bfloat16)
    lay_rows(xf, tv, 0)
    m_scr[...] = jnp.full(m_scr.shape, LOWEST, F32)
    l_scr[...] = jnp.zeros_like(l_scr)
    k_scr[...] = jnp.zeros_like(k_scr)

    pl.semaphore_wait(barrier, 4)
    core = lax.rem(tp, 2)
    sibling = (dp, tp + 1 - 2 * core)

    def width_half(ref, c):
        return ref.at[:, :, pl.ds(pl.multiple_of(c * (width // 2), width // 2), width // 2)]

    def x_copy(src, c, to, k):
        return pltpu.make_async_remote_copy(
            src_ref=width_half(src, c), dst_ref=width_half(xp, c), send_sem=x_sem.at[0, k], recv_sem=x_sem.at[1, k],
            device_id=to, device_id_type=MESH,
        )

    x_direct = x_copy(xf, core, partner, 0)
    x_relay = x_copy(xp, core, sibling, 1)
    t_copy = pltpu.make_async_remote_copy(
        src_ref=tv, dst_ref=tp_recv, send_sem=t_sem.at[0], recv_sem=t_sem.at[1], device_id=partner, device_id_type=MESH
    )
    x_direct.start()
    t_copy.start()

    def by_rows(w, depth):
        return lax.dot_general(xb[:, depth], w, (((1,), (1,)), ((), ())), preferred_element_type=F32)

    def by_ids(w, depth):
        return lax.dot_general(w, xt[depth, :], (((1,), (0,)), ((), ())), preferred_element_type=F32)

    def products(slot, lo, size):
        block = min(SUB, size // 2)
        starts = range(lo, lo + size, block)
        fixed = len(starts) // 2
        sums = [None] * len(starts)
        for k in range(0, width, DEPTH):
            depth = slice(k, k + DEPTH)
            for n, start in enumerate(starts):
                w = wbuf[slot, start : start + block, depth]
                z = by_rows(w, depth) if n < fixed else by_ids(w, depth)
                sums[n] = z if k == 0 else sums[n] + z
        pieces = []
        for n, z in enumerate(sums):
            for at in range(0, block, 128):
                pieces.append(z[:, at : at + 128] if n < fixed else z[at : at + 128, :].T[0:64])
        return pieces

    def fold(rows, parts):
        m_old = m_scr[0:rows, :]
        m_new = m_old
        for p in parts:
            m_new = jnp.maximum(m_new, p)
        total = l_scr[0:rows, :] * jnp.exp(m_old - m_new)
        for p in parts:
            total = total + jnp.exp(p - m_new)
        m_scr[0:rows, :] = m_new
        l_scr[0:rows, :] = total

    tail_copy.wait()
    s = by_rows(wtail[...], slice(0, width))[0:32] * ct[0:32, 0:tail]
    for b in range(4):
        s_scr[b, :, tail_at : tail_at + tail] = s[8 * b : 8 * b + 4, :]
    k_scr[0:32, 0:tail] = jnp.where(dl[0:32, 0:tail] == float(tail_at), s, 0.0)
    m_tail = jnp.max(s, axis=1, keepdims=True)
    l_tail = jnp.sum(jnp.exp(s - m_tail), axis=1, keepdims=True)
    lane0 = lax.broadcasted_iota(jnp.int32, (32, 128), 1) == 0
    m_scr[0:32, :] = jnp.where(lane0, m_tail, LOWEST)
    l_scr[0:32, :] = jnp.where(lane0, l_tail, 0.0)

    def z_copy(k):
        at = column(FIRST + k)
        return pltpu.make_async_remote_copy(
            src_ref=zsend.at[k], dst_ref=s_scr.at[:, :, pl.ds(at, TILE)], send_sem=zs_sem.at[k], recv_sem=zr_sem.at[k],
            device_id=partner, device_id_type=MESH,
        )

    def consume(slot, at, lo, size, rows, k):
        kept = k_scr[0:rows, :]
        parts = []
        for n, z in enumerate(products(slot, lo, size)):
            s = z[0:rows] * ct[0:rows, :]
            parts.append(s)
            off = lo + n * 128
            kept = jnp.where(dl[0:rows, :] == (at + off).astype(F32), s, kept)
            for b in range(4):
                s_scr[b, :, pl.ds(at + off, 128)] = s[8 * b : 8 * b + 4, :]
                if rows == 64:
                    zsend[k, b, :, off : off + 128] = s[32 + 8 * b : 32 + 8 * b + 4, :]
            if n % 2:
                fold(rows, parts)
                parts = []
        k_scr[0:rows, :] = kept

    def step(i, rows):
        slot = i % SLOTS
        for c in tile_copies(i, slot):
            c.wait()
        k = i - FIRST
        consume(slot, column(i), 0, TILE, rows, k)

        @pl.when(i + SLOTS < steps)
        def _():
            for c in tile_copies(i + SLOTS, slot):
                c.start()

        if rows == 64:

            @pl.when(k < SHARED - HELD)
            def _():
                z_copy(k).start()

    group = lax.broadcasted_iota(jnp.int32, (8, 128), 1) // 32

    def pack(cols):
        size = cols[0].shape[0]
        packed = jnp.broadcast_to(cols[0], (size, 128))
        for b in range(1, 4):
            packed = jnp.where(group[:size] == b, cols[b], packed)
        return packed

    def unpack(packed, b):
        size = packed.shape[0]
        lane = lax.broadcasted_iota(jnp.int32, (size, 128), 1)
        return jnp.sum(jnp.where(lane == 32 * b, packed, 0.0), axis=1, keepdims=True)

    def packed_lse(at):
        m = m_scr[at : at + 32, :]
        top = jnp.max(m, axis=1, keepdims=True)
        lse = top + jnp.log(jnp.sum(l_scr[at : at + 32, :] * jnp.exp(m - top), axis=1, keepdims=True))
        return pack([lse[8 * b : 8 * b + 8, :] for b in range(4)])

    def packed_token(at):
        kept = jnp.sum(k_scr[at : at + 32, :], axis=1, keepdims=True)
        return pack([kept[8 * b : 8 * b + 8, :] for b in range(4)])

    lax.fori_loop(0, RELAY, lambda i, _: step(i, 32), None)
    x_direct.wait()
    x_relay.start()
    lax.fori_loop(RELAY, FIRST, lambda i, _: step(i, 32), None)
    x_copy(xp, 1 - core, sibling, 1).wait_recv()
    x_relay.wait_send()
    t_copy.wait()
    lay_rows(xp, tp_recv, 32)
    lax.fori_loop(FIRST, FIRST + SHARED, lambda i, _: step(i, 64), None)
    q_copy.start()
    pstat_s[0] = packed_lse(32)
    pstat_s[1] = packed_token(32)
    stat_copy = pltpu.make_async_remote_copy(
        src_ref=pstat_s, dst_ref=pstat_r, send_sem=ps_sem.at[0], recv_sem=ps_sem.at[1],
        device_id=partner, device_id_type=MESH,
    )
    stat_copy.start()
    for k in range(SHARED - HELD, SHARED):
        z_copy(k).start()
    lax.fori_loop(FIRST + SHARED, steps - 1, lambda i, _: step(i, 32), None)
    end, slot = steps - 1, (steps - 1) % SLOTS
    copies = tile_copies(end, slot)
    for lo, size in ((0, 2 * part), (2 * part, part), (3 * part, part)):
        for c in copies[lo // part : (lo + size) // part]:
            c.wait()
        consume(slot, column(end), lo, size, 32, 0)

    def exchange(src, dst, sem):
        return [
            pltpu.make_async_remote_copy(
                src_ref=src, dst_ref=dst.at[d], send_sem=sem.at[0, d], recv_sem=sem.at[1, d],
                device_id=peers[d], device_id_type=MESH,
            )
            for d in range(3)
        ]

    mine = packed_lse(0)
    stat_copy.wait()
    theirs = pstat_r[0]
    top = jnp.maximum(mine, theirs)
    near = top + jnp.log(jnp.exp(mine - top) + jnp.exp(theirs - top))
    e1s[...] = near
    e1 = exchange(e1s, e1r, e1_sem)
    for c in e1:
        c.start()

    own = [dl[8 * b : 8 * b + 4, :] for b in range(4)]

    row_m = [jnp.broadcast_to(unpack(near[0:4, :], b), (4, 128)) for b in range(4)]

    def prepare(at, size):
        places = [(b, at + off, min(size, 128)) for b in range(4) for off in range(0, size, 128)]
        values = [s_scr[b, :, pl.ds(a, n)] for b, a, n in places]
        values = [jnp.exp(v - row_m[b][:, :n]) for v, (b, _, n) in zip(values, places)]
        for v, (b, a, n) in zip(values, places):
            s_scr[b, :, pl.ds(a, n)] = v

    def pick(at, size, found):
        out = []
        for b in range(4):
            f = found[b]
            for off in range(0, size, 128):
                n = min(size, 128)
                f = jnp.where(own[b][:, :n] == jnp.asarray(at + off).astype(F32), qv[b, :, pl.ds(at + off, n)], f)
            out.append(f)
        return tuple(out)

    zero = jnp.zeros((4, 128), F32)
    lax.fori_loop(0, steps, lambda i, _: prepare(column(i), TILE), None)
    prepare(tail_at, tail)
    q_copy.wait()
    found = lax.fori_loop(0, tail_at // PASS, lambda i, f: pick(pl.multiple_of(i * PASS, 128), PASS, f), (zero,) * 4)
    found_tail = pick(tail_at, tail, (jnp.zeros((4, tail), F32),) * 4)
    token_q = []
    for b in range(4):
        f = found_tail[b]
        token_q.append(jnp.sum(found[b], axis=1, keepdims=True) + jnp.sum(f, axis=1, keepdims=True))
    e3s[0] = (packed_token(0) + pstat_r[1])[0:4, :]
    e3s[1] = pack(token_q)
    e3 = exchange(e3s, e3r, e3_sem)
    for c in e3:
        c.start()

    def take_z(k, _):
        z_copy(k).wait_send()
        at = pl.multiple_of((FIRST + (1 - dp) * SHARED + k) * TILE, TILE)
        pltpu.make_async_remote_copy(
            src_ref=zsend.at[k], dst_ref=s_scr.at[:, :, pl.ds(at, TILE)], send_sem=zs_sem.at[k], recv_sem=zr_sem.at[k],
            device_id=partner, device_id_type=MESH,
        ).wait_recv()
        prepare(at, TILE)

    lax.fori_loop(0, SHARED, take_z, None)

    for c in e1:
        c.wait()
    lses = [near] + [e1r[d] for d in range(3)]
    top = jnp.maximum(jnp.maximum(lses[0], lses[1]), jnp.maximum(lses[2], lses[3]))
    sums = jnp.exp(lses[0] - top) + jnp.exp(lses[1] - top) + jnp.exp(lses[2] - top) + jnp.exp(lses[3] - top)
    lse = top + jnp.log(sums)
    lse_ref[...] = lse
    scale = [jnp.exp(row_m[b] - jnp.broadcast_to(unpack(lse[0:4, :], b), (4, 128))) for b in range(4)]

    def excess(b, at, size):
        e = jnp.maximum(s_scr[b, :, pl.ds(at, size)] * scale[b][:, :size] - qv[b, :, pl.ds(at, size)], 0.0)
        ex_ref[b, :, pl.ds(at, size)] = e
        return e

    def last_pass(i, sums):
        at = pl.multiple_of(i * PASS, 128)
        out = []
        for b in range(4):
            acc = sums[b]
            for off in range(0, PASS, 128):
                acc = acc + excess(b, at + off, 128)
            out.append(acc)
        return tuple(out)

    sums = lax.fori_loop(0, tail_at // PASS, last_pass, (zero,) * 4)
    rows = []
    for b in range(4):
        e = excess(b, tail_at, tail)
        rows.append(jnp.sum(sums[b], axis=1, keepdims=True) + jnp.sum(e, axis=1, keepdims=True))
    e2s[...] = pack(rows)
    e2 = exchange(e2s, e2r, e2_sem)
    for c in e2:
        c.start()

    for c in e3:
        c.wait()
    at_token = (e3s[...] + e3r[0]) + (e3r[1] + e3r[2])
    acc_ref[...] = jnp.minimum(jnp.exp(at_token[0] - lse[0:4, :]) / at_token[1], 1.0)

    for c in e2:
        c.wait()
    norm_ref[...] = (e2s[...] + e2r[0]) + (e2r[1] + e2r[2])


def finish_kernel(
    ex_ref, norm_ref, acc_ref, lse_ref, acc_out, norm_out, res_out, bonus_out, acc_v, norm_v, bonus_v, stage, sem, r_sem
):
    n_ids = ex_ref.shape[2]
    lane = lax.broadcasted_iota(jnp.int32, (4, 128), 1)
    norm = norm_ref[...]
    writes = []
    for b in range(4):
        total = jnp.sum(jnp.where(lane == 32 * b, norm, 0.0), axis=1, keepdims=True)
        scale = jnp.broadcast_to(1.0 / jnp.broadcast_to(total, (4, 128)), (4, 128))

        for at in range(0, n_ids, 128):
            size = min(128, n_ids - at)
            stage[b, :, at : at + size] = ex_ref[b, :, at : at + size] * scale[:, :size]
        writes.append(pltpu.make_async_copy(stage.at[b], res_out.at[b], r_sem.at[b]))
        writes[-1].start()

    sub = lax.broadcasted_iota(jnp.int32, (4, 128), 0)
    for src, dst, out, k in ((acc_ref[...], acc_v, acc_out, 0), (norm, norm_v, norm_out, 1)):
        row = jnp.sum(jnp.where(lane % 32 == sub, src, 0.0), axis=0, keepdims=True)
        for b in range(4):
            dst[b : b + 1, :] = (row if b == 0 else pltpu.roll(row, 128 - 32 * b, 1))[:, 0:4]
        writes.append(pltpu.make_async_copy(dst, out, sem.at[k]))
        writes[-1].start()
    row = lse_ref[4:5, :]
    lane = lane[0:1, :]
    packed = row
    for b in range(1, 4):
        packed = jnp.where(lane == b, pltpu.roll(row, 128 - 31 * b, 1), packed)
    bonus_v[...] = packed[:, 0:4]
    writes.append(pltpu.make_async_copy(bonus_v, bonus_out, sem.at[2]))
    writes[-1].start()
    for c in writes:
        c.wait()


def solution(mesh):
    def local_step(hidden, norm_gain, w_head, draft_probs, draft_tokens, temperature):
        n_ids = w_head.shape[1]
        width = w_head.shape[0]
        pad_ids = -(-n_ids // 128) * 128
        tail = n_ids % TILE
        vmem, smem, hbm = pltpu.VMEM, pltpu.SMEM, pltpu.HBM
        dma = pltpu.SemaphoreType.DMA
        ex, norm, acc, lse = pl.pallas_call(
            verify_kernel,
            out_shape=[vmem((4, 4, n_ids), F32), vmem((4, 128), F32), vmem((4, 128), F32), vmem((8, 128), F32)],
            in_specs=[pl.BlockSpec(memory_space=s) for s in (hbm,) * 6],
            out_specs=[pl.BlockSpec(memory_space=vmem)] * 4,
            scratch_shapes=[
                vmem((5, 4, width), jnp.bfloat16),
                vmem((1, width), F32),
                smem((4,), F32),
                smem((4, 4), jnp.int32),
                vmem((SLOTS, TILE, width), jnp.bfloat16),
                vmem((tail, width), jnp.bfloat16),
                vmem((4, 4, n_ids), F32),
                vmem((4, 4, pad_ids), F32),
                vmem((5, 4, width), F32),
                vmem((5, 4, width), F32),
                vmem((32, width), F32),
                vmem((64, width), jnp.bfloat16),
                vmem((width, 128), jnp.bfloat16),
                vmem((5, 4, 128), F32),
                vmem((5, 4, 128), F32),
                vmem((64, 128), F32),
                vmem((64, 128), F32),
                vmem((64, 128), F32),
                vmem((64, 128), F32),
                vmem((64, 128), F32),
                vmem((SHARED, 4, 4, TILE), F32),
                vmem((2, 8, 128), F32),
                vmem((2, 8, 128), F32),
                vmem((8, 128), F32),
                vmem((3, 8, 128), F32),
                vmem((4, 128), F32),
                vmem((3, 4, 128), F32),
                vmem((2, 4, 128), F32),
                vmem((3, 2, 4, 128), F32),
                dma((4,)), dma((SLOTS, PARTS)), dma, dma, dma((2, 2)), dma((2,)), dma((SHARED,)), dma((SHARED,)), dma((2,)),
                dma((2, 3)), dma((2, 3)), dma((2, 3)),
            ],
            compiler_params=pltpu.CompilerParams(collective_id=0, has_side_effects=True),
            name="verify",
        )(
            hidden.transpose(1, 0, 2), norm_gain.reshape(1, width), temperature, draft_tokens,
            w_head.T, draft_probs,
        )
        acc, norm, residual, bonus = pl.pallas_call(
            finish_kernel,
            out_shape=[
                jax.ShapeDtypeStruct((4, 4), F32),
                jax.ShapeDtypeStruct((4, 4), F32),
                jax.ShapeDtypeStruct((4, 4, n_ids), F32),
                jax.ShapeDtypeStruct((1, 4), F32),
            ],
            in_specs=[pl.BlockSpec(memory_space=vmem)] * 4,
            out_specs=[pl.BlockSpec(memory_space=hbm)] * 4,
            scratch_shapes=[
                vmem((4, 4), F32), vmem((4, 4), F32), vmem((1, 4), F32), vmem((4, 4, n_ids), F32), dma((3,)), dma((4,)),
            ],
            compiler_params=pltpu.CompilerParams(vmem_limit_bytes=16 * 1024 * 1024),
            name="finish",
        )(ex, norm, acc, lse)
        return acc, norm, residual, bonus.reshape(4)

    return jax.shard_map(
        local_step,
        mesh=mesh,
        in_specs=(P("dp", None, None), P(), P(None, "tp"), P("dp", None, "tp"), P("dp", None), P("dp")),
        out_specs=(P("dp", None), P("dp", None), P("dp", None, "tp"), P("dp")),
        check_vma=False,
    )
```

```python
import jax
import jax.numpy as jnp
from jax import lax
from jax.experimental import pallas as pl
from jax.experimental.pallas import tpu as pltpu
from jax.sharding import PartitionSpec as P

MESH = pl.DeviceIdType.MESH
F32 = jnp.float32
LOWEST = float(jnp.finfo(jnp.float32).min)

TILE = 1024
SUB = 256
DEPTH = 256
SLOTS = 3
SHARED = 14
FIRST = 6
HELD = 2
RELAY = 4
PARTS = 2
PASS = 2048


def verify_kernel(
    h_hbm, g_hbm, t_hbm, dt_hbm, w_ref, q_ref,
    ex_ref, norm_ref, acc_ref, lse_ref,
    h_ref, g_ref, t_ref, dt_ref, wbuf, wtail, qv, s_scr, xf, xp, xrows, xb, xt, tv, tp_recv, ct, dl, m_scr, l_scr, k_scr,
    zsend, pstat_s, pstat_r, e1s, e1r, e2s, e2r, e3s, e3r,
    in_sem, w_sem, wt_sem, q_sem, x_sem, t_sem, zs_sem, zr_sem, ps_sem, e1_sem, e2_sem, e3_sem,
):
    dp, tp = lax.axis_index("dp"), lax.axis_index("tp")
    partner = (1 - dp, tp)
    peers = [(dp, lax.rem(tp + d, 4)) for d in (1, 2, 3)]
    n_ids, width = w_ref.shape
    n_full = n_ids // TILE
    tail = n_ids - n_full * TILE
    tail_at = n_full * TILE
    last = n_full - 2 * SHARED - FIRST
    steps = FIRST + SHARED + last

    def column(i):
        in_shared = (i + steps - FIRST) // steps
        past_shared = (i + steps - FIRST - SHARED) // steps
        return pl.multiple_of((i + in_shared * dp * SHARED + past_shared * (SHARED - dp * SHARED)) * TILE, TILE)

    part = TILE // PARTS

    def tile_copies(i, slot):
        at = column(i)
        return [
            pltpu.make_async_copy(
                w_ref.at[pl.ds(at + k * part, part), :], wbuf.at[slot, pl.ds(k * part, part), :], w_sem.at[slot, k]
            )
            for k in range(PARTS)
        ]

    tail_copy = pltpu.make_async_copy(w_ref.at[pl.ds(tail_at, tail), :], wtail, wt_sem)
    q_copy = pltpu.make_async_copy(q_ref, qv, q_sem)
    small = [
        pltpu.make_async_copy(src, dst, in_sem.at[k])
        for k, (src, dst) in enumerate(((h_hbm, h_ref), (g_hbm, g_ref), (t_hbm, t_ref), (dt_hbm, dt_ref)))
    ]
    for c in small:
        c.start()
    tail_copy.start()
    for c in tile_copies(0, 0):
        c.start()

    barrier = pltpu.get_barrier_semaphore()
    for other in [partner] + peers:
        pl.semaphore_signal(barrier, inc=1, device_id=other, device_id_type=MESH)

    for c in small:
        c.wait()
    for c in tile_copies(1, 1):
        c.start()
    h = h_ref[...].astype(F32)
    inv_rms = lax.rsqrt(jnp.mean(h * h, axis=-1, keepdims=True) + 1e-5)
    xf[...] = h * inv_rms * g_ref[...][None]
    for b in range(4):
        tv[0, b : b + 1, :] = jnp.full((1, 128), 1.0, F32) / jnp.full((1, 128), t_ref[b], F32)
        for j in range(4):
            tv[1 + j, b : b + 1, :] = jnp.full((1, 128), dt_ref[b, j].astype(F32), F32)

    def lay_rows(src, t_src, at):
        xrows[...] = jnp.zeros_like(xrows)
        lane = lax.broadcasted_iota(jnp.int32, (1, 128), 1) + tp * n_ids
        for b in range(4):
            for j in range(5):
                xrows[8 * b + j : 8 * b + j + 1, :] = src[j, b : b + 1, :]
            ct[at + 8 * b : at + 8 * b + 8, :] = jnp.broadcast_to(t_src[0, b : b + 1, :], (8, 128))
            dl[at + 8 * b : at + 8 * b + 8, :] = jnp.full((8, 128), -1.0, F32)
            for j in range(4):
                dl[at + 8 * b + j : at + 8 * b + j + 1, :] = t_src[1 + j, b : b + 1, :] - lane.astype(F32)
        rows = xrows[...].astype(jnp.bfloat16)
        xb[at : at + 32, :] = rows
        for k in range(0, width, 128):
            xt[k : k + 128, at : at + 32] = xrows[:, k : k + 128].T.astype(jnp.bfloat16)

    xt[:, 32:128] = jnp.zeros((width, 96), jnp.bfloat16)
    xb[32:64, :] = jnp.zeros((32, width), jnp.bfloat16)
    lay_rows(xf, tv, 0)
    for i in range(2, SLOTS):
        for c in tile_copies(i, i):
            c.start()
    m_scr[...] = jnp.full(m_scr.shape, LOWEST, F32)
    l_scr[...] = jnp.zeros_like(l_scr)
    k_scr[...] = jnp.zeros_like(k_scr)

    pl.semaphore_wait(barrier, 4)
    core = lax.rem(tp, 2)
    sibling = (dp, tp + 1 - 2 * core)

    def width_half(ref, c):
        return ref.at[:, :, pl.ds(pl.multiple_of(c * (width // 2), width // 2), width // 2)]

    def x_copy(src, c, to, k):
        return pltpu.make_async_remote_copy(
            src_ref=width_half(src, c), dst_ref=width_half(xp, c), send_sem=x_sem.at[0, k], recv_sem=x_sem.at[1, k],
            device_id=to, device_id_type=MESH,
        )

    x_direct = x_copy(xf, core, partner, 0)
    x_relay = x_copy(xp, core, sibling, 1)
    t_copy = pltpu.make_async_remote_copy(
        src_ref=tv, dst_ref=tp_recv, send_sem=t_sem.at[0], recv_sem=t_sem.at[1], device_id=partner, device_id_type=MESH
    )
    x_direct.start()
    t_copy.start()

    def by_rows(w, depth):
        return lax.dot_general(xb[:, depth], w, (((1,), (1,)), ((), ())), preferred_element_type=F32)

    def by_ids(w, depth):
        return lax.dot_general(w, xt[depth, :], (((1,), (0,)), ((), ())), preferred_element_type=F32)

    def products(slot, lo, size):
        block = min(SUB, size // 2)
        starts = range(lo, lo + size, block)
        fixed = len(starts) // 2
        sums = [None] * len(starts)
        for k in range(0, width, DEPTH):
            depth = slice(k, k + DEPTH)
            for n, start in enumerate(starts):
                w = wbuf[slot, start : start + block, depth]
                z = by_rows(w, depth) if n < fixed else by_ids(w, depth)
                sums[n] = z if k == 0 else sums[n] + z
        pieces = []
        for n, z in enumerate(sums):
            for at in range(0, block, 128):
                pieces.append(z[:, at : at + 128] if n < fixed else z[at : at + 128, :].T[0:64])
        return pieces

    def fold(rows, parts):
        m_old = m_scr[0:rows, :]
        m_new = m_old
        for p in parts:
            m_new = jnp.maximum(m_new, p)
        total = l_scr[0:rows, :] * jnp.exp(m_old - m_new)
        for p in parts:
            total = total + jnp.exp(p - m_new)
        m_scr[0:rows, :] = m_new
        l_scr[0:rows, :] = total

    tail_copy.wait()
    s = by_rows(wtail[...], slice(0, width))[0:32] * ct[0:32, 0:tail]
    for b in range(4):
        s_scr[b, :, tail_at : tail_at + tail] = s[8 * b : 8 * b + 4, :]
    k_scr[0:32, 0:tail] = jnp.where(dl[0:32, 0:tail] == float(tail_at), s, 0.0)
    m_tail = jnp.max(s, axis=1, keepdims=True)
    l_tail = jnp.sum(jnp.exp(s - m_tail), axis=1, keepdims=True)
    lane0 = lax.broadcasted_iota(jnp.int32, (32, 128), 1) == 0
    m_scr[0:32, :] = jnp.where(lane0, m_tail, LOWEST)
    l_scr[0:32, :] = jnp.where(lane0, l_tail, 0.0)

    def z_copy(k):
        at = column(FIRST + k)
        return pltpu.make_async_remote_copy(
            src_ref=zsend.at[k], dst_ref=s_scr.at[:, :, pl.ds(at, TILE)], send_sem=zs_sem.at[k], recv_sem=zr_sem.at[k],
            device_id=partner, device_id_type=MESH,
        )

    def consume(slot, at, lo, size, rows, k):
        kept = k_scr[0:rows, :]
        parts = []
        for n, z in enumerate(products(slot, lo, size)):
            s = z[0:rows] * ct[0:rows, :]
            parts.append(s)
            off = lo + n * 128
            kept = jnp.where(dl[0:rows, :] == (at + off).astype(F32), s, kept)
            for b in range(4):
                s_scr[b, :, pl.ds(at + off, 128)] = s[8 * b : 8 * b + 4, :]
                if rows == 64:
                    zsend[k, b, :, off : off + 128] = s[32 + 8 * b : 32 + 8 * b + 4, :]
            if n % 2:
                fold(rows, parts)
                parts = []
        k_scr[0:rows, :] = kept

    def step(i, rows):
        slot = i % SLOTS
        for c in tile_copies(i, slot):
            c.wait()
        k = i - FIRST
        consume(slot, column(i), 0, TILE, rows, k)

        @pl.when(i + SLOTS < steps)
        def _():
            for c in tile_copies(i + SLOTS, slot):
                c.start()

        if rows == 64:

            @pl.when(k < SHARED - HELD)
            def _():
                z_copy(k).start()

    group = lax.broadcasted_iota(jnp.int32, (8, 128), 1) // 32

    def pack(cols):
        size = cols[0].shape[0]
        packed = jnp.broadcast_to(cols[0], (size, 128))
        for b in range(1, 4):
            packed = jnp.where(group[:size] == b, cols[b], packed)
        return packed

    def unpack(packed, b):
        size = packed.shape[0]
        lane = lax.broadcasted_iota(jnp.int32, (size, 128), 1)
        return jnp.sum(jnp.where(lane == 32 * b, packed, 0.0), axis=1, keepdims=True)

    def packed_lse(at):
        m = m_scr[at : at + 32, :]
        top = jnp.max(m, axis=1, keepdims=True)
        lse = top + jnp.log(jnp.sum(l_scr[at : at + 32, :] * jnp.exp(m - top), axis=1, keepdims=True))
        return pack([lse[8 * b : 8 * b + 8, :] for b in range(4)])

    def packed_token(at):
        kept = jnp.sum(k_scr[at : at + 32, :], axis=1, keepdims=True)
        return pack([kept[8 * b : 8 * b + 8, :] for b in range(4)])

    lax.fori_loop(0, RELAY, lambda i, _: step(i, 32), None)
    x_direct.wait()
    x_relay.start()
    lax.fori_loop(RELAY, FIRST, lambda i, _: step(i, 32), None)
    x_copy(xp, 1 - core, sibling, 1).wait_recv()
    x_relay.wait_send()
    t_copy.wait()
    lay_rows(xp, tp_recv, 32)
    lax.fori_loop(FIRST, FIRST + SHARED, lambda i, _: step(i, 64), None)
    q_copy.start()
    pstat_s[0] = packed_lse(32)
    pstat_s[1] = packed_token(32)
    stat_copy = pltpu.make_async_remote_copy(
        src_ref=pstat_s, dst_ref=pstat_r, send_sem=ps_sem.at[0], recv_sem=ps_sem.at[1],
        device_id=partner, device_id_type=MESH,
    )
    stat_copy.start()
    for k in range(SHARED - HELD, SHARED):
        z_copy(k).start()
    lax.fori_loop(FIRST + SHARED, steps - 1, lambda i, _: step(i, 32), None)
    end, slot = steps - 1, (steps - 1) % SLOTS
    copies = tile_copies(end, slot)
    for lo, size in ((0, part), (part, part)):
        for c in copies[lo // part : (lo + size) // part]:
            c.wait()
        consume(slot, column(end), lo, size, 32, 0)

    def exchange(src, dst, sem):
        return [
            pltpu.make_async_remote_copy(
                src_ref=src, dst_ref=dst.at[d], send_sem=sem.at[0, d], recv_sem=sem.at[1, d],
                device_id=peers[d], device_id_type=MESH,
            )
            for d in range(3)
        ]

    mine = packed_lse(0)
    stat_copy.wait()
    theirs = pstat_r[0]
    top = jnp.maximum(mine, theirs)
    near = top + jnp.log(jnp.exp(mine - top) + jnp.exp(theirs - top))
    e1s[...] = near
    e1 = exchange(e1s, e1r, e1_sem)
    for c in e1:
        c.start()

    own = [dl[8 * b : 8 * b + 4, :] for b in range(4)]

    row_m = [jnp.broadcast_to(unpack(near[0:4, :], b), (4, 128)) for b in range(4)]

    def prepare(at, size):
        places = [(b, at + off, min(size, 128)) for b in range(4) for off in range(0, size, 128)]
        values = [s_scr[b, :, pl.ds(a, n)] for b, a, n in places]
        values = [jnp.exp(v - row_m[b][:, :n]) for v, (b, _, n) in zip(values, places)]
        for v, (b, a, n) in zip(values, places):
            s_scr[b, :, pl.ds(a, n)] = v

    def pick(at, size, found):
        out = []
        for b in range(4):
            f = found[b]
            for off in range(0, size, 128):
                n = min(size, 128)
                f = jnp.where(own[b][:, :n] == jnp.asarray(at + off).astype(F32), qv[b, :, pl.ds(at + off, n)], f)
            out.append(f)
        return tuple(out)

    zero = jnp.zeros((4, 128), F32)
    lax.fori_loop(0, steps, lambda i, _: prepare(column(i), TILE), None)
    prepare(tail_at, tail)
    q_copy.wait()
    whole = tail_at // PASS * PASS
    found = lax.fori_loop(0, whole // PASS, lambda i, f: pick(pl.multiple_of(i * PASS, 128), PASS, f), (zero,) * 4)
    found = pick(whole, tail_at - whole, found)
    found_tail = pick(tail_at, tail, (jnp.zeros((4, tail), F32),) * 4)
    token_q = []
    for b in range(4):
        f = found_tail[b]
        token_q.append(jnp.sum(found[b], axis=1, keepdims=True) + jnp.sum(f, axis=1, keepdims=True))
    e3s[0] = (packed_token(0) + pstat_r[1])[0:4, :]
    e3s[1] = pack(token_q)
    e3 = exchange(e3s, e3r, e3_sem)
    for c in e3:
        c.start()

    def take_z(k, _):
        z_copy(k).wait_send()
        at = pl.multiple_of((FIRST + (1 - dp) * SHARED + k) * TILE, TILE)
        pltpu.make_async_remote_copy(
            src_ref=zsend.at[k], dst_ref=s_scr.at[:, :, pl.ds(at, TILE)], send_sem=zs_sem.at[k], recv_sem=zr_sem.at[k],
            device_id=partner, device_id_type=MESH,
        ).wait_recv()
        prepare(at, TILE)

    lax.fori_loop(0, SHARED, take_z, None)

    for c in e1:
        c.wait()
    lses = [near] + [e1r[d] for d in range(3)]
    top = jnp.maximum(jnp.maximum(lses[0], lses[1]), jnp.maximum(lses[2], lses[3]))
    sums = jnp.exp(lses[0] - top) + jnp.exp(lses[1] - top) + jnp.exp(lses[2] - top) + jnp.exp(lses[3] - top)
    lse = top + jnp.log(sums)
    lse_ref[...] = lse
    scale = [jnp.exp(row_m[b] - jnp.broadcast_to(unpack(lse[0:4, :], b), (4, 128))) for b in range(4)]

    def excess(b, at, size):
        e = jnp.maximum(s_scr[b, :, pl.ds(at, size)] * scale[b][:, :size] - qv[b, :, pl.ds(at, size)], 0.0)
        ex_ref[b, :, pl.ds(at, size)] = e
        return e

    def last_pass(at, size, sums):
        out = []
        for b in range(4):
            acc = sums[b]
            for off in range(0, size, 128):
                acc = acc + excess(b, at + off, 128)
            out.append(acc)
        return tuple(out)

    sums = lax.fori_loop(0, whole // PASS, lambda i, t: last_pass(pl.multiple_of(i * PASS, 128), PASS, t), (zero,) * 4)
    sums = last_pass(whole, tail_at - whole, sums)
    rows = []
    for b in range(4):
        e = excess(b, tail_at, tail)
        rows.append(jnp.sum(sums[b], axis=1, keepdims=True) + jnp.sum(e, axis=1, keepdims=True))
    e2s[...] = pack(rows)
    e2 = exchange(e2s, e2r, e2_sem)
    for c in e2:
        c.start()

    for c in e3:
        c.wait()
    at_token = (e3s[...] + e3r[0]) + (e3r[1] + e3r[2])
    acc_ref[...] = jnp.minimum(jnp.exp(at_token[0] - lse[0:4, :]) / at_token[1], 1.0)

    for c in e2:
        c.wait()
    norm_ref[...] = (e2s[...] + e2r[0]) + (e2r[1] + e2r[2])


def finish_kernel(
    ex_ref, norm_ref, acc_ref, lse_ref, acc_out, norm_out, res_out, bonus_out, acc_v, norm_v, bonus_v, stage, sem, r_sem
):
    n_ids = ex_ref.shape[2]
    lane = lax.broadcasted_iota(jnp.int32, (4, 128), 1)
    norm = norm_ref[...]
    writes = []
    for b in range(4):
        total = jnp.sum(jnp.where(lane == 32 * b, norm, 0.0), axis=1, keepdims=True)
        scale = jnp.broadcast_to(1.0 / jnp.broadcast_to(total, (4, 128)), (4, 128))

        for at in range(0, n_ids, 128):
            size = min(128, n_ids - at)
            stage[b, :, at : at + size] = ex_ref[b, :, at : at + size] * scale[:, :size]
        writes.append(pltpu.make_async_copy(stage.at[b], res_out.at[b], r_sem.at[b]))
        writes[-1].start()

    sub = lax.broadcasted_iota(jnp.int32, (4, 128), 0)
    for src, dst, out, k in ((acc_ref[...], acc_v, acc_out, 0), (norm, norm_v, norm_out, 1)):
        row = jnp.sum(jnp.where(lane % 32 == sub, src, 0.0), axis=0, keepdims=True)
        for b in range(4):
            dst[b : b + 1, :] = (row if b == 0 else pltpu.roll(row, 128 - 32 * b, 1))[:, 0:4]
        writes.append(pltpu.make_async_copy(dst, out, sem.at[k]))
        writes[-1].start()
    row = lse_ref[4:5, :]
    lane = lane[0:1, :]
    packed = row
    for b in range(1, 4):
        packed = jnp.where(lane == b, pltpu.roll(row, 128 - 31 * b, 1), packed)
    bonus_v[...] = packed[:, 0:4]
    writes.append(pltpu.make_async_copy(bonus_v, bonus_out, sem.at[2]))
    writes[-1].start()
    for c in writes:
        c.wait()


def solution(mesh):
    def local_step(hidden, norm_gain, w_head, draft_probs, draft_tokens, temperature):
        n_ids = w_head.shape[1]
        width = w_head.shape[0]
        pad_ids = -(-n_ids // 128) * 128
        tail = n_ids % TILE
        vmem, smem, hbm = pltpu.VMEM, pltpu.SMEM, pltpu.HBM
        dma = pltpu.SemaphoreType.DMA
        ex, norm, acc, lse = pl.pallas_call(
            verify_kernel,
            out_shape=[vmem((4, 4, n_ids), F32), vmem((4, 128), F32), vmem((4, 128), F32), vmem((8, 128), F32)],
            in_specs=[pl.BlockSpec(memory_space=s) for s in (hbm,) * 6],
            out_specs=[pl.BlockSpec(memory_space=vmem)] * 4,
            scratch_shapes=[
                vmem((5, 4, width), jnp.bfloat16),
                vmem((1, width), F32),
                smem((4,), F32),
                smem((4, 4), jnp.int32),
                vmem((SLOTS, TILE, width), jnp.bfloat16),
                vmem((tail, width), jnp.bfloat16),
                vmem((4, 4, n_ids), F32),
                vmem((4, 4, pad_ids), F32),
                vmem((5, 4, width), F32),
                vmem((5, 4, width), F32),
                vmem((32, width), F32),
                vmem((64, width), jnp.bfloat16),
                vmem((width, 128), jnp.bfloat16),
                vmem((5, 4, 128), F32),
                vmem((5, 4, 128), F32),
                vmem((64, 128), F32),
                vmem((64, 128), F32),
                vmem((64, 128), F32),
                vmem((64, 128), F32),
                vmem((64, 128), F32),
                vmem((SHARED, 4, 4, TILE), F32),
                vmem((2, 8, 128), F32),
                vmem((2, 8, 128), F32),
                vmem((8, 128), F32),
                vmem((3, 8, 128), F32),
                vmem((4, 128), F32),
                vmem((3, 4, 128), F32),
                vmem((2, 4, 128), F32),
                vmem((3, 2, 4, 128), F32),
                dma((4,)), dma((SLOTS, PARTS)), dma, dma, dma((2, 2)), dma((2,)), dma((SHARED,)), dma((SHARED,)), dma((2,)),
                dma((2, 3)), dma((2, 3)), dma((2, 3)),
            ],
            compiler_params=pltpu.CompilerParams(collective_id=0, has_side_effects=True),
            name="verify",
        )(
            hidden.transpose(1, 0, 2), norm_gain.reshape(1, width), temperature, draft_tokens,
            w_head.T, draft_probs,
        )
        acc, norm, residual, bonus = pl.pallas_call(
            finish_kernel,
            out_shape=[
                jax.ShapeDtypeStruct((4, 4), F32),
                jax.ShapeDtypeStruct((4, 4), F32),
                jax.ShapeDtypeStruct((4, 4, n_ids), F32),
                jax.ShapeDtypeStruct((1, 4), F32),
            ],
            in_specs=[pl.BlockSpec(memory_space=vmem)] * 4,
            out_specs=[pl.BlockSpec(memory_space=hbm)] * 4,
            scratch_shapes=[
                vmem((4, 4), F32), vmem((4, 4), F32), vmem((1, 4), F32), vmem((4, 4, n_ids), F32), dma((3,)), dma((4,)),
            ],
            compiler_params=pltpu.CompilerParams(vmem_limit_bytes=16 * 1024 * 1024),
            name="finish",
        )(ex, norm, acc, lse)
        return acc, norm, residual, bonus.reshape(4)

    return jax.shard_map(
        local_step,
        mesh=mesh,
        in_specs=(P("dp", None, None), P(), P(None, "tp"), P("dp", None, "tp"), P("dp", None), P("dp")),
        out_specs=(P("dp", None), P("dp", None), P("dp", None, "tp"), P("dp")),
        check_vma=False,
    )
```

```python
import jax
import jax.numpy as jnp
from jax import lax
from jax.experimental import pallas as pl
from jax.experimental.pallas import tpu as pltpu
from jax.sharding import PartitionSpec as P

MESH = pl.DeviceIdType.MESH
F32 = jnp.float32
LOWEST = float(jnp.finfo(jnp.float32).min)

TILE = 1024
SUB = 256
DEPTH = 256
SLOTS = 3
SHARED = 14
FIRST = 6
HELD = 2
RELAY = 4
PARTS = 1
PASS = 2048


def verify_kernel(
    h_hbm, g_hbm, t_hbm, dt_hbm, w_ref, q_ref,
    ex_ref, norm_ref, acc_ref, lse_ref,
    h_ref, g_ref, t_ref, dt_ref, wbuf, wtail, qv, s_scr, xf, xp, xrows, xb, xt, tv, tp_recv, ct, dl, m_scr, l_scr, k_scr,
    zsend, pstat_s, pstat_r, e1s, e1r, e2s, e2r, e3s, e3r,
    in_sem, w_sem, wt_sem, q_sem, x_sem, t_sem, zs_sem, zr_sem, ps_sem, e1_sem, e2_sem, e3_sem,
):
    dp, tp = lax.axis_index("dp"), lax.axis_index("tp")
    partner = (1 - dp, tp)
    peers = [(dp, lax.rem(tp + d, 4)) for d in (1, 2, 3)]
    n_ids, width = w_ref.shape
    n_full = n_ids // TILE
    tail = n_ids - n_full * TILE
    tail_at = n_full * TILE
    last = n_full - 2 * SHARED - FIRST
    steps = FIRST + SHARED + last

    def column(i):
        in_shared = (i + steps - FIRST) // steps
        past_shared = (i + steps - FIRST - SHARED) // steps
        return pl.multiple_of((i + in_shared * dp * SHARED + past_shared * (SHARED - dp * SHARED)) * TILE, TILE)

    part = TILE // PARTS

    def tile_copies(i, slot):
        at = column(i)
        return [
            pltpu.make_async_copy(
                w_ref.at[pl.ds(at + k * part, part), :], wbuf.at[slot, pl.ds(k * part, part), :], w_sem.at[slot, k]
            )
            for k in range(PARTS)
        ]

    tail_copy = pltpu.make_async_copy(w_ref.at[pl.ds(tail_at, tail), :], wtail, wt_sem)
    q_copy = pltpu.make_async_copy(q_ref, qv, q_sem)
    small = [
        pltpu.make_async_copy(src, dst, in_sem.at[k])
        for k, (src, dst) in enumerate(((h_hbm, h_ref), (g_hbm, g_ref), (t_hbm, t_ref), (dt_hbm, dt_ref)))
    ]
    for c in small:
        c.start()
    tail_copy.start()
    for c in tile_copies(0, 0):
        c.start()

    barrier = pltpu.get_barrier_semaphore()
    for other in [partner] + peers:
        pl.semaphore_signal(barrier, inc=1, device_id=other, device_id_type=MESH)

    for c in small:
        c.wait()
    for c in tile_copies(1, 1):
        c.start()
    h = h_ref[...].astype(F32)
    inv_rms = lax.rsqrt(jnp.mean(h * h, axis=-1, keepdims=True) + 1e-5)
    xf[...] = h * inv_rms * g_ref[...][None]
    for b in range(4):
        tv[0, b : b + 1, :] = jnp.full((1, 128), 1.0, F32) / jnp.full((1, 128), t_ref[b], F32)
        for j in range(4):
            tv[1 + j, b : b + 1, :] = jnp.full((1, 128), dt_ref[b, j].astype(F32), F32)

    def lay_rows(src, t_src, at):
        xrows[...] = jnp.zeros_like(xrows)
        lane = lax.broadcasted_iota(jnp.int32, (1, 128), 1) + tp * n_ids
        for b in range(4):
            for j in range(5):
                xrows[8 * b + j : 8 * b + j + 1, :] = src[j, b : b + 1, :]
            ct[at + 8 * b : at + 8 * b + 8, :] = jnp.broadcast_to(t_src[0, b : b + 1, :], (8, 128))
            dl[at + 8 * b : at + 8 * b + 8, :] = jnp.full((8, 128), -1.0, F32)
            for j in range(4):
                dl[at + 8 * b + j : at + 8 * b + j + 1, :] = t_src[1 + j, b : b + 1, :] - lane.astype(F32)
        rows = xrows[...].astype(jnp.bfloat16)
        xb[at : at + 32, :] = rows
        for k in range(0, width, 128):
            xt[k : k + 128, at : at + 32] = xrows[:, k : k + 128].T.astype(jnp.bfloat16)

    xt[:, 32:128] = jnp.zeros((width, 96), jnp.bfloat16)
    xb[32:64, :] = jnp.zeros((32, width), jnp.bfloat16)
    lay_rows(xf, tv, 0)
    for i in range(2, SLOTS):
        for c in tile_copies(i, i):
            c.start()
    m_scr[...] = jnp.full(m_scr.shape, LOWEST, F32)
    l_scr[...] = jnp.zeros_like(l_scr)
    k_scr[...] = jnp.zeros_like(k_scr)

    pl.semaphore_wait(barrier, 4)
    core = lax.rem(tp, 2)
    sibling = (dp, tp + 1 - 2 * core)

    def width_half(ref, c):
        return ref.at[:, :, pl.ds(pl.multiple_of(c * (width // 2), width // 2), width // 2)]

    def x_copy(src, c, to, k):
        return pltpu.make_async_remote_copy(
            src_ref=width_half(src, c), dst_ref=width_half(xp, c), send_sem=x_sem.at[0, k], recv_sem=x_sem.at[1, k],
            device_id=to, device_id_type=MESH,
        )

    x_direct = x_copy(xf, core, partner, 0)
    x_relay = x_copy(xp, core, sibling, 1)
    t_copy = pltpu.make_async_remote_copy(
        src_ref=tv, dst_ref=tp_recv, send_sem=t_sem.at[0], recv_sem=t_sem.at[1], device_id=partner, device_id_type=MESH
    )
    x_direct.start()
    t_copy.start()

    def by_rows(w, depth):
        return lax.dot_general(xb[:, depth], w, (((1,), (1,)), ((), ())), preferred_element_type=F32)

    def by_ids(w, depth):
        return lax.dot_general(w, xt[depth, :], (((1,), (0,)), ((), ())), preferred_element_type=F32)

    def products(slot, lo, size):
        block = min(SUB, size // 2)
        starts = range(lo, lo + size, block)
        fixed = len(starts) // 2
        sums = [None] * len(starts)
        for k in range(0, width, DEPTH):
            depth = slice(k, k + DEPTH)
            for n, start in enumerate(starts):
                w = wbuf[slot, start : start + block, depth]
                z = by_rows(w, depth) if n < fixed else by_ids(w, depth)
                sums[n] = z if k == 0 else sums[n] + z
        pieces = []
        for n, z in enumerate(sums):
            for at in range(0, block, 128):
                pieces.append(z[:, at : at + 128] if n < fixed else z[at : at + 128, :].T[0:64])
        return pieces

    def fold(rows, parts):
        m_old = m_scr[0:rows, :]
        m_new = m_old
        for p in parts:
            m_new = jnp.maximum(m_new, p)
        total = l_scr[0:rows, :] * jnp.exp(m_old - m_new)
        for p in parts:
            total = total + jnp.exp(p - m_new)
        m_scr[0:rows, :] = m_new
        l_scr[0:rows, :] = total

    tail_copy.wait()
    s = by_rows(wtail[...], slice(0, width))[0:32] * ct[0:32, 0:tail]
    for b in range(4):
        s_scr[b, :, tail_at : tail_at + tail] = s[8 * b : 8 * b + 4, :]
    k_scr[0:32, 0:tail] = jnp.where(dl[0:32, 0:tail] == float(tail_at), s, 0.0)
    m_tail = jnp.max(s, axis=1, keepdims=True)
    l_tail = jnp.sum(jnp.exp(s - m_tail), axis=1, keepdims=True)
    lane0 = lax.broadcasted_iota(jnp.int32, (32, 128), 1) == 0
    m_scr[0:32, :] = jnp.where(lane0, m_tail, LOWEST)
    l_scr[0:32, :] = jnp.where(lane0, l_tail, 0.0)

    def z_copy(k):
        at = column(FIRST + k)
        return pltpu.make_async_remote_copy(
            src_ref=zsend.at[k], dst_ref=s_scr.at[:, :, pl.ds(at, TILE)], send_sem=zs_sem.at[k], recv_sem=zr_sem.at[k],
            device_id=partner, device_id_type=MESH,
        )

    def consume(slot, at, lo, size, rows, k):
        kept = k_scr[0:rows, :]
        parts = []
        for n, z in enumerate(products(slot, lo, size)):
            s = z[0:rows] * ct[0:rows, :]
            parts.append(s)
            off = lo + n * 128
            kept = jnp.where(dl[0:rows, :] == (at + off).astype(F32), s, kept)
            for b in range(4):
                s_scr[b, :, pl.ds(at + off, 128)] = s[8 * b : 8 * b + 4, :]
                if rows == 64:
                    zsend[k, b, :, off : off + 128] = s[32 + 8 * b : 32 + 8 * b + 4, :]
            if n % 2:
                fold(rows, parts)
                parts = []
        k_scr[0:rows, :] = kept

    def step(i, rows):
        slot = i % SLOTS
        for c in tile_copies(i, slot):
            c.wait()
        k = i - FIRST
        consume(slot, column(i), 0, TILE, rows, k)

        @pl.when(i + SLOTS < steps)
        def _():
            for c in tile_copies(i + SLOTS, slot):
                c.start()

        if rows == 64:

            @pl.when(k < SHARED - HELD)
            def _():
                z_copy(k).start()

    group = lax.broadcasted_iota(jnp.int32, (8, 128), 1) // 32

    def pack(cols):
        size = cols[0].shape[0]
        packed = jnp.broadcast_to(cols[0], (size, 128))
        for b in range(1, 4):
            packed = jnp.where(group[:size] == b, cols[b], packed)
        return packed

    def unpack(packed, b):
        size = packed.shape[0]
        lane = lax.broadcasted_iota(jnp.int32, (size, 128), 1)
        return jnp.sum(jnp.where(lane == 32 * b, packed, 0.0), axis=1, keepdims=True)

    def packed_lse(at):
        m = m_scr[at : at + 32, :]
        top = jnp.max(m, axis=1, keepdims=True)
        lse = top + jnp.log(jnp.sum(l_scr[at : at + 32, :] * jnp.exp(m - top), axis=1, keepdims=True))
        return pack([lse[8 * b : 8 * b + 8, :] for b in range(4)])

    def packed_token(at):
        kept = jnp.sum(k_scr[at : at + 32, :], axis=1, keepdims=True)
        return pack([kept[8 * b : 8 * b + 8, :] for b in range(4)])

    lax.fori_loop(0, RELAY, lambda i, _: step(i, 32), None)
    x_direct.wait()
    x_relay.start()
    lax.fori_loop(RELAY, FIRST, lambda i, _: step(i, 32), None)
    x_copy(xp, 1 - core, sibling, 1).wait_recv()
    x_relay.wait_send()
    t_copy.wait()
    lay_rows(xp, tp_recv, 32)
    lax.fori_loop(FIRST, FIRST + SHARED, lambda i, _: step(i, 64), None)
    q_copy.start()
    pstat_s[0] = packed_lse(32)
    pstat_s[1] = packed_token(32)
    stat_copy = pltpu.make_async_remote_copy(
        src_ref=pstat_s, dst_ref=pstat_r, send_sem=ps_sem.at[0], recv_sem=ps_sem.at[1],
        device_id=partner, device_id_type=MESH,
    )
    stat_copy.start()
    for k in range(SHARED - HELD, SHARED):
        z_copy(k).start()
    lax.fori_loop(FIRST + SHARED, steps - 1, lambda i, _: step(i, 32), None)
    end, slot = steps - 1, (steps - 1) % SLOTS
    copies = tile_copies(end, slot)
    for lo, size in [(k * part, part) for k in range(PARTS)]:
        for c in copies[lo // part : (lo + size) // part]:
            c.wait()
        consume(slot, column(end), lo, size, 32, 0)

    def exchange(src, dst, sem):
        return [
            pltpu.make_async_remote_copy(
                src_ref=src, dst_ref=dst.at[d], send_sem=sem.at[0, d], recv_sem=sem.at[1, d],
                device_id=peers[d], device_id_type=MESH,
            )
            for d in range(3)
        ]

    mine = packed_lse(0)
    stat_copy.wait()
    theirs = pstat_r[0]
    top = jnp.maximum(mine, theirs)
    near = top + jnp.log(jnp.exp(mine - top) + jnp.exp(theirs - top))
    e1s[...] = near
    e1 = exchange(e1s, e1r, e1_sem)
    for c in e1:
        c.start()

    own = [dl[8 * b : 8 * b + 4, :] for b in range(4)]

    row_m = [jnp.broadcast_to(unpack(near[0:4, :], b), (4, 128)) for b in range(4)]

    def prepare(at, size):
        places = [(b, at + off, min(size, 128)) for b in range(4) for off in range(0, size, 128)]
        values = [s_scr[b, :, pl.ds(a, n)] for b, a, n in places]
        values = [jnp.exp(v - row_m[b][:, :n]) for v, (b, _, n) in zip(values, places)]
        for v, (b, a, n) in zip(values, places):
            s_scr[b, :, pl.ds(a, n)] = v

    def pick(at, size, found):
        out = []
        for b in range(4):
            f = found[b]
            for off in range(0, size, 128):
                n = min(size, 128)
                f = jnp.where(own[b][:, :n] == jnp.asarray(at + off).astype(F32), qv[b, :, pl.ds(at + off, n)], f)
            out.append(f)
        return tuple(out)

    zero = jnp.zeros((4, 128), F32)
    lax.fori_loop(0, steps, lambda i, _: prepare(column(i), TILE), None)
    prepare(tail_at, tail)
    q_copy.wait()
    whole = tail_at // PASS * PASS
    found = lax.fori_loop(0, whole // PASS, lambda i, f: pick(pl.multiple_of(i * PASS, 128), PASS, f), (zero,) * 4)
    found = pick(whole, tail_at - whole, found)
    found_tail = pick(tail_at, tail, (jnp.zeros((4, tail), F32),) * 4)
    token_q = []
    for b in range(4):
        f = found_tail[b]
        token_q.append(jnp.sum(found[b], axis=1, keepdims=True) + jnp.sum(f, axis=1, keepdims=True))
    e3s[0] = (packed_token(0) + pstat_r[1])[0:4, :]
    e3s[1] = pack(token_q)
    e3 = exchange(e3s, e3r, e3_sem)
    for c in e3:
        c.start()

    def take_z(k, _):
        z_copy(k).wait_send()
        at = pl.multiple_of((FIRST + (1 - dp) * SHARED + k) * TILE, TILE)
        pltpu.make_async_remote_copy(
            src_ref=zsend.at[k], dst_ref=s_scr.at[:, :, pl.ds(at, TILE)], send_sem=zs_sem.at[k], recv_sem=zr_sem.at[k],
            device_id=partner, device_id_type=MESH,
        ).wait_recv()
        prepare(at, TILE)

    lax.fori_loop(0, SHARED, take_z, None)

    for c in e1:
        c.wait()
    lses = [near] + [e1r[d] for d in range(3)]
    top = jnp.maximum(jnp.maximum(lses[0], lses[1]), jnp.maximum(lses[2], lses[3]))
    sums = jnp.exp(lses[0] - top) + jnp.exp(lses[1] - top) + jnp.exp(lses[2] - top) + jnp.exp(lses[3] - top)
    lse = top + jnp.log(sums)
    lse_ref[...] = lse
    scale = [jnp.exp(row_m[b] - jnp.broadcast_to(unpack(lse[0:4, :], b), (4, 128))) for b in range(4)]

    def excess(b, at, size):
        e = jnp.maximum(s_scr[b, :, pl.ds(at, size)] * scale[b][:, :size] - qv[b, :, pl.ds(at, size)], 0.0)
        ex_ref[b, :, pl.ds(at, size)] = e
        return e

    def last_pass(at, size, sums):
        out = []
        for b in range(4):
            acc = sums[b]
            for off in range(0, size, 128):
                acc = acc + excess(b, at + off, 128)
            out.append(acc)
        return tuple(out)

    sums = lax.fori_loop(0, whole // PASS, lambda i, t: last_pass(pl.multiple_of(i * PASS, 128), PASS, t), (zero,) * 4)
    sums = last_pass(whole, tail_at - whole, sums)
    rows = []
    for b in range(4):
        e = excess(b, tail_at, tail)
        rows.append(jnp.sum(sums[b], axis=1, keepdims=True) + jnp.sum(e, axis=1, keepdims=True))
    e2s[...] = pack(rows)
    e2 = exchange(e2s, e2r, e2_sem)
    for c in e2:
        c.start()

    for c in e3:
        c.wait()
    at_token = (e3s[...] + e3r[0]) + (e3r[1] + e3r[2])
    acc_ref[...] = jnp.minimum(jnp.exp(at_token[0] - lse[0:4, :]) / at_token[1], 1.0)

    for c in e2:
        c.wait()
    norm_ref[...] = (e2s[...] + e2r[0]) + (e2r[1] + e2r[2])


def finish_kernel(
    ex_ref, norm_ref, acc_ref, lse_ref, acc_out, norm_out, res_out, bonus_out, acc_v, norm_v, bonus_v, stage, sem, r_sem
):
    n_ids = ex_ref.shape[2]
    lane = lax.broadcasted_iota(jnp.int32, (4, 128), 1)
    norm = norm_ref[...]
    writes = []
    for b in range(4):
        total = jnp.sum(jnp.where(lane == 32 * b, norm, 0.0), axis=1, keepdims=True)
        scale = jnp.broadcast_to(1.0 / jnp.broadcast_to(total, (4, 128)), (4, 128))

        for at in range(0, n_ids, 128):
            size = min(128, n_ids - at)
            stage[b, :, at : at + size] = ex_ref[b, :, at : at + size] * scale[:, :size]
        writes.append(pltpu.make_async_copy(stage.at[b], res_out.at[b], r_sem.at[b]))
        writes[-1].start()

    sub = lax.broadcasted_iota(jnp.int32, (4, 128), 0)
    for src, dst, out, k in ((acc_ref[...], acc_v, acc_out, 0), (norm, norm_v, norm_out, 1)):
        row = jnp.sum(jnp.where(lane % 32 == sub, src, 0.0), axis=0, keepdims=True)
        for b in range(4):
            dst[b : b + 1, :] = (row if b == 0 else pltpu.roll(row, 128 - 32 * b, 1))[:, 0:4]
        writes.append(pltpu.make_async_copy(dst, out, sem.at[k]))
        writes[-1].start()
    row = lse_ref[4:5, :]
    lane = lane[0:1, :]
    packed = row
    for b in range(1, 4):
        packed = jnp.where(lane == b, pltpu.roll(row, 128 - 31 * b, 1), packed)
    bonus_v[...] = packed[:, 0:4]
    writes.append(pltpu.make_async_copy(bonus_v, bonus_out, sem.at[2]))
    writes[-1].start()
    for c in writes:
        c.wait()


def solution(mesh):
    def local_step(hidden, norm_gain, w_head, draft_probs, draft_tokens, temperature):
        n_ids = w_head.shape[1]
        width = w_head.shape[0]
        pad_ids = -(-n_ids // 128) * 128
        tail = n_ids % TILE
        vmem, smem, hbm = pltpu.VMEM, pltpu.SMEM, pltpu.HBM
        dma = pltpu.SemaphoreType.DMA
        ex, norm, acc, lse = pl.pallas_call(
            verify_kernel,
            out_shape=[vmem((4, 4, n_ids), F32), vmem((4, 128), F32), vmem((4, 128), F32), vmem((8, 128), F32)],
            in_specs=[pl.BlockSpec(memory_space=s) for s in (hbm,) * 6],
            out_specs=[pl.BlockSpec(memory_space=vmem)] * 4,
            scratch_shapes=[
                vmem((5, 4, width), jnp.bfloat16),
                vmem((1, width), F32),
                smem((4,), F32),
                smem((4, 4), jnp.int32),
                vmem((SLOTS, TILE, width), jnp.bfloat16),
                vmem((tail, width), jnp.bfloat16),
                vmem((4, 4, n_ids), F32),
                vmem((4, 4, pad_ids), F32),
                vmem((5, 4, width), F32),
                vmem((5, 4, width), F32),
                vmem((32, width), F32),
                vmem((64, width), jnp.bfloat16),
                vmem((width, 128), jnp.bfloat16),
                vmem((5, 4, 128), F32),
                vmem((5, 4, 128), F32),
                vmem((64, 128), F32),
                vmem((64, 128), F32),
                vmem((64, 128), F32),
                vmem((64, 128), F32),
                vmem((64, 128), F32),
                vmem((SHARED, 4, 4, TILE), F32),
                vmem((2, 8, 128), F32),
                vmem((2, 8, 128), F32),
                vmem((8, 128), F32),
                vmem((3, 8, 128), F32),
                vmem((4, 128), F32),
                vmem((3, 4, 128), F32),
                vmem((2, 4, 128), F32),
                vmem((3, 2, 4, 128), F32),
                dma((4,)), dma((SLOTS, PARTS)), dma, dma, dma((2, 2)), dma((2,)), dma((SHARED,)), dma((SHARED,)), dma((2,)),
                dma((2, 3)), dma((2, 3)), dma((2, 3)),
            ],
            compiler_params=pltpu.CompilerParams(collective_id=0, has_side_effects=True),
            name="verify",
        )(
            hidden.transpose(1, 0, 2), norm_gain.reshape(1, width), temperature, draft_tokens,
            w_head.T, draft_probs,
        )
        acc, norm, residual, bonus = pl.pallas_call(
            finish_kernel,
            out_shape=[
                jax.ShapeDtypeStruct((4, 4), F32),
                jax.ShapeDtypeStruct((4, 4), F32),
                jax.ShapeDtypeStruct((4, 4, n_ids), F32),
                jax.ShapeDtypeStruct((1, 4), F32),
            ],
            in_specs=[pl.BlockSpec(memory_space=vmem)] * 4,
            out_specs=[pl.BlockSpec(memory_space=hbm)] * 4,
            scratch_shapes=[
                vmem((4, 4), F32), vmem((4, 4), F32), vmem((1, 4), F32), vmem((4, 4, n_ids), F32), dma((3,)), dma((4,)),
            ],
            compiler_params=pltpu.CompilerParams(vmem_limit_bytes=16 * 1024 * 1024),
            name="finish",
        )(ex, norm, acc, lse)
        return acc, norm, residual, bonus.reshape(4)

    return jax.shard_map(
        local_step,
        mesh=mesh,
        in_specs=(P("dp", None, None), P(), P(None, "tp"), P("dp", None, "tp"), P("dp", None), P("dp")),
        out_specs=(P("dp", None), P("dp", None), P("dp", None, "tp"), P("dp")),
        check_vma=False,
    )
```

```python
import jax
import jax.numpy as jnp
from jax import lax
from jax.experimental import pallas as pl
from jax.experimental.pallas import tpu as pltpu
from jax.sharding import PartitionSpec as P

MESH = pl.DeviceIdType.MESH
F32 = jnp.float32
LOWEST = float(jnp.finfo(jnp.float32).min)

TILE = 1024
SUB = 256
DEPTH = 256
SLOTS = 3
SHARED = 15
FIRST = 5
HELD = 2
RELAY = 4
PARTS = 1
PASS = 2048


def verify_kernel(
    h_hbm, g_hbm, t_hbm, dt_hbm, w_ref, q_ref,
    ex_ref, norm_ref, acc_ref, lse_ref,
    h_ref, g_ref, t_ref, dt_ref, wbuf, wtail, qv, s_scr, xf, xp, xrows, xb, xt, tv, tp_recv, ct, dl, m_scr, l_scr, k_scr,
    zsend, pstat_s, pstat_r, e1s, e1r, e2s, e2r, e3s, e3r,
    in_sem, w_sem, wt_sem, q_sem, x_sem, t_sem, zs_sem, zr_sem, ps_sem, e1_sem, e2_sem, e3_sem,
):
    dp, tp = lax.axis_index("dp"), lax.axis_index("tp")
    partner = (1 - dp, tp)
    peers = [(dp, lax.rem(tp + d, 4)) for d in (1, 2, 3)]
    n_ids, width = w_ref.shape
    n_full = n_ids // TILE
    tail = n_ids - n_full * TILE
    tail_at = n_full * TILE
    last = n_full - 2 * SHARED - FIRST
    steps = FIRST + SHARED + last

    def column(i):
        in_shared = (i + steps - FIRST) // steps
        past_shared = (i + steps - FIRST - SHARED) // steps
        return pl.multiple_of((i + in_shared * dp * SHARED + past_shared * (SHARED - dp * SHARED)) * TILE, TILE)

    part = TILE // PARTS

    def tile_copies(i, slot):
        at = column(i)
        return [
            pltpu.make_async_copy(
                w_ref.at[pl.ds(at + k * part, part), :], wbuf.at[slot, pl.ds(k * part, part), :], w_sem.at[slot, k]
            )
            for k in range(PARTS)
        ]

    tail_copy = pltpu.make_async_copy(w_ref.at[pl.ds(tail_at, tail), :], wtail, wt_sem)
    q_copy = pltpu.make_async_copy(q_ref, qv, q_sem)
    small = [
        pltpu.make_async_copy(src, dst, in_sem.at[k])
        for k, (src, dst) in enumerate(((h_hbm, h_ref), (g_hbm, g_ref), (t_hbm, t_ref), (dt_hbm, dt_ref)))
    ]
    for c in small:
        c.start()
    tail_copy.start()
    for c in tile_copies(0, 0):
        c.start()

    barrier = pltpu.get_barrier_semaphore()
    for other in [partner] + peers:
        pl.semaphore_signal(barrier, inc=1, device_id=other, device_id_type=MESH)

    for c in small:
        c.wait()
    for c in tile_copies(1, 1):
        c.start()
    h = h_ref[...].astype(F32)
    inv_rms = lax.rsqrt(jnp.mean(h * h, axis=-1, keepdims=True) + 1e-5)
    xf[...] = h * inv_rms * g_ref[...][None]
    for b in range(4):
        tv[0, b : b + 1, :] = jnp.full((1, 128), 1.0, F32) / jnp.full((1, 128), t_ref[b], F32)
        for j in range(4):
            tv[1 + j, b : b + 1, :] = jnp.full((1, 128), dt_ref[b, j].astype(F32), F32)

    def lay_rows(src, t_src, at):
        xrows[...] = jnp.zeros_like(xrows)
        lane = lax.broadcasted_iota(jnp.int32, (1, 128), 1) + tp * n_ids
        for b in range(4):
            for j in range(5):
                xrows[8 * b + j : 8 * b + j + 1, :] = src[j, b : b + 1, :]
            ct[at + 8 * b : at + 8 * b + 8, :] = jnp.broadcast_to(t_src[0, b : b + 1, :], (8, 128))
            dl[at + 8 * b : at + 8 * b + 8, :] = jnp.full((8, 128), -1.0, F32)
            for j in range(4):
                dl[at + 8 * b + j : at + 8 * b + j + 1, :] = t_src[1 + j, b : b + 1, :] - lane.astype(F32)
        rows = xrows[...].astype(jnp.bfloat16)
        xb[at : at + 32, :] = rows
        for k in range(0, width, 128):
            xt[k : k + 128, at : at + 32] = xrows[:, k : k + 128].T.astype(jnp.bfloat16)

    xt[:, 32:128] = jnp.zeros((width, 96), jnp.bfloat16)
    xb[32:64, :] = jnp.zeros((32, width), jnp.bfloat16)
    lay_rows(xf, tv, 0)
    for i in range(2, SLOTS):
        for c in tile_copies(i, i):
            c.start()
    m_scr[...] = jnp.full(m_scr.shape, LOWEST, F32)
    l_scr[...] = jnp.zeros_like(l_scr)
    k_scr[...] = jnp.zeros_like(k_scr)

    pl.semaphore_wait(barrier, 4)
    core = lax.rem(tp, 2)
    sibling = (dp, tp + 1 - 2 * core)

    def width_half(ref, c):
        return ref.at[:, :, pl.ds(pl.multiple_of(c * (width // 2), width // 2), width // 2)]

    def x_copy(src, c, to, k):
        return pltpu.make_async_remote_copy(
            src_ref=width_half(src, c), dst_ref=width_half(xp, c), send_sem=x_sem.at[0, k], recv_sem=x_sem.at[1, k],
            device_id=to, device_id_type=MESH,
        )

    x_direct = x_copy(xf, core, partner, 0)
    x_relay = x_copy(xp, core, sibling, 1)
    t_copy = pltpu.make_async_remote_copy(
        src_ref=tv, dst_ref=tp_recv, send_sem=t_sem.at[0], recv_sem=t_sem.at[1], device_id=partner, device_id_type=MESH
    )
    x_direct.start()
    t_copy.start()

    def by_rows(w, depth):
        return lax.dot_general(xb[:, depth], w, (((1,), (1,)), ((), ())), preferred_element_type=F32)

    def by_ids(w, depth):
        return lax.dot_general(w, xt[depth, :], (((1,), (0,)), ((), ())), preferred_element_type=F32)

    def products(slot, lo, size):
        block = min(SUB, size // 2)
        starts = range(lo, lo + size, block)
        fixed = len(starts) // 2
        sums = [None] * len(starts)
        for k in range(0, width, DEPTH):
            depth = slice(k, k + DEPTH)
            for n, start in enumerate(starts):
                w = wbuf[slot, start : start + block, depth]
                z = by_rows(w, depth) if n < fixed else by_ids(w, depth)
                sums[n] = z if k == 0 else sums[n] + z
        pieces = []
        for n, z in enumerate(sums):
            for at in range(0, block, 128):
                pieces.append(z[:, at : at + 128] if n < fixed else z[at : at + 128, :].T[0:64])
        return pieces

    def fold(rows, parts):
        m_old = m_scr[0:rows, :]
        m_new = m_old
        for p in parts:
            m_new = jnp.maximum(m_new, p)
        total = l_scr[0:rows, :] * jnp.exp(m_old - m_new)
        for p in parts:
            total = total + jnp.exp(p - m_new)
        m_scr[0:rows, :] = m_new
        l_scr[0:rows, :] = total

    tail_copy.wait()
    s = by_rows(wtail[...], slice(0, width))[0:32] * ct[0:32, 0:tail]
    for b in range(4):
        s_scr[b, :, tail_at : tail_at + tail] = s[8 * b : 8 * b + 4, :]
    k_scr[0:32, 0:tail] = jnp.where(dl[0:32, 0:tail] == float(tail_at), s, 0.0)
    m_tail = jnp.max(s, axis=1, keepdims=True)
    l_tail = jnp.sum(jnp.exp(s - m_tail), axis=1, keepdims=True)
    lane0 = lax.broadcasted_iota(jnp.int32, (32, 128), 1) == 0
    m_scr[0:32, :] = jnp.where(lane0, m_tail, LOWEST)
    l_scr[0:32, :] = jnp.where(lane0, l_tail, 0.0)

    def z_copy(k):
        at = column(FIRST + k)
        return pltpu.make_async_remote_copy(
            src_ref=zsend.at[k], dst_ref=s_scr.at[:, :, pl.ds(at, TILE)], send_sem=zs_sem.at[k], recv_sem=zr_sem.at[k],
            device_id=partner, device_id_type=MESH,
        )

    def consume(slot, at, lo, size, rows, k):
        kept = k_scr[0:rows, :]
        parts = []
        for n, z in enumerate(products(slot, lo, size)):
            s = z[0:rows] * ct[0:rows, :]
            parts.append(s)
            off = lo + n * 128
            kept = jnp.where(dl[0:rows, :] == (at + off).astype(F32), s, kept)
            for b in range(4):
                s_scr[b, :, pl.ds(at + off, 128)] = s[8 * b : 8 * b + 4, :]
                if rows == 64:
                    zsend[k, b, :, off : off + 128] = s[32 + 8 * b : 32 + 8 * b + 4, :]
            if n % 2:
                fold(rows, parts)
                parts = []
        k_scr[0:rows, :] = kept

    def step(i, rows):
        slot = i % SLOTS
        for c in tile_copies(i, slot):
            c.wait()
        k = i - FIRST
        consume(slot, column(i), 0, TILE, rows, k)

        @pl.when(i + SLOTS < steps)
        def _():
            for c in tile_copies(i + SLOTS, slot):
                c.start()

        if rows == 64:

            @pl.when(k < SHARED - HELD)
            def _():
                z_copy(k).start()

    group = lax.broadcasted_iota(jnp.int32, (8, 128), 1) // 32

    def pack(cols):
        size = cols[0].shape[0]
        packed = jnp.broadcast_to(cols[0], (size, 128))
        for b in range(1, 4):
            packed = jnp.where(group[:size] == b, cols[b], packed)
        return packed

    def unpack(packed, b):
        size = packed.shape[0]
        lane = lax.broadcasted_iota(jnp.int32, (size, 128), 1)
        return jnp.sum(jnp.where(lane == 32 * b, packed, 0.0), axis=1, keepdims=True)

    def packed_lse(at):
        m = m_scr[at : at + 32, :]
        top = jnp.max(m, axis=1, keepdims=True)
        lse = top + jnp.log(jnp.sum(l_scr[at : at + 32, :] * jnp.exp(m - top), axis=1, keepdims=True))
        return pack([lse[8 * b : 8 * b + 8, :] for b in range(4)])

    def packed_token(at):
        kept = jnp.sum(k_scr[at : at + 32, :], axis=1, keepdims=True)
        return pack([kept[8 * b : 8 * b + 8, :] for b in range(4)])

    lax.fori_loop(0, RELAY, lambda i, _: step(i, 32), None)
    x_direct.wait()
    x_relay.start()
    lax.fori_loop(RELAY, FIRST, lambda i, _: step(i, 32), None)
    x_copy(xp, 1 - core, sibling, 1).wait_recv()
    x_relay.wait_send()
    t_copy.wait()
    lay_rows(xp, tp_recv, 32)
    lax.fori_loop(FIRST, FIRST + SHARED, lambda i, _: step(i, 64), None)
    q_copy.start()
    pstat_s[0] = packed_lse(32)
    pstat_s[1] = packed_token(32)
    stat_copy = pltpu.make_async_remote_copy(
        src_ref=pstat_s, dst_ref=pstat_r, send_sem=ps_sem.at[0], recv_sem=ps_sem.at[1],
        device_id=partner, device_id_type=MESH,
    )
    stat_copy.start()
    for k in range(SHARED - HELD, SHARED):
        z_copy(k).start()
    lax.fori_loop(FIRST + SHARED, steps - 1, lambda i, _: step(i, 32), None)
    end, slot = steps - 1, (steps - 1) % SLOTS
    copies = tile_copies(end, slot)
    for lo, size in [(k * part, part) for k in range(PARTS)]:
        for c in copies[lo // part : (lo + size) // part]:
            c.wait()
        consume(slot, column(end), lo, size, 32, 0)

    def exchange(src, dst, sem):
        return [
            pltpu.make_async_remote_copy(
                src_ref=src, dst_ref=dst.at[d], send_sem=sem.at[0, d], recv_sem=sem.at[1, d],
                device_id=peers[d], device_id_type=MESH,
            )
            for d in range(3)
        ]

    mine = packed_lse(0)
    stat_copy.wait()
    theirs = pstat_r[0]
    top = jnp.maximum(mine, theirs)
    near = top + jnp.log(jnp.exp(mine - top) + jnp.exp(theirs - top))
    e1s[...] = near
    e1 = exchange(e1s, e1r, e1_sem)
    for c in e1:
        c.start()

    own = [dl[8 * b : 8 * b + 4, :] for b in range(4)]

    row_m = [jnp.broadcast_to(unpack(near[0:4, :], b), (4, 128)) for b in range(4)]

    def prepare(at, size):
        places = [(b, at + off, min(size, 128)) for b in range(4) for off in range(0, size, 128)]
        values = [s_scr[b, :, pl.ds(a, n)] for b, a, n in places]
        values = [jnp.exp(v - row_m[b][:, :n]) for v, (b, _, n) in zip(values, places)]
        for v, (b, a, n) in zip(values, places):
            s_scr[b, :, pl.ds(a, n)] = v

    def pick(at, size, found):
        out = []
        for b in range(4):
            f = found[b]
            for off in range(0, size, 128):
                n = min(size, 128)
                f = jnp.where(own[b][:, :n] == jnp.asarray(at + off).astype(F32), qv[b, :, pl.ds(at + off, n)], f)
            out.append(f)
        return tuple(out)

    zero = jnp.zeros((4, 128), F32)
    lax.fori_loop(0, steps, lambda i, _: prepare(column(i), TILE), None)
    prepare(tail_at, tail)
    q_copy.wait()
    whole = tail_at // PASS * PASS
    found = lax.fori_loop(0, whole // PASS, lambda i, f: pick(pl.multiple_of(i * PASS, 128), PASS, f), (zero,) * 4)
    found = pick(whole, tail_at - whole, found)
    found_tail = pick(tail_at, tail, (jnp.zeros((4, tail), F32),) * 4)
    token_q = []
    for b in range(4):
        f = found_tail[b]
        token_q.append(jnp.sum(found[b], axis=1, keepdims=True) + jnp.sum(f, axis=1, keepdims=True))
    e3s[0] = (packed_token(0) + pstat_r[1])[0:4, :]
    e3s[1] = pack(token_q)
    e3 = exchange(e3s, e3r, e3_sem)
    for c in e3:
        c.start()

    def take_z(k, _):
        z_copy(k).wait_send()
        at = pl.multiple_of((FIRST + (1 - dp) * SHARED + k) * TILE, TILE)
        pltpu.make_async_remote_copy(
            src_ref=zsend.at[k], dst_ref=s_scr.at[:, :, pl.ds(at, TILE)], send_sem=zs_sem.at[k], recv_sem=zr_sem.at[k],
            device_id=partner, device_id_type=MESH,
        ).wait_recv()
        prepare(at, TILE)

    lax.fori_loop(0, SHARED, take_z, None)

    for c in e1:
        c.wait()
    lses = [near] + [e1r[d] for d in range(3)]
    top = jnp.maximum(jnp.maximum(lses[0], lses[1]), jnp.maximum(lses[2], lses[3]))
    sums = jnp.exp(lses[0] - top) + jnp.exp(lses[1] - top) + jnp.exp(lses[2] - top) + jnp.exp(lses[3] - top)
    lse = top + jnp.log(sums)
    lse_ref[...] = lse
    scale = [jnp.exp(row_m[b] - jnp.broadcast_to(unpack(lse[0:4, :], b), (4, 128))) for b in range(4)]

    def excess(b, at, size):
        e = jnp.maximum(s_scr[b, :, pl.ds(at, size)] * scale[b][:, :size] - qv[b, :, pl.ds(at, size)], 0.0)
        ex_ref[b, :, pl.ds(at, size)] = e
        return e

    def last_pass(at, size, sums):
        out = []
        for b in range(4):
            acc = sums[b]
            for off in range(0, size, 128):
                acc = acc + excess(b, at + off, 128)
            out.append(acc)
        return tuple(out)

    sums = lax.fori_loop(0, whole // PASS, lambda i, t: last_pass(pl.multiple_of(i * PASS, 128), PASS, t), (zero,) * 4)
    sums = last_pass(whole, tail_at - whole, sums)
    rows = []
    for b in range(4):
        e = excess(b, tail_at, tail)
        rows.append(jnp.sum(sums[b], axis=1, keepdims=True) + jnp.sum(e, axis=1, keepdims=True))
    e2s[...] = pack(rows)
    e2 = exchange(e2s, e2r, e2_sem)
    for c in e2:
        c.start()

    for c in e3:
        c.wait()
    at_token = (e3s[...] + e3r[0]) + (e3r[1] + e3r[2])
    acc_ref[...] = jnp.minimum(jnp.exp(at_token[0] - lse[0:4, :]) / at_token[1], 1.0)

    for c in e2:
        c.wait()
    norm_ref[...] = (e2s[...] + e2r[0]) + (e2r[1] + e2r[2])


def finish_kernel(
    ex_ref, norm_ref, acc_ref, lse_ref, acc_out, norm_out, res_out, bonus_out, acc_v, norm_v, bonus_v, stage, sem, r_sem
):
    n_ids = ex_ref.shape[2]
    lane = lax.broadcasted_iota(jnp.int32, (4, 128), 1)
    norm = norm_ref[...]
    writes = []
    for b in range(4):
        total = jnp.sum(jnp.where(lane == 32 * b, norm, 0.0), axis=1, keepdims=True)
        scale = jnp.broadcast_to(1.0 / jnp.broadcast_to(total, (4, 128)), (4, 128))

        for at in range(0, n_ids, 128):
            size = min(128, n_ids - at)
            stage[b, :, at : at + size] = ex_ref[b, :, at : at + size] * scale[:, :size]
        writes.append(pltpu.make_async_copy(stage.at[b], res_out.at[b], r_sem.at[b]))
        writes[-1].start()

    sub = lax.broadcasted_iota(jnp.int32, (4, 128), 0)
    for src, dst, out, k in ((acc_ref[...], acc_v, acc_out, 0), (norm, norm_v, norm_out, 1)):
        row = jnp.sum(jnp.where(lane % 32 == sub, src, 0.0), axis=0, keepdims=True)
        for b in range(4):
            dst[b : b + 1, :] = (row if b == 0 else pltpu.roll(row, 128 - 32 * b, 1))[:, 0:4]
        writes.append(pltpu.make_async_copy(dst, out, sem.at[k]))
        writes[-1].start()
    row = lse_ref[4:5, :]
    lane = lane[0:1, :]
    packed = row
    for b in range(1, 4):
        packed = jnp.where(lane == b, pltpu.roll(row, 128 - 31 * b, 1), packed)
    bonus_v[...] = packed[:, 0:4]
    writes.append(pltpu.make_async_copy(bonus_v, bonus_out, sem.at[2]))
    writes[-1].start()
    for c in writes:
        c.wait()


def solution(mesh):
    def local_step(hidden, norm_gain, w_head, draft_probs, draft_tokens, temperature):
        n_ids = w_head.shape[1]
        width = w_head.shape[0]
        pad_ids = -(-n_ids // 128) * 128
        tail = n_ids % TILE
        vmem, smem, hbm = pltpu.VMEM, pltpu.SMEM, pltpu.HBM
        dma = pltpu.SemaphoreType.DMA
        ex, norm, acc, lse = pl.pallas_call(
            verify_kernel,
            out_shape=[vmem((4, 4, n_ids), F32), vmem((4, 128), F32), vmem((4, 128), F32), vmem((8, 128), F32)],
            in_specs=[pl.BlockSpec(memory_space=s) for s in (hbm,) * 6],
            out_specs=[pl.BlockSpec(memory_space=vmem)] * 4,
            scratch_shapes=[
                vmem((5, 4, width), jnp.bfloat16),
                vmem((1, width), F32),
                smem((4,), F32),
                smem((4, 4), jnp.int32),
                vmem((SLOTS, TILE, width), jnp.bfloat16),
                vmem((tail, width), jnp.bfloat16),
                vmem((4, 4, n_ids), F32),
                vmem((4, 4, pad_ids), F32),
                vmem((5, 4, width), F32),
                vmem((5, 4, width), F32),
                vmem((32, width), F32),
                vmem((64, width), jnp.bfloat16),
                vmem((width, 128), jnp.bfloat16),
                vmem((5, 4, 128), F32),
                vmem((5, 4, 128), F32),
                vmem((64, 128), F32),
                vmem((64, 128), F32),
                vmem((64, 128), F32),
                vmem((64, 128), F32),
                vmem((64, 128), F32),
                vmem((SHARED, 4, 4, TILE), F32),
                vmem((2, 8, 128), F32),
                vmem((2, 8, 128), F32),
                vmem((8, 128), F32),
                vmem((3, 8, 128), F32),
                vmem((4, 128), F32),
                vmem((3, 4, 128), F32),
                vmem((2, 4, 128), F32),
                vmem((3, 2, 4, 128), F32),
                dma((4,)), dma((SLOTS, PARTS)), dma, dma, dma((2, 2)), dma((2,)), dma((SHARED,)), dma((SHARED,)), dma((2,)),
                dma((2, 3)), dma((2, 3)), dma((2, 3)),
            ],
            compiler_params=pltpu.CompilerParams(collective_id=0, has_side_effects=True),
            name="verify",
        )(
            hidden.transpose(1, 0, 2), norm_gain.reshape(1, width), temperature, draft_tokens,
            w_head.T, draft_probs,
        )
        acc, norm, residual, bonus = pl.pallas_call(
            finish_kernel,
            out_shape=[
                jax.ShapeDtypeStruct((4, 4), F32),
                jax.ShapeDtypeStruct((4, 4), F32),
                jax.ShapeDtypeStruct((4, 4, n_ids), F32),
                jax.ShapeDtypeStruct((1, 4), F32),
            ],
            in_specs=[pl.BlockSpec(memory_space=vmem)] * 4,
            out_specs=[pl.BlockSpec(memory_space=hbm)] * 4,
            scratch_shapes=[
                vmem((4, 4), F32), vmem((4, 4), F32), vmem((1, 4), F32), vmem((4, 4, n_ids), F32), dma((3,)), dma((4,)),
            ],
            compiler_params=pltpu.CompilerParams(vmem_limit_bytes=16 * 1024 * 1024),
            name="finish",
        )(ex, norm, acc, lse)
        return acc, norm, residual, bonus.reshape(4)

    return jax.shard_map(
        local_step,
        mesh=mesh,
        in_specs=(P("dp", None, None), P(), P(None, "tp"), P("dp", None, "tp"), P("dp", None), P("dp")),
        out_specs=(P("dp", None), P("dp", None), P("dp", None, "tp"), P("dp")),
        check_vma=False,
    )
```

```python
import jax
import jax.numpy as jnp
from jax import lax
from jax.experimental import pallas as pl
from jax.experimental.pallas import tpu as pltpu
from jax.sharding import PartitionSpec as P

MESH = pl.DeviceIdType.MESH
F32 = jnp.float32
LOWEST = float(jnp.finfo(jnp.float32).min)

TILE = 1024
SUB = 256
DEPTH = 256
SLOTS = 3
SHARED = 15
FIRST = 4
LATE = 5
HELD = 2
RELAY = 3
PARTS = 1
PASS = 2048


def verify_kernel(
    h_hbm, g_hbm, t_hbm, dt_hbm, w_ref, q_ref,
    ex_ref, norm_ref, acc_ref, lse_ref,
    h_ref, g_ref, t_ref, dt_ref, wbuf, wtail, qv, s_scr, xf, xp, xrows, xb, xt, tv, tp_recv, ct, dl, m_scr, l_scr, k_scr,
    zsend, pstat_s, pstat_r, e1s, e1r, e2s, e2r, e3s, e3r,
    in_sem, w_sem, wt_sem, q_sem, x_sem, t_sem, zs_sem, zr_sem, ps_sem, e1_sem, e2_sem, e3_sem,
):
    dp, tp = lax.axis_index("dp"), lax.axis_index("tp")
    partner = (1 - dp, tp)
    peers = [(dp, lax.rem(tp + d, 4)) for d in (1, 2, 3)]
    n_ids, width = w_ref.shape
    n_full = n_ids // TILE
    tail = n_ids - n_full * TILE
    tail_at = n_full * TILE
    last = n_full - 2 * SHARED - FIRST
    steps = FIRST + SHARED + last

    def column(i):
        in_shared = (i + steps - FIRST) // steps
        past_shared = (i + steps - FIRST - SHARED) // steps
        return pl.multiple_of((i + in_shared * dp * SHARED + past_shared * (SHARED - dp * SHARED)) * TILE, TILE)

    part = TILE // PARTS

    def tile_copies(i, slot):
        at = column(i)
        return [
            pltpu.make_async_copy(
                w_ref.at[pl.ds(at + k * part, part), :], wbuf.at[slot, pl.ds(k * part, part), :], w_sem.at[slot, k]
            )
            for k in range(PARTS)
        ]

    tail_copy = pltpu.make_async_copy(w_ref.at[pl.ds(tail_at, tail), :], wtail, wt_sem)
    q_copy = pltpu.make_async_copy(q_ref, qv, q_sem)
    small = [
        pltpu.make_async_copy(src, dst, in_sem.at[k])
        for k, (src, dst) in enumerate(((h_hbm, h_ref), (g_hbm, g_ref), (t_hbm, t_ref), (dt_hbm, dt_ref)))
    ]
    for c in small:
        c.start()
    tail_copy.start()
    for c in tile_copies(0, 0):
        c.start()

    barrier = pltpu.get_barrier_semaphore()
    for other in [partner] + peers:
        pl.semaphore_signal(barrier, inc=1, device_id=other, device_id_type=MESH)

    for c in small:
        c.wait()
    for c in tile_copies(1, 1):
        c.start()
    h = h_ref[...].astype(F32)
    inv_rms = lax.rsqrt(jnp.mean(h * h, axis=-1, keepdims=True) + 1e-5)
    xf[...] = h * inv_rms * g_ref[...][None]
    for b in range(4):
        tv[0, b : b + 1, :] = jnp.full((1, 128), 1.0, F32) / jnp.full((1, 128), t_ref[b], F32)
        for j in range(4):
            tv[1 + j, b : b + 1, :] = jnp.full((1, 128), dt_ref[b, j].astype(F32), F32)

    def lay_rows(src, t_src, at):
        xrows[...] = jnp.zeros_like(xrows)
        lane = lax.broadcasted_iota(jnp.int32, (1, 128), 1) + tp * n_ids
        for b in range(4):
            for j in range(5):
                xrows[8 * b + j : 8 * b + j + 1, :] = src[j, b : b + 1, :]
            ct[at + 8 * b : at + 8 * b + 8, :] = jnp.broadcast_to(t_src[0, b : b + 1, :], (8, 128))
            dl[at + 8 * b : at + 8 * b + 8, :] = jnp.full((8, 128), -1.0, F32)
            for j in range(4):
                dl[at + 8 * b + j : at + 8 * b + j + 1, :] = t_src[1 + j, b : b + 1, :] - lane.astype(F32)
        rows = xrows[...].astype(jnp.bfloat16)
        xb[at : at + 32, :] = rows
        for k in range(0, width, 128):
            xt[k : k + 128, at : at + 32] = xrows[:, k : k + 128].T.astype(jnp.bfloat16)

    xt[:, 32:128] = jnp.zeros((width, 96), jnp.bfloat16)
    xb[32:64, :] = jnp.zeros((32, width), jnp.bfloat16)
    lay_rows(xf, tv, 0)
    for i in range(2, SLOTS):
        for c in tile_copies(i, i):
            c.start()
    m_scr[...] = jnp.full(m_scr.shape, LOWEST, F32)
    l_scr[...] = jnp.zeros_like(l_scr)
    k_scr[...] = jnp.zeros_like(k_scr)

    pl.semaphore_wait(barrier, 4)
    core = lax.rem(tp, 2)
    sibling = (dp, tp + 1 - 2 * core)

    def width_half(ref, c):
        return ref.at[:, :, pl.ds(pl.multiple_of(c * (width // 2), width // 2), width // 2)]

    def x_copy(src, c, to, k):
        return pltpu.make_async_remote_copy(
            src_ref=width_half(src, c), dst_ref=width_half(xp, c), send_sem=x_sem.at[0, k], recv_sem=x_sem.at[1, k],
            device_id=to, device_id_type=MESH,
        )

    x_direct = x_copy(xf, core, partner, 0)
    x_relay = x_copy(xp, core, sibling, 1)
    t_copy = pltpu.make_async_remote_copy(
        src_ref=tv, dst_ref=tp_recv, send_sem=t_sem.at[0], recv_sem=t_sem.at[1], device_id=partner, device_id_type=MESH
    )
    x_direct.start()
    t_copy.start()

    def by_rows(w, depth):
        return lax.dot_general(xb[:, depth], w, (((1,), (1,)), ((), ())), preferred_element_type=F32)

    def by_ids(w, depth):
        return lax.dot_general(w, xt[depth, :], (((1,), (0,)), ((), ())), preferred_element_type=F32)

    def products(slot, lo, size):
        block = min(SUB, size // 2)
        starts = range(lo, lo + size, block)
        fixed = len(starts) // 2
        sums = [None] * len(starts)
        for k in range(0, width, DEPTH):
            depth = slice(k, k + DEPTH)
            for n, start in enumerate(starts):
                w = wbuf[slot, start : start + block, depth]
                z = by_rows(w, depth) if n < fixed else by_ids(w, depth)
                sums[n] = z if k == 0 else sums[n] + z
        pieces = []
        for n, z in enumerate(sums):
            for at in range(0, block, 128):
                pieces.append(z[:, at : at + 128] if n < fixed else z[at : at + 128, :].T[0:64])
        return pieces

    def fold(rows, parts):
        m_old = m_scr[0:rows, :]
        m_new = m_old
        for p in parts:
            m_new = jnp.maximum(m_new, p)
        total = l_scr[0:rows, :] * jnp.exp(m_old - m_new)
        for p in parts:
            total = total + jnp.exp(p - m_new)
        m_scr[0:rows, :] = m_new
        l_scr[0:rows, :] = total

    tail_copy.wait()
    s = by_rows(wtail[...], slice(0, width))[0:32] * ct[0:32, 0:tail]
    for b in range(4):
        s_scr[b, :, tail_at : tail_at + tail] = s[8 * b : 8 * b + 4, :]
    k_scr[0:32, 0:tail] = jnp.where(dl[0:32, 0:tail] == float(tail_at), s, 0.0)
    m_tail = jnp.max(s, axis=1, keepdims=True)
    l_tail = jnp.sum(jnp.exp(s - m_tail), axis=1, keepdims=True)
    lane0 = lax.broadcasted_iota(jnp.int32, (32, 128), 1) == 0
    m_scr[0:32, :] = jnp.where(lane0, m_tail, LOWEST)
    l_scr[0:32, :] = jnp.where(lane0, l_tail, 0.0)

    def z_copy(k):
        at = column(FIRST + k)
        return pltpu.make_async_remote_copy(
            src_ref=zsend.at[k], dst_ref=s_scr.at[:, :, pl.ds(at, TILE)], send_sem=zs_sem.at[k], recv_sem=zr_sem.at[k],
            device_id=partner, device_id_type=MESH,
        )

    def consume(slot, at, lo, size, rows, k):
        kept = k_scr[0:rows, :]
        parts = []
        for n, z in enumerate(products(slot, lo, size)):
            s = z[0:rows] * ct[0:rows, :]
            parts.append(s)
            off = lo + n * 128
            kept = jnp.where(dl[0:rows, :] == (at + off).astype(F32), s, kept)
            for b in range(4):
                s_scr[b, :, pl.ds(at + off, 128)] = s[8 * b : 8 * b + 4, :]
                if rows == 64:
                    zsend[k, b, :, off : off + 128] = s[32 + 8 * b : 32 + 8 * b + 4, :]
            if n % 2:
                fold(rows, parts)
                parts = []
        k_scr[0:rows, :] = kept

    def step(i, rows):
        slot = i % SLOTS
        for c in tile_copies(i, slot):
            c.wait()
        k = i - FIRST
        consume(slot, column(i), 0, TILE, rows, k)

        @pl.when(i + SLOTS < steps)
        def _():
            for c in tile_copies(i + SLOTS, slot):
                c.start()

        if rows == 64:

            @pl.when(k < SHARED - HELD)
            def _():
                z_copy(k).start()

    group = lax.broadcasted_iota(jnp.int32, (8, 128), 1) // 32

    def pack(cols):
        size = cols[0].shape[0]
        packed = jnp.broadcast_to(cols[0], (size, 128))
        for b in range(1, 4):
            packed = jnp.where(group[:size] == b, cols[b], packed)
        return packed

    def unpack(packed, b):
        size = packed.shape[0]
        lane = lax.broadcasted_iota(jnp.int32, (size, 128), 1)
        return jnp.sum(jnp.where(lane == 32 * b, packed, 0.0), axis=1, keepdims=True)

    def packed_lse(at):
        m = m_scr[at : at + 32, :]
        top = jnp.max(m, axis=1, keepdims=True)
        lse = top + jnp.log(jnp.sum(l_scr[at : at + 32, :] * jnp.exp(m - top), axis=1, keepdims=True))
        return pack([lse[8 * b : 8 * b + 8, :] for b in range(4)])

    def packed_token(at):
        kept = jnp.sum(k_scr[at : at + 32, :], axis=1, keepdims=True)
        return pack([kept[8 * b : 8 * b + 8, :] for b in range(4)])

    lax.fori_loop(0, RELAY, lambda i, _: step(i, 32), None)
    x_direct.wait()
    x_relay.start()
    lax.fori_loop(RELAY, FIRST, lambda i, _: step(i, 32), None)
    x_copy(xp, 1 - core, sibling, 1).wait_recv()
    x_relay.wait_send()
    t_copy.wait()
    lay_rows(xp, tp_recv, 32)
    lax.fori_loop(FIRST, FIRST + SHARED, lambda i, _: step(i, 64), None)
    q_copy.start()
    pstat_s[0] = packed_lse(32)
    pstat_s[1] = packed_token(32)
    stat_copy = pltpu.make_async_remote_copy(
        src_ref=pstat_s, dst_ref=pstat_r, send_sem=ps_sem.at[0], recv_sem=ps_sem.at[1],
        device_id=partner, device_id_type=MESH,
    )
    stat_copy.start()
    for k in range(SHARED - HELD, SHARED):
        z_copy(k).start()
    lax.fori_loop(FIRST + SHARED, steps - 1, lambda i, _: step(i, 32), None)
    end, slot = steps - 1, (steps - 1) % SLOTS
    copies = tile_copies(end, slot)
    for lo, size in [(k * part, part) for k in range(PARTS)]:
        for c in copies[lo // part : (lo + size) // part]:
            c.wait()
        consume(slot, column(end), lo, size, 32, 0)

    def exchange(src, dst, sem):
        return [
            pltpu.make_async_remote_copy(
                src_ref=src, dst_ref=dst.at[d], send_sem=sem.at[0, d], recv_sem=sem.at[1, d],
                device_id=peers[d], device_id_type=MESH,
            )
            for d in range(3)
        ]

    mine = packed_lse(0)
    stat_copy.wait()
    theirs = pstat_r[0]
    top = jnp.maximum(mine, theirs)
    near = top + jnp.log(jnp.exp(mine - top) + jnp.exp(theirs - top))
    e1s[...] = near
    e1 = exchange(e1s, e1r, e1_sem)
    for c in e1:
        c.start()

    own = [dl[8 * b : 8 * b + 4, :] for b in range(4)]

    row_m = [jnp.broadcast_to(unpack(near[0:4, :], b), (4, 128)) for b in range(4)]

    def prepare(at, size):
        places = [(b, at + off, min(size, 128)) for b in range(4) for off in range(0, size, 128)]
        values = [s_scr[b, :, pl.ds(a, n)] for b, a, n in places]
        values = [jnp.exp(v - row_m[b][:, :n]) for v, (b, _, n) in zip(values, places)]
        for v, (b, a, n) in zip(values, places):
            s_scr[b, :, pl.ds(a, n)] = v

    def pick(at, size, found):
        out = []
        for b in range(4):
            f = found[b]
            for off in range(0, size, 128):
                n = min(size, 128)
                f = jnp.where(own[b][:, :n] == jnp.asarray(at + off).astype(F32), qv[b, :, pl.ds(at + off, n)], f)
            out.append(f)
        return tuple(out)

    zero = jnp.zeros((4, 128), F32)
    lax.fori_loop(0, steps, lambda i, _: prepare(column(i), TILE), None)
    prepare(tail_at, tail)
    q_copy.wait()
    whole = tail_at // PASS * PASS
    found = lax.fori_loop(0, whole // PASS, lambda i, f: pick(pl.multiple_of(i * PASS, 128), PASS, f), (zero,) * 4)
    found = pick(whole, tail_at - whole, found)
    found_tail = pick(tail_at, tail, (jnp.zeros((4, tail), F32),) * 4)
    token_q = []
    for b in range(4):
        f = found_tail[b]
        token_q.append(jnp.sum(found[b], axis=1, keepdims=True) + jnp.sum(f, axis=1, keepdims=True))
    e3s[0] = (packed_token(0) + pstat_r[1])[0:4, :]
    e3s[1] = pack(token_q)
    e3 = exchange(e3s, e3r, e3_sem)
    for c in e3:
        c.start()

    def theirs_at(k):
        return pl.multiple_of((FIRST + (1 - dp) * SHARED + k) * TILE, TILE)

    def await_z(k):
        z_copy(k).wait_send()
        pltpu.make_async_remote_copy(
            src_ref=zsend.at[k], dst_ref=s_scr.at[:, :, pl.ds(theirs_at(k), TILE)],
            send_sem=zs_sem.at[k], recv_sem=zr_sem.at[k], device_id=partner, device_id_type=MESH,
        ).wait_recv()

    def take_early(k, _):
        await_z(k)
        prepare(theirs_at(k), TILE)

    lax.fori_loop(0, SHARED - LATE, take_early, None)
    for c in e1:
        c.wait()
    lses = [near] + [e1r[d] for d in range(3)]
    top = jnp.maximum(jnp.maximum(lses[0], lses[1]), jnp.maximum(lses[2], lses[3]))
    sums = jnp.exp(lses[0] - top) + jnp.exp(lses[1] - top) + jnp.exp(lses[2] - top) + jnp.exp(lses[3] - top)
    lse = top + jnp.log(sums)
    lse_ref[...] = lse
    row_l = [jnp.broadcast_to(unpack(lse[0:4, :], b), (4, 128)) for b in range(4)]
    scale = [jnp.exp(row_m[b] - row_l[b]) for b in range(4)]

    def excess(b, at, size, p):
        e = jnp.maximum(p - qv[b, :, pl.ds(at, size)], 0.0)
        ex_ref[b, :, pl.ds(at, size)] = e
        return e

    def close(at, sums, prepared):
        out = []
        for b in range(4):
            acc = sums[b]
            for off in range(0, TILE, 128):
                v = s_scr[b, :, pl.ds(at + off, 128)]
                acc = acc + excess(b, at + off, 128, v * scale[b] if prepared else jnp.exp(v - row_l[b]))
            out.append(acc)
        return tuple(out)

    def close_late(k, sums):
        await_z(k)
        return close(theirs_at(k), sums, False)

    sums = lax.fori_loop(0, steps, lambda i, t: close(column(i), t, True), (zero,) * 4)
    rows = []
    for b in range(4):
        e = excess(b, tail_at, tail, s_scr[b, :, tail_at : tail_at + tail] * scale[b][:, :tail])
        rows.append(jnp.sum(e, axis=1, keepdims=True))
    sums = lax.fori_loop(0, SHARED - LATE, lambda k, t: close(theirs_at(k), t, True), sums)
    sums = lax.fori_loop(SHARED - LATE, SHARED, close_late, sums)
    rows = [jnp.sum(sums[b], axis=1, keepdims=True) + rows[b] for b in range(4)]
    e2s[...] = pack(rows)
    e2 = exchange(e2s, e2r, e2_sem)
    for c in e2:
        c.start()

    for c in e3:
        c.wait()
    at_token = (e3s[...] + e3r[0]) + (e3r[1] + e3r[2])
    acc_ref[...] = jnp.minimum(jnp.exp(at_token[0] - lse[0:4, :]) / at_token[1], 1.0)

    for c in e2:
        c.wait()
    norm_ref[...] = (e2s[...] + e2r[0]) + (e2r[1] + e2r[2])


def finish_kernel(
    ex_ref, norm_ref, acc_ref, lse_ref, acc_out, norm_out, res_out, bonus_out, acc_v, norm_v, bonus_v, stage, sem, r_sem
):
    n_ids = ex_ref.shape[2]
    lane = lax.broadcasted_iota(jnp.int32, (4, 128), 1)
    norm = norm_ref[...]
    writes = []
    for b in range(4):
        total = jnp.sum(jnp.where(lane == 32 * b, norm, 0.0), axis=1, keepdims=True)
        scale = jnp.broadcast_to(1.0 / jnp.broadcast_to(total, (4, 128)), (4, 128))

        for at in range(0, n_ids, 128):
            size = min(128, n_ids - at)
            stage[b, :, at : at + size] = ex_ref[b, :, at : at + size] * scale[:, :size]
        writes.append(pltpu.make_async_copy(stage.at[b], res_out.at[b], r_sem.at[b]))
        writes[-1].start()

    sub = lax.broadcasted_iota(jnp.int32, (4, 128), 0)
    for src, dst, out, k in ((acc_ref[...], acc_v, acc_out, 0), (norm, norm_v, norm_out, 1)):
        row = jnp.sum(jnp.where(lane % 32 == sub, src, 0.0), axis=0, keepdims=True)
        for b in range(4):
            dst[b : b + 1, :] = (row if b == 0 else pltpu.roll(row, 128 - 32 * b, 1))[:, 0:4]
        writes.append(pltpu.make_async_copy(dst, out, sem.at[k]))
        writes[-1].start()
    row = lse_ref[4:5, :]
    lane = lane[0:1, :]
    packed = row
    for b in range(1, 4):
        packed = jnp.where(lane == b, pltpu.roll(row, 128 - 31 * b, 1), packed)
    bonus_v[...] = packed[:, 0:4]
    writes.append(pltpu.make_async_copy(bonus_v, bonus_out, sem.at[2]))
    writes[-1].start()
    for c in writes:
        c.wait()


def solution(mesh):
    def local_step(hidden, norm_gain, w_head, draft_probs, draft_tokens, temperature):
        n_ids = w_head.shape[1]
        width = w_head.shape[0]
        pad_ids = -(-n_ids // 128) * 128
        tail = n_ids % TILE
        vmem, smem, hbm = pltpu.VMEM, pltpu.SMEM, pltpu.HBM
        dma = pltpu.SemaphoreType.DMA
        ex, norm, acc, lse = pl.pallas_call(
            verify_kernel,
            out_shape=[vmem((4, 4, n_ids), F32), vmem((4, 128), F32), vmem((4, 128), F32), vmem((8, 128), F32)],
            in_specs=[pl.BlockSpec(memory_space=s) for s in (hbm,) * 6],
            out_specs=[pl.BlockSpec(memory_space=vmem)] * 4,
            scratch_shapes=[
                vmem((5, 4, width), jnp.bfloat16),
                vmem((1, width), F32),
                smem((4,), F32),
                smem((4, 4), jnp.int32),
                vmem((SLOTS, TILE, width), jnp.bfloat16),
                vmem((tail, width), jnp.bfloat16),
                vmem((4, 4, n_ids), F32),
                vmem((4, 4, pad_ids), F32),
                vmem((5, 4, width), F32),
                vmem((5, 4, width), F32),
                vmem((32, width), F32),
                vmem((64, width), jnp.bfloat16),
                vmem((width, 128), jnp.bfloat16),
                vmem((5, 4, 128), F32),
                vmem((5, 4, 128), F32),
                vmem((64, 128), F32),
                vmem((64, 128), F32),
                vmem((64, 128), F32),
                vmem((64, 128), F32),
                vmem((64, 128), F32),
                vmem((SHARED, 4, 4, TILE), F32),
                vmem((2, 8, 128), F32),
                vmem((2, 8, 128), F32),
                vmem((8, 128), F32),
                vmem((3, 8, 128), F32),
                vmem((4, 128), F32),
                vmem((3, 4, 128), F32),
                vmem((2, 4, 128), F32),
                vmem((3, 2, 4, 128), F32),
                dma((4,)), dma((SLOTS, PARTS)), dma, dma, dma((2, 2)), dma((2,)), dma((SHARED,)), dma((SHARED,)), dma((2,)),
                dma((2, 3)), dma((2, 3)), dma((2, 3)),
            ],
            compiler_params=pltpu.CompilerParams(collective_id=0, has_side_effects=True),
            name="verify",
        )(
            hidden.transpose(1, 0, 2), norm_gain.reshape(1, width), temperature, draft_tokens,
            w_head.T, draft_probs,
        )
        acc, norm, residual, bonus = pl.pallas_call(
            finish_kernel,
            out_shape=[
                jax.ShapeDtypeStruct((4, 4), F32),
                jax.ShapeDtypeStruct((4, 4), F32),
                jax.ShapeDtypeStruct((4, 4, n_ids), F32),
                jax.ShapeDtypeStruct((1, 4), F32),
            ],
            in_specs=[pl.BlockSpec(memory_space=vmem)] * 4,
            out_specs=[pl.BlockSpec(memory_space=hbm)] * 4,
            scratch_shapes=[
                vmem((4, 4), F32), vmem((4, 4), F32), vmem((1, 4), F32), vmem((4, 4, n_ids), F32), dma((3,)), dma((4,)),
            ],
            compiler_params=pltpu.CompilerParams(vmem_limit_bytes=16 * 1024 * 1024),
            name="finish",
        )(ex, norm, acc, lse)
        return acc, norm, residual, bonus.reshape(4)

    return jax.shard_map(
        local_step,
        mesh=mesh,
        in_specs=(P("dp", None, None), P(), P(None, "tp"), P("dp", None, "tp"), P("dp", None), P("dp")),
        out_specs=(P("dp", None), P("dp", None), P("dp", None, "tp"), P("dp")),
        check_vma=False,
    )
```

```python
import jax
import jax.numpy as jnp
from jax import lax
from jax.experimental import pallas as pl
from jax.experimental.pallas import tpu as pltpu
from jax.sharding import PartitionSpec as P

MESH = pl.DeviceIdType.MESH
F32 = jnp.float32
LOWEST = float(jnp.finfo(jnp.float32).min)

TILE = 1024
SUB = 256
DEPTH = 256
SLOTS = 3
SHARED = 15
FIRST = 4
LATE = 5
HELD = 2
RELAY = 3
PARTS = 1
PASS = 2048


def verify_kernel(
    h_hbm, g_hbm, t_hbm, dt_hbm, w_ref, q_ref,
    ex_ref, norm_ref, acc_ref, lse_ref,
    h_ref, g_ref, t_ref, dt_ref, wbuf, wtail, qv, s_scr, xf, xp, xrows, xb, xt, tv, tp_recv, ct, dl, m_scr, l_scr, k_scr,
    zsend, pstat_s, pstat_r, e1s, e1r, e2s, e2r, e3s, e3r,
    in_sem, w_sem, wt_sem, q_sem, x_sem, t_sem, zs_sem, zr_sem, ps_sem, e1_sem, e2_sem, e3_sem,
):
    dp, tp = lax.axis_index("dp"), lax.axis_index("tp")
    partner = (1 - dp, tp)
    peers = [(dp, lax.rem(tp + d, 4)) for d in (1, 2, 3)]
    n_ids, width = w_ref.shape
    n_full = n_ids // TILE
    tail = n_ids - n_full * TILE
    tail_at = n_full * TILE
    last = n_full - 2 * SHARED - FIRST
    steps = FIRST + SHARED + last

    def column(i):
        in_shared = (i + steps - FIRST) // steps
        past_shared = (i + steps - FIRST - SHARED) // steps
        return pl.multiple_of((i + in_shared * dp * SHARED + past_shared * (SHARED - dp * SHARED)) * TILE, TILE)

    part = TILE // PARTS

    def tile_copies(i, slot):
        at = column(i)
        return [
            pltpu.make_async_copy(
                w_ref.at[pl.ds(at + k * part, part), :], wbuf.at[slot, pl.ds(k * part, part), :], w_sem.at[slot, k]
            )
            for k in range(PARTS)
        ]

    tail_copy = pltpu.make_async_copy(w_ref.at[pl.ds(tail_at, tail), :], wtail, wt_sem)
    q_copy = pltpu.make_async_copy(q_ref, qv, q_sem)
    small = [
        pltpu.make_async_copy(src, dst, in_sem.at[k])
        for k, (src, dst) in enumerate(((h_hbm, h_ref), (g_hbm, g_ref), (t_hbm, t_ref), (dt_hbm, dt_ref)))
    ]
    for c in small:
        c.start()
    tail_copy.start()
    for c in tile_copies(0, 0):
        c.start()

    barrier = pltpu.get_barrier_semaphore()
    for other in [partner] + peers:
        pl.semaphore_signal(barrier, inc=1, device_id=other, device_id_type=MESH)

    for c in small:
        c.wait()
    for c in tile_copies(1, 1):
        c.start()
    h = h_ref[...].astype(F32)
    inv_rms = lax.rsqrt(jnp.mean(h * h, axis=-1, keepdims=True) + 1e-5)
    xf[...] = h * inv_rms * g_ref[...][None]
    for b in range(4):
        tv[0, b : b + 1, :] = jnp.full((1, 128), 1.0, F32) / jnp.full((1, 128), t_ref[b], F32)
        for j in range(4):
            tv[1 + j, b : b + 1, :] = jnp.full((1, 128), dt_ref[b, j].astype(F32), F32)

    def lay_rows(src, t_src, at):
        xrows[...] = jnp.zeros_like(xrows)
        lane = lax.broadcasted_iota(jnp.int32, (1, 128), 1) + tp * n_ids
        for b in range(4):
            for j in range(5):
                xrows[8 * b + j : 8 * b + j + 1, :] = src[j, b : b + 1, :]
            ct[at + 8 * b : at + 8 * b + 8, :] = jnp.broadcast_to(t_src[0, b : b + 1, :], (8, 128))
            dl[at + 8 * b : at + 8 * b + 8, :] = jnp.full((8, 128), -1.0, F32)
            for j in range(4):
                dl[at + 8 * b + j : at + 8 * b + j + 1, :] = t_src[1 + j, b : b + 1, :] - lane.astype(F32)
        rows = xrows[...].astype(jnp.bfloat16)
        xb[at : at + 32, :] = rows
        for k in range(0, width, 128):
            xt[k : k + 128, at : at + 32] = xrows[:, k : k + 128].T.astype(jnp.bfloat16)

    pl.semaphore_wait(barrier, 4)
    core = lax.rem(tp, 2)
    sibling = (dp, tp + 1 - 2 * core)

    def width_half(ref, c):
        return ref.at[:, :, pl.ds(pl.multiple_of(c * (width // 2), width // 2), width // 2)]

    def x_copy(src, c, to, k):
        return pltpu.make_async_remote_copy(
            src_ref=width_half(src, c), dst_ref=width_half(xp, c), send_sem=x_sem.at[0, k], recv_sem=x_sem.at[1, k],
            device_id=to, device_id_type=MESH,
        )

    x_direct = x_copy(xf, core, partner, 0)
    x_relay = x_copy(xp, core, sibling, 1)
    t_copy = pltpu.make_async_remote_copy(
        src_ref=tv, dst_ref=tp_recv, send_sem=t_sem.at[0], recv_sem=t_sem.at[1], device_id=partner, device_id_type=MESH
    )
    x_direct.start()
    t_copy.start()

    xt[:, 32:128] = jnp.zeros((width, 96), jnp.bfloat16)
    xb[32:64, :] = jnp.zeros((32, width), jnp.bfloat16)
    lay_rows(xf, tv, 0)
    for i in range(2, SLOTS):
        for c in tile_copies(i, i):
            c.start()
    m_scr[...] = jnp.full(m_scr.shape, LOWEST, F32)
    l_scr[...] = jnp.zeros_like(l_scr)
    k_scr[...] = jnp.zeros_like(k_scr)

    def by_rows(w, depth):
        return lax.dot_general(xb[:, depth], w, (((1,), (1,)), ((), ())), preferred_element_type=F32)

    def by_ids(w, depth):
        return lax.dot_general(w, xt[depth, :], (((1,), (0,)), ((), ())), preferred_element_type=F32)

    def products(slot, lo, size):
        block = min(SUB, size // 2)
        starts = range(lo, lo + size, block)
        fixed = len(starts) // 2
        sums = [None] * len(starts)
        for k in range(0, width, DEPTH):
            depth = slice(k, k + DEPTH)
            for n, start in enumerate(starts):
                w = wbuf[slot, start : start + block, depth]
                z = by_rows(w, depth) if n < fixed else by_ids(w, depth)
                sums[n] = z if k == 0 else sums[n] + z
        pieces = []
        for n, z in enumerate(sums):
            for at in range(0, block, 128):
                pieces.append(z[:, at : at + 128] if n < fixed else z[at : at + 128, :].T[0:64])
        return pieces

    def fold(rows, parts):
        m_old = m_scr[0:rows, :]
        m_new = m_old
        for p in parts:
            m_new = jnp.maximum(m_new, p)
        total = l_scr[0:rows, :] * jnp.exp(m_old - m_new)
        for p in parts:
            total = total + jnp.exp(p - m_new)
        m_scr[0:rows, :] = m_new
        l_scr[0:rows, :] = total

    tail_copy.wait()
    s = by_rows(wtail[...], slice(0, width))[0:32] * ct[0:32, 0:tail]
    for b in range(4):
        s_scr[b, :, tail_at : tail_at + tail] = s[8 * b : 8 * b + 4, :]
    k_scr[0:32, 0:tail] = jnp.where(dl[0:32, 0:tail] == float(tail_at), s, 0.0)
    m_tail = jnp.max(s, axis=1, keepdims=True)
    l_tail = jnp.sum(jnp.exp(s - m_tail), axis=1, keepdims=True)
    lane0 = lax.broadcasted_iota(jnp.int32, (32, 128), 1) == 0
    m_scr[0:32, :] = jnp.where(lane0, m_tail, LOWEST)
    l_scr[0:32, :] = jnp.where(lane0, l_tail, 0.0)

    def z_copy(k):
        at = column(FIRST + k)
        return pltpu.make_async_remote_copy(
            src_ref=zsend.at[k], dst_ref=s_scr.at[:, :, pl.ds(at, TILE)], send_sem=zs_sem.at[k], recv_sem=zr_sem.at[k],
            device_id=partner, device_id_type=MESH,
        )

    def consume(slot, at, lo, size, rows, k):
        kept = k_scr[0:rows, :]
        parts = []
        for n, z in enumerate(products(slot, lo, size)):
            s = z[0:rows] * ct[0:rows, :]
            parts.append(s)
            off = lo + n * 128
            kept = jnp.where(dl[0:rows, :] == (at + off).astype(F32), s, kept)
            for b in range(4):
                s_scr[b, :, pl.ds(at + off, 128)] = s[8 * b : 8 * b + 4, :]
                if rows == 64:
                    zsend[k, b, :, off : off + 128] = s[32 + 8 * b : 32 + 8 * b + 4, :]
            if n % 2:
                fold(rows, parts)
                parts = []
        k_scr[0:rows, :] = kept

    def step(i, rows):
        slot = i % SLOTS
        for c in tile_copies(i, slot):
            c.wait()
        k = i - FIRST
        consume(slot, column(i), 0, TILE, rows, k)

        @pl.when(i + SLOTS < steps)
        def _():
            for c in tile_copies(i + SLOTS, slot):
                c.start()

        if rows == 64:

            @pl.when(k < SHARED - HELD)
            def _():
                z_copy(k).start()

    group = lax.broadcasted_iota(jnp.int32, (8, 128), 1) // 32

    def pack(cols):
        size = cols[0].shape[0]
        packed = jnp.broadcast_to(cols[0], (size, 128))
        for b in range(1, 4):
            packed = jnp.where(group[:size] == b, cols[b], packed)
        return packed

    def unpack(packed, b):
        size = packed.shape[0]
        lane = lax.broadcasted_iota(jnp.int32, (size, 128), 1)
        return jnp.sum(jnp.where(lane == 32 * b, packed, 0.0), axis=1, keepdims=True)

    def packed_lse(at):
        m = m_scr[at : at + 32, :]
        top = jnp.max(m, axis=1, keepdims=True)
        lse = top + jnp.log(jnp.sum(l_scr[at : at + 32, :] * jnp.exp(m - top), axis=1, keepdims=True))
        return pack([lse[8 * b : 8 * b + 8, :] for b in range(4)])

    def packed_token(at):
        kept = jnp.sum(k_scr[at : at + 32, :], axis=1, keepdims=True)
        return pack([kept[8 * b : 8 * b + 8, :] for b in range(4)])

    lax.fori_loop(0, RELAY, lambda i, _: step(i, 32), None)
    x_direct.wait()
    x_relay.start()
    lax.fori_loop(RELAY, FIRST, lambda i, _: step(i, 32), None)
    x_copy(xp, 1 - core, sibling, 1).wait_recv()
    x_relay.wait_send()
    t_copy.wait()
    lay_rows(xp, tp_recv, 32)
    lax.fori_loop(FIRST, FIRST + SHARED, lambda i, _: step(i, 64), None)
    q_copy.start()
    pstat_s[0] = packed_lse(32)
    pstat_s[1] = packed_token(32)
    stat_copy = pltpu.make_async_remote_copy(
        src_ref=pstat_s, dst_ref=pstat_r, send_sem=ps_sem.at[0], recv_sem=ps_sem.at[1],
        device_id=partner, device_id_type=MESH,
    )
    stat_copy.start()
    for k in range(SHARED - HELD, SHARED):
        z_copy(k).start()
    lax.fori_loop(FIRST + SHARED, steps - 1, lambda i, _: step(i, 32), None)
    end, slot = steps - 1, (steps - 1) % SLOTS
    copies = tile_copies(end, slot)
    for lo, size in [(k * part, part) for k in range(PARTS)]:
        for c in copies[lo // part : (lo + size) // part]:
            c.wait()
        consume(slot, column(end), lo, size, 32, 0)

    def exchange(src, dst, sem):
        return [
            pltpu.make_async_remote_copy(
                src_ref=src, dst_ref=dst.at[d], send_sem=sem.at[0, d], recv_sem=sem.at[1, d],
                device_id=peers[d], device_id_type=MESH,
            )
            for d in range(3)
        ]

    mine = packed_lse(0)
    stat_copy.wait()
    theirs = pstat_r[0]
    top = jnp.maximum(mine, theirs)
    near = top + jnp.log(jnp.exp(mine - top) + jnp.exp(theirs - top))
    e1s[...] = near
    e1 = exchange(e1s, e1r, e1_sem)
    for c in e1:
        c.start()

    own = [dl[8 * b : 8 * b + 4, :] for b in range(4)]

    row_m = [jnp.broadcast_to(unpack(near[0:4, :], b), (4, 128)) for b in range(4)]

    def prepare(at, size):
        places = [(b, at + off, min(size, 128)) for b in range(4) for off in range(0, size, 128)]
        values = [s_scr[b, :, pl.ds(a, n)] for b, a, n in places]
        values = [jnp.exp(v - row_m[b][:, :n]) for v, (b, _, n) in zip(values, places)]
        for v, (b, a, n) in zip(values, places):
            s_scr[b, :, pl.ds(a, n)] = v

    def pick(at, size, found):
        out = []
        for b in range(4):
            f = found[b]
            for off in range(0, size, 128):
                n = min(size, 128)
                f = jnp.where(own[b][:, :n] == jnp.asarray(at + off).astype(F32), qv[b, :, pl.ds(at + off, n)], f)
            out.append(f)
        return tuple(out)

    zero = jnp.zeros((4, 128), F32)
    lax.fori_loop(0, steps, lambda i, _: prepare(column(i), TILE), None)
    prepare(tail_at, tail)
    q_copy.wait()
    whole = tail_at // PASS * PASS
    found = lax.fori_loop(0, whole // PASS, lambda i, f: pick(pl.multiple_of(i * PASS, 128), PASS, f), (zero,) * 4)
    found = pick(whole, tail_at - whole, found)
    found_tail = pick(tail_at, tail, (jnp.zeros((4, tail), F32),) * 4)
    token_q = []
    for b in range(4):
        f = found_tail[b]
        token_q.append(jnp.sum(found[b], axis=1, keepdims=True) + jnp.sum(f, axis=1, keepdims=True))
    e3s[0] = (packed_token(0) + pstat_r[1])[0:4, :]
    e3s[1] = pack(token_q)
    e3 = exchange(e3s, e3r, e3_sem)
    for c in e3:
        c.start()

    def theirs_at(k):
        return pl.multiple_of((FIRST + (1 - dp) * SHARED + k) * TILE, TILE)

    def await_z(k):
        z_copy(k).wait_send()
        pltpu.make_async_remote_copy(
            src_ref=zsend.at[k], dst_ref=s_scr.at[:, :, pl.ds(theirs_at(k), TILE)],
            send_sem=zs_sem.at[k], recv_sem=zr_sem.at[k], device_id=partner, device_id_type=MESH,
        ).wait_recv()

    def take_early(k, _):
        await_z(k)
        prepare(theirs_at(k), TILE)

    lax.fori_loop(0, SHARED - LATE, take_early, None)
    for c in e1:
        c.wait()
    lses = [near] + [e1r[d] for d in range(3)]
    top = jnp.maximum(jnp.maximum(lses[0], lses[1]), jnp.maximum(lses[2], lses[3]))
    sums = jnp.exp(lses[0] - top) + jnp.exp(lses[1] - top) + jnp.exp(lses[2] - top) + jnp.exp(lses[3] - top)
    lse = top + jnp.log(sums)
    lse_ref[...] = lse
    row_l = [jnp.broadcast_to(unpack(lse[0:4, :], b), (4, 128)) for b in range(4)]
    scale = [jnp.exp(row_m[b] - row_l[b]) for b in range(4)]

    def excess(b, at, size, p):
        e = jnp.maximum(p - qv[b, :, pl.ds(at, size)], 0.0)
        ex_ref[b, :, pl.ds(at, size)] = e
        return e

    def close(at, sums, prepared):
        out = []
        for b in range(4):
            acc = sums[b]
            for off in range(0, TILE, 128):
                v = s_scr[b, :, pl.ds(at + off, 128)]
                acc = acc + excess(b, at + off, 128, v * scale[b] if prepared else jnp.exp(v - row_l[b]))
            out.append(acc)
        return tuple(out)

    def close_late(k, sums):
        await_z(k)
        return close(theirs_at(k), sums, False)

    def close_from(first, count, sums):
        return lax.fori_loop(0, count, lambda i, t: close(pl.multiple_of((first + i) * TILE, TILE), t, True), sums)

    sums = close_from(0, FIRST, (zero,) * 4)
    sums = close_from(FIRST + dp * SHARED, SHARED, sums)
    sums = close_from(FIRST + 2 * SHARED, last, sums)
    rows = []
    for b in range(4):
        e = excess(b, tail_at, tail, s_scr[b, :, tail_at : tail_at + tail] * scale[b][:, :tail])
        rows.append(jnp.sum(e, axis=1, keepdims=True))
    sums = close_from(FIRST + (1 - dp) * SHARED, SHARED - LATE, sums)
    sums = lax.fori_loop(SHARED - LATE, SHARED, close_late, sums)
    rows = [jnp.sum(sums[b], axis=1, keepdims=True) + rows[b] for b in range(4)]
    e2s[...] = pack(rows)
    e2 = exchange(e2s, e2r, e2_sem)
    for c in e2:
        c.start()

    for c in e3:
        c.wait()
    at_token = (e3s[...] + e3r[0]) + (e3r[1] + e3r[2])
    acc_ref[...] = jnp.minimum(jnp.exp(at_token[0] - lse[0:4, :]) / at_token[1], 1.0)

    for c in e2:
        c.wait()
    norm_ref[...] = (e2s[...] + e2r[0]) + (e2r[1] + e2r[2])


def finish_kernel(
    ex_ref, norm_ref, acc_ref, lse_ref, acc_out, norm_out, res_out, bonus_out, acc_v, norm_v, bonus_v, stage, sem, r_sem
):
    n_ids = ex_ref.shape[2]
    lane = lax.broadcasted_iota(jnp.int32, (4, 128), 1)
    norm = norm_ref[...]
    writes = []
    for b in range(4):
        total = jnp.sum(jnp.where(lane == 32 * b, norm, 0.0), axis=1, keepdims=True)
        scale = jnp.broadcast_to(1.0 / jnp.broadcast_to(total, (4, 128)), (4, 128))

        for at in range(0, n_ids, 128):
            size = min(128, n_ids - at)
            stage[b, :, at : at + size] = ex_ref[b, :, at : at + size] * scale[:, :size]
        writes.append(pltpu.make_async_copy(stage.at[b], res_out.at[b], r_sem.at[b]))
        writes[-1].start()

    sub = lax.broadcasted_iota(jnp.int32, (4, 128), 0)
    for src, dst, out, k in ((acc_ref[...], acc_v, acc_out, 0), (norm, norm_v, norm_out, 1)):
        row = jnp.sum(jnp.where(lane % 32 == sub, src, 0.0), axis=0, keepdims=True)
        for b in range(4):
            dst[b : b + 1, :] = (row if b == 0 else pltpu.roll(row, 128 - 32 * b, 1))[:, 0:4]
        writes.append(pltpu.make_async_copy(dst, out, sem.at[k]))
        writes[-1].start()
    row = lse_ref[4:5, :]
    lane = lane[0:1, :]
    packed = row
    for b in range(1, 4):
        packed = jnp.where(lane == b, pltpu.roll(row, 128 - 31 * b, 1), packed)
    bonus_v[...] = packed[:, 0:4]
    writes.append(pltpu.make_async_copy(bonus_v, bonus_out, sem.at[2]))
    writes[-1].start()
    for c in writes:
        c.wait()


def solution(mesh):
    def local_step(hidden, norm_gain, w_head, draft_probs, draft_tokens, temperature):
        n_ids = w_head.shape[1]
        width = w_head.shape[0]
        pad_ids = -(-n_ids // 128) * 128
        tail = n_ids % TILE
        vmem, smem, hbm = pltpu.VMEM, pltpu.SMEM, pltpu.HBM
        dma = pltpu.SemaphoreType.DMA
        ex, norm, acc, lse = pl.pallas_call(
            verify_kernel,
            out_shape=[vmem((4, 4, n_ids), F32), vmem((4, 128), F32), vmem((4, 128), F32), vmem((8, 128), F32)],
            in_specs=[pl.BlockSpec(memory_space=s) for s in (hbm,) * 6],
            out_specs=[pl.BlockSpec(memory_space=vmem)] * 4,
            scratch_shapes=[
                vmem((5, 4, width), jnp.bfloat16),
                vmem((1, width), F32),
                smem((4,), F32),
                smem((4, 4), jnp.int32),
                vmem((SLOTS, TILE, width), jnp.bfloat16),
                vmem((tail, width), jnp.bfloat16),
                vmem((4, 4, n_ids), F32),
                vmem((4, 4, pad_ids), F32),
                vmem((5, 4, width), F32),
                vmem((5, 4, width), F32),
                vmem((32, width), F32),
                vmem((64, width), jnp.bfloat16),
                vmem((width, 128), jnp.bfloat16),
                vmem((5, 4, 128), F32),
                vmem((5, 4, 128), F32),
                vmem((64, 128), F32),
                vmem((64, 128), F32),
                vmem((64, 128), F32),
                vmem((64, 128), F32),
                vmem((64, 128), F32),
                vmem((SHARED, 4, 4, TILE), F32),
                vmem((2, 8, 128), F32),
                vmem((2, 8, 128), F32),
                vmem((8, 128), F32),
                vmem((3, 8, 128), F32),
                vmem((4, 128), F32),
                vmem((3, 4, 128), F32),
                vmem((2, 4, 128), F32),
                vmem((3, 2, 4, 128), F32),
                dma((4,)), dma((SLOTS, PARTS)), dma, dma, dma((2, 2)), dma((2,)), dma((SHARED,)), dma((SHARED,)), dma((2,)),
                dma((2, 3)), dma((2, 3)), dma((2, 3)),
            ],
            compiler_params=pltpu.CompilerParams(collective_id=0, has_side_effects=True),
            name="verify",
        )(
            hidden.transpose(1, 0, 2), norm_gain.reshape(1, width), temperature, draft_tokens,
            w_head.T, draft_probs,
        )
        acc, norm, residual, bonus = pl.pallas_call(
            finish_kernel,
            out_shape=[
                jax.ShapeDtypeStruct((4, 4), F32),
                jax.ShapeDtypeStruct((4, 4), F32),
                jax.ShapeDtypeStruct((4, 4, n_ids), F32),
                jax.ShapeDtypeStruct((1, 4), F32),
            ],
            in_specs=[pl.BlockSpec(memory_space=vmem)] * 4,
            out_specs=[pl.BlockSpec(memory_space=hbm)] * 4,
            scratch_shapes=[
                vmem((4, 4), F32), vmem((4, 4), F32), vmem((1, 4), F32), vmem((4, 4, n_ids), F32), dma((3,)), dma((4,)),
            ],
            compiler_params=pltpu.CompilerParams(vmem_limit_bytes=16 * 1024 * 1024),
            name="finish",
        )(ex, norm, acc, lse)
        return acc, norm, residual, bonus.reshape(4)

    return jax.shard_map(
        local_step,
        mesh=mesh,
        in_specs=(P("dp", None, None), P(), P(None, "tp"), P("dp", None, "tp"), P("dp", None), P("dp")),
        out_specs=(P("dp", None), P("dp", None), P("dp", None, "tp"), P("dp")),
        check_vma=False,
    )
```

```python
import jax
import jax.numpy as jnp
from jax import lax
from jax.experimental import pallas as pl
from jax.experimental.pallas import tpu as pltpu
from jax.sharding import PartitionSpec as P

MESH = pl.DeviceIdType.MESH
F32 = jnp.float32
LOWEST = float(jnp.finfo(jnp.float32).min)

TILE = 1024
SUB = 256
DEPTH = 256
SLOTS = 3
SHARED = 16
FIRST = 4
LATE = 6
HELD = 3
RELAY = 3
PARTS = 1
PASS = 2048


def verify_kernel(
    h_hbm, g_hbm, t_hbm, dt_hbm, w_ref, q_ref,
    ex_ref, norm_ref, acc_ref, lse_ref,
    h_ref, g_ref, t_ref, dt_ref, wbuf, wtail, qv, s_scr, xf, xp, xrows, xb, xt, tv, tp_recv, ct, dl, m_scr, l_scr, k_scr,
    zsend, pstat_s, pstat_r, e1s, e1r, e2s, e2r, e3s, e3r,
    in_sem, w_sem, wt_sem, q_sem, x_sem, t_sem, zs_sem, zr_sem, ps_sem, e1_sem, e2_sem, e3_sem,
):
    dp, tp = lax.axis_index("dp"), lax.axis_index("tp")
    partner = (1 - dp, tp)
    peers = [(dp, lax.rem(tp + d, 4)) for d in (1, 2, 3)]
    n_ids, width = w_ref.shape
    n_full = n_ids // TILE
    tail = n_ids - n_full * TILE
    tail_at = n_full * TILE
    last = n_full - 2 * SHARED - FIRST
    steps = FIRST + SHARED + last

    def column(i):
        in_shared = (i + steps - FIRST) // steps
        past_shared = (i + steps - FIRST - SHARED) // steps
        return pl.multiple_of((i + in_shared * dp * SHARED + past_shared * (SHARED - dp * SHARED)) * TILE, TILE)

    part = TILE // PARTS

    def tile_copies(i, slot):
        at = column(i)
        return [
            pltpu.make_async_copy(
                w_ref.at[pl.ds(at + k * part, part), :], wbuf.at[slot, pl.ds(k * part, part), :], w_sem.at[slot, k]
            )
            for k in range(PARTS)
        ]

    tail_copy = pltpu.make_async_copy(w_ref.at[pl.ds(tail_at, tail), :], wtail, wt_sem)
    q_copy = pltpu.make_async_copy(q_ref, qv, q_sem)
    small = [
        pltpu.make_async_copy(src, dst, in_sem.at[k])
        for k, (src, dst) in enumerate(((h_hbm, h_ref), (g_hbm, g_ref), (t_hbm, t_ref), (dt_hbm, dt_ref)))
    ]
    for c in small:
        c.start()
    tail_copy.start()
    for c in tile_copies(0, 0):
        c.start()

    barrier = pltpu.get_barrier_semaphore()
    for other in [partner] + peers:
        pl.semaphore_signal(barrier, inc=1, device_id=other, device_id_type=MESH)

    for c in small:
        c.wait()
    for c in tile_copies(1, 1):
        c.start()
    h = h_ref[...].astype(F32)
    inv_rms = lax.rsqrt(jnp.mean(h * h, axis=-1, keepdims=True) + 1e-5)
    xf[...] = h * inv_rms * g_ref[...][None]
    for b in range(4):
        tv[0, b : b + 1, :] = jnp.full((1, 128), 1.0, F32) / jnp.full((1, 128), t_ref[b], F32)
        for j in range(4):
            tv[1 + j, b : b + 1, :] = jnp.full((1, 128), dt_ref[b, j].astype(F32), F32)

    def lay_rows(src, t_src, at):
        xrows[...] = jnp.zeros_like(xrows)
        lane = lax.broadcasted_iota(jnp.int32, (1, 128), 1) + tp * n_ids
        for b in range(4):
            for j in range(5):
                xrows[8 * b + j : 8 * b + j + 1, :] = src[j, b : b + 1, :]
            ct[at + 8 * b : at + 8 * b + 8, :] = jnp.broadcast_to(t_src[0, b : b + 1, :], (8, 128))
            dl[at + 8 * b : at + 8 * b + 8, :] = jnp.full((8, 128), -1.0, F32)
            for j in range(4):
                dl[at + 8 * b + j : at + 8 * b + j + 1, :] = t_src[1 + j, b : b + 1, :] - lane.astype(F32)
        rows = xrows[...].astype(jnp.bfloat16)
        xb[at : at + 32, :] = rows
        for k in range(0, width, 128):
            xt[k : k + 128, at : at + 32] = xrows[:, k : k + 128].T.astype(jnp.bfloat16)

    pl.semaphore_wait(barrier, 4)
    core = lax.rem(tp, 2)
    sibling = (dp, tp + 1 - 2 * core)

    def width_half(ref, c):
        return ref.at[:, :, pl.ds(pl.multiple_of(c * (width // 2), width // 2), width // 2)]

    def x_copy(src, c, to, k):
        return pltpu.make_async_remote_copy(
            src_ref=width_half(src, c), dst_ref=width_half(xp, c), send_sem=x_sem.at[0, k], recv_sem=x_sem.at[1, k],
            device_id=to, device_id_type=MESH,
        )

    x_direct = x_copy(xf, core, partner, 0)
    x_relay = x_copy(xp, core, sibling, 1)
    t_copy = pltpu.make_async_remote_copy(
        src_ref=tv, dst_ref=tp_recv, send_sem=t_sem.at[0], recv_sem=t_sem.at[1], device_id=partner, device_id_type=MESH
    )
    x_direct.start()
    t_copy.start()

    xt[:, 32:128] = jnp.zeros((width, 96), jnp.bfloat16)
    xb[32:64, :] = jnp.zeros((32, width), jnp.bfloat16)
    lay_rows(xf, tv, 0)
    for i in range(2, SLOTS):
        for c in tile_copies(i, i):
            c.start()
    m_scr[...] = jnp.full(m_scr.shape, LOWEST, F32)
    l_scr[...] = jnp.zeros_like(l_scr)
    k_scr[...] = jnp.zeros_like(k_scr)

    def by_rows(w, depth):
        return lax.dot_general(xb[:, depth], w, (((1,), (1,)), ((), ())), preferred_element_type=F32)

    def by_ids(w, depth):
        return lax.dot_general(w, xt[depth, :], (((1,), (0,)), ((), ())), preferred_element_type=F32)

    def products(slot, lo, size):
        block = min(SUB, size // 2)
        starts = range(lo, lo + size, block)
        fixed = len(starts) // 2
        sums = [None] * len(starts)
        for k in range(0, width, DEPTH):
            depth = slice(k, k + DEPTH)
            for n, start in enumerate(starts):
                w = wbuf[slot, start : start + block, depth]
                z = by_rows(w, depth) if n < fixed else by_ids(w, depth)
                sums[n] = z if k == 0 else sums[n] + z
        pieces = []
        for n, z in enumerate(sums):
            for at in range(0, block, 128):
                pieces.append(z[:, at : at + 128] if n < fixed else z[at : at + 128, :].T[0:64])
        return pieces

    def fold(rows, parts):
        m_old = m_scr[0:rows, :]
        m_new = m_old
        for p in parts:
            m_new = jnp.maximum(m_new, p)
        total = l_scr[0:rows, :] * jnp.exp(m_old - m_new)
        for p in parts:
            total = total + jnp.exp(p - m_new)
        m_scr[0:rows, :] = m_new
        l_scr[0:rows, :] = total

    tail_copy.wait()
    s = by_rows(wtail[...], slice(0, width))[0:32] * ct[0:32, 0:tail]
    for b in range(4):
        s_scr[b, :, tail_at : tail_at + tail] = s[8 * b : 8 * b + 4, :]
    k_scr[0:32, 0:tail] = jnp.where(dl[0:32, 0:tail] == float(tail_at), s, 0.0)
    m_tail = jnp.max(s, axis=1, keepdims=True)
    l_tail = jnp.sum(jnp.exp(s - m_tail), axis=1, keepdims=True)
    lane0 = lax.broadcasted_iota(jnp.int32, (32, 128), 1) == 0
    m_scr[0:32, :] = jnp.where(lane0, m_tail, LOWEST)
    l_scr[0:32, :] = jnp.where(lane0, l_tail, 0.0)

    def z_copy(k):
        at = column(FIRST + k)
        return pltpu.make_async_remote_copy(
            src_ref=zsend.at[k], dst_ref=s_scr.at[:, :, pl.ds(at, TILE)], send_sem=zs_sem.at[k], recv_sem=zr_sem.at[k],
            device_id=partner, device_id_type=MESH,
        )

    def consume(slot, at, lo, size, rows, k):
        kept = k_scr[0:rows, :]
        parts = []
        for n, z in enumerate(products(slot, lo, size)):
            s = z[0:rows] * ct[0:rows, :]
            parts.append(s)
            off = lo + n * 128
            kept = jnp.where(dl[0:rows, :] == (at + off).astype(F32), s, kept)
            for b in range(4):
                s_scr[b, :, pl.ds(at + off, 128)] = s[8 * b : 8 * b + 4, :]
                if rows == 64:
                    zsend[k, b, :, off : off + 128] = s[32 + 8 * b : 32 + 8 * b + 4, :]
            if n % 2:
                fold(rows, parts)
                parts = []
        k_scr[0:rows, :] = kept

    def step(i, rows):
        slot = i % SLOTS
        for c in tile_copies(i, slot):
            c.wait()
        k = i - FIRST
        consume(slot, column(i), 0, TILE, rows, k)

        @pl.when(i + SLOTS < steps)
        def _():
            for c in tile_copies(i + SLOTS, slot):
                c.start()

        if rows == 64:

            @pl.when(k < SHARED - HELD)
            def _():
                z_copy(k).start()

    group = lax.broadcasted_iota(jnp.int32, (8, 128), 1) // 32

    def pack(cols):
        size = cols[0].shape[0]
        packed = jnp.broadcast_to(cols[0], (size, 128))
        for b in range(1, 4):
            packed = jnp.where(group[:size] == b, cols[b], packed)
        return packed

    def unpack(packed, b):
        size = packed.shape[0]
        lane = lax.broadcasted_iota(jnp.int32, (size, 128), 1)
        return jnp.sum(jnp.where(lane == 32 * b, packed, 0.0), axis=1, keepdims=True)

    def packed_lse(at):
        m = m_scr[at : at + 32, :]
        top = jnp.max(m, axis=1, keepdims=True)
        lse = top + jnp.log(jnp.sum(l_scr[at : at + 32, :] * jnp.exp(m - top), axis=1, keepdims=True))
        return pack([lse[8 * b : 8 * b + 8, :] for b in range(4)])

    def packed_token(at):
        kept = jnp.sum(k_scr[at : at + 32, :], axis=1, keepdims=True)
        return pack([kept[8 * b : 8 * b + 8, :] for b in range(4)])

    lax.fori_loop(0, RELAY, lambda i, _: step(i, 32), None)
    x_direct.wait()
    x_relay.start()
    lax.fori_loop(RELAY, FIRST, lambda i, _: step(i, 32), None)
    x_copy(xp, 1 - core, sibling, 1).wait_recv()
    x_relay.wait_send()
    t_copy.wait()
    lay_rows(xp, tp_recv, 32)
    lax.fori_loop(FIRST, FIRST + SHARED, lambda i, _: step(i, 64), None)
    q_copy.start()
    pstat_s[0] = packed_lse(32)
    pstat_s[1] = packed_token(32)
    stat_copy = pltpu.make_async_remote_copy(
        src_ref=pstat_s, dst_ref=pstat_r, send_sem=ps_sem.at[0], recv_sem=ps_sem.at[1],
        device_id=partner, device_id_type=MESH,
    )
    stat_copy.start()
    for k in range(SHARED - HELD, SHARED):
        z_copy(k).start()
    lax.fori_loop(FIRST + SHARED, steps - 1, lambda i, _: step(i, 32), None)
    end, slot = steps - 1, (steps - 1) % SLOTS
    copies = tile_copies(end, slot)
    for lo, size in [(k * part, part) for k in range(PARTS)]:
        for c in copies[lo // part : (lo + size) // part]:
            c.wait()
        consume(slot, column(end), lo, size, 32, 0)

    def exchange(src, dst, sem):
        return [
            pltpu.make_async_remote_copy(
                src_ref=src, dst_ref=dst.at[d], send_sem=sem.at[0, d], recv_sem=sem.at[1, d],
                device_id=peers[d], device_id_type=MESH,
            )
            for d in range(3)
        ]

    mine = packed_lse(0)
    stat_copy.wait()
    theirs = pstat_r[0]
    top = jnp.maximum(mine, theirs)
    near = top + jnp.log(jnp.exp(mine - top) + jnp.exp(theirs - top))
    e1s[...] = near
    e1 = exchange(e1s, e1r, e1_sem)
    for c in e1:
        c.start()

    own = [dl[8 * b : 8 * b + 4, :] for b in range(4)]

    row_m = [jnp.broadcast_to(unpack(near[0:4, :], b), (4, 128)) for b in range(4)]

    def prepare(at, size):
        places = [(b, at + off, min(size, 128)) for b in range(4) for off in range(0, size, 128)]
        values = [s_scr[b, :, pl.ds(a, n)] for b, a, n in places]
        values = [jnp.exp(v - row_m[b][:, :n]) for v, (b, _, n) in zip(values, places)]
        for v, (b, a, n) in zip(values, places):
            s_scr[b, :, pl.ds(a, n)] = v

    def pick(at, size, found):
        out = []
        for b in range(4):
            f = found[b]
            for off in range(0, size, 128):
                n = min(size, 128)
                f = jnp.where(own[b][:, :n] == jnp.asarray(at + off).astype(F32), qv[b, :, pl.ds(at + off, n)], f)
            out.append(f)
        return tuple(out)

    zero = jnp.zeros((4, 128), F32)
    lax.fori_loop(0, steps, lambda i, _: prepare(column(i), TILE), None)
    prepare(tail_at, tail)
    q_copy.wait()
    whole = tail_at // PASS * PASS
    found = lax.fori_loop(0, whole // PASS, lambda i, f: pick(pl.multiple_of(i * PASS, 128), PASS, f), (zero,) * 4)
    found = pick(whole, tail_at - whole, found)
    found_tail = pick(tail_at, tail, (jnp.zeros((4, tail), F32),) * 4)
    token_q = []
    for b in range(4):
        f = found_tail[b]
        token_q.append(jnp.sum(found[b], axis=1, keepdims=True) + jnp.sum(f, axis=1, keepdims=True))
    e3s[0] = (packed_token(0) + pstat_r[1])[0:4, :]
    e3s[1] = pack(token_q)
    e3 = exchange(e3s, e3r, e3_sem)
    for c in e3:
        c.start()

    def theirs_at(k):
        return pl.multiple_of((FIRST + (1 - dp) * SHARED + k) * TILE, TILE)

    def await_z(k):
        z_copy(k).wait_send()
        pltpu.make_async_remote_copy(
            src_ref=zsend.at[k], dst_ref=s_scr.at[:, :, pl.ds(theirs_at(k), TILE)],
            send_sem=zs_sem.at[k], recv_sem=zr_sem.at[k], device_id=partner, device_id_type=MESH,
        ).wait_recv()

    def take_early(k, _):
        await_z(k)
        prepare(theirs_at(k), TILE)

    lax.fori_loop(0, SHARED - LATE, take_early, None)
    for c in e1:
        c.wait()
    lses = [near] + [e1r[d] for d in range(3)]
    top = jnp.maximum(jnp.maximum(lses[0], lses[1]), jnp.maximum(lses[2], lses[3]))
    sums = jnp.exp(lses[0] - top) + jnp.exp(lses[1] - top) + jnp.exp(lses[2] - top) + jnp.exp(lses[3] - top)
    lse = top + jnp.log(sums)
    lse_ref[...] = lse
    row_l = [jnp.broadcast_to(unpack(lse[0:4, :], b), (4, 128)) for b in range(4)]
    scale = [jnp.exp(row_m[b] - row_l[b]) for b in range(4)]

    def excess(b, at, size, p):
        e = jnp.maximum(p - qv[b, :, pl.ds(at, size)], 0.0)
        ex_ref[b, :, pl.ds(at, size)] = e
        return e

    def close(at, sums, prepared):
        out = []
        for b in range(4):
            acc = sums[b]
            for off in range(0, TILE, 128):
                v = s_scr[b, :, pl.ds(at + off, 128)]
                acc = acc + excess(b, at + off, 128, v * scale[b] if prepared else jnp.exp(v - row_l[b]))
            out.append(acc)
        return tuple(out)

    def close_late(k, sums):
        await_z(k)
        return close(theirs_at(k), sums, False)

    def close_from(first, count, sums):
        return lax.fori_loop(0, count, lambda i, t: close(pl.multiple_of((first + i) * TILE, TILE), t, True), sums)

    sums = close_from(0, FIRST, (zero,) * 4)
    sums = close_from(FIRST + dp * SHARED, SHARED, sums)
    sums = close_from(FIRST + 2 * SHARED, last, sums)
    rows = []
    for b in range(4):
        e = excess(b, tail_at, tail, s_scr[b, :, tail_at : tail_at + tail] * scale[b][:, :tail])
        rows.append(jnp.sum(e, axis=1, keepdims=True))
    sums = close_from(FIRST + (1 - dp) * SHARED, SHARED - LATE, sums)
    sums = lax.fori_loop(SHARED - LATE, SHARED, close_late, sums)
    rows = [jnp.sum(sums[b], axis=1, keepdims=True) + rows[b] for b in range(4)]
    e2s[...] = pack(rows)
    e2 = exchange(e2s, e2r, e2_sem)
    for c in e2:
        c.start()

    for c in e3:
        c.wait()
    at_token = (e3s[...] + e3r[0]) + (e3r[1] + e3r[2])
    acc_ref[...] = jnp.minimum(jnp.exp(at_token[0] - lse[0:4, :]) / at_token[1], 1.0)

    for c in e2:
        c.wait()
    norm_ref[...] = (e2s[...] + e2r[0]) + (e2r[1] + e2r[2])


def finish_kernel(
    ex_ref, norm_ref, acc_ref, lse_ref, acc_out, norm_out, res_out, bonus_out, acc_v, norm_v, bonus_v, stage, sem, r_sem
):
    n_ids = ex_ref.shape[2]
    lane = lax.broadcasted_iota(jnp.int32, (4, 128), 1)
    norm = norm_ref[...]
    writes = []
    for b in range(4):
        total = jnp.sum(jnp.where(lane == 32 * b, norm, 0.0), axis=1, keepdims=True)
        scale = jnp.broadcast_to(1.0 / jnp.broadcast_to(total, (4, 128)), (4, 128))

        for at in range(0, n_ids, 128):
            size = min(128, n_ids - at)
            stage[b, :, at : at + size] = ex_ref[b, :, at : at + size] * scale[:, :size]
        writes.append(pltpu.make_async_copy(stage.at[b], res_out.at[b], r_sem.at[b]))
        writes[-1].start()

    sub = lax.broadcasted_iota(jnp.int32, (4, 128), 0)
    for src, dst, out, k in ((acc_ref[...], acc_v, acc_out, 0), (norm, norm_v, norm_out, 1)):
        row = jnp.sum(jnp.where(lane % 32 == sub, src, 0.0), axis=0, keepdims=True)
        for b in range(4):
            dst[b : b + 1, :] = (row if b == 0 else pltpu.roll(row, 128 - 32 * b, 1))[:, 0:4]
        writes.append(pltpu.make_async_copy(dst, out, sem.at[k]))
        writes[-1].start()
    row = lse_ref[4:5, :]
    lane = lane[0:1, :]
    packed = row
    for b in range(1, 4):
        packed = jnp.where(lane == b, pltpu.roll(row, 128 - 31 * b, 1), packed)
    bonus_v[...] = packed[:, 0:4]
    writes.append(pltpu.make_async_copy(bonus_v, bonus_out, sem.at[2]))
    writes[-1].start()
    for c in writes:
        c.wait()


def solution(mesh):
    def local_step(hidden, norm_gain, w_head, draft_probs, draft_tokens, temperature):
        n_ids = w_head.shape[1]
        width = w_head.shape[0]
        pad_ids = -(-n_ids // 128) * 128
        tail = n_ids % TILE
        vmem, smem, hbm = pltpu.VMEM, pltpu.SMEM, pltpu.HBM
        dma = pltpu.SemaphoreType.DMA
        ex, norm, acc, lse = pl.pallas_call(
            verify_kernel,
            out_shape=[vmem((4, 4, n_ids), F32), vmem((4, 128), F32), vmem((4, 128), F32), vmem((8, 128), F32)],
            in_specs=[pl.BlockSpec(memory_space=s) for s in (hbm,) * 6],
            out_specs=[pl.BlockSpec(memory_space=vmem)] * 4,
            scratch_shapes=[
                vmem((5, 4, width), jnp.bfloat16),
                vmem((1, width), F32),
                smem((4,), F32),
                smem((4, 4), jnp.int32),
                vmem((SLOTS, TILE, width), jnp.bfloat16),
                vmem((tail, width), jnp.bfloat16),
                vmem((4, 4, n_ids), F32),
                vmem((4, 4, pad_ids), F32),
                vmem((5, 4, width), F32),
                vmem((5, 4, width), F32),
                vmem((32, width), F32),
                vmem((64, width), jnp.bfloat16),
                vmem((width, 128), jnp.bfloat16),
                vmem((5, 4, 128), F32),
                vmem((5, 4, 128), F32),
                vmem((64, 128), F32),
                vmem((64, 128), F32),
                vmem((64, 128), F32),
                vmem((64, 128), F32),
                vmem((64, 128), F32),
                vmem((SHARED, 4, 4, TILE), F32),
                vmem((2, 8, 128), F32),
                vmem((2, 8, 128), F32),
                vmem((8, 128), F32),
                vmem((3, 8, 128), F32),
                vmem((4, 128), F32),
                vmem((3, 4, 128), F32),
                vmem((2, 4, 128), F32),
                vmem((3, 2, 4, 128), F32),
                dma((4,)), dma((SLOTS, PARTS)), dma, dma, dma((2, 2)), dma((2,)), dma((SHARED,)), dma((SHARED,)), dma((2,)),
                dma((2, 3)), dma((2, 3)), dma((2, 3)),
            ],
            compiler_params=pltpu.CompilerParams(collective_id=0, has_side_effects=True),
            name="verify",
        )(
            hidden.transpose(1, 0, 2), norm_gain.reshape(1, width), temperature, draft_tokens,
            w_head.T, draft_probs,
        )
        acc, norm, residual, bonus = pl.pallas_call(
            finish_kernel,
            out_shape=[
                jax.ShapeDtypeStruct((4, 4), F32),
                jax.ShapeDtypeStruct((4, 4), F32),
                jax.ShapeDtypeStruct((4, 4, n_ids), F32),
                jax.ShapeDtypeStruct((1, 4), F32),
            ],
            in_specs=[pl.BlockSpec(memory_space=vmem)] * 4,
            out_specs=[pl.BlockSpec(memory_space=hbm)] * 4,
            scratch_shapes=[
                vmem((4, 4), F32), vmem((4, 4), F32), vmem((1, 4), F32), vmem((4, 4, n_ids), F32), dma((3,)), dma((4,)),
            ],
            compiler_params=pltpu.CompilerParams(vmem_limit_bytes=16 * 1024 * 1024),
            name="finish",
        )(ex, norm, acc, lse)
        return acc, norm, residual, bonus.reshape(4)

    return jax.shard_map(
        local_step,
        mesh=mesh,
        in_specs=(P("dp", None, None), P(), P(None, "tp"), P("dp", None, "tp"), P("dp", None), P("dp")),
        out_specs=(P("dp", None), P("dp", None), P("dp", None, "tp"), P("dp")),
        check_vma=False,
    )
```

```python
import jax
import jax.numpy as jnp
from jax import lax
from jax.experimental import pallas as pl
from jax.experimental.pallas import tpu as pltpu
from jax.sharding import PartitionSpec as P

MESH = pl.DeviceIdType.MESH
F32 = jnp.float32
LOWEST = float(jnp.finfo(jnp.float32).min)

TILE = 1024
SUB = 256
DEPTH = 256
SLOTS = 3
SHARED = 15
FIRST = 4
LATE = 5
HELD = 2
RELAY = 3
PARTS = 2
PASS = 2048


def verify_kernel(
    h_hbm, g_hbm, t_hbm, dt_hbm, w_ref, q_ref,
    ex_ref, norm_ref, acc_ref, lse_ref,
    h_ref, g_ref, t_ref, dt_ref, wbuf, wtail, qv, s_scr, xf, xp, xrows, xb, xt, tv, tp_recv, ct, dl, m_scr, l_scr, k_scr,
    zsend, pstat_s, pstat_r, e1s, e1r, e2s, e2r, e3s, e3r,
    in_sem, w_sem, wt_sem, q_sem, x_sem, t_sem, zs_sem, zr_sem, ps_sem, e1_sem, e2_sem, e3_sem,
):
    dp, tp = lax.axis_index("dp"), lax.axis_index("tp")
    partner = (1 - dp, tp)
    peers = [(dp, lax.rem(tp + d, 4)) for d in (1, 2, 3)]
    n_ids, width = w_ref.shape
    n_full = n_ids // TILE
    tail = n_ids - n_full * TILE
    tail_at = n_full * TILE
    last = n_full - 2 * SHARED - FIRST
    steps = FIRST + SHARED + last

    def column(i):
        in_shared = (i + steps - FIRST) // steps
        past_shared = (i + steps - FIRST - SHARED) // steps
        return pl.multiple_of((i + in_shared * dp * SHARED + past_shared * (SHARED - dp * SHARED)) * TILE, TILE)

    part = TILE // PARTS

    def tile_copies(i, slot):
        at = column(i)
        return [
            pltpu.make_async_copy(
                w_ref.at[pl.ds(at + k * part, part), :], wbuf.at[slot, pl.ds(k * part, part), :], w_sem.at[slot, k]
            )
            for k in range(PARTS)
        ]

    tail_copy = pltpu.make_async_copy(w_ref.at[pl.ds(tail_at, tail), :], wtail, wt_sem)
    q_copy = pltpu.make_async_copy(q_ref, qv, q_sem)
    small = [
        pltpu.make_async_copy(src, dst, in_sem.at[k])
        for k, (src, dst) in enumerate(((h_hbm, h_ref), (g_hbm, g_ref), (t_hbm, t_ref), (dt_hbm, dt_ref)))
    ]
    for c in small:
        c.start()
    tail_copy.start()
    for c in tile_copies(0, 0):
        c.start()

    barrier = pltpu.get_barrier_semaphore()
    for other in [partner] + peers:
        pl.semaphore_signal(barrier, inc=1, device_id=other, device_id_type=MESH)

    for c in small:
        c.wait()
    for c in tile_copies(1, 1):
        c.start()
    h = h_ref[...].astype(F32)
    inv_rms = lax.rsqrt(jnp.mean(h * h, axis=-1, keepdims=True) + 1e-5)
    xf[...] = h * inv_rms * g_ref[...][None]
    for b in range(4):
        tv[0, b : b + 1, :] = jnp.full((1, 128), 1.0, F32) / jnp.full((1, 128), t_ref[b], F32)
        for j in range(4):
            tv[1 + j, b : b + 1, :] = jnp.full((1, 128), dt_ref[b, j].astype(F32), F32)

    def lay_rows(src, t_src, at):
        xrows[...] = jnp.zeros_like(xrows)
        lane = lax.broadcasted_iota(jnp.int32, (1, 128), 1) + tp * n_ids
        for b in range(4):
            for j in range(5):
                xrows[8 * b + j : 8 * b + j + 1, :] = src[j, b : b + 1, :]
            ct[at + 8 * b : at + 8 * b + 8, :] = jnp.broadcast_to(t_src[0, b : b + 1, :], (8, 128))
            dl[at + 8 * b : at + 8 * b + 8, :] = jnp.full((8, 128), -1.0, F32)
            for j in range(4):
                dl[at + 8 * b + j : at + 8 * b + j + 1, :] = t_src[1 + j, b : b + 1, :] - lane.astype(F32)
        rows = xrows[...].astype(jnp.bfloat16)
        xb[at : at + 32, :] = rows
        for k in range(0, width, 128):
            xt[k : k + 128, at : at + 32] = xrows[:, k : k + 128].T.astype(jnp.bfloat16)

    pl.semaphore_wait(barrier, 4)
    core = lax.rem(tp, 2)
    sibling = (dp, tp + 1 - 2 * core)

    def width_half(ref, c):
        return ref.at[:, :, pl.ds(pl.multiple_of(c * (width // 2), width // 2), width // 2)]

    def x_copy(src, c, to, k):
        return pltpu.make_async_remote_copy(
            src_ref=width_half(src, c), dst_ref=width_half(xp, c), send_sem=x_sem.at[0, k], recv_sem=x_sem.at[1, k],
            device_id=to, device_id_type=MESH,
        )

    x_direct = x_copy(xf, core, partner, 0)
    x_relay = x_copy(xp, core, sibling, 1)
    t_copy = pltpu.make_async_remote_copy(
        src_ref=tv, dst_ref=tp_recv, send_sem=t_sem.at[0], recv_sem=t_sem.at[1], device_id=partner, device_id_type=MESH
    )
    x_direct.start()
    t_copy.start()

    xt[:, 32:128] = jnp.zeros((width, 96), jnp.bfloat16)
    xb[32:64, :] = jnp.zeros((32, width), jnp.bfloat16)
    lay_rows(xf, tv, 0)
    for i in range(2, SLOTS):
        for c in tile_copies(i, i):
            c.start()
    m_scr[...] = jnp.full(m_scr.shape, LOWEST, F32)
    l_scr[...] = jnp.zeros_like(l_scr)
    k_scr[...] = jnp.zeros_like(k_scr)

    def by_rows(w, depth):
        return lax.dot_general(xb[:, depth], w, (((1,), (1,)), ((), ())), preferred_element_type=F32)

    def by_ids(w, depth):
        return lax.dot_general(w, xt[depth, :], (((1,), (0,)), ((), ())), preferred_element_type=F32)

    def products(slot, lo, size):
        block = min(SUB, size // 2)
        starts = range(lo, lo + size, block)
        fixed = len(starts) // 2
        sums = [None] * len(starts)
        for k in range(0, width, DEPTH):
            depth = slice(k, k + DEPTH)
            for n, start in enumerate(starts):
                w = wbuf[slot, start : start + block, depth]
                z = by_rows(w, depth) if n < fixed else by_ids(w, depth)
                sums[n] = z if k == 0 else sums[n] + z
        pieces = []
        for n, z in enumerate(sums):
            for at in range(0, block, 128):
                pieces.append(z[:, at : at + 128] if n < fixed else z[at : at + 128, :].T[0:64])
        return pieces

    def fold(rows, parts):
        m_old = m_scr[0:rows, :]
        m_new = m_old
        for p in parts:
            m_new = jnp.maximum(m_new, p)
        total = l_scr[0:rows, :] * jnp.exp(m_old - m_new)
        for p in parts:
            total = total + jnp.exp(p - m_new)
        m_scr[0:rows, :] = m_new
        l_scr[0:rows, :] = total

    tail_copy.wait()
    s = by_rows(wtail[...], slice(0, width))[0:32] * ct[0:32, 0:tail]
    for b in range(4):
        s_scr[b, :, tail_at : tail_at + tail] = s[8 * b : 8 * b + 4, :]
    k_scr[0:32, 0:tail] = jnp.where(dl[0:32, 0:tail] == float(tail_at), s, 0.0)
    m_tail = jnp.max(s, axis=1, keepdims=True)
    l_tail = jnp.sum(jnp.exp(s - m_tail), axis=1, keepdims=True)
    lane0 = lax.broadcasted_iota(jnp.int32, (32, 128), 1) == 0
    m_scr[0:32, :] = jnp.where(lane0, m_tail, LOWEST)
    l_scr[0:32, :] = jnp.where(lane0, l_tail, 0.0)

    def z_copy(k):
        at = column(FIRST + k)
        return pltpu.make_async_remote_copy(
            src_ref=zsend.at[k], dst_ref=s_scr.at[:, :, pl.ds(at, TILE)], send_sem=zs_sem.at[k], recv_sem=zr_sem.at[k],
            device_id=partner, device_id_type=MESH,
        )

    def consume(slot, at, lo, size, rows, k):
        kept = k_scr[0:rows, :]
        parts = []
        for n, z in enumerate(products(slot, lo, size)):
            s = z[0:rows] * ct[0:rows, :]
            parts.append(s)
            off = lo + n * 128
            kept = jnp.where(dl[0:rows, :] == (at + off).astype(F32), s, kept)
            for b in range(4):
                s_scr[b, :, pl.ds(at + off, 128)] = s[8 * b : 8 * b + 4, :]
                if rows == 64:
                    zsend[k, b, :, off : off + 128] = s[32 + 8 * b : 32 + 8 * b + 4, :]
            if n % 2:
                fold(rows, parts)
                parts = []
        k_scr[0:rows, :] = kept

    def step(i, rows):
        slot = i % SLOTS
        for c in tile_copies(i, slot):
            c.wait()
        k = i - FIRST
        consume(slot, column(i), 0, TILE, rows, k)

        @pl.when(i + SLOTS < steps)
        def _():
            tile_copies(i + SLOTS, slot)[0].start()

        @pl.when(i + SLOTS < steps - 1)
        def _():
            tile_copies(i + SLOTS, slot)[1].start()

        @pl.when(i + SLOTS == steps)
        def _():
            tile_copies(steps - 1, (steps - 1) % SLOTS)[1].start()

        if rows == 64:

            @pl.when(k < SHARED - HELD)
            def _():
                z_copy(k).start()

    group = lax.broadcasted_iota(jnp.int32, (8, 128), 1) // 32

    def pack(cols):
        size = cols[0].shape[0]
        packed = jnp.broadcast_to(cols[0], (size, 128))
        for b in range(1, 4):
            packed = jnp.where(group[:size] == b, cols[b], packed)
        return packed

    def unpack(packed, b):
        size = packed.shape[0]
        lane = lax.broadcasted_iota(jnp.int32, (size, 128), 1)
        return jnp.sum(jnp.where(lane == 32 * b, packed, 0.0), axis=1, keepdims=True)

    def packed_lse(at):
        m = m_scr[at : at + 32, :]
        top = jnp.max(m, axis=1, keepdims=True)
        lse = top + jnp.log(jnp.sum(l_scr[at : at + 32, :] * jnp.exp(m - top), axis=1, keepdims=True))
        return pack([lse[8 * b : 8 * b + 8, :] for b in range(4)])

    def packed_token(at):
        kept = jnp.sum(k_scr[at : at + 32, :], axis=1, keepdims=True)
        return pack([kept[8 * b : 8 * b + 8, :] for b in range(4)])

    lax.fori_loop(0, RELAY, lambda i, _: step(i, 32), None)
    x_direct.wait()
    x_relay.start()
    lax.fori_loop(RELAY, FIRST, lambda i, _: step(i, 32), None)
    x_copy(xp, 1 - core, sibling, 1).wait_recv()
    x_relay.wait_send()
    t_copy.wait()
    lay_rows(xp, tp_recv, 32)
    lax.fori_loop(FIRST, FIRST + SHARED, lambda i, _: step(i, 64), None)
    q_copy.start()
    pstat_s[0] = packed_lse(32)
    pstat_s[1] = packed_token(32)
    stat_copy = pltpu.make_async_remote_copy(
        src_ref=pstat_s, dst_ref=pstat_r, send_sem=ps_sem.at[0], recv_sem=ps_sem.at[1],
        device_id=partner, device_id_type=MESH,
    )
    stat_copy.start()
    for k in range(SHARED - HELD, SHARED):
        z_copy(k).start()
    lax.fori_loop(FIRST + SHARED, steps - 1, lambda i, _: step(i, 32), None)
    end, slot = steps - 1, (steps - 1) % SLOTS
    copies = tile_copies(end, slot)
    for lo, size in [(k * part, part) for k in range(PARTS)]:
        for c in copies[lo // part : (lo + size) // part]:
            c.wait()
        consume(slot, column(end), lo, size, 32, 0)

    def exchange(src, dst, sem):
        return [
            pltpu.make_async_remote_copy(
                src_ref=src, dst_ref=dst.at[d], send_sem=sem.at[0, d], recv_sem=sem.at[1, d],
                device_id=peers[d], device_id_type=MESH,
            )
            for d in range(3)
        ]

    mine = packed_lse(0)
    stat_copy.wait()
    theirs = pstat_r[0]
    top = jnp.maximum(mine, theirs)
    near = top + jnp.log(jnp.exp(mine - top) + jnp.exp(theirs - top))
    e1s[...] = near
    e1 = exchange(e1s, e1r, e1_sem)
    for c in e1:
        c.start()

    own = [dl[8 * b : 8 * b + 4, :] for b in range(4)]

    row_m = [jnp.broadcast_to(unpack(near[0:4, :], b), (4, 128)) for b in range(4)]

    def prepare(at, size):
        places = [(b, at + off, min(size, 128)) for b in range(4) for off in range(0, size, 128)]
        values = [s_scr[b, :, pl.ds(a, n)] for b, a, n in places]
        values = [jnp.exp(v - row_m[b][:, :n]) for v, (b, _, n) in zip(values, places)]
        for v, (b, a, n) in zip(values, places):
            s_scr[b, :, pl.ds(a, n)] = v

    def pick(at, size, found):
        out = []
        for b in range(4):
            f = found[b]
            for off in range(0, size, 128):
                n = min(size, 128)
                f = jnp.where(own[b][:, :n] == jnp.asarray(at + off).astype(F32), qv[b, :, pl.ds(at + off, n)], f)
            out.append(f)
        return tuple(out)

    zero = jnp.zeros((4, 128), F32)
    lax.fori_loop(0, steps, lambda i, _: prepare(column(i), TILE), None)
    prepare(tail_at, tail)
    q_copy.wait()
    whole = tail_at // PASS * PASS
    found = lax.fori_loop(0, whole // PASS, lambda i, f: pick(pl.multiple_of(i * PASS, 128), PASS, f), (zero,) * 4)
    found = pick(whole, tail_at - whole, found)
    found_tail = pick(tail_at, tail, (jnp.zeros((4, tail), F32),) * 4)
    token_q = []
    for b in range(4):
        f = found_tail[b]
        token_q.append(jnp.sum(found[b], axis=1, keepdims=True) + jnp.sum(f, axis=1, keepdims=True))
    e3s[0] = (packed_token(0) + pstat_r[1])[0:4, :]
    e3s[1] = pack(token_q)
    e3 = exchange(e3s, e3r, e3_sem)
    for c in e3:
        c.start()

    def theirs_at(k):
        return pl.multiple_of((FIRST + (1 - dp) * SHARED + k) * TILE, TILE)

    def await_z(k):
        z_copy(k).wait_send()
        pltpu.make_async_remote_copy(
            src_ref=zsend.at[k], dst_ref=s_scr.at[:, :, pl.ds(theirs_at(k), TILE)],
            send_sem=zs_sem.at[k], recv_sem=zr_sem.at[k], device_id=partner, device_id_type=MESH,
        ).wait_recv()

    def take_early(k, _):
        await_z(k)
        prepare(theirs_at(k), TILE)

    lax.fori_loop(0, SHARED - LATE, take_early, None)
    for c in e1:
        c.wait()
    lses = [near] + [e1r[d] for d in range(3)]
    top = jnp.maximum(jnp.maximum(lses[0], lses[1]), jnp.maximum(lses[2], lses[3]))
    sums = jnp.exp(lses[0] - top) + jnp.exp(lses[1] - top) + jnp.exp(lses[2] - top) + jnp.exp(lses[3] - top)
    lse = top + jnp.log(sums)
    lse_ref[...] = lse
    row_l = [jnp.broadcast_to(unpack(lse[0:4, :], b), (4, 128)) for b in range(4)]
    scale = [jnp.exp(row_m[b] - row_l[b]) for b in range(4)]

    def excess(b, at, size, p):
        e = jnp.maximum(p - qv[b, :, pl.ds(at, size)], 0.0)
        ex_ref[b, :, pl.ds(at, size)] = e
        return e

    def close(at, sums, prepared):
        out = []
        for b in range(4):
            acc = sums[b]
            for off in range(0, TILE, 128):
                v = s_scr[b, :, pl.ds(at + off, 128)]
                acc = acc + excess(b, at + off, 128, v * scale[b] if prepared else jnp.exp(v - row_l[b]))
            out.append(acc)
        return tuple(out)

    def close_late(k, sums):
        await_z(k)
        return close(theirs_at(k), sums, False)

    def close_from(first, count, sums):
        return lax.fori_loop(0, count, lambda i, t: close(pl.multiple_of((first + i) * TILE, TILE), t, True), sums)

    sums = close_from(0, FIRST, (zero,) * 4)
    sums = close_from(FIRST + dp * SHARED, SHARED, sums)
    sums = close_from(FIRST + 2 * SHARED, last, sums)
    rows = []
    for b in range(4):
        e = excess(b, tail_at, tail, s_scr[b, :, tail_at : tail_at + tail] * scale[b][:, :tail])
        rows.append(jnp.sum(e, axis=1, keepdims=True))
    sums = close_from(FIRST + (1 - dp) * SHARED, SHARED - LATE, sums)
    sums = lax.fori_loop(SHARED - LATE, SHARED, close_late, sums)
    rows = [jnp.sum(sums[b], axis=1, keepdims=True) + rows[b] for b in range(4)]
    e2s[...] = pack(rows)
    e2 = exchange(e2s, e2r, e2_sem)
    for c in e2:
        c.start()

    for c in e3:
        c.wait()
    at_token = (e3s[...] + e3r[0]) + (e3r[1] + e3r[2])
    acc_ref[...] = jnp.minimum(jnp.exp(at_token[0] - lse[0:4, :]) / at_token[1], 1.0)

    for c in e2:
        c.wait()
    norm_ref[...] = (e2s[...] + e2r[0]) + (e2r[1] + e2r[2])


def finish_kernel(
    ex_ref, norm_ref, acc_ref, lse_ref, acc_out, norm_out, res_out, bonus_out, acc_v, norm_v, bonus_v, stage, sem, r_sem
):
    n_ids = ex_ref.shape[2]
    lane = lax.broadcasted_iota(jnp.int32, (4, 128), 1)
    norm = norm_ref[...]
    writes = []
    for b in range(4):
        total = jnp.sum(jnp.where(lane == 32 * b, norm, 0.0), axis=1, keepdims=True)
        scale = jnp.broadcast_to(1.0 / jnp.broadcast_to(total, (4, 128)), (4, 128))

        for at in range(0, n_ids, 128):
            size = min(128, n_ids - at)
            stage[b, :, at : at + size] = ex_ref[b, :, at : at + size] * scale[:, :size]
        writes.append(pltpu.make_async_copy(stage.at[b], res_out.at[b], r_sem.at[b]))
        writes[-1].start()

    sub = lax.broadcasted_iota(jnp.int32, (4, 128), 0)
    for src, dst, out, k in ((acc_ref[...], acc_v, acc_out, 0), (norm, norm_v, norm_out, 1)):
        row = jnp.sum(jnp.where(lane % 32 == sub, src, 0.0), axis=0, keepdims=True)
        for b in range(4):
            dst[b : b + 1, :] = (row if b == 0 else pltpu.roll(row, 128 - 32 * b, 1))[:, 0:4]
        writes.append(pltpu.make_async_copy(dst, out, sem.at[k]))
        writes[-1].start()
    row = lse_ref[4:5, :]
    lane = lane[0:1, :]
    packed = row
    for b in range(1, 4):
        packed = jnp.where(lane == b, pltpu.roll(row, 128 - 31 * b, 1), packed)
    bonus_v[...] = packed[:, 0:4]
    writes.append(pltpu.make_async_copy(bonus_v, bonus_out, sem.at[2]))
    writes[-1].start()
    for c in writes:
        c.wait()


def solution(mesh):
    def local_step(hidden, norm_gain, w_head, draft_probs, draft_tokens, temperature):
        n_ids = w_head.shape[1]
        width = w_head.shape[0]
        pad_ids = -(-n_ids // 128) * 128
        tail = n_ids % TILE
        vmem, smem, hbm = pltpu.VMEM, pltpu.SMEM, pltpu.HBM
        dma = pltpu.SemaphoreType.DMA
        ex, norm, acc, lse = pl.pallas_call(
            verify_kernel,
            out_shape=[vmem((4, 4, n_ids), F32), vmem((4, 128), F32), vmem((4, 128), F32), vmem((8, 128), F32)],
            in_specs=[pl.BlockSpec(memory_space=s) for s in (hbm,) * 6],
            out_specs=[pl.BlockSpec(memory_space=vmem)] * 4,
            scratch_shapes=[
                vmem((5, 4, width), jnp.bfloat16),
                vmem((1, width), F32),
                smem((4,), F32),
                smem((4, 4), jnp.int32),
                vmem((SLOTS, TILE, width), jnp.bfloat16),
                vmem((tail, width), jnp.bfloat16),
                vmem((4, 4, n_ids), F32),
                vmem((4, 4, pad_ids), F32),
                vmem((5, 4, width), F32),
                vmem((5, 4, width), F32),
                vmem((32, width), F32),
                vmem((64, width), jnp.bfloat16),
                vmem((width, 128), jnp.bfloat16),
                vmem((5, 4, 128), F32),
                vmem((5, 4, 128), F32),
                vmem((64, 128), F32),
                vmem((64, 128), F32),
                vmem((64, 128), F32),
                vmem((64, 128), F32),
                vmem((64, 128), F32),
                vmem((SHARED, 4, 4, TILE), F32),
                vmem((2, 8, 128), F32),
                vmem((2, 8, 128), F32),
                vmem((8, 128), F32),
                vmem((3, 8, 128), F32),
                vmem((4, 128), F32),
                vmem((3, 4, 128), F32),
                vmem((2, 4, 128), F32),
                vmem((3, 2, 4, 128), F32),
                dma((4,)), dma((SLOTS, PARTS)), dma, dma, dma((2, 2)), dma((2,)), dma((SHARED,)), dma((SHARED,)), dma((2,)),
                dma((2, 3)), dma((2, 3)), dma((2, 3)),
            ],
            compiler_params=pltpu.CompilerParams(collective_id=0, has_side_effects=True),
            name="verify",
        )(
            hidden.transpose(1, 0, 2), norm_gain.reshape(1, width), temperature, draft_tokens,
            w_head.T, draft_probs,
        )
        acc, norm, residual, bonus = pl.pallas_call(
            finish_kernel,
            out_shape=[
                jax.ShapeDtypeStruct((4, 4), F32),
                jax.ShapeDtypeStruct((4, 4), F32),
                jax.ShapeDtypeStruct((4, 4, n_ids), F32),
                jax.ShapeDtypeStruct((1, 4), F32),
            ],
            in_specs=[pl.BlockSpec(memory_space=vmem)] * 4,
            out_specs=[pl.BlockSpec(memory_space=hbm)] * 4,
            scratch_shapes=[
                vmem((4, 4), F32), vmem((4, 4), F32), vmem((1, 4), F32), vmem((4, 4, n_ids), F32), dma((3,)), dma((4,)),
            ],
            compiler_params=pltpu.CompilerParams(vmem_limit_bytes=16 * 1024 * 1024),
            name="finish",
        )(ex, norm, acc, lse)
        return acc, norm, residual, bonus.reshape(4)

    return jax.shard_map(
        local_step,
        mesh=mesh,
        in_specs=(P("dp", None, None), P(), P(None, "tp"), P("dp", None, "tp"), P("dp", None), P("dp")),
        out_specs=(P("dp", None), P("dp", None), P("dp", None, "tp"), P("dp")),
        check_vma=False,
    )
```

```python
import jax
import jax.numpy as jnp
from jax import lax
from jax.experimental import pallas as pl
from jax.experimental.pallas import tpu as pltpu
from jax.sharding import PartitionSpec as P

MESH = pl.DeviceIdType.MESH
F32 = jnp.float32
LOWEST = float(jnp.finfo(jnp.float32).min)

TILE = 1024
SUB = 256
DEPTH = 256
SLOTS = 3
SHARED = 15
FIRST = 3
LATE = 5
HELD = 3
RELAY = 2
PARTS = 1
PASS = 2048


def verify_kernel(
    h_hbm, g_hbm, t_hbm, dt_hbm, w_ref, q_ref,
    ex_ref, norm_ref, acc_ref, lse_ref,
    h_ref, g_ref, t_ref, dt_ref, wbuf, wtail, qv, s_scr, xf, xp, xrows, xb, xt, tv, tp_recv, ct, dl, m_scr, l_scr, k_scr,
    zsend, pstat_s, pstat_r, e1s, e1r, e2s, e2r, e3s, e3r,
    in_sem, w_sem, wt_sem, q_sem, x_sem, t_sem, zs_sem, zr_sem, ps_sem, e1_sem, e2_sem, e3_sem,
):
    dp, tp = lax.axis_index("dp"), lax.axis_index("tp")
    partner = (1 - dp, tp)
    peers = [(dp, lax.rem(tp + d, 4)) for d in (1, 2, 3)]
    n_ids, width = w_ref.shape
    n_full = n_ids // TILE
    tail = n_ids - n_full * TILE
    tail_at = n_full * TILE
    last = n_full - 2 * SHARED - FIRST
    steps = FIRST + SHARED + last

    def column(i):
        in_shared = (i + steps - FIRST) // steps
        past_shared = (i + steps - FIRST - SHARED) // steps
        return pl.multiple_of((i + in_shared * dp * SHARED + past_shared * (SHARED - dp * SHARED)) * TILE, TILE)

    part = TILE // PARTS

    def tile_copies(i, slot):
        at = column(i)
        return [
            pltpu.make_async_copy(
                w_ref.at[pl.ds(at + k * part, part), :], wbuf.at[slot, pl.ds(k * part, part), :], w_sem.at[slot, k]
            )
            for k in range(PARTS)
        ]

    tail_copy = pltpu.make_async_copy(w_ref.at[pl.ds(tail_at, tail), :], wtail, wt_sem)
    q_copy = pltpu.make_async_copy(q_ref, qv, q_sem)
    small = [
        pltpu.make_async_copy(src, dst, in_sem.at[k])
        for k, (src, dst) in enumerate(((h_hbm, h_ref), (g_hbm, g_ref), (t_hbm, t_ref), (dt_hbm, dt_ref)))
    ]
    for c in small:
        c.start()
    tail_copy.start()
    for c in tile_copies(0, 0):
        c.start()

    barrier = pltpu.get_barrier_semaphore()
    for other in [partner] + peers:
        pl.semaphore_signal(barrier, inc=1, device_id=other, device_id_type=MESH)

    for c in small:
        c.wait()
    for c in tile_copies(1, 1):
        c.start()
    h = h_ref[...].astype(F32)
    inv_rms = lax.rsqrt(jnp.mean(h * h, axis=-1, keepdims=True) + 1e-5)
    xf[...] = h * inv_rms * g_ref[...][None]
    for b in range(4):
        tv[0, b : b + 1, :] = jnp.full((1, 128), 1.0, F32) / jnp.full((1, 128), t_ref[b], F32)
        for j in range(4):
            tv[1 + j, b : b + 1, :] = jnp.full((1, 128), dt_ref[b, j].astype(F32), F32)

    def lay_rows(src, t_src, at):
        xrows[...] = jnp.zeros_like(xrows)
        lane = lax.broadcasted_iota(jnp.int32, (1, 128), 1) + tp * n_ids
        for b in range(4):
            for j in range(5):
                xrows[8 * b + j : 8 * b + j + 1, :] = src[j, b : b + 1, :]
            ct[at + 8 * b : at + 8 * b + 8, :] = jnp.broadcast_to(t_src[0, b : b + 1, :], (8, 128))
            dl[at + 8 * b : at + 8 * b + 8, :] = jnp.full((8, 128), -1.0, F32)
            for j in range(4):
                dl[at + 8 * b + j : at + 8 * b + j + 1, :] = t_src[1 + j, b : b + 1, :] - lane.astype(F32)
        rows = xrows[...].astype(jnp.bfloat16)
        xb[at : at + 32, :] = rows
        for k in range(0, width, 128):
            xt[k : k + 128, at : at + 32] = xrows[:, k : k + 128].T.astype(jnp.bfloat16)

    pl.semaphore_wait(barrier, 4)
    core = lax.rem(tp, 2)
    sibling = (dp, tp + 1 - 2 * core)

    def width_half(ref, c):
        return ref.at[:, :, pl.ds(pl.multiple_of(c * (width // 2), width // 2), width // 2)]

    def x_copy(src, c, to, k):
        return pltpu.make_async_remote_copy(
            src_ref=width_half(src, c), dst_ref=width_half(xp, c), send_sem=x_sem.at[0, k], recv_sem=x_sem.at[1, k],
            device_id=to, device_id_type=MESH,
        )

    x_direct = x_copy(xf, core, partner, 0)
    x_relay = x_copy(xp, core, sibling, 1)
    t_copy = pltpu.make_async_remote_copy(
        src_ref=tv, dst_ref=tp_recv, send_sem=t_sem.at[0], recv_sem=t_sem.at[1], device_id=partner, device_id_type=MESH
    )
    x_direct.start()
    t_copy.start()

    xt[:, 32:128] = jnp.zeros((width, 96), jnp.bfloat16)
    xb[32:64, :] = jnp.zeros((32, width), jnp.bfloat16)
    lay_rows(xf, tv, 0)
    for i in range(2, SLOTS):
        for c in tile_copies(i, i):
            c.start()
    m_scr[...] = jnp.full(m_scr.shape, LOWEST, F32)
    l_scr[...] = jnp.zeros_like(l_scr)
    k_scr[...] = jnp.zeros_like(k_scr)

    def by_rows(w, depth):
        return lax.dot_general(xb[:, depth], w, (((1,), (1,)), ((), ())), preferred_element_type=F32)

    def by_ids(w, depth):
        return lax.dot_general(w, xt[depth, :], (((1,), (0,)), ((), ())), preferred_element_type=F32)

    def products(slot, lo, size):
        block = min(SUB, size // 2)
        starts = range(lo, lo + size, block)
        fixed = len(starts) // 2
        sums = [None] * len(starts)
        for k in range(0, width, DEPTH):
            depth = slice(k, k + DEPTH)
            for n, start in enumerate(starts):
                w = wbuf[slot, start : start + block, depth]
                z = by_rows(w, depth) if n < fixed else by_ids(w, depth)
                sums[n] = z if k == 0 else sums[n] + z
        pieces = []
        for n, z in enumerate(sums):
            for at in range(0, block, 128):
                pieces.append(z[:, at : at + 128] if n < fixed else z[at : at + 128, :].T[0:64])
        return pieces

    def fold(rows, parts):
        m_old = m_scr[0:rows, :]
        m_new = m_old
        for p in parts:
            m_new = jnp.maximum(m_new, p)
        total = l_scr[0:rows, :] * jnp.exp(m_old - m_new)
        for p in parts:
            total = total + jnp.exp(p - m_new)
        m_scr[0:rows, :] = m_new
        l_scr[0:rows, :] = total

    tail_copy.wait()
    s = by_rows(wtail[...], slice(0, width))[0:32] * ct[0:32, 0:tail]
    for b in range(4):
        s_scr[b, :, tail_at : tail_at + tail] = s[8 * b : 8 * b + 4, :]
    k_scr[0:32, 0:tail] = jnp.where(dl[0:32, 0:tail] == float(tail_at), s, 0.0)
    m_tail = jnp.max(s, axis=1, keepdims=True)
    l_tail = jnp.sum(jnp.exp(s - m_tail), axis=1, keepdims=True)
    lane0 = lax.broadcasted_iota(jnp.int32, (32, 128), 1) == 0
    m_scr[0:32, :] = jnp.where(lane0, m_tail, LOWEST)
    l_scr[0:32, :] = jnp.where(lane0, l_tail, 0.0)

    def z_copy(k):
        at = column(FIRST + k)
        return pltpu.make_async_remote_copy(
            src_ref=zsend.at[k], dst_ref=s_scr.at[:, :, pl.ds(at, TILE)], send_sem=zs_sem.at[k], recv_sem=zr_sem.at[k],
            device_id=partner, device_id_type=MESH,
        )

    def consume(slot, at, lo, size, rows, k):
        kept = k_scr[0:rows, :]
        parts = []
        for n, z in enumerate(products(slot, lo, size)):
            s = z[0:rows] * ct[0:rows, :]
            parts.append(s)
            off = lo + n * 128
            kept = jnp.where(dl[0:rows, :] == (at + off).astype(F32), s, kept)
            for b in range(4):
                s_scr[b, :, pl.ds(at + off, 128)] = s[8 * b : 8 * b + 4, :]
                if rows == 64:
                    zsend[k, b, :, off : off + 128] = s[32 + 8 * b : 32 + 8 * b + 4, :]
            if n % 2:
                fold(rows, parts)
                parts = []
        k_scr[0:rows, :] = kept

    def step(i, rows):
        slot = i % SLOTS
        for c in tile_copies(i, slot):
            c.wait()
        k = i - FIRST
        consume(slot, column(i), 0, TILE, rows, k)

        @pl.when(i + SLOTS < steps)
        def _():
            for c in tile_copies(i + SLOTS, slot):
                c.start()

        if rows == 64:

            @pl.when(k < SHARED - HELD)
            def _():
                z_copy(k).start()

    group = lax.broadcasted_iota(jnp.int32, (8, 128), 1) // 32

    def pack(cols):
        size = cols[0].shape[0]
        packed = jnp.broadcast_to(cols[0], (size, 128))
        for b in range(1, 4):
            packed = jnp.where(group[:size] == b, cols[b], packed)
        return packed

    def unpack(packed, b):
        size = packed.shape[0]
        lane = lax.broadcasted_iota(jnp.int32, (size, 128), 1)
        return jnp.sum(jnp.where(lane == 32 * b, packed, 0.0), axis=1, keepdims=True)

    def packed_lse(at):
        m = m_scr[at : at + 32, :]
        top = jnp.max(m, axis=1, keepdims=True)
        lse = top + jnp.log(jnp.sum(l_scr[at : at + 32, :] * jnp.exp(m - top), axis=1, keepdims=True))
        return pack([lse[8 * b : 8 * b + 8, :] for b in range(4)])

    def packed_token(at):
        kept = jnp.sum(k_scr[at : at + 32, :], axis=1, keepdims=True)
        return pack([kept[8 * b : 8 * b + 8, :] for b in range(4)])

    lax.fori_loop(0, RELAY, lambda i, _: step(i, 32), None)
    x_direct.wait()
    x_relay.start()
    lax.fori_loop(RELAY, FIRST, lambda i, _: step(i, 32), None)
    x_copy(xp, 1 - core, sibling, 1).wait_recv()
    x_relay.wait_send()
    t_copy.wait()
    lay_rows(xp, tp_recv, 32)
    lax.fori_loop(FIRST, FIRST + SHARED, lambda i, _: step(i, 64), None)
    q_copy.start()
    pstat_s[0] = packed_lse(32)
    pstat_s[1] = packed_token(32)
    stat_copy = pltpu.make_async_remote_copy(
        src_ref=pstat_s, dst_ref=pstat_r, send_sem=ps_sem.at[0], recv_sem=ps_sem.at[1],
        device_id=partner, device_id_type=MESH,
    )
    stat_copy.start()
    for k in range(SHARED - HELD, SHARED):
        z_copy(k).start()
    lax.fori_loop(FIRST + SHARED, steps - 1, lambda i, _: step(i, 32), None)
    end, slot = steps - 1, (steps - 1) % SLOTS
    copies = tile_copies(end, slot)
    for lo, size in [(k * part, part) for k in range(PARTS)]:
        for c in copies[lo // part : (lo + size) // part]:
            c.wait()
        consume(slot, column(end), lo, size, 32, 0)

    def exchange(src, dst, sem):
        return [
            pltpu.make_async_remote_copy(
                src_ref=src, dst_ref=dst.at[d], send_sem=sem.at[0, d], recv_sem=sem.at[1, d],
                device_id=peers[d], device_id_type=MESH,
            )
            for d in range(3)
        ]

    mine = packed_lse(0)
    stat_copy.wait()
    theirs = pstat_r[0]
    top = jnp.maximum(mine, theirs)
    near = top + jnp.log(jnp.exp(mine - top) + jnp.exp(theirs - top))
    e1s[...] = near
    e1 = exchange(e1s, e1r, e1_sem)
    for c in e1:
        c.start()

    own = [dl[8 * b : 8 * b + 4, :] for b in range(4)]

    row_m = [jnp.broadcast_to(unpack(near[0:4, :], b), (4, 128)) for b in range(4)]

    def prepare(at, size):
        places = [(b, at + off, min(size, 128)) for b in range(4) for off in range(0, size, 128)]
        values = [s_scr[b, :, pl.ds(a, n)] for b, a, n in places]
        values = [jnp.exp(v - row_m[b][:, :n]) for v, (b, _, n) in zip(values, places)]
        for v, (b, a, n) in zip(values, places):
            s_scr[b, :, pl.ds(a, n)] = v

    def pick(at, size, found):
        out = []
        for b in range(4):
            f = found[b]
            for off in range(0, size, 128):
                n = min(size, 128)
                f = jnp.where(own[b][:, :n] == jnp.asarray(at + off).astype(F32), qv[b, :, pl.ds(at + off, n)], f)
            out.append(f)
        return tuple(out)

    zero = jnp.zeros((4, 128), F32)
    lax.fori_loop(0, steps, lambda i, _: prepare(column(i), TILE), None)
    prepare(tail_at, tail)
    q_copy.wait()
    whole = tail_at // PASS * PASS
    found = lax.fori_loop(0, whole // PASS, lambda i, f: pick(pl.multiple_of(i * PASS, 128), PASS, f), (zero,) * 4)
    found = pick(whole, tail_at - whole, found)
    found_tail = pick(tail_at, tail, (jnp.zeros((4, tail), F32),) * 4)
    token_q = []
    for b in range(4):
        f = found_tail[b]
        token_q.append(jnp.sum(found[b], axis=1, keepdims=True) + jnp.sum(f, axis=1, keepdims=True))
    e3s[0] = (packed_token(0) + pstat_r[1])[0:4, :]
    e3s[1] = pack(token_q)
    e3 = exchange(e3s, e3r, e3_sem)
    for c in e3:
        c.start()

    def theirs_at(k):
        return pl.multiple_of((FIRST + (1 - dp) * SHARED + k) * TILE, TILE)

    def await_z(k):
        z_copy(k).wait_send()
        pltpu.make_async_remote_copy(
            src_ref=zsend.at[k], dst_ref=s_scr.at[:, :, pl.ds(theirs_at(k), TILE)],
            send_sem=zs_sem.at[k], recv_sem=zr_sem.at[k], device_id=partner, device_id_type=MESH,
        ).wait_recv()

    def take_early(k, _):
        await_z(k)
        prepare(theirs_at(k), TILE)

    lax.fori_loop(0, SHARED - LATE, take_early, None)
    for c in e1:
        c.wait()
    lses = [near] + [e1r[d] for d in range(3)]
    top = jnp.maximum(jnp.maximum(lses[0], lses[1]), jnp.maximum(lses[2], lses[3]))
    sums = jnp.exp(lses[0] - top) + jnp.exp(lses[1] - top) + jnp.exp(lses[2] - top) + jnp.exp(lses[3] - top)
    lse = top + jnp.log(sums)
    lse_ref[...] = lse
    row_l = [jnp.broadcast_to(unpack(lse[0:4, :], b), (4, 128)) for b in range(4)]
    scale = [jnp.exp(row_m[b] - row_l[b]) for b in range(4)]

    def excess(b, at, size, p):
        e = jnp.maximum(p - qv[b, :, pl.ds(at, size)], 0.0)
        ex_ref[b, :, pl.ds(at, size)] = e
        return e

    def close(at, sums, prepared):
        out = []
        for b in range(4):
            acc = sums[b]
            for off in range(0, TILE, 128):
                v = s_scr[b, :, pl.ds(at + off, 128)]
                acc = acc + excess(b, at + off, 128, v * scale[b] if prepared else jnp.exp(v - row_l[b]))
            out.append(acc)
        return tuple(out)

    def close_late(k, sums):
        await_z(k)
        return close(theirs_at(k), sums, False)

    def close_from(first, count, sums):
        return lax.fori_loop(0, count, lambda i, t: close(pl.multiple_of((first + i) * TILE, TILE), t, True), sums)

    sums = close_from(0, FIRST, (zero,) * 4)
    sums = close_from(FIRST + dp * SHARED, SHARED, sums)
    sums = close_from(FIRST + 2 * SHARED, last, sums)
    rows = []
    for b in range(4):
        e = excess(b, tail_at, tail, s_scr[b, :, tail_at : tail_at + tail] * scale[b][:, :tail])
        rows.append(jnp.sum(e, axis=1, keepdims=True))
    sums = close_from(FIRST + (1 - dp) * SHARED, SHARED - LATE, sums)
    sums = lax.fori_loop(SHARED - LATE, SHARED, close_late, sums)
    rows = [jnp.sum(sums[b], axis=1, keepdims=True) + rows[b] for b in range(4)]
    e2s[...] = pack(rows)
    e2 = exchange(e2s, e2r, e2_sem)
    for c in e2:
        c.start()

    for c in e3:
        c.wait()
    at_token = (e3s[...] + e3r[0]) + (e3r[1] + e3r[2])
    acc_ref[...] = jnp.minimum(jnp.exp(at_token[0] - lse[0:4, :]) / at_token[1], 1.0)

    for c in e2:
        c.wait()
    norm_ref[...] = (e2s[...] + e2r[0]) + (e2r[1] + e2r[2])


def finish_kernel(
    ex_ref, norm_ref, acc_ref, lse_ref, acc_out, norm_out, res_out, bonus_out, acc_v, norm_v, bonus_v, stage, sem, r_sem
):
    n_ids = ex_ref.shape[2]
    lane = lax.broadcasted_iota(jnp.int32, (4, 128), 1)
    norm = norm_ref[...]
    writes = []
    for b in range(4):
        total = jnp.sum(jnp.where(lane == 32 * b, norm, 0.0), axis=1, keepdims=True)
        scale = jnp.broadcast_to(1.0 / jnp.broadcast_to(total, (4, 128)), (4, 128))

        for at in range(0, n_ids, 128):
            size = min(128, n_ids - at)
            stage[b, :, at : at + size] = ex_ref[b, :, at : at + size] * scale[:, :size]
        writes.append(pltpu.make_async_copy(stage.at[b], res_out.at[b], r_sem.at[b]))
        writes[-1].start()

    sub = lax.broadcasted_iota(jnp.int32, (4, 128), 0)
    for src, dst, out, k in ((acc_ref[...], acc_v, acc_out, 0), (norm, norm_v, norm_out, 1)):
        row = jnp.sum(jnp.where(lane % 32 == sub, src, 0.0), axis=0, keepdims=True)
        for b in range(4):
            dst[b : b + 1, :] = (row if b == 0 else pltpu.roll(row, 128 - 32 * b, 1))[:, 0:4]
        writes.append(pltpu.make_async_copy(dst, out, sem.at[k]))
        writes[-1].start()
    row = lse_ref[4:5, :]
    lane = lane[0:1, :]
    packed = row
    for b in range(1, 4):
        packed = jnp.where(lane == b, pltpu.roll(row, 128 - 31 * b, 1), packed)
    bonus_v[...] = packed[:, 0:4]
    writes.append(pltpu.make_async_copy(bonus_v, bonus_out, sem.at[2]))
    writes[-1].start()
    for c in writes:
        c.wait()


def solution(mesh):
    def local_step(hidden, norm_gain, w_head, draft_probs, draft_tokens, temperature):
        n_ids = w_head.shape[1]
        width = w_head.shape[0]
        pad_ids = -(-n_ids // 128) * 128
        tail = n_ids % TILE
        vmem, smem, hbm = pltpu.VMEM, pltpu.SMEM, pltpu.HBM
        dma = pltpu.SemaphoreType.DMA
        ex, norm, acc, lse = pl.pallas_call(
            verify_kernel,
            out_shape=[vmem((4, 4, n_ids), F32), vmem((4, 128), F32), vmem((4, 128), F32), vmem((8, 128), F32)],
            in_specs=[pl.BlockSpec(memory_space=s) for s in (hbm,) * 6],
            out_specs=[pl.BlockSpec(memory_space=vmem)] * 4,
            scratch_shapes=[
                vmem((5, 4, width), jnp.bfloat16),
                vmem((1, width), F32),
                smem((4,), F32),
                smem((4, 4), jnp.int32),
                vmem((SLOTS, TILE, width), jnp.bfloat16),
                vmem((tail, width), jnp.bfloat16),
                vmem((4, 4, n_ids), F32),
                vmem((4, 4, pad_ids), F32),
                vmem((5, 4, width), F32),
                vmem((5, 4, width), F32),
                vmem((32, width), F32),
                vmem((64, width), jnp.bfloat16),
                vmem((width, 128), jnp.bfloat16),
                vmem((5, 4, 128), F32),
                vmem((5, 4, 128), F32),
                vmem((64, 128), F32),
                vmem((64, 128), F32),
                vmem((64, 128), F32),
                vmem((64, 128), F32),
                vmem((64, 128), F32),
                vmem((SHARED, 4, 4, TILE), F32),
                vmem((2, 8, 128), F32),
                vmem((2, 8, 128), F32),
                vmem((8, 128), F32),
                vmem((3, 8, 128), F32),
                vmem((4, 128), F32),
                vmem((3, 4, 128), F32),
                vmem((2, 4, 128), F32),
                vmem((3, 2, 4, 128), F32),
                dma((4,)), dma((SLOTS, PARTS)), dma, dma, dma((2, 2)), dma((2,)), dma((SHARED,)), dma((SHARED,)), dma((2,)),
                dma((2, 3)), dma((2, 3)), dma((2, 3)),
            ],
            compiler_params=pltpu.CompilerParams(collective_id=0, has_side_effects=True),
            name="verify",
        )(
            hidden.transpose(1, 0, 2), norm_gain.reshape(1, width), temperature, draft_tokens,
            w_head.T, draft_probs,
        )
        acc, norm, residual, bonus = pl.pallas_call(
            finish_kernel,
            out_shape=[
                jax.ShapeDtypeStruct((4, 4), F32),
                jax.ShapeDtypeStruct((4, 4), F32),
                jax.ShapeDtypeStruct((4, 4, n_ids), F32),
                jax.ShapeDtypeStruct((1, 4), F32),
            ],
            in_specs=[pl.BlockSpec(memory_space=vmem)] * 4,
            out_specs=[pl.BlockSpec(memory_space=hbm)] * 4,
            scratch_shapes=[
                vmem((4, 4), F32), vmem((4, 4), F32), vmem((1, 4), F32), vmem((4, 4, n_ids), F32), dma((3,)), dma((4,)),
            ],
            compiler_params=pltpu.CompilerParams(vmem_limit_bytes=16 * 1024 * 1024),
            name="finish",
        )(ex, norm, acc, lse)
        return acc, norm, residual, bonus.reshape(4)

    return jax.shard_map(
        local_step,
        mesh=mesh,
        in_specs=(P("dp", None, None), P(), P(None, "tp"), P("dp", None, "tp"), P("dp", None), P("dp")),
        out_specs=(P("dp", None), P("dp", None), P("dp", None, "tp"), P("dp")),
        check_vma=False,
    )
```

```python
import jax
import jax.numpy as jnp
from jax import lax
from jax.experimental import pallas as pl
from jax.experimental.pallas import tpu as pltpu
from jax.sharding import PartitionSpec as P

MESH = pl.DeviceIdType.MESH
F32 = jnp.float32
LOWEST = float(jnp.finfo(jnp.float32).min)

TILE = 1024
SUB = 256
DEPTH = 256
SLOTS = 3
SHARED = 15
FIRST = 4
LATE = 5
HELD = 3
RELAY = 3
PARTS = 1
PASS = 2048


def verify_kernel(
    h_hbm, g_hbm, t_hbm, dt_hbm, w_ref, q_ref,
    ex_ref, norm_ref, acc_ref, lse_ref,
    h_ref, g_ref, t_ref, dt_ref, wbuf, wtail, qv, s_scr, xf, xp, xrows, xb, xt, tv, tp_recv, ct, dl, m_scr, l_scr, k_scr,
    zsend, pstat_s, pstat_r, e1s, e1r, e2s, e2r, e3s, e3r,
    in_sem, w_sem, wt_sem, q_sem, x_sem, t_sem, zs_sem, zr_sem, ps_sem, e1_sem, e2_sem, e3_sem,
):
    dp, tp = lax.axis_index("dp"), lax.axis_index("tp")
    partner = (1 - dp, tp)
    peers = [(dp, lax.rem(tp + d, 4)) for d in (1, 2, 3)]
    n_ids, width = w_ref.shape
    n_full = n_ids // TILE
    tail = n_ids - n_full * TILE
    tail_at = n_full * TILE
    last = n_full - 2 * SHARED - FIRST
    steps = FIRST + SHARED + last

    def column(i):
        in_shared = (i + steps - FIRST) // steps
        past_shared = (i + steps - FIRST - SHARED) // steps
        return pl.multiple_of((i + in_shared * dp * SHARED + past_shared * (SHARED - dp * SHARED)) * TILE, TILE)

    part = TILE // PARTS

    def tile_copies(i, slot):
        at = column(i)
        return [
            pltpu.make_async_copy(
                w_ref.at[pl.ds(at + k * part, part), :], wbuf.at[slot, pl.ds(k * part, part), :], w_sem.at[slot, k]
            )
            for k in range(PARTS)
        ]

    tail_copy = pltpu.make_async_copy(w_ref.at[pl.ds(tail_at, tail), :], wtail, wt_sem)
    q_copy = pltpu.make_async_copy(q_ref, qv, q_sem)
    small = [
        pltpu.make_async_copy(src, dst, in_sem.at[k])
        for k, (src, dst) in enumerate(((h_hbm, h_ref), (g_hbm, g_ref), (t_hbm, t_ref), (dt_hbm, dt_ref)))
    ]
    for c in small:
        c.start()
    tail_copy.start()
    for c in tile_copies(0, 0):
        c.start()

    barrier = pltpu.get_barrier_semaphore()
    for other in [partner] + peers:
        pl.semaphore_signal(barrier, inc=1, device_id=other, device_id_type=MESH)

    for c in small:
        c.wait()
    for c in tile_copies(1, 1):
        c.start()
    h = h_ref[...].astype(F32)
    inv_rms = lax.rsqrt(jnp.mean(h * h, axis=-1, keepdims=True) + 1e-5)
    xf[...] = h * inv_rms * g_ref[...][None]
    for b in range(4):
        tv[0, b : b + 1, :] = jnp.full((1, 128), 1.0, F32) / jnp.full((1, 128), t_ref[b], F32)
        for j in range(4):
            tv[1 + j, b : b + 1, :] = jnp.full((1, 128), dt_ref[b, j].astype(F32), F32)

    def lay_rows(src, t_src, at):
        xrows[...] = jnp.zeros_like(xrows)
        lane = lax.broadcasted_iota(jnp.int32, (1, 128), 1) + tp * n_ids
        for b in range(4):
            for j in range(5):
                xrows[8 * b + j : 8 * b + j + 1, :] = src[j, b : b + 1, :]
            ct[at + 8 * b : at + 8 * b + 8, :] = jnp.broadcast_to(t_src[0, b : b + 1, :], (8, 128))
            dl[at + 8 * b : at + 8 * b + 8, :] = jnp.full((8, 128), -1.0, F32)
            for j in range(4):
                dl[at + 8 * b + j : at + 8 * b + j + 1, :] = t_src[1 + j, b : b + 1, :] - lane.astype(F32)
        rows = xrows[...].astype(jnp.bfloat16)
        xb[at : at + 32, :] = rows
        for k in range(0, width, 128):
            xt[k : k + 128, at : at + 32] = xrows[:, k : k + 128].T.astype(jnp.bfloat16)

    pl.semaphore_wait(barrier, 4)
    core = lax.rem(tp, 2)
    sibling = (dp, tp + 1 - 2 * core)

    def width_half(ref, c):
        return ref.at[:, :, pl.ds(pl.multiple_of(c * (width // 2), width // 2), width // 2)]

    def x_copy(src, c, to, k):
        return pltpu.make_async_remote_copy(
            src_ref=width_half(src, c), dst_ref=width_half(xp, c), send_sem=x_sem.at[0, k], recv_sem=x_sem.at[1, k],
            device_id=to, device_id_type=MESH,
        )

    x_direct = x_copy(xf, core, partner, 0)
    x_relay = x_copy(xp, core, sibling, 1)
    t_copy = pltpu.make_async_remote_copy(
        src_ref=tv, dst_ref=tp_recv, send_sem=t_sem.at[0], recv_sem=t_sem.at[1], device_id=partner, device_id_type=MESH
    )
    x_direct.start()
    t_copy.start()

    xt[:, 32:128] = jnp.zeros((width, 96), jnp.bfloat16)
    xb[32:64, :] = jnp.zeros((32, width), jnp.bfloat16)
    lay_rows(xf, tv, 0)
    for i in range(2, SLOTS):
        for c in tile_copies(i, i):
            c.start()
    m_scr[...] = jnp.full(m_scr.shape, LOWEST, F32)
    l_scr[...] = jnp.zeros_like(l_scr)
    k_scr[...] = jnp.zeros_like(k_scr)

    def by_rows(w, depth):
        return lax.dot_general(xb[:, depth], w, (((1,), (1,)), ((), ())), preferred_element_type=F32)

    def by_ids(w, depth):
        return lax.dot_general(w, xt[depth, :], (((1,), (0,)), ((), ())), preferred_element_type=F32)

    def products(slot, lo, size):
        block = min(SUB, size // 2)
        starts = range(lo, lo + size, block)
        fixed = len(starts) // 2
        sums = [None] * len(starts)
        for k in range(0, width, DEPTH):
            depth = slice(k, k + DEPTH)
            for n, start in enumerate(starts):
                w = wbuf[slot, start : start + block, depth]
                z = by_rows(w, depth) if n < fixed else by_ids(w, depth)
                sums[n] = z if k == 0 else sums[n] + z
        pieces = []
        for n, z in enumerate(sums):
            for at in range(0, block, 128):
                pieces.append(z[:, at : at + 128] if n < fixed else z[at : at + 128, :].T[0:64])
        return pieces

    def fold(rows, parts):
        m_old = m_scr[0:rows, :]
        m_new = m_old
        for p in parts:
            m_new = jnp.maximum(m_new, p)
        total = l_scr[0:rows, :] * jnp.exp(m_old - m_new)
        for p in parts:
            total = total + jnp.exp(p - m_new)
        m_scr[0:rows, :] = m_new
        l_scr[0:rows, :] = total

    tail_copy.wait()
    s = by_rows(wtail[...], slice(0, width))[0:32] * ct[0:32, 0:tail]
    for b in range(4):
        s_scr[b, :, tail_at : tail_at + tail] = s[8 * b : 8 * b + 4, :]
    k_scr[0:32, 0:tail] = jnp.where(dl[0:32, 0:tail] == float(tail_at), s, 0.0)
    m_tail = jnp.max(s, axis=1, keepdims=True)
    l_tail = jnp.sum(jnp.exp(s - m_tail), axis=1, keepdims=True)
    lane0 = lax.broadcasted_iota(jnp.int32, (32, 128), 1) == 0
    m_scr[0:32, :] = jnp.where(lane0, m_tail, LOWEST)
    l_scr[0:32, :] = jnp.where(lane0, l_tail, 0.0)

    def z_copy(k):
        at = column(FIRST + k)
        return pltpu.make_async_remote_copy(
            src_ref=zsend.at[k], dst_ref=s_scr.at[:, :, pl.ds(at, TILE)], send_sem=zs_sem.at[k], recv_sem=zr_sem.at[k],
            device_id=partner, device_id_type=MESH,
        )

    def consume(slot, at, lo, size, rows, k):
        kept = k_scr[0:rows, :]
        parts = []
        for n, z in enumerate(products(slot, lo, size)):
            s = z[0:rows] * ct[0:rows, :]
            parts.append(s)
            off = lo + n * 128
            kept = jnp.where(dl[0:rows, :] == (at + off).astype(F32), s, kept)
            for b in range(4):
                s_scr[b, :, pl.ds(at + off, 128)] = s[8 * b : 8 * b + 4, :]
                if rows == 64:
                    zsend[k, b, :, off : off + 128] = s[32 + 8 * b : 32 + 8 * b + 4, :]
            if n % 2:
                fold(rows, parts)
                parts = []
        k_scr[0:rows, :] = kept

    def step(i, rows):
        slot = i % SLOTS
        for c in tile_copies(i, slot):
            c.wait()
        k = i - FIRST
        consume(slot, column(i), 0, TILE, rows, k)

        @pl.when(i + SLOTS < steps)
        def _():
            for c in tile_copies(i + SLOTS, slot):
                c.start()

        if rows == 64:

            @pl.when(k < SHARED - HELD)
            def _():
                z_copy(k).start()

    group = lax.broadcasted_iota(jnp.int32, (8, 128), 1) // 32

    def pack(cols):
        size = cols[0].shape[0]
        packed = jnp.broadcast_to(cols[0], (size, 128))
        for b in range(1, 4):
            packed = jnp.where(group[:size] == b, cols[b], packed)
        return packed

    def unpack(packed, b):
        size = packed.shape[0]
        lane = lax.broadcasted_iota(jnp.int32, (size, 128), 1)
        return jnp.sum(jnp.where(lane == 32 * b, packed, 0.0), axis=1, keepdims=True)

    def packed_lse(at):
        m = m_scr[at : at + 32, :]
        top = jnp.max(m, axis=1, keepdims=True)
        lse = top + jnp.log(jnp.sum(l_scr[at : at + 32, :] * jnp.exp(m - top), axis=1, keepdims=True))
        return pack([lse[8 * b : 8 * b + 8, :] for b in range(4)])

    def packed_token(at):
        kept = jnp.sum(k_scr[at : at + 32, :], axis=1, keepdims=True)
        return pack([kept[8 * b : 8 * b + 8, :] for b in range(4)])

    lax.fori_loop(0, RELAY, lambda i, _: step(i, 32), None)
    x_direct.wait()
    x_relay.start()
    lax.fori_loop(RELAY, FIRST, lambda i, _: step(i, 32), None)
    x_copy(xp, 1 - core, sibling, 1).wait_recv()
    x_relay.wait_send()
    t_copy.wait()
    lay_rows(xp, tp_recv, 32)
    lax.fori_loop(FIRST, FIRST + SHARED, lambda i, _: step(i, 64), None)
    q_copy.start()
    pstat_s[0] = packed_lse(32)
    pstat_s[1] = packed_token(32)
    stat_copy = pltpu.make_async_remote_copy(
        src_ref=pstat_s, dst_ref=pstat_r, send_sem=ps_sem.at[0], recv_sem=ps_sem.at[1],
        device_id=partner, device_id_type=MESH,
    )
    stat_copy.start()
    for k in range(SHARED - HELD, SHARED):
        z_copy(k).start()
    lax.fori_loop(FIRST + SHARED, steps - 1, lambda i, _: step(i, 32), None)
    end, slot = steps - 1, (steps - 1) % SLOTS
    copies = tile_copies(end, slot)
    for lo, size in [(k * part, part) for k in range(PARTS)]:
        for c in copies[lo // part : (lo + size) // part]:
            c.wait()
        consume(slot, column(end), lo, size, 32, 0)

    def exchange(src, dst, sem):
        return [
            pltpu.make_async_remote_copy(
                src_ref=src, dst_ref=dst.at[d], send_sem=sem.at[0, d], recv_sem=sem.at[1, d],
                device_id=peers[d], device_id_type=MESH,
            )
            for d in range(3)
        ]

    mine = packed_lse(0)
    stat_copy.wait()
    theirs = pstat_r[0]
    top = jnp.maximum(mine, theirs)
    near = top + jnp.log(jnp.exp(mine - top) + jnp.exp(theirs - top))
    e1s[...] = near
    e1 = exchange(e1s, e1r, e1_sem)
    for c in e1:
        c.start()

    own = [dl[8 * b : 8 * b + 4, :] for b in range(4)]

    row_m = [jnp.broadcast_to(unpack(near[0:4, :], b), (4, 128)) for b in range(4)]

    def prepare(at, size):
        places = [(b, at + off, min(size, 128)) for b in range(4) for off in range(0, size, 128)]
        values = [s_scr[b, :, pl.ds(a, n)] for b, a, n in places]
        values = [jnp.exp(v - row_m[b][:, :n]) for v, (b, _, n) in zip(values, places)]
        for v, (b, a, n) in zip(values, places):
            s_scr[b, :, pl.ds(a, n)] = v

    def pick(at, size, found):
        out = []
        for b in range(4):
            f = found[b]
            for off in range(0, size, 128):
                n = min(size, 128)
                f = jnp.where(own[b][:, :n] == jnp.asarray(at + off).astype(F32), qv[b, :, pl.ds(at + off, n)], f)
            out.append(f)
        return tuple(out)

    zero = jnp.zeros((4, 128), F32)
    lax.fori_loop(0, steps, lambda i, _: prepare(column(i), TILE), None)
    prepare(tail_at, tail)
    q_copy.wait()
    whole = tail_at // PASS * PASS
    found = lax.fori_loop(0, whole // PASS, lambda i, f: pick(pl.multiple_of(i * PASS, 128), PASS, f), (zero,) * 4)
    found = pick(whole, tail_at - whole, found)
    found_tail = pick(tail_at, tail, (jnp.zeros((4, tail), F32),) * 4)
    token_q = []
    for b in range(4):
        f = found_tail[b]
        token_q.append(jnp.sum(found[b], axis=1, keepdims=True) + jnp.sum(f, axis=1, keepdims=True))
    e3s[0] = (packed_token(0) + pstat_r[1])[0:4, :]
    e3s[1] = pack(token_q)
    e3 = exchange(e3s, e3r, e3_sem)
    for c in e3:
        c.start()

    def theirs_at(k):
        return pl.multiple_of((FIRST + (1 - dp) * SHARED + k) * TILE, TILE)

    def await_z(k):
        z_copy(k).wait_send()
        pltpu.make_async_remote_copy(
            src_ref=zsend.at[k], dst_ref=s_scr.at[:, :, pl.ds(theirs_at(k), TILE)],
            send_sem=zs_sem.at[k], recv_sem=zr_sem.at[k], device_id=partner, device_id_type=MESH,
        ).wait_recv()

    def take_early(k, _):
        await_z(k)
        prepare(theirs_at(k), TILE)

    lax.fori_loop(0, SHARED - LATE, take_early, None)
    for c in e1:
        c.wait()
    lses = [near] + [e1r[d] for d in range(3)]
    top = jnp.maximum(jnp.maximum(lses[0], lses[1]), jnp.maximum(lses[2], lses[3]))
    sums = jnp.exp(lses[0] - top) + jnp.exp(lses[1] - top) + jnp.exp(lses[2] - top) + jnp.exp(lses[3] - top)
    lse = top + jnp.log(sums)
    lse_ref[...] = lse
    row_l = [jnp.broadcast_to(unpack(lse[0:4, :], b), (4, 128)) for b in range(4)]
    scale = [jnp.exp(row_m[b] - row_l[b]) for b in range(4)]

    def excess(b, at, size, p):
        e = jnp.maximum(p - qv[b, :, pl.ds(at, size)], 0.0)
        ex_ref[b, :, pl.ds(at, size)] = e
        return e

    def close(at, sums, prepared):
        out = []
        for b in range(4):
            acc = sums[b]
            for off in range(0, TILE, 128):
                v = s_scr[b, :, pl.ds(at + off, 128)]
                acc = acc + excess(b, at + off, 128, v * scale[b] if prepared else jnp.exp(v - row_l[b]))
            out.append(acc)
        return tuple(out)

    def close_late(k, sums):
        await_z(k)
        return close(theirs_at(k), sums, False)

    def close_from(first, count, sums):
        return lax.fori_loop(0, count, lambda i, t: close(pl.multiple_of((first + i) * TILE, TILE), t, True), sums)

    sums = close_from(0, FIRST, (zero,) * 4)
    sums = close_from(FIRST + dp * SHARED, SHARED, sums)
    sums = close_from(FIRST + 2 * SHARED, last, sums)
    rows = []
    for b in range(4):
        e = excess(b, tail_at, tail, s_scr[b, :, tail_at : tail_at + tail] * scale[b][:, :tail])
        rows.append(jnp.sum(e, axis=1, keepdims=True))
    sums = close_from(FIRST + (1 - dp) * SHARED, SHARED - LATE, sums)
    sums = lax.fori_loop(SHARED - LATE, SHARED, close_late, sums)
    rows = [jnp.sum(sums[b], axis=1, keepdims=True) + rows[b] for b in range(4)]
    e2s[...] = pack(rows)
    e2 = exchange(e2s, e2r, e2_sem)
    for c in e2:
        c.start()

    for c in e3:
        c.wait()
    at_token = (e3s[...] + e3r[0]) + (e3r[1] + e3r[2])
    acc_ref[...] = jnp.minimum(jnp.exp(at_token[0] - lse[0:4, :]) / at_token[1], 1.0)

    for c in e2:
        c.wait()
    norm_ref[...] = (e2s[...] + e2r[0]) + (e2r[1] + e2r[2])


def finish_kernel(
    ex_ref, norm_ref, acc_ref, lse_ref, acc_out, norm_out, res_out, bonus_out, acc_v, norm_v, bonus_v, stage, sem, r_sem
):
    n_ids = ex_ref.shape[2]
    lane = lax.broadcasted_iota(jnp.int32, (4, 128), 1)
    norm = norm_ref[...]
    writes = []
    for b in range(4):
        total = jnp.sum(jnp.where(lane == 32 * b, norm, 0.0), axis=1, keepdims=True)
        scale = jnp.broadcast_to(1.0 / jnp.broadcast_to(total, (4, 128)), (4, 128))

        for at in range(0, n_ids, 128):
            size = min(128, n_ids - at)
            stage[b, :, at : at + size] = ex_ref[b, :, at : at + size] * scale[:, :size]
        writes.append(pltpu.make_async_copy(stage.at[b], res_out.at[b], r_sem.at[b]))
        writes[-1].start()

    sub = lax.broadcasted_iota(jnp.int32, (4, 128), 0)
    for src, dst, out, k in ((acc_ref[...], acc_v, acc_out, 0), (norm, norm_v, norm_out, 1)):
        row = jnp.sum(jnp.where(lane % 32 == sub, src, 0.0), axis=0, keepdims=True)
        for b in range(4):
            dst[b : b + 1, :] = (row if b == 0 else pltpu.roll(row, 128 - 32 * b, 1))[:, 0:4]
        writes.append(pltpu.make_async_copy(dst, out, sem.at[k]))
        writes[-1].start()
    row = lse_ref[4:5, :]
    lane = lane[0:1, :]
    packed = row
    for b in range(1, 4):
        packed = jnp.where(lane == b, pltpu.roll(row, 128 - 31 * b, 1), packed)
    bonus_v[...] = packed[:, 0:4]
    writes.append(pltpu.make_async_copy(bonus_v, bonus_out, sem.at[2]))
    writes[-1].start()
    for c in writes:
        c.wait()


def solution(mesh):
    def local_step(hidden, norm_gain, w_head, draft_probs, draft_tokens, temperature):
        n_ids = w_head.shape[1]
        width = w_head.shape[0]
        pad_ids = -(-n_ids // 128) * 128
        tail = n_ids % TILE
        vmem, smem, hbm = pltpu.VMEM, pltpu.SMEM, pltpu.HBM
        dma = pltpu.SemaphoreType.DMA
        ex, norm, acc, lse = pl.pallas_call(
            verify_kernel,
            out_shape=[vmem((4, 4, n_ids), F32), vmem((4, 128), F32), vmem((4, 128), F32), vmem((8, 128), F32)],
            in_specs=[pl.BlockSpec(memory_space=s) for s in (hbm,) * 6],
            out_specs=[pl.BlockSpec(memory_space=vmem)] * 4,
            scratch_shapes=[
                vmem((5, 4, width), jnp.bfloat16),
                vmem((1, width), F32),
                smem((4,), F32),
                smem((4, 4), jnp.int32),
                vmem((SLOTS, TILE, width), jnp.bfloat16),
                vmem((tail, width), jnp.bfloat16),
                vmem((4, 4, n_ids), F32),
                vmem((4, 4, pad_ids), F32),
                vmem((5, 4, width), F32),
                vmem((5, 4, width), F32),
                vmem((32, width), F32),
                vmem((64, width), jnp.bfloat16),
                vmem((width, 128), jnp.bfloat16),
                vmem((5, 4, 128), F32),
                vmem((5, 4, 128), F32),
                vmem((64, 128), F32),
                vmem((64, 128), F32),
                vmem((64, 128), F32),
                vmem((64, 128), F32),
                vmem((64, 128), F32),
                vmem((SHARED, 4, 4, TILE), F32),
                vmem((2, 8, 128), F32),
                vmem((2, 8, 128), F32),
                vmem((8, 128), F32),
                vmem((3, 8, 128), F32),
                vmem((4, 128), F32),
                vmem((3, 4, 128), F32),
                vmem((2, 4, 128), F32),
                vmem((3, 2, 4, 128), F32),
                dma((4,)), dma((SLOTS, PARTS)), dma, dma, dma((2, 2)), dma((2,)), dma((SHARED,)), dma((SHARED,)), dma((2,)),
                dma((2, 3)), dma((2, 3)), dma((2, 3)),
            ],
            compiler_params=pltpu.CompilerParams(collective_id=0, has_side_effects=True),
            name="verify",
        )(
            hidden.transpose(1, 0, 2), norm_gain.reshape(1, width), temperature, draft_tokens,
            w_head.T, draft_probs,
        )
        acc, norm, residual, bonus = pl.pallas_call(
            finish_kernel,
            out_shape=[
                jax.ShapeDtypeStruct((4, 4), F32),
                jax.ShapeDtypeStruct((4, 4), F32),
                jax.ShapeDtypeStruct((4, 4, n_ids), F32),
                jax.ShapeDtypeStruct((1, 4), F32),
            ],
            in_specs=[pl.BlockSpec(memory_space=vmem)] * 4,
            out_specs=[pl.BlockSpec(memory_space=hbm)] * 4,
            scratch_shapes=[
                vmem((4, 4), F32), vmem((4, 4), F32), vmem((1, 4), F32), vmem((4, 4, n_ids), F32), dma((3,)), dma((4,)),
            ],
            compiler_params=pltpu.CompilerParams(vmem_limit_bytes=16 * 1024 * 1024),
            name="finish",
        )(ex, norm, acc, lse)
        return acc, norm, residual, bonus.reshape(4)

    return jax.shard_map(
        local_step,
        mesh=mesh,
        in_specs=(P("dp", None, None), P(), P(None, "tp"), P("dp", None, "tp"), P("dp", None), P("dp")),
        out_specs=(P("dp", None), P("dp", None), P("dp", None, "tp"), P("dp")),
        check_vma=False,
    )
```
